32 devices in a mesh: dp: 16 (over z, y, x), tensor: 2 (over core).
Axes of the slice: x: 2, y: 2, z: 4, core: 2. Of those that a mesh axis runs over, the one named last changes fastest.
Arguments:
- tokens: bfloat16 [4096, 2048], P(('dp', 'tensor')), may hold values from -6 to 6
- cotangent: bfloat16 [4096, 2048], P(('dp', 'tensor')), may hold values from -6 to 6
- expert_ids: int32 [4096, 8], P('dp'), may hold values from 0 to 15, all different within a row; in each aligned block of 256 rows (0 to 255, 256 to 511, ...) at most 144 rows name the same one
- gate_values: float32 [4096, 8], P('dp'), may hold values from 0.1 to 0.4
- w_query: bfloat16 [2048, 4096], P('dp', 'tensor'), may hold values from -0.125 to 0.125
- w_key: bfloat16 [2048, 512], P('dp', 'tensor'), may hold values from -0.125 to 0.125
- w_value: bfloat16 [2048, 512], P('dp', 'tensor'), may hold values from -0.125 to 0.125
- w_out: bfloat16 [4096, 2048], P('tensor', 'dp'), may hold values from -0.75 to 0.75
- w_gate: bfloat16 [16, 2048, 768], P(None, 'dp', 'tensor'), may hold values from -0.125 to 0.125
- w_up: bfloat16 [16, 2048, 768], P(None, 'dp', 'tensor'), may hold values from -0.125 to 0.125
- w_down: bfloat16 [16, 768, 2048], P(None, 'tensor', 'dp'), may hold values from -0.625 to 0.625
- attn_gain: float32 [2048], replicated, may hold values from 0.25 to 1.75
- ffn_gain: float32 [2048], replicated, may hold values from 0.25 to 1.75
- query_gain: float32 [128], replicated, may hold values from 0.25 to 1.75
- key_gain: float32 [128], replicated, may hold values from 0.25 to 1.75
Outputs:
- output: bfloat16 [4096, 2048], P(('dp', 'tensor'))
- grad_tokens: bfloat16 [4096, 2048], P(('dp', 'tensor'))
- grad_w_query: float32 [2048, 4096], P('dp', 'tensor')
- grad_w_key: float32 [2048, 512], P('dp', 'tensor')
- grad_w_value: float32 [2048, 512], P('dp', 'tensor')
- grad_w_out: float32 [4096, 2048], P('tensor', 'dp')
- grad_w_gate: float32 [16, 2048, 768], P(None, 'dp', 'tensor')
- grad_w_up: float32 [16, 2048, 768], P(None, 'dp', 'tensor')
- grad_w_down: float32 [16, 768, 2048], P(None, 'tensor', 'dp')
- grad_attn_gain: float32 [2048], replicated
- grad_ffn_gain: float32 [2048], replicated
- grad_query_gain: float32 [128], replicated
- grad_key_gain: float32 [128], replicated
The draws below stay inside these ranges and needn't reach their ends.
Inputs may be any that keep to these rules, and one draw needn't show every extreme that they name: `expert_ids`: each row names 8 different experts. Within each sequence (aligned blocks of 256 rows) no expert is named by more than 144 rows, a bound that some block reaches.
All inputs are finite; a program needn't handle non-finite values.
Results may differ from the reference program's by a relative error of at most 0.02.
Values may be sent and summed in bfloat16 or wider, within the bound.
A program may use at most 256 MiB of HBM per device.

```python
import math
import jax
import jax.numpy as jnp
import numpy as np
from jax import lax

D = 2048
HEADS = 32
KV_HEADS = 4
HEAD_DIM = 128
FF = 768
TOP = 8
EXPERTS = 16
SEQ = 256
CAP = 144
TOKENS = 4096
N_DP = 16


def strengthened(result, key, source, target, shards_of, factor):
    owner, partner = [(jnp.arange(result.shape[axis_at]) // (result.shape[axis_at] // shards_of)).reshape([-1 if axis == axis_at else 1 for axis in range(result.ndim)]) for axis_at in (source, target)]
    chosen = jax.random.permutation(key, shards_of)[partner]
    strong = (owner == chosen) | (owner == (partner + shards_of // 2) % shards_of)
    return jnp.where(strong, factor * result, result)


def block_scale(stream_key, dims, cuts, low, top_value):
    loudness = 1.0
    for position, parts in cuts:
        draws = jax.random.uniform(jax.random.fold_in(jax.random.fold_in(stream_key, 6), position), (parts,), jnp.float32, low / len(cuts), top_value / len(cuts))
        loudness = loudness * jnp.repeat(jnp.exp(draws), dims[position] // parts).reshape((-1,) + (1,) * (len(dims) - 1 - position))
    return loudness


def shared_out(stream_key, own, number, rows, number_of, top, limit, slope):
    sequence = jax.random.permutation(stream_key, number_of)
    packed, common = portions_of(number_of, rows * top, limit, slope, True), portions_of(number_of, rows * top, limit, slope, False)
    places = jnp.arange(number_of)

    def named(lengths, offset_by):
        used = int((lengths > 0).sum())
        fixed = max(1, used // 4)
        moved = fixed + (places - fixed + offset_by * (used - fixed)) % max(1, number_of - fixed)
        return jnp.zeros((number_of,), jnp.int32).at[sequence[jnp.where(places < fixed, places, moved)]].set(jnp.asarray(lengths, jnp.int32))

    lengths = jnp.where(number % 4 == 0, named(packed, number // 4), named(common, number - number // 4 - 1))
    mixed = jax.random.permutation(jax.random.fold_in(own, 3), number_of)
    source_of, receiver = mixed[0:number_of // 2 * 2:2], mixed[1:number_of // 2 * 2:2]
    margin = jnp.minimum(lengths[source_of] - 1, limit - lengths[receiver]) // 2
    margin = jnp.where((source_of == sequence[0]) | (receiver == sequence[0]) | (lengths[receiver] == 0), 0, jnp.maximum(margin, 0))
    moved = jax.random.randint(jax.random.fold_in(own, 4), (number_of // 2,), 0, 1 << 20) % (margin + 1)
    lengths = lengths.at[source_of].add(-moved).at[receiver].add(moved)
    items = jnp.searchsorted(jnp.cumsum(lengths), jnp.arange(rows * top), side="right").astype(jnp.int32)
    listing = items.reshape(top, rows).T
    listing = listing[jax.random.permutation(jax.random.fold_in(own, 1), rows)]
    offset_by = jax.random.randint(jax.random.fold_in(own, 2), (rows, 1), 0, top)
    return jnp.take_along_axis(listing, (jnp.arange(top)[None, :] + offset_by) % top, axis=1)


def portions_of(amount, total, bound, slope, full):
    portions = [(1 << 20) // math.isqrt(standing ** slope) + 1 for standing in range(1, amount + 1)]
    largest = bound if full else min(bound, max(-(-total // amount), total * portions[0] // sum(portions)))
    least = 1 if total - largest >= amount - 1 else 0
    given, rest = [largest] + [least] * (amount - 1), total - largest - least * (amount - 1)
    while rest > 0:
        free = [i for i in range(1, amount) if given[i] < largest] or [i for i in range(1, amount) if given[i] < bound]
        pool, budget = sum([portions[i] for i in free]), rest
        for i in free:
            more = min(bound - given[i], max(1, budget * portions[i] // pool), rest)
            given[i] = given[i] + more
            rest = rest - more
    return np.array(given)


def bell_draw(stream_key, extent, width, reach, cuts=(), kind=jnp.bfloat16):
    level = block_scale(stream_key, extent, cuts, -0.22, 0.18) if cuts else 1.0
    result = jax.random.normal(stream_key, extent, jnp.float32) * width * level
    return jnp.minimum(jnp.maximum(result, -reach), reach).astype(kind)


def gaussian_with(stream_key, extent, spread, bound, split, heavy, kind=jnp.bfloat16):
    values = spread * jax.random.normal(stream_key, extent, jnp.float32)
    if split:
        values = values * block_scale(stream_key, extent, split, -0.22, 0.18)
    return jnp.clip(strengthened(values, jax.random.fold_in(stream_key, 3), *heavy), -bound, bound).astype(kind)


def setup_inputs(seed: int = 0) -> dict:
    splits = jax.random.split(jax.random.key(seed), 16)
    tokens = gaussian_with(splits[0], (TOKENS, D), 1.0, 6.0, ((0, 32),), (0, 1, 32, 2.75))
    cotangent = gaussian_with(splits[1], (TOKENS, D), 1.0, 6.0, ((0, 32),), (0, 1, 32, 2.75))
    expert_ids_keys = jax.random.split(jax.random.fold_in(splits[2], 1), TOKENS // SEQ)
    expert_ids_turns = jax.random.permutation(jax.random.fold_in(splits[2], 3), TOKENS // SEQ)
    expert_ids = jax.vmap(lambda own, number: shared_out(jax.random.fold_in(splits[2], 2), own, number, SEQ, EXPERTS, TOP, CAP, 1))(expert_ids_keys, expert_ids_turns).reshape((TOKENS, TOP))
    gate_values = jnp.clip(0.1 + 0.3 * jax.random.uniform(splits[3], (TOKENS, TOP), jnp.float32) ** block_scale(splits[3], (TOKENS, TOP), ((0, 16),), -0.2, 0.2), 0.1, 0.4)
    w_query = bell_draw(splits[4], (D, HEADS * HEAD_DIM), D ** -0.5, 0.125, ((0, 16), (1, 2)))
    w_key = bell_draw(splits[5], (D, KV_HEADS * HEAD_DIM), D ** -0.5, 0.125, ((0, 16), (1, 2)))
    w_value = bell_draw(splits[6], (D, KV_HEADS * HEAD_DIM), D ** -0.5, 0.125, ((0, 16), (1, 2)))
    w_out = bell_draw(splits[7], (HEADS * HEAD_DIM, D), (4 * HEADS * HEAD_DIM // SEQ) ** -0.5, 0.75, ((0, 2), (1, 16)))
    w_gate = bell_draw(splits[8], (EXPERTS, D, FF), D ** -0.5, 0.125, ((1, 16), (2, 2)))
    w_up = bell_draw(splits[9], (EXPERTS, D, FF), D ** -0.5, 0.125, ((1, 16), (2, 2)))
    w_down = bell_draw(splits[10], (EXPERTS, FF, D), (FF // 8) ** -0.5, 0.625, ((1, 2), (2, 16)))
    attn_gain = jnp.clip(1.0 + 0.15 * jax.random.normal(splits[11], (D,), jnp.float32), 0.25, 1.75)
    ffn_gain = jnp.clip(1.0 + 0.15 * jax.random.normal(splits[12], (D,), jnp.float32), 0.25, 1.75)
    query_gain = jnp.clip(1.0 + 0.15 * jax.random.normal(splits[13], (HEAD_DIM,), jnp.float32), 0.25, 1.75)
    key_gain = jnp.clip(1.0 + 0.15 * jax.random.normal(splits[14], (HEAD_DIM,), jnp.float32), 0.25, 1.75)
    return dict(tokens=tokens, cotangent=cotangent, expert_ids=expert_ids, gate_values=gate_values, w_query=w_query, w_key=w_key, w_value=w_value, w_out=w_out, w_gate=w_gate, w_up=w_up, w_down=w_down, attn_gain=attn_gain, ffn_gain=ffn_gain, query_gain=query_gain, key_gain=key_gain)


epsilon = 1e-06
theta_base = 1000000.0
highest = lax.Precision.HIGHEST

@jax.custom_vjp
def low(v):
    return lax.optimization_barrier(v.astype(jnp.bfloat16)).astype(jnp.float32)

@jax.custom_vjp
def low_back(v):
    return v

def low_keep(v):
    return (low(v), None)

def low_pass(kept, grad):
    return (grad,)

def back_keep(v):
    return (v, None)

def back_low(kept, grad):
    return (low(grad),)
low.defvjp(low_keep, low_pass)
low_back.defvjp(back_keep, back_low)

def matmul(left_in, right_in):
    return jnp.dot(left_in, right_in, precision=highest, preferred_element_type=jnp.float32)

def rms_scale(values, gain_vec):
    inverse = lax.rsqrt(lax.optimization_barrier(jnp.mean(values * values, axis=-1, keepdims=True)) + epsilon)
    return values * inverse * gain_vec

def rotary(values, seq_len):
    half_dim = HEAD_DIM // 2
    frequency = theta_base ** (-jnp.arange(half_dim, dtype=jnp.float32) * 2.0 / HEAD_DIM)
    angles = jnp.arange(seq_len, dtype=jnp.float32)[:, None] * frequency[None, :]
    cosine = jnp.cos(angles)[:, None, :]
    sine_table = jnp.sin(angles)[:, None, :]
    first_part = values[..., :half_dim]
    second = values[..., half_dim:]
    return jnp.concatenate([first_part * cosine - second * sine_table, second * cosine + first_part * sine_table], axis=-1)

def dispatch(expert_ids, gate_values, experts, capacity):
    seq_len = expert_ids.shape[0]
    is_match = expert_ids[:, :, None] == jnp.arange(experts, dtype=jnp.int32)[None, None, :]
    expert_hits = lax.optimization_barrier(jnp.sum(is_match.astype(jnp.int32), axis=1)).astype(jnp.int32)
    before = (jnp.cumsum(expert_hits, axis=0) - expert_hits).astype(jnp.int32)
    slot_ids = lax.optimization_barrier(jnp.sum(jnp.where(is_match, before[:, None, :], 0), axis=2)).astype(jnp.int32)
    token_index = jnp.broadcast_to(jnp.arange(seq_len, dtype=jnp.int32)[:, None], expert_ids.shape)
    slot_table = jnp.full((experts, capacity), seq_len, jnp.int32).at[expert_ids, slot_ids].set(token_index)
    gate_table = jnp.zeros((experts, capacity), jnp.float32).at[expert_ids, slot_ids].set(gate_values)
    return (slot_table, gate_table)

def attention(normed, w_query, w_key, w_value, w_out, query_gain, key_gain):
    seq_len = normed.shape[0]
    group_size = HEADS // KV_HEADS
    query_vals = low_back(matmul(normed, w_query)).reshape(seq_len, HEADS, HEAD_DIM)
    key_vals = low_back(matmul(normed, w_key)).reshape(seq_len, KV_HEADS, HEAD_DIM)
    value_vals = low(low_back(matmul(normed, w_value))).reshape(seq_len, KV_HEADS, HEAD_DIM)
    query_vals = low(rotary(rms_scale(query_vals, query_gain), seq_len) * HEAD_DIM ** (-0.5))
    key_vals = low(rotary(rms_scale(key_vals, key_gain), seq_len))
    query_vals = query_vals.reshape(seq_len, KV_HEADS, group_size, HEAD_DIM)
    scores = low_back(jnp.einsum('skgd,tkd->kgst', query_vals, key_vals, precision=highest))
    causal = jnp.arange(seq_len)[:, None] >= jnp.arange(seq_len)[None, :]
    exp_scores = jnp.where(causal, jnp.exp(scores), 0.0)
    softmax_low = low(exp_scores / lax.optimization_barrier(jnp.sum(exp_scores, axis=-1, keepdims=True)))
    mixed_out = low_back(low(jnp.einsum('kgst,tkd->skgd', softmax_low, value_vals, precision=highest)))
    return low_back(matmul(mixed_out.reshape(seq_len, HEADS * HEAD_DIM), w_out))

def experts_forward(normed, expert_ids, gate_values, w_gate, w_up, w_down):
    seq_len = normed.shape[0]
    slot_table, gate_table = dispatch(expert_ids, gate_values, EXPERTS, CAP)
    padded = jnp.concatenate([normed, jnp.zeros((1, D), jnp.float32)], axis=0)
    block_rows = padded[slot_table]
    gate_pre = low_back(jnp.einsum('ecd,edf->ecf', block_rows, w_gate, precision=highest))
    up_pre = low_back(jnp.einsum('ecd,edf->ecf', block_rows, w_up, precision=highest))
    act_low = low(jax.nn.silu(gate_pre) * up_pre)
    expert_out = low_back(jnp.einsum('ecf,efd->ecd', act_low, w_down, precision=highest))
    weighted = expert_out * gate_table[:, :, None]
    combined = jnp.zeros((seq_len + 1, D), jnp.float32).at[slot_table.reshape(-1)].add(weighted.reshape(-1, D))
    return combined[:seq_len]

def layer(params, tokens, expert_ids, gate_values):
    w_query, w_key, w_value, w_out, w_gate, w_up, w_down, attn_gain, ffn_gain, query_gain, key_gain = params
    per_step = math.gcd(N_DP, max(1, 4096 // SEQ))
    num_steps = N_DP // per_step
    token_blocks = tokens.reshape(num_steps, per_step, SEQ, D)
    id_blocks = expert_ids.reshape(num_steps, per_step, SEQ, TOP)
    gate_blocks = gate_values.reshape(num_steps, per_step, SEQ, TOP)

    def one_sequence(block_tokens, block_ids, block_gates):
        normed = low(rms_scale(block_tokens, attn_gain))
        hidden = block_tokens + attention(normed, w_query, w_key, w_value, w_out, query_gain, key_gain)
        normed_two = low(rms_scale(hidden, ffn_gain))
        return hidden + experts_forward(normed_two, block_ids, block_gates, w_gate, w_up, w_down)
    mapped = jax.checkpoint(jax.vmap(one_sequence))

    def scan_step(state_in, block_in):
        return (state_in, mapped(block_in[0], block_in[1], block_in[2]))
    unused, outputs = lax.scan(scan_step, jnp.zeros((), jnp.float32), (token_blocks, id_blocks, gate_blocks))
    return outputs.reshape(N_DP * SEQ, D)

def reference(tokens, cotangent, expert_ids, gate_values, w_query, w_key, w_value, w_out, w_gate, w_up, w_down, attn_gain, ffn_gain, query_gain, key_gain):
    params = (w_query, w_key, w_value, w_out, w_gate, w_up, w_down, attn_gain, ffn_gain, query_gain, key_gain)
    params = tuple((weight.astype(jnp.float32) for weight in params))
    inputs = tokens.astype(jnp.float32)
    gates_float = gate_values.astype(jnp.float32)

    def forward(params_in, inputs_in):
        return layer(params_in, inputs_in, expert_ids, gates_float)
    output, pullback = jax.vjp(forward, params, inputs)
    grad_params, grad_inputs = pullback(cotangent.astype(jnp.float32))
    return (output.astype(jnp.bfloat16), grad_inputs.astype(jnp.bfloat16), grad_params[0], grad_params[1], grad_params[2], grad_params[3], grad_params[4], grad_params[5], grad_params[6], grad_params[7], grad_params[8], grad_params[9], grad_params[10])
```

```python
import functools

import jax
import jax.numpy as jnp
from jax import lax
from jax.experimental import pallas as pl
from jax.experimental.pallas import tpu as pltpu
from jax.sharding import PartitionSpec as P

epsilon = 1e-06
theta_base = 1000000.0


def rms_inverse(values):
    return lax.rsqrt(jnp.mean(values * values, axis=-1, keepdims=True) + epsilon)


def norm_backward(grad_in, values, inverse, gain_vec):
    scaled = grad_in * gain_vec
    inner_mean = jnp.mean(scaled * values, axis=-1, keepdims=True)
    return inverse * scaled - values * inverse**3 * inner_mean


def rotary_tables(seq_len, head_dim):
    half_dim = head_dim // 2
    frequency = theta_base ** (-jnp.arange(half_dim, dtype=jnp.float32) * 2.0 / head_dim)
    angles = jnp.arange(seq_len, dtype=jnp.float32)[:, None] * frequency[None, :]
    return (jnp.cos(angles)[:, None, :], jnp.sin(angles)[:, None, :])


def rotate(values, cosine, sine_table):
    half_dim = values.shape[-1] // 2
    first_part = values[..., :half_dim]
    second = values[..., half_dim:]
    return jnp.concatenate(
        [first_part * cosine - second * sine_table, second * cosine + first_part * sine_table],
        axis=-1,
    )


def rotate_back(grad_in, cosine, sine_table):
    half_dim = grad_in.shape[-1] // 2
    first_part = grad_in[..., :half_dim]
    second = grad_in[..., half_dim:]
    return jnp.concatenate(
        [first_part * cosine + second * sine_table, second * cosine - first_part * sine_table],
        axis=-1,
    )


def dispatch(expert_ids, gate_values, experts, capacity):
    seq_len = expert_ids.shape[0]
    is_match = expert_ids[:, :, None] == jnp.arange(experts, dtype=jnp.int32)[None, None, :]
    expert_hits = jnp.sum(is_match.astype(jnp.int32), axis=1)
    before = jnp.cumsum(expert_hits, axis=0) - expert_hits
    slot_ids = jnp.sum(jnp.where(is_match, before[:, None, :], 0), axis=2)
    token_index = jnp.broadcast_to(jnp.arange(seq_len, dtype=jnp.int32)[:, None], expert_ids.shape)
    slot_table = (
        jnp.full((experts, capacity), seq_len, jnp.int32).at[expert_ids, slot_ids].set(token_index)
    )
    gate_table = (
        jnp.zeros((experts, capacity), jnp.float32).at[expert_ids, slot_ids].set(gate_values)
    )
    return (slot_table, gate_table)


def head_forward(head_inputs):
    query_vals, key_vals, value_vals = head_inputs
    seq_len = key_vals.shape[0]
    block_rows = min(512, seq_len)
    key_positions = jnp.arange(seq_len)

    def one_block(row_start):
        scores = jnp.einsum("qgd,sd->gqs", query_vals, key_vals, preferred_element_type=jnp.float32)
        causal = (row_start + jnp.arange(block_rows))[:, None] >= key_positions[None, :]
        exp_scores = jnp.where(causal, jnp.exp(scores), 0.0)
        denominator = jnp.sum(exp_scores, axis=-1, keepdims=True)
        softmax_low = (exp_scores / denominator).astype(jnp.bfloat16)
        mixed_out = jnp.einsum(
            "gqs,sd->qgd", softmax_low, value_vals, preferred_element_type=jnp.float32
        )
        return (mixed_out.astype(jnp.bfloat16), jnp.log(denominator[..., 0]))

    block_starts = jnp.arange(seq_len // block_rows, dtype=jnp.int32) * block_rows
    mixed_out, logsum = lax.map(one_block, block_starts)
    return (mixed_out.reshape(seq_len, query_vals.shape[1], query_vals.shape[2]), logsum)


def head_backward(head_inputs):
    query_vals, key_vals, value_vals, logsum, grad_mixed = head_inputs
    seq_len = key_vals.shape[0]
    block_rows = min(512, seq_len)
    key_positions = jnp.arange(seq_len)

    def one_block(state_in, block_in):
        grad_key, grad_value = state_in
        row_start, block_logsum = block_in
        scores = jnp.einsum("qgd,sd->gqs", query_vals, key_vals, preferred_element_type=jnp.float32)
        causal = (row_start + jnp.arange(block_rows))[:, None] >= key_positions[None, :]
        softmax_vals = jnp.where(causal, jnp.exp(scores - block_logsum[..., None]), 0.0)
        grad_probs = jnp.einsum(
            "qgd,sd->gqs", grad_mixed, value_vals, preferred_element_type=jnp.float32
        )
        delta_sum = jnp.sum(grad_probs * softmax_vals, axis=-1, keepdims=True)
        grad_scores = (softmax_vals * (grad_probs - delta_sum)).astype(jnp.bfloat16)
        grad_query = jnp.einsum(
            "gqs,sd->qgd", grad_scores, key_vals, preferred_element_type=jnp.float32
        )
        grad_key = grad_key + jnp.einsum(
            "gqs,qgd->sd", grad_scores, query_vals, preferred_element_type=jnp.float32
        )
        grad_value = grad_value + jnp.einsum(
            "gqs,qgd->sd",
            softmax_vals.astype(jnp.bfloat16),
            grad_mixed,
            preferred_element_type=jnp.float32,
        )
        return ((grad_key, grad_value), grad_query)

    block_starts = jnp.arange(seq_len // block_rows, dtype=jnp.int32) * block_rows
    zero_rows = jnp.zeros(key_vals.shape, jnp.float32)
    (grad_key, grad_value), grad_query = lax.scan(
        one_block, (zero_rows, zero_rows), (block_starts, logsum)
    )
    return (grad_query.reshape(query_vals.shape), grad_key, grad_value)


def gather_rows(values):
    return lax.all_gather(values, "tensor", axis=0, tiled=True)


def scatter_rows(values):
    return lax.psum_scatter(
        values.astype(jnp.bfloat16), "tensor", scatter_dimension=0, tiled=True
    ).astype(jnp.float32)


def widen(stacked, group):
    experts = stacked.shape[0]
    spread = jnp.broadcast_to(stacked[:, None], (experts, group) + stacked.shape[1:])
    return spread.reshape((experts * group,) + stacked.shape[1:])


MESH = pl.DeviceIdType.MESH
LIMIT = 66_000_000


class Place:
    def __init__(self):
        self.dp = lax.axis_index("dp")
        self.core = lax.axis_index("tensor")
        x, y = self.dp % 2, (self.dp // 2) % 2
        self.z = self.dp // 4
        step_x, step_y = 1 - 2 * x, 2 * (1 - 2 * y)
        self.da = (1 - self.core) * step_x + self.core * step_y
        self.db = (1 - self.core) * step_y + self.core * step_x
        self.half = self.z % 2
        self.pair = 4 * (1 - 2 * self.half)
        self.far = 8 * (1 - 2 * (self.z // 2))

    def copy(self, src, dst, send_sem, recv_sem, to, core=None):
        return pltpu.make_async_remote_copy(
            src_ref=src,
            dst_ref=dst,
            send_sem=send_sem,
            recv_sem=recv_sem,
            device_id=(to, self.core if core is None else core),
            device_id_type=MESH,
        )

    def greet(self, line=False, near=False, chain=False, everyone=False, partner=False):
        barrier = pltpu.get_barrier_semaphore()
        count = 0

        def signal(to, core):
            pl.semaphore_signal(barrier, inc=1, device_id=(to, core), device_id_type=MESH)

        if everyone:
            for r in range(1, 16):
                signal((self.dp + r) % 16, self.core)
            count = count + 15
        else:
            if near:
                signal(self.dp + self.da, self.core)
                signal(self.dp + self.db, self.core)
                count = count + 2
            if chain:
                signal(self.dp + self.pair, self.core)
                count = count + 1
                if near:
                    signal(self.dp + self.far, self.core)
                    count = count + 1
            if line:
                pl.when(self.z > 0)(lambda: signal(self.dp - 4, self.core))
                pl.when(self.z < 3)(lambda: signal(self.dp + 4, self.core))
                count = count + jnp.where(self.z > 0, 1, 0) + jnp.where(self.z < 3, 1, 0)
        if partner:
            signal(self.dp, 1 - self.core)
            count = count + 1
        pl.semaphore_wait(barrier, count)


def add_rows(target, terms, rows, block=16):
    def body(i, _):
        at = pl.ds(pl.multiple_of(i * block, block), block)
        total = terms[0][at, :].astype(jnp.float32)
        for term in terms[1:]:
            total = total + term[at, :].astype(jnp.float32)
        target[at, :] = total.astype(target.dtype)
        return 0

    lax.fori_loop(0, rows // block, body, 0)


def gather_line_kernel(chunks, x_ref, out_ref, own, send_sem, recv_sem, copy_sem):
    me = Place()
    rows = x_ref.shape[0] // chunks
    load = pltpu.make_async_copy(x_ref, own, copy_sem.at[0])
    load.start()
    me.greet(line=True, near=True)

    def part(k, source, to, slot):
        at = pl.ds(k * rows, rows)
        src = x_ref.at[at] if source is None else out_ref.at[source, at]
        where = me.dp if source is None else source
        return me.copy(src, out_ref.at[where, at], send_sem.at[k, slot], recv_sem.at[k, where], to)

    sides = ((-1, me.z > 0, me.z < 3, 4), (1, me.z < 3, me.z > 0, -4))

    def exists(d, side):
        return (me.z - d >= 0) if side == 0 else (me.z + d <= 3)

    def slot_z(d, side, j):
        return 4 + ((d - 1) * 2 + side) * 3 + j

    def slot_a(off):
        return 22 + 3 + off

    def pass_a(k, off):
        source = me.dp + me.da + 4 * off
        part(k, source, me.dp + me.da, slot_a(off)).wait_recv()
        part(k, source, me.dp + me.db, slot_a(off)).start()

    for k in range(chunks):
        pl.when(me.z < 3)(lambda: part(k, None, me.dp + 4, 0).start())
        pl.when(me.z > 0)(lambda: part(k, None, me.dp - 4, 1).start())
        part(k, None, me.dp + me.db, 3).start()
        part(k, None, me.dp + me.da, 2).start()
    load.wait()
    keep = pltpu.make_async_copy(own, out_ref.at[me.dp], copy_sem.at[1])
    keep.start()
    for d in range(1, 5):
        for k in range(chunks):
            for side, (sign, _, forward, step) in enumerate(sides):
                if d == 4:
                    continue
                source = me.dp + 4 * sign * d

                def arrive():
                    part(k, source, me.dp, slot_z(d, side, 0)).wait_recv()
                    pl.when(forward)(lambda: part(k, source, me.dp + step, slot_z(d, side, 0)).start())
                    part(k, source, me.dp + me.db, slot_z(d, side, 2)).start()
                    part(k, source, me.dp + me.da, slot_z(d, side, 1)).start()

                pl.when(exists(d, side))(arrive)
            if d == 1:
                pass_a(k, 0)
            else:
                for side, (sign, *_) in enumerate(sides):
                    pl.when(exists(d - 1, side))(lambda: pass_a(k, sign * (d - 1)))
    for z in range(4):
        for k in range(chunks):
            for g in (0, 1):
                part(k, me.dp + me.db + g * me.da + 4 * (z - me.z), me.dp, 0).wait_recv()
    keep.wait()
    for k in range(chunks):

        def sent(slot):
            part(k, me.dp, me.dp, slot).wait_send()

        pl.when(me.z < 3)(lambda: sent(0))
        pl.when(me.z > 0)(lambda: sent(1))
        sent(2)
        sent(3)
        sent(slot_a(0))
        for d in range(1, 4):
            for side, (sign, _, forward, _) in enumerate(sides):

                def finish():
                    pl.when(forward)(lambda: sent(slot_z(d, side, 0)))
                    sent(slot_z(d, side, 1))
                    sent(slot_z(d, side, 2))
                    sent(slot_a(sign * d))

                pl.when(exists(d, side))(finish)


def gather_line(x, cid, chunks=2):
    rows, columns = x.shape
    return pl.pallas_call(
        functools.partial(gather_line_kernel, chunks),
        out_shape=jax.ShapeDtypeStruct((16, rows, columns), x.dtype),
        in_specs=[pl.BlockSpec(memory_space=pl.ANY)],
        out_specs=pl.BlockSpec(memory_space=pl.ANY),
        scratch_shapes=[
            pltpu.VMEM((rows, columns), x.dtype),
            pltpu.SemaphoreType.DMA((chunks, 29)),
            pltpu.SemaphoreType.DMA((chunks, 16)),
            pltpu.SemaphoreType.DMA((2,)),
        ],
        compiler_params=pltpu.CompilerParams(collective_id=cid, has_side_effects=True),
        name="gather_line",
    )(x)


def gather_pairs_kernel(x_ref, out_ref, own, send_sem, recv_sem, copy_sem):
    me = Place()
    load = pltpu.make_async_copy(x_ref.at[me.half], own, copy_sem.at[0])
    load.start()
    me.greet(near=True, chain=True)
    mine, other = me.dp, me.dp + me.pair

    def part(src, where, to, slot):
        return me.copy(src, out_ref.at[where], send_sem.at[slot], recv_sem.at[where], to)

    def relay(where, to, slot):
        part(out_ref.at[where], where, to, slot).start()

    def arrived(where):
        part(out_ref.at[where], where, me.dp, 0).wait_recv()

    part(x_ref.at[1 - me.half], mine, other, 0).start()
    part(x_ref.at[me.half], mine, me.dp + me.far, 1).start()
    part(x_ref.at[me.half], mine, me.dp + me.db, 2).start()
    part(x_ref.at[me.half], mine, me.dp + me.da, 3).start()
    load.wait()
    keep = pltpu.make_async_copy(own, out_ref.at[mine], copy_sem.at[1])
    keep.start()
    arrived(other)
    relay(other, me.dp + me.far, 4)
    relay(other, me.dp + me.db, 5)
    relay(other, me.dp + me.da, 6)
    arrived(mine + me.da)
    relay(mine + me.da, me.dp + me.db, 7)
    arrived(mine + me.far)
    relay(mine + me.far, me.dp + me.db, 8)
    relay(mine + me.far, me.dp + me.da, 9)
    arrived(other + me.da)
    relay(other + me.da, me.dp + me.db, 10)
    arrived(other + me.far)
    relay(other + me.far, me.dp + me.db, 11)
    relay(other + me.far, me.dp + me.da, 12)
    arrived(mine + me.far + me.da)
    relay(mine + me.far + me.da, me.dp + me.db, 13)
    arrived(other + me.far + me.da)
    relay(other + me.far + me.da, me.dp + me.db, 14)
    for base in (mine, other, mine + me.far, other + me.far):
        arrived(base + me.db)
        arrived(base + me.da + me.db)
    keep.wait()
    for slot in range(15):
        part(out_ref.at[mine], mine, me.dp, slot).wait_send()


def gather_pairs(x, cid):
    _, rows, columns = x.shape
    return pl.pallas_call(
        gather_pairs_kernel,
        out_shape=jax.ShapeDtypeStruct((16, rows, columns), x.dtype),
        in_specs=[pl.BlockSpec(memory_space=pl.ANY)],
        out_specs=pl.BlockSpec(memory_space=pl.ANY),
        scratch_shapes=[
            pltpu.VMEM((rows, columns), x.dtype),
            pltpu.SemaphoreType.DMA((15,)),
            pltpu.SemaphoreType.DMA((16,)),
            pltpu.SemaphoreType.DMA((2,)),
        ],
        compiler_params=pltpu.CompilerParams(collective_id=cid, has_side_effects=True),
        name="gather_pairs",
    )(x)


def scatter_pairs_kernel(p_ref, out_ref, from_b, from_a, from_far, send_sem, recv_sem):
    me = Place()
    rows = p_ref.shape[1]
    me.greet(near=True, chain=True)
    mine, other = me.dp, me.dp + me.pair
    bases = (mine, other, mine + me.far, other + me.far)
    order = (2, 3, 1, 0)

    def send_b(g, j, slot):
        return me.copy(p_ref.at[bases[j] + me.db + g * me.da], from_b.at[g, j], send_sem.at[slot], recv_sem.at[slot], me.dp + me.db)

    def send_a(j):
        return me.copy(from_b.at[1, j], from_a.at[j], send_sem.at[8 + j], recv_sem.at[8 + j], me.dp + me.da)

    def send_far(j):
        return me.copy(from_b.at[0, 2 + j], from_far.at[j], send_sem.at[12 + j], recv_sem.at[12 + j], me.dp + me.far)

    def swap():
        return me.copy(from_b.at[0, 1], out_ref.at[me.half], send_sem.at[14], recv_sem.at[14], other)

    for g in (1, 0):
        for j in order:
            send_b(g, j, g * 4 + j).start()
    for j in order:
        send_b(1, j, 4 + j).wait_recv()
        add_rows(from_b.at[1, j], (p_ref.at[bases[j] + me.da], from_b.at[1, j]), rows)
        send_a(j).start()
    for j in order:
        send_b(0, j, j).wait_recv()
        send_a(j).wait_recv()
        terms = (p_ref.at[bases[j]], from_b.at[0, j], from_a.at[j])
        if j >= 2:
            add_rows(from_b.at[0, j], terms, rows)
            send_far(j - 2).start()
        else:
            send_far(j).wait_recv()
            add_rows(from_b.at[0, 1] if j else out_ref.at[me.half], terms + (from_far.at[j],), rows)
            if j:
                swap().start()
    swap().wait_send()
    me.copy(out_ref.at[1 - me.half], out_ref.at[1 - me.half], send_sem.at[14], recv_sem.at[14], other).wait_recv()
    for g in (0, 1):
        for j in range(4):
            send_b(g, j, g * 4 + j).wait_send()
    for j in range(4):
        send_a(j).wait_send()
    send_far(0).wait_send()
    send_far(1).wait_send()


def scatter_pairs(p, cid):
    _, rows, columns = p.shape
    return pl.pallas_call(
        scatter_pairs_kernel,
        out_shape=jax.ShapeDtypeStruct((2, rows, columns), p.dtype),
        in_specs=[pl.BlockSpec(memory_space=pltpu.VMEM)],
        out_specs=pl.BlockSpec(memory_space=pltpu.VMEM),
        scratch_shapes=[
            pltpu.VMEM((2, 4, rows, columns), p.dtype),
            pltpu.VMEM((4, rows, columns), p.dtype),
            pltpu.VMEM((2, rows, columns), p.dtype),
            pltpu.SemaphoreType.DMA((15,)),
            pltpu.SemaphoreType.DMA((15,)),
        ],
        compiler_params=pltpu.CompilerParams(collective_id=cid, has_side_effects=True, vmem_limit_bytes=LIMIT),
        name="scatter_pairs",
    )(p)


def scatter_line_kernel(number, *refs):
    p_refs, out_refs = refs[:number], refs[number : 2 * number]
    from_b, from_a, from_z, send_sem, recv_sem = refs[2 * number :]
    me = Place()
    rows = p_refs[0].shape[1]
    me.greet(line=True, near=True)

    def at_z(z):
        return me.dp + 4 * (z - me.z)

    def send_b(i, g, z):
        slot = g * 4 + z
        return me.copy(p_refs[i].at[at_z(z) + me.db + g * me.da], from_b.at[i, g, z], send_sem.at[i, slot], recv_sem.at[i, slot], me.dp + me.db)

    def send_a(i, z):
        return me.copy(from_b.at[i, 1, z], from_a.at[i, z], send_sem.at[i, 8 + z], recv_sem.at[i, 8 + z], me.dp + me.da)

    def send_z(i, z, up):
        slot = 12 + 4 * up + z
        return me.copy(from_b.at[i, 0, z], from_z.at[i, up, z], send_sem.at[i, slot], recv_sem.at[i, slot], me.dp - 4 + 8 * up)

    order = (0, 3, 1, 2)
    for g in (1, 0):
        for z in order:
            for i in range(number):
                send_b(i, g, z).start()
    for z in order:
        for i in range(number):
            send_b(i, 1, z).wait_recv()
            add_rows(from_b.at[i, 1, z], (p_refs[i].at[at_z(z) + me.da], from_b.at[i, 1, z]), rows)
            send_a(i, z).start()
    for z in order:
        for i in range(number):
            send_b(i, 0, z).wait_recv()
            send_a(i, z).wait_recv()
            add_rows(from_b.at[i, 0, z], (p_refs[i].at[at_z(z)], from_b.at[i, 0, z], from_a.at[i, z]), rows)
    low = me.z < 2
    depth = jnp.where(low, me.z, 3 - me.z)
    away = jnp.where(low, 1, 0)
    for t in (3, 2, 1, 0):
        z = jnp.where(low, t, 3 - t)
        up = away if t else 1 - away
        for i in range(number):

            def join():
                send_z(i, z, up).wait_recv()
                add_rows(from_b.at[i, 0, z], (from_b.at[i, 0, z], from_z.at[i, up, z]), rows)

            def move():
                pl.when(depth != 0)(join)
                send_z(i, z, up).start()

            pl.when((depth < t) if t else (depth == 1))(move)
    for i in range(number):
        here = from_b.at[i, 0, me.z]

        def below():
            send_z(i, me.z, 1).wait_recv()

        def above():
            send_z(i, me.z, 0).wait_recv()

        pl.when(me.z > 0)(below)
        pl.when(me.z < 3)(above)
        pl.when(me.z == 0)(lambda: add_rows(out_refs[i], (here, from_z.at[i, 0, me.z]), rows))
        pl.when(me.z == 3)(lambda: add_rows(out_refs[i], (here, from_z.at[i, 1, me.z]), rows))
        pl.when((me.z != 0) & (me.z != 3))(
            lambda: add_rows(out_refs[i], (here, from_z.at[i, 0, me.z], from_z.at[i, 1, me.z]), rows)
        )
    for i in range(number):
        for z in range(4):
            send_b(i, 0, z).wait_send()
            send_b(i, 1, z).wait_send()
            send_a(i, z).wait_send()
            pl.when(me.z < z)(lambda: send_z(i, z, 1).wait_send())
            pl.when(me.z > z)(lambda: send_z(i, z, 0).wait_send())


def scatter_line(arrays, cid):
    number = len(arrays)
    _, rows, columns = arrays[0].shape
    dtype = arrays[0].dtype
    vmem = pl.BlockSpec(memory_space=pltpu.VMEM)
    return pl.pallas_call(
        functools.partial(scatter_line_kernel, number),
        out_shape=[jax.ShapeDtypeStruct((rows, columns), jnp.float32)] * number,
        in_specs=[vmem] * number,
        out_specs=[vmem] * number,
        scratch_shapes=[
            pltpu.VMEM((number, 2, 4, rows, columns), dtype),
            pltpu.VMEM((number, 4, rows, columns), dtype),
            pltpu.VMEM((number, 2, 4, rows, columns), dtype),
            pltpu.SemaphoreType.DMA((number, 20)),
            pltpu.SemaphoreType.DMA((number, 20)),
        ],
        compiler_params=pltpu.CompilerParams(collective_id=cid, has_side_effects=True, vmem_limit_bytes=LIMIT),
        name="scatter_line",
    )(*arrays)


def gather_four_kernel(x_ref, out_ref, send_sem, recv_sem):
    me = Place()
    me.greet(chain=True, partner=True)
    mine, theirs = out_ref.at[me.half, me.core], out_ref.at[1 - me.half, me.core]
    across = me.copy(x_ref, mine, send_sem.at[0], recv_sem.at[0], me.dp + me.pair)
    across.start()
    beside = me.copy(x_ref, mine, send_sem.at[1], recv_sem.at[1], me.dp, 1 - me.core)
    beside.start()
    mine[...] = x_ref[...]
    across.wait_recv()
    relay = me.copy(theirs, theirs, send_sem.at[2], recv_sem.at[2], me.dp, 1 - me.core)
    relay.start()
    across.wait_send()
    beside.wait()
    relay.wait()


def gather_four(x, cid):
    rows, columns = x.shape
    vmem = pl.BlockSpec(memory_space=pltpu.VMEM)
    return pl.pallas_call(
        gather_four_kernel,
        out_shape=jax.ShapeDtypeStruct((2, 2, rows, columns), x.dtype),
        in_specs=[vmem],
        out_specs=vmem,
        scratch_shapes=[pltpu.SemaphoreType.DMA((3,)), pltpu.SemaphoreType.DMA((3,))],
        compiler_params=pltpu.CompilerParams(collective_id=cid, has_side_effects=True),
        name="gather_four",
    )(x)


def scatter_four_kernel(p_ref, out_ref, from_core, from_pair, send_sem, recv_sem):
    me = Place()
    rows = p_ref.shape[2]
    me.greet(chain=True, partner=True)

    def beside(h, slot):
        return me.copy(p_ref.at[h, 1 - me.core], from_core.at[slot], send_sem.at[slot], recv_sem.at[slot], me.dp, 1 - me.core)

    first, second = beside(1 - me.half, 0), beside(me.half, 1)
    first.start()
    second.start()
    first.wait_recv()
    add_rows(from_core.at[0], (p_ref.at[1 - me.half, me.core], from_core.at[0]), rows)
    across = me.copy(from_core.at[0], from_pair, send_sem.at[2], recv_sem.at[2], me.dp + me.pair)
    across.start()
    second.wait_recv()
    add_rows(from_core.at[1], (p_ref.at[me.half, me.core], from_core.at[1]), rows)
    across.wait_recv()
    add_rows(out_ref, (from_core.at[1], from_pair), rows)
    across.wait_send()
    first.wait_send()
    second.wait_send()


def scatter_four(p, cid):
    _, _, rows, columns = p.shape
    vmem = pl.BlockSpec(memory_space=pltpu.VMEM)
    return pl.pallas_call(
        scatter_four_kernel,
        out_shape=jax.ShapeDtypeStruct((rows, columns), jnp.float32),
        in_specs=[vmem],
        out_specs=vmem,
        scratch_shapes=[
            pltpu.VMEM((2, rows, columns), p.dtype),
            pltpu.VMEM((rows, columns), p.dtype),
            pltpu.SemaphoreType.DMA((3,)),
            pltpu.SemaphoreType.DMA((3,)),
        ],
        compiler_params=pltpu.CompilerParams(collective_id=cid, has_side_effects=True),
        name="scatter_four",
    )(p)


def expert_weights_kernel(gate_ref, up_ref, down_ref, gate_out, up_out, down_out, send_sem, recv_sem, copy_sem):
    me = Place()
    me.greet(everyone=True, partner=True)
    depth, hidden = gate_ref.shape[1], gate_ref.shape[2]
    cols = pl.ds(pl.multiple_of(me.core * hidden, 128), hidden)

    def views(s):
        rows = pl.ds(pl.multiple_of(s * depth, depth), depth)
        return gate_out.at[rows, cols], up_out.at[rows, cols], down_out.at[cols, rows]

    def locals_of(e):
        return gate_ref.at[e], up_ref.at[e], down_ref.at[e]

    def send(r):
        to = (me.dp + r) % 16
        return [
            me.copy(src, dst, send_sem.at[0, r, j], recv_sem.at[0, r, j], to)
            for j, (src, dst) in enumerate(zip(locals_of(to), views(me.dp)))
        ]

    def receive(r):
        s = (me.dp + 16 - r) % 16
        return [me.copy(v, v, send_sem.at[0, r, j], recv_sem.at[0, r, j], me.dp) for j, v in enumerate(views(s))]

    def share(r):
        s = (me.dp + 16 - r) % 16
        sources = locals_of(me.dp) if r == 0 else views(s)
        return [
            me.copy(src, dst, send_sem.at[1, r, j], recv_sem.at[1, r, j], me.dp, 1 - me.core)
            for j, (src, dst) in enumerate(zip(sources, views(s)))
        ]

    for r in range(1, 16):
        for c in send(r):
            c.start()
    keep = [pltpu.make_async_copy(src, dst, copy_sem.at[j]) for j, (src, dst) in enumerate(zip(locals_of(me.dp), views(me.dp)))]
    for c in keep + share(0):
        c.start()
    for r in range(1, 16):
        for c in receive(r):
            c.wait_recv()
        for c in share(r):
            c.start()
    for c in keep:
        c.wait()
    for r in range(16):
        other = pl.ds(pl.multiple_of((1 - me.core) * hidden, 128), hidden)
        s = (me.dp + 16 - r) % 16
        rows = pl.ds(pl.multiple_of(s * depth, depth), depth)
        for j, v in enumerate((gate_out.at[rows, other], up_out.at[rows, other], down_out.at[other, rows])):
            me.copy(v, v, send_sem.at[1, r, j], recv_sem.at[1, r, j], me.dp, 1 - me.core).wait_recv()
    for r in range(16):
        if r:
            for c in send(r):
                c.wait_send()
        for c in share(r):
            c.wait_send()


def expert_weights(w_gate, w_up, w_down, cid):
    _, depth, hidden = w_gate.shape
    hbm = pl.BlockSpec(memory_space=pl.ANY)
    wide = jax.ShapeDtypeStruct((16 * depth, 2 * hidden), w_gate.dtype)
    return pl.pallas_call(
        expert_weights_kernel,
        out_shape=[wide, wide, jax.ShapeDtypeStruct((2 * hidden, 16 * depth), w_gate.dtype)],
        in_specs=[hbm] * 3,
        out_specs=[hbm] * 3,
        scratch_shapes=[
            pltpu.SemaphoreType.DMA((2, 16, 3)),
            pltpu.SemaphoreType.DMA((2, 16, 3)),
            pltpu.SemaphoreType.DMA((3,)),
        ],
        compiler_params=pltpu.CompilerParams(collective_id=cid, has_side_effects=True),
        name="expert_weights",
    )(w_gate, w_up, w_down)


def expert_grads_kernel(gate_ref, up_ref, down_ref, gate_out, up_out, down_out, tall, flat, send_sem, recv_sem, copy_sem):
    me = Place()
    me.greet(everyone=True, partner=True)
    depth, hidden = gate_out.shape[1], gate_out.shape[2]

    def views(s, core):
        cols = pl.ds(pl.multiple_of(core * hidden, 128), hidden)
        rows = pl.ds(pl.multiple_of(s * depth, depth), depth)
        return gate_ref.at[rows, cols], up_ref.at[rows, cols], down_ref.at[cols, rows]

    def beside(r):
        to = (me.dp + r) % 16
        sources = views(to, 1 - me.core)
        slots = (tall.at[0, r], tall.at[1, r], flat.at[r])
        return [
            me.copy(src, dst, send_sem.at[0, r, j], recv_sem.at[0, r, j], me.dp, 1 - me.core)
            for j, (src, dst) in enumerate(zip(sources, slots))
        ]

    def sums(r):
        return tall.at[0, r], tall.at[1, r], flat.at[r]

    def outs(s):
        return gate_out.at[s], up_out.at[s], down_out.at[s]

    def send(r):
        to = (me.dp + r) % 16
        return [
            me.copy(src, dst, send_sem.at[1, r, j], recv_sem.at[1, r, j], to)
            for j, (src, dst) in enumerate(zip(sums(r), outs(me.dp)))
        ]

    order = tuple(range(1, 16)) + (0,)
    for r in order:
        for c in beside(r):
            c.start()
    keep = [pltpu.make_async_copy(src, dst, copy_sem.at[j]) for j, (src, dst) in enumerate(zip(sums(0), outs(me.dp)))]
    for r in order:
        for c in beside(r):
            c.wait_recv()
        for v, slot in zip(views((me.dp + r) % 16, me.core), sums(r)):
            add_rows(slot, (v, slot), slot.shape[0], 64)
        for c in send(r) if r else keep:
            c.start()
    for r in range(1, 16):
        s = (me.dp + 16 - r) % 16
        for j, v in enumerate(outs(s)):
            me.copy(v, v, send_sem.at[1, r, j], recv_sem.at[1, r, j], me.dp).wait_recv()
    for c in keep:
        c.wait()
    for r in range(16):
        for c in beside(r):
            c.wait_send()
        if r:
            for c in send(r):
                c.wait_send()


def expert_grads(gate, up, down, cid):
    depth, hidden = gate.shape[0] // 16, gate.shape[1] // 2
    hbm = pl.BlockSpec(memory_space=pl.ANY)
    vmem = pl.BlockSpec(memory_space=pltpu.VMEM)
    tall = jax.ShapeDtypeStruct((16, depth, hidden), gate.dtype)
    return pl.pallas_call(
        expert_grads_kernel,
        out_shape=[tall, tall, jax.ShapeDtypeStruct((16, hidden, depth), gate.dtype)],
        in_specs=[vmem] * 3,
        out_specs=[hbm] * 3,
        scratch_shapes=[
            pltpu.VMEM((2, 16, depth, hidden), gate.dtype),
            pltpu.VMEM((16, hidden, depth), gate.dtype),
            pltpu.SemaphoreType.DMA((2, 16, 3)),
            pltpu.SemaphoreType.DMA((2, 16, 3)),
            pltpu.SemaphoreType.DMA((3,)),
        ],
        compiler_params=pltpu.CompilerParams(collective_id=cid, has_side_effects=True, vmem_limit_bytes=LIMIT),
        name="expert_grads",
    )(gate, up, down)


def per_device_any(
    tokens,
    cotangent,
    expert_ids,
    gate_values,
    w_query,
    w_key,
    w_value,
    w_out,
    w_gate,
    w_up,
    w_down,
    attn_gain,
    ffn_gain,
    query_gain,
    key_gain,
):
    contract = (((1,), (1,)), ((), ()))
    contract_rows = (((0,), (0,)), ((), ()))
    residual = tokens.astype(jnp.float32)
    model_width = residual.shape[1]
    inverse_one = rms_inverse(residual)
    seq_normed = gather_rows((residual * inverse_one * attn_gain).astype(jnp.bfloat16))
    full_query, full_key, full_value, full_out = (
        lax.all_gather(w_query, "dp", axis=0, tiled=True),
        lax.all_gather(w_key, "dp", axis=0, tiled=True),
        lax.all_gather(w_value, "dp", axis=0, tiled=True),
        lax.all_gather(w_out, "dp", axis=1, tiled=True),
    )
    seq_len = seq_normed.shape[0]
    head_dim = query_gain.shape[0]
    local_heads = full_query.shape[1] // head_dim
    local_kv = full_key.shape[1] // head_dim
    group_size = local_heads // local_kv
    attn_scale = head_dim ** (-0.5)
    cosine, sine_table = rotary_tables(seq_len, head_dim)
    query_raw = jnp.dot(seq_normed, full_query, preferred_element_type=jnp.float32).reshape(
        seq_len, local_heads, head_dim
    )
    key_raw = jnp.dot(seq_normed, full_key, preferred_element_type=jnp.float32).reshape(
        seq_len, local_kv, head_dim
    )
    value_low = (
        jnp.dot(seq_normed, full_value, preferred_element_type=jnp.float32)
        .astype(jnp.bfloat16)
        .reshape(seq_len, local_kv, head_dim)
    )
    query_inverse = rms_inverse(query_raw)
    key_inverse = rms_inverse(key_raw)
    query_low = (
        rotate(query_raw * query_inverse * query_gain, cosine, sine_table) * attn_scale
    ).astype(jnp.bfloat16)
    key_low = rotate(key_raw * key_inverse * key_gain, cosine, sine_table).astype(jnp.bfloat16)
    query_heads = query_low.reshape(seq_len, local_kv, group_size, head_dim).transpose(1, 0, 2, 3)
    key_heads = key_low.transpose(1, 0, 2)
    value_heads = value_low.transpose(1, 0, 2)
    mixed_heads, logsum = lax.map(head_forward, (query_heads, key_heads, value_heads))
    mixed_flat = mixed_heads.transpose(1, 0, 2, 3).reshape(seq_len, local_heads * head_dim)
    hidden = residual + scatter_rows(
        jnp.dot(mixed_flat, full_out, preferred_element_type=jnp.float32)
    )
    inverse_two = rms_inverse(hidden)
    seq_two = gather_rows((hidden * inverse_two * ffn_gain).astype(jnp.bfloat16))
    seq_grad = gather_rows(cotangent)
    experts = w_gate.shape[0]
    dp_rows = w_gate.shape[1]
    hidden_units = w_gate.shape[2]
    dp_count = lax.axis_size("dp")
    group = dp_count // experts
    routed_rows = seq_len * expert_ids.shape[1] * 9 // 8
    capacity = (routed_rows + experts * group - 1) // (experts * group) * group
    slot_table, gate_table = dispatch(expert_ids, gate_values, experts, capacity)
    blank_row = jnp.zeros((1, model_width), jnp.bfloat16)
    padded_in = jnp.concatenate([seq_two, blank_row], axis=0)
    padded_grad = jnp.concatenate([seq_grad, blank_row], axis=0)
    empty_rows = jnp.zeros((seq_len + 1, model_width), jnp.float32)
    piece_rows = capacity // group
    down_rows = jnp.transpose(w_down, (0, 2, 1))
    gate_mine, up_mine, down_mine = (
        lax.all_to_all(widen(w_gate, group), "dp", split_axis=0, concat_axis=1, tiled=True),
        lax.all_to_all(widen(w_up, group), "dp", split_axis=0, concat_axis=1, tiled=True),
        lax.all_to_all(widen(down_rows, group), "dp", split_axis=0, concat_axis=1, tiled=True),
    )
    gate_mine = gate_mine[0]
    up_mine = up_mine[0]
    down_mine = down_mine[0]
    blocks_in = padded_in[slot_table]
    grad_blocks = (padded_grad[slot_table].astype(jnp.float32) * gate_table[:, :, None]).astype(
        jnp.bfloat16
    )
    recv_in, recv_grad = (
        lax.all_to_all(
            blocks_in.reshape(dp_count, piece_rows, model_width),
            "dp",
            split_axis=0,
            concat_axis=0,
            tiled=True,
        ),
        lax.all_to_all(
            grad_blocks.reshape(dp_count, piece_rows, model_width),
            "dp",
            split_axis=0,
            concat_axis=0,
            tiled=True,
        ),
    )
    rows_in = recv_in.reshape(-1, model_width)
    rows_grad = recv_grad.reshape(-1, model_width)
    gate_pre = jnp.dot(rows_in, gate_mine, preferred_element_type=jnp.float32)
    up_pre = jnp.dot(rows_in, up_mine, preferred_element_type=jnp.float32)
    act_low = (jax.nn.silu(gate_pre) * up_pre).astype(jnp.bfloat16)
    expert_out = lax.dot_general(act_low, down_mine, contract, preferred_element_type=jnp.float32)
    grad_act = jnp.dot(rows_grad, down_mine, preferred_element_type=jnp.float32)
    sigmoid_gate = jax.nn.sigmoid(gate_pre)
    grad_gate = (grad_act * up_pre * sigmoid_gate * (1.0 + gate_pre * (1.0 - sigmoid_gate))).astype(
        jnp.bfloat16
    )
    grad_up = (grad_act * gate_pre * sigmoid_gate).astype(jnp.bfloat16)
    grad_input = lax.dot_general(
        grad_gate, gate_mine, contract, preferred_element_type=jnp.float32
    ) + lax.dot_general(grad_up, up_mine, contract, preferred_element_type=jnp.float32)
    back_out, back_grad = (
        lax.all_to_all(
            expert_out.reshape(dp_count, piece_rows, model_width).astype(jnp.bfloat16),
            "dp",
            split_axis=0,
            concat_axis=0,
            tiled=True,
        ).astype(jnp.float32),
        lax.all_to_all(
            grad_input.reshape(dp_count, piece_rows, model_width).astype(jnp.bfloat16),
            "dp",
            split_axis=0,
            concat_axis=0,
            tiled=True,
        ).astype(jnp.float32),
    )
    back_out = back_out.reshape(experts, capacity, model_width)
    back_grad = back_grad.reshape(experts * capacity, model_width)
    flat_slots = slot_table.reshape(-1)
    combined = empty_rows.at[flat_slots].add(
        (back_out * gate_table[:, :, None]).reshape(-1, model_width)
    )
    grad_acc = empty_rows.at[flat_slots].add(back_grad)
    grad_both = jnp.concatenate([grad_gate, grad_up], axis=1)
    grad_cols = jnp.concatenate(
        [
            lax.dot_general(rows_in, grad_both, contract_rows, preferred_element_type=jnp.float32),
            lax.dot_general(rows_grad, act_low, contract_rows, preferred_element_type=jnp.float32),
        ],
        axis=1,
    )
    returned = lax.all_to_all(
        grad_cols[None].astype(jnp.bfloat16), "dp", split_axis=1, concat_axis=0, tiled=True
    ).astype(jnp.float32)
    summed = jnp.sum(returned.reshape(experts, group, dp_rows, 3 * hidden_units), axis=1)
    grad_w_gate = summed[:, :, :hidden_units]
    grad_w_up = summed[:, :, hidden_units : 2 * hidden_units]
    grad_w_down = jnp.transpose(summed[:, :, 2 * hidden_units :], (0, 2, 1))
    output = (hidden + scatter_rows(combined[:seq_len])).astype(jnp.bfloat16)
    grad_two = scatter_rows(grad_acc[:seq_len])
    ffn_gain_part = jnp.sum(grad_two * hidden * inverse_two, axis=0)
    grad_hidden = cotangent.astype(jnp.float32) + norm_backward(
        grad_two, hidden, inverse_two, ffn_gain
    )
    grad_attn = gather_rows(grad_hidden.astype(jnp.bfloat16))
    grad_mixed = lax.dot_general(
        grad_attn, full_out, contract, preferred_element_type=jnp.float32
    ).astype(jnp.bfloat16)
    grad_mixed_heads = grad_mixed.reshape(seq_len, local_kv, group_size, head_dim).transpose(
        1, 0, 2, 3
    )
    grad_query_heads, grad_key_heads, grad_value_heads = lax.map(
        head_backward, (query_heads, key_heads, value_heads, logsum, grad_mixed_heads)
    )
    grad_query_rot = (
        grad_query_heads.transpose(1, 0, 2, 3).reshape(seq_len, local_heads, head_dim) * attn_scale
    )
    grad_query_norm = rotate_back(grad_query_rot, cosine, sine_table)
    query_gain_part = jnp.sum(grad_query_norm * query_raw * query_inverse, axis=(0, 1))
    grad_query_low = (
        norm_backward(grad_query_norm, query_raw, query_inverse, query_gain)
        .astype(jnp.bfloat16)
        .reshape(seq_len, local_heads * head_dim)
    )
    grad_key_norm = rotate_back(grad_key_heads.transpose(1, 0, 2), cosine, sine_table)
    key_gain_part = jnp.sum(grad_key_norm * key_raw * key_inverse, axis=(0, 1))
    grad_key_low = (
        norm_backward(grad_key_norm, key_raw, key_inverse, key_gain)
        .astype(jnp.bfloat16)
        .reshape(seq_len, local_kv * head_dim)
    )
    grad_value_low = (
        grad_value_heads.transpose(1, 0, 2)
        .reshape(seq_len, local_kv * head_dim)
        .astype(jnp.bfloat16)
    )
    grad_proj = jnp.concatenate([grad_query_low, grad_key_low, grad_value_low], axis=1)
    full_proj = jnp.concatenate([full_query, full_key, full_value], axis=1)
    grad_one = scatter_rows(
        lax.dot_general(grad_proj, full_proj, contract, preferred_element_type=jnp.float32)
    )
    first_part = jnp.einsum("sd,sf->df", seq_normed, grad_proj, preferred_element_type=jnp.float32)
    second = jnp.einsum("sd,sf->df", grad_attn, mixed_flat, preferred_element_type=jnp.float32)
    shares = lax.psum_scatter(
        jnp.concatenate([first_part, second], axis=1), "dp", scatter_dimension=0, tiled=True
    )
    query_cols = w_query.shape[1]
    key_cols = w_key.shape[1]
    grad_w_query = shares[:, :query_cols]
    grad_w_key = shares[:, query_cols : query_cols + key_cols]
    grad_w_value = shares[:, query_cols + key_cols : query_cols + 2 * key_cols]
    grad_w_out = jnp.transpose(shares[:, query_cols + 2 * key_cols :])
    attn_gain_part = jnp.sum(grad_one * residual * inverse_one, axis=0)
    grad_tokens = (grad_hidden + norm_backward(grad_one, residual, inverse_one, attn_gain)).astype(
        jnp.bfloat16
    )
    total_gains = lax.psum(
        (attn_gain_part, ffn_gain_part, query_gain_part, key_gain_part), ("dp", "tensor")
    )
    return (
        output,
        grad_tokens,
        grad_w_query,
        grad_w_key,
        grad_w_value,
        grad_w_out,
        grad_w_gate,
        grad_w_up,
        grad_w_down,
        total_gains[0],
        total_gains[1],
        total_gains[2],
        total_gains[3],
    )


def per_device_relay(
    tokens,
    cotangent,
    expert_ids,
    gate_values,
    w_query,
    w_key,
    w_value,
    w_out,
    w_gate,
    w_up,
    w_down,
    attn_gain,
    ffn_gain,
    query_gain,
    key_gain,
):
    dot = functools.partial(jnp.dot, preferred_element_type=jnp.float32)
    dot_t = functools.partial(lax.dot_general, dimension_numbers=(((1,), (1,)), ((), ())), preferred_element_type=jnp.float32)
    t_dot = functools.partial(lax.dot_general, dimension_numbers=(((0,), (0,)), ((), ())), preferred_element_type=jnp.float32)
    low = jnp.bfloat16
    rows, width = tokens.shape
    head_dim = query_gain.shape[0]
    experts = w_gate.shape[0]
    me, core = lax.axis_index("dp"), lax.axis_index("tensor")
    mine = lax.dynamic_slice_in_dim(expert_ids, core * rows, rows, 0)
    values = lax.dynamic_slice_in_dim(gate_values, core * rows, rows, 0)
    match = mine[None] == jnp.arange(experts, dtype=jnp.int32)[:, None, None]
    gates = jnp.sum(jnp.where(match, values[None], 0.0), axis=2)
    gates = lax.dynamic_index_in_dim(lax.all_gather(gates, "dp", axis=1, tiled=True), me, 0, keepdims=False)[:, None]

    q_cols, kv_cols = w_query.shape[1] // 2, w_key.shape[1] // 2
    w_out_rows = jnp.transpose(w_out)
    halves = jnp.stack(
        [
            jnp.concatenate([w[:, h * (w.shape[1] // 2) : (h + 1) * (w.shape[1] // 2)] for w in (w_query, w_key, w_value, w_out_rows)], axis=1)
            for h in range(2)
        ]
    )
    weights = gather_pairs(halves, 1)
    weights = weights.reshape(-1, weights.shape[2])
    proj_cols = q_cols + 2 * kv_cols
    w_proj, w_back = weights[:, :proj_cols], weights[:, proj_cols:]
    gate_full, up_full, down_full = expert_weights(w_gate, w_up, w_down, 2)
    rows_grad = gather_line(cotangent, 3).reshape(-1, width)

    residual = tokens.astype(jnp.float32)
    inverse_one = rms_inverse(residual)
    seq_normed = gather_four((residual * inverse_one * attn_gain).astype(low), 4).reshape(-1, width)
    seq_len = 2 * rows
    group = q_cols // head_dim
    scale = head_dim ** (-0.5)
    cosine, sine_table = rotary_tables(seq_len, head_dim)
    proj = dot(seq_normed, w_proj)
    query_raw = proj[:, :q_cols].reshape(2, seq_len, group, head_dim)
    key_raw = proj[:, q_cols : q_cols + kv_cols].reshape(2, seq_len, 1, head_dim)
    value_low = proj[:, q_cols + kv_cols :].astype(low).reshape(2, seq_len, head_dim)
    query_inverse, key_inverse = rms_inverse(query_raw), rms_inverse(key_raw)
    query_low = (rotate(query_raw * query_inverse * query_gain, cosine, sine_table) * scale).astype(low)
    key_low = rotate(key_raw * key_inverse * key_gain, cosine, sine_table).astype(low)[:, :, 0]
    causal = jnp.arange(seq_len)[:, None] >= jnp.arange(seq_len)[None, :]
    scores = jnp.einsum("bqgd,bsd->bgqs", query_low, key_low, preferred_element_type=jnp.float32)
    exp_scores = jnp.where(causal, jnp.exp(scores), 0.0)
    probs = exp_scores / jnp.sum(exp_scores, axis=-1, keepdims=True)
    probs_low = probs.astype(low)
    mixed = jnp.einsum("bgqs,bsd->bqgd", probs_low, value_low, preferred_element_type=jnp.float32).astype(low).reshape(2 * seq_len, q_cols)
    hidden = residual + scatter_four(dot_t(mixed, w_back).astype(low).reshape(2, 2, rows, width), 5)
    inverse_two = rms_inverse(hidden)
    rows_in = gather_line((hidden * inverse_two * ffn_gain).astype(low), 6).reshape(-1, width)

    gate_pre = dot(rows_in, gate_full)
    up_pre = dot(rows_in, up_full)
    sigmoid_gate = jax.nn.sigmoid(gate_pre)
    act = (gate_pre * sigmoid_gate * up_pre).astype(low)
    expert_out = (dot(act, down_full) * gates).astype(low)
    grad_out = (rows_grad.astype(jnp.float32) * gates).astype(low)
    grad_act = dot_t(grad_out, down_full)
    grad_gate = (grad_act * up_pre * sigmoid_gate * (1.0 + gate_pre * (1.0 - sigmoid_gate))).astype(low)
    grad_up = (grad_act * gate_pre * sigmoid_gate).astype(low)
    grad_in = (dot_t(grad_gate, gate_full) + dot_t(grad_up, up_full)).astype(low)
    moe, grad_two = scatter_line([v.reshape(-1, rows, width) for v in (expert_out, grad_in)], 7)
    w_gate_part = t_dot(rows_in, grad_gate).astype(low)
    w_up_part = t_dot(rows_in, grad_up).astype(low)
    w_down_part = t_dot(act, grad_out).astype(low)
    grad_w_gate, grad_w_up, grad_w_down = [v.astype(jnp.float32) for v in expert_grads(w_gate_part, w_up_part, w_down_part, 8)]

    output = (hidden + moe).astype(low)
    ffn_gain_part = jnp.sum(grad_two * hidden * inverse_two, axis=0)
    grad_hidden = cotangent.astype(jnp.float32) + norm_backward(grad_two, hidden, inverse_two, ffn_gain)
    grad_attn = gather_four(grad_hidden.astype(low), 9).reshape(-1, width)
    grad_mixed = dot(grad_attn, w_back).astype(low).reshape(2, seq_len, group, head_dim)
    grad_probs = jnp.einsum("bqgd,bsd->bgqs", grad_mixed, value_low, preferred_element_type=jnp.float32)
    delta_sum = jnp.sum(grad_probs * probs, axis=-1, keepdims=True)
    grad_scores = (probs * (grad_probs - delta_sum)).astype(low)
    grad_query = jnp.einsum("bgqs,bsd->bqgd", grad_scores, key_low, preferred_element_type=jnp.float32)
    grad_key = jnp.einsum("bgqs,bqgd->bsd", grad_scores, query_low, preferred_element_type=jnp.float32)
    grad_value = jnp.einsum("bgqs,bqgd->bsd", probs_low, grad_mixed, preferred_element_type=jnp.float32)
    grad_query_norm = rotate_back(grad_query * scale, cosine, sine_table)
    query_gain_part = jnp.sum(grad_query_norm * query_raw * query_inverse, axis=(0, 1, 2))
    grad_query_low = norm_backward(grad_query_norm, query_raw, query_inverse, query_gain).astype(low)
    grad_key_norm = rotate_back(grad_key[:, :, None], cosine, sine_table)
    key_gain_part = jnp.sum(grad_key_norm * key_raw * key_inverse, axis=(0, 1, 2))
    grad_key_low = norm_backward(grad_key_norm, key_raw, key_inverse, key_gain).astype(low)
    grad_proj = jnp.concatenate([v.astype(low).reshape(2 * seq_len, -1) for v in (grad_query_low, grad_key_low, grad_value)], axis=1)
    grad_one = scatter_four(dot_t(grad_proj, w_proj).astype(low).reshape(2, 2, rows, width), 10)
    w_parts = jnp.concatenate([t_dot(seq_normed, grad_proj), t_dot(grad_attn, mixed)], axis=1).astype(low)
    shares = scatter_pairs(w_parts.reshape(-1, rows, w_parts.shape[1]), 11).astype(jnp.float32)
    stops = (0, q_cols, q_cols + kv_cols, proj_cols, proj_cols + q_cols)
    grads = [jnp.concatenate([shares[0, :, a:b], shares[1, :, a:b]], axis=1) for a, b in zip(stops, stops[1:])]
    attn_gain_part = jnp.sum(grad_one * residual * inverse_one, axis=0)
    grad_tokens = (grad_hidden + norm_backward(grad_one, residual, inverse_one, attn_gain)).astype(low)
    totals = lax.psum((attn_gain_part, ffn_gain_part, query_gain_part, key_gain_part), ("dp", "tensor"))
    return (output, grad_tokens, grads[0], grads[1], grads[2], jnp.transpose(grads[3]), grad_w_gate, grad_w_up, grad_w_down, *totals)


def solution(mesh):
    return jax.shard_map(
        per_device_relay if tuple(mesh.shape.values()) == (16, 2) else per_device_any,
        mesh=mesh,
        in_specs=(
            P(("dp", "tensor"), None),
            P(("dp", "tensor"), None),
            P("dp", None),
            P("dp", None),
            P("dp", "tensor"),
            P("dp", "tensor"),
            P("dp", "tensor"),
            P("tensor", "dp"),
            P(None, "dp", "tensor"),
            P(None, "dp", "tensor"),
            P(None, "tensor", "dp"),
            P(),
            P(),
            P(),
            P(),
        ),
        out_specs=(
            P(("dp", "tensor"), None),
            P(("dp", "tensor"), None),
            P("dp", "tensor"),
            P("dp", "tensor"),
            P("dp", "tensor"),
            P("tensor", "dp"),
            P(None, "dp", "tensor"),
            P(None, "dp", "tensor"),
            P(None, "tensor", "dp"),
            P(),
            P(),
            P(),
            P(),
        ),
        check_vma=False,
    )
```

```python
import functools

import jax
import jax.numpy as jnp
from jax import lax
from jax.experimental import pallas as pl
from jax.experimental.pallas import tpu as pltpu
from jax.sharding import PartitionSpec as P

epsilon = 1e-06
theta_base = 1000000.0


def rms_inverse(values):
    return lax.rsqrt(jnp.mean(values * values, axis=-1, keepdims=True) + epsilon)


def norm_backward(grad_in, values, inverse, gain_vec):
    scaled = grad_in * gain_vec
    inner_mean = jnp.mean(scaled * values, axis=-1, keepdims=True)
    return inverse * scaled - values * inverse**3 * inner_mean


def rotary_tables(seq_len, head_dim):
    half_dim = head_dim // 2
    frequency = theta_base ** (-jnp.arange(half_dim, dtype=jnp.float32) * 2.0 / head_dim)
    angles = jnp.arange(seq_len, dtype=jnp.float32)[:, None] * frequency[None, :]
    return (jnp.cos(angles)[:, None, :], jnp.sin(angles)[:, None, :])


def rotate(values, cosine, sine_table):
    half_dim = values.shape[-1] // 2
    first_part = values[..., :half_dim]
    second = values[..., half_dim:]
    return jnp.concatenate(
        [first_part * cosine - second * sine_table, second * cosine + first_part * sine_table],
        axis=-1,
    )


def rotate_back(grad_in, cosine, sine_table):
    half_dim = grad_in.shape[-1] // 2
    first_part = grad_in[..., :half_dim]
    second = grad_in[..., half_dim:]
    return jnp.concatenate(
        [first_part * cosine + second * sine_table, second * cosine - first_part * sine_table],
        axis=-1,
    )


def dispatch(expert_ids, gate_values, experts, capacity):
    seq_len = expert_ids.shape[0]
    is_match = expert_ids[:, :, None] == jnp.arange(experts, dtype=jnp.int32)[None, None, :]
    expert_hits = jnp.sum(is_match.astype(jnp.int32), axis=1)
    before = jnp.cumsum(expert_hits, axis=0) - expert_hits
    slot_ids = jnp.sum(jnp.where(is_match, before[:, None, :], 0), axis=2)
    token_index = jnp.broadcast_to(jnp.arange(seq_len, dtype=jnp.int32)[:, None], expert_ids.shape)
    slot_table = (
        jnp.full((experts, capacity), seq_len, jnp.int32).at[expert_ids, slot_ids].set(token_index)
    )
    gate_table = (
        jnp.zeros((experts, capacity), jnp.float32).at[expert_ids, slot_ids].set(gate_values)
    )
    return (slot_table, gate_table)


def head_forward(head_inputs):
    query_vals, key_vals, value_vals = head_inputs
    seq_len = key_vals.shape[0]
    block_rows = min(512, seq_len)
    key_positions = jnp.arange(seq_len)

    def one_block(row_start):
        scores = jnp.einsum("qgd,sd->gqs", query_vals, key_vals, preferred_element_type=jnp.float32)
        causal = (row_start + jnp.arange(block_rows))[:, None] >= key_positions[None, :]
        exp_scores = jnp.where(causal, jnp.exp(scores), 0.0)
        denominator = jnp.sum(exp_scores, axis=-1, keepdims=True)
        softmax_low = (exp_scores / denominator).astype(jnp.bfloat16)
        mixed_out = jnp.einsum(
            "gqs,sd->qgd", softmax_low, value_vals, preferred_element_type=jnp.float32
        )
        return (mixed_out.astype(jnp.bfloat16), jnp.log(denominator[..., 0]))

    block_starts = jnp.arange(seq_len // block_rows, dtype=jnp.int32) * block_rows
    mixed_out, logsum = lax.map(one_block, block_starts)
    return (mixed_out.reshape(seq_len, query_vals.shape[1], query_vals.shape[2]), logsum)


def head_backward(head_inputs):
    query_vals, key_vals, value_vals, logsum, grad_mixed = head_inputs
    seq_len = key_vals.shape[0]
    block_rows = min(512, seq_len)
    key_positions = jnp.arange(seq_len)

    def one_block(state_in, block_in):
        grad_key, grad_value = state_in
        row_start, block_logsum = block_in
        scores = jnp.einsum("qgd,sd->gqs", query_vals, key_vals, preferred_element_type=jnp.float32)
        causal = (row_start + jnp.arange(block_rows))[:, None] >= key_positions[None, :]
        softmax_vals = jnp.where(causal, jnp.exp(scores - block_logsum[..., None]), 0.0)
        grad_probs = jnp.einsum(
            "qgd,sd->gqs", grad_mixed, value_vals, preferred_element_type=jnp.float32
        )
        delta_sum = jnp.sum(grad_probs * softmax_vals, axis=-1, keepdims=True)
        grad_scores = (softmax_vals * (grad_probs - delta_sum)).astype(jnp.bfloat16)
        grad_query = jnp.einsum(
            "gqs,sd->qgd", grad_scores, key_vals, preferred_element_type=jnp.float32
        )
        grad_key = grad_key + jnp.einsum(
            "gqs,qgd->sd", grad_scores, query_vals, preferred_element_type=jnp.float32
        )
        grad_value = grad_value + jnp.einsum(
            "gqs,qgd->sd",
            softmax_vals.astype(jnp.bfloat16),
            grad_mixed,
            preferred_element_type=jnp.float32,
        )
        return ((grad_key, grad_value), grad_query)

    block_starts = jnp.arange(seq_len // block_rows, dtype=jnp.int32) * block_rows
    zero_rows = jnp.zeros(key_vals.shape, jnp.float32)
    (grad_key, grad_value), grad_query = lax.scan(
        one_block, (zero_rows, zero_rows), (block_starts, logsum)
    )
    return (grad_query.reshape(query_vals.shape), grad_key, grad_value)


def gather_rows(values):
    return lax.all_gather(values, "tensor", axis=0, tiled=True)


def scatter_rows(values):
    return lax.psum_scatter(
        values.astype(jnp.bfloat16), "tensor", scatter_dimension=0, tiled=True
    ).astype(jnp.float32)


def widen(stacked, group):
    experts = stacked.shape[0]
    spread = jnp.broadcast_to(stacked[:, None], (experts, group) + stacked.shape[1:])
    return spread.reshape((experts * group,) + stacked.shape[1:])


MESH = pl.DeviceIdType.MESH
LIMIT = 66_000_000


class Place:
    def __init__(self):
        self.dp = lax.axis_index("dp")
        self.core = lax.axis_index("tensor")
        x, y = self.dp % 2, (self.dp // 2) % 2
        self.z = self.dp // 4
        step_x, step_y = 1 - 2 * x, 2 * (1 - 2 * y)
        self.da = (1 - self.core) * step_x + self.core * step_y
        self.db = (1 - self.core) * step_y + self.core * step_x
        self.half = self.z % 2
        self.pair = 4 * (1 - 2 * self.half)
        self.far = 8 * (1 - 2 * (self.z // 2))

    def copy(self, src, dst, send_sem, recv_sem, to, core=None):
        return pltpu.make_async_remote_copy(
            src_ref=src,
            dst_ref=dst,
            send_sem=send_sem,
            recv_sem=recv_sem,
            device_id=(to, self.core if core is None else core),
            device_id_type=MESH,
        )

    def at_z(self, z):
        return self.dp + 4 * (z - self.z)

    def greet(self, line=False, near=False, chain=False, everyone=False, partner=False):
        barrier = pltpu.get_barrier_semaphore()
        count = 0

        def signal(to, core):
            pl.semaphore_signal(barrier, inc=1, device_id=(to, core), device_id_type=MESH)

        if everyone:
            for r in range(1, 16):
                signal((self.dp + r) % 16, self.core)
            count = count + 15
        else:
            if near:
                signal(self.dp + self.da, self.core)
                signal(self.dp + self.db, self.core)
                count = count + 2
            if chain:
                signal(self.dp + self.pair, self.core)
                count = count + 1
                if near:
                    signal(self.dp + self.far, self.core)
                    count = count + 1
            if line:
                pl.when(self.z > 0)(lambda: signal(self.dp - 4, self.core))
                pl.when(self.z < 3)(lambda: signal(self.dp + 4, self.core))
                count = count + jnp.where(self.z > 0, 1, 0) + jnp.where(self.z < 3, 1, 0)
        if partner:
            signal(self.dp, 1 - self.core)
            count = count + 1
        pl.semaphore_wait(barrier, count)


def add_rows(target, terms, rows, block=16):
    def body(i, _):
        at = pl.ds(pl.multiple_of(i * block, block), block)
        total = terms[0][at, :].astype(jnp.float32)
        for term in terms[1:]:
            total = total + term[at, :].astype(jnp.float32)
        target[at, :] = total.astype(target.dtype)
        return 0

    lax.fori_loop(0, rows // block, body, 0)


def gather_four_kernel(x_ref, out_ref, send_sem, recv_sem):
    me = Place()
    me.greet(chain=True, partner=True)
    mine, theirs = out_ref.at[me.half, me.core], out_ref.at[1 - me.half, me.core]
    across = me.copy(x_ref, mine, send_sem.at[0], recv_sem.at[0], me.dp + me.pair)
    across.start()
    beside = me.copy(x_ref, mine, send_sem.at[1], recv_sem.at[1], me.dp, 1 - me.core)
    beside.start()
    mine[...] = x_ref[...]
    across.wait_recv()
    relay = me.copy(theirs, theirs, send_sem.at[2], recv_sem.at[2], me.dp, 1 - me.core)
    relay.start()
    across.wait_send()
    beside.wait()
    relay.wait()


def gather_four(x, cid):
    rows, columns = x.shape
    vmem = pl.BlockSpec(memory_space=pltpu.VMEM)
    return pl.pallas_call(
        gather_four_kernel,
        out_shape=jax.ShapeDtypeStruct((2, 2, rows, columns), x.dtype),
        in_specs=[vmem],
        out_specs=vmem,
        scratch_shapes=[pltpu.SemaphoreType.DMA((3,)), pltpu.SemaphoreType.DMA((3,))],
        compiler_params=pltpu.CompilerParams(collective_id=cid, has_side_effects=True),
        name="gather_four",
    )(x)


def scatter_four_kernel(p_ref, out_ref, from_core, from_pair, send_sem, recv_sem):
    me = Place()
    rows = p_ref.shape[2]
    me.greet(chain=True, partner=True)

    def beside(h, slot):
        return me.copy(p_ref.at[h, 1 - me.core], from_core.at[slot], send_sem.at[slot], recv_sem.at[slot], me.dp, 1 - me.core)

    first, second = beside(1 - me.half, 0), beside(me.half, 1)
    first.start()
    second.start()
    first.wait_recv()
    add_rows(from_core.at[0], (p_ref.at[1 - me.half, me.core], from_core.at[0]), rows)
    across = me.copy(from_core.at[0], from_pair, send_sem.at[2], recv_sem.at[2], me.dp + me.pair)
    across.start()
    second.wait_recv()
    add_rows(from_core.at[1], (p_ref.at[me.half, me.core], from_core.at[1]), rows)
    across.wait_recv()
    add_rows(out_ref, (from_core.at[1], from_pair), rows)
    across.wait_send()
    first.wait_send()
    second.wait_send()


def scatter_four(p, cid):
    _, _, rows, columns = p.shape
    vmem = pl.BlockSpec(memory_space=pltpu.VMEM)
    return pl.pallas_call(
        scatter_four_kernel,
        out_shape=jax.ShapeDtypeStruct((rows, columns), jnp.float32),
        in_specs=[vmem],
        out_specs=vmem,
        scratch_shapes=[
            pltpu.VMEM((2, rows, columns), p.dtype),
            pltpu.VMEM((rows, columns), p.dtype),
            pltpu.SemaphoreType.DMA((3,)),
            pltpu.SemaphoreType.DMA((3,)),
        ],
        compiler_params=pltpu.CompilerParams(collective_id=cid, has_side_effects=True),
        name="scatter_four",
    )(p)


def run(*threads):
    threads = list(threads)
    while threads:
        for thread in list(threads):
            if next(thread, "end") == "end":
                threads.remove(thread)


def lagged(items, first, second, lag):
    for n in range(len(items) + lag):
        if n < len(items):
            first(items[n])
            yield
        if n >= lag:
            second(items[n - lag])
            yield


def gather_line(me, x_ref, out_ref, send_sem, recv_sem):
    def part(source, to, slot, own=False):
        return me.copy(x_ref if own else out_ref.at[source], out_ref.at[source], send_sem.at[slot], recv_sem.at[source], to)

    sides = ((-1, me.z < 3, 4), (1, me.z > 0, -4))

    def exists(d, side):
        return (me.z - d >= 0) if side == 0 else (me.z + d <= 3)

    def slot_z(d, side, j):
        return 4 + ((d - 1) * 2 + side) * 3 + j

    def slot_a(off):
        return 25 + off

    def pass_a(off):
        source = me.dp + me.da + 4 * off
        part(source, me.dp, slot_a(off)).wait_recv()
        part(source, me.dp + me.db, slot_a(off)).start()

    pl.when(me.z < 3)(lambda: part(me.dp, me.dp + 4, 0, True).start())
    pl.when(me.z > 0)(lambda: part(me.dp, me.dp - 4, 1, True).start())
    part(me.dp, me.dp + me.db, 3, True).start()
    part(me.dp, me.dp + me.da, 2, True).start()
    yield
    for d in range(1, 5):
        if d < 4:
            for side, (sign, forward, step) in enumerate(sides):
                source = me.dp + 4 * sign * d

                def arrive():
                    part(source, me.dp, slot_z(d, side, 0)).wait_recv()
                    pl.when(forward)(lambda: part(source, me.dp + step, slot_z(d, side, 0)).start())
                    part(source, me.dp + me.db, slot_z(d, side, 2)).start()
                    part(source, me.dp + me.da, slot_z(d, side, 1)).start()

                pl.when(exists(d, side))(arrive)
                yield
        if d == 1:
            pass_a(0)
            yield
        else:
            for side, (sign, *_) in enumerate(sides):
                pl.when(exists(d - 1, side))(lambda: pass_a(sign * (d - 1)))
                yield
    for z in range(4):
        for g in (0, 1):
            part(me.at_z(z) + me.db + g * me.da, me.dp, 0).wait_recv()
            yield

    def sent(slot):
        part(me.dp, me.dp, slot).wait_send()

    pl.when(me.z < 3)(lambda: sent(0))
    pl.when(me.z > 0)(lambda: sent(1))
    sent(2)
    sent(3)
    sent(slot_a(0))
    for d in range(1, 4):
        for side, (sign, forward, _) in enumerate(sides):

            def finish():
                pl.when(forward)(lambda: sent(slot_z(d, side, 0)))
                sent(slot_z(d, side, 1))
                sent(slot_z(d, side, 2))
                sent(slot_a(sign * d))

            pl.when(exists(d, side))(finish)


def gather_pairs(me, x_ref, out_ref, send_sem, recv_sem):
    mine, other = me.dp, me.dp + me.pair

    def part(src, where, to, slot):
        return me.copy(src, out_ref.at[where], send_sem.at[slot], recv_sem.at[where], to)

    def relay(where, to, slot):
        part(out_ref.at[where], where, to, slot).start()

    def arrived(where):
        part(out_ref.at[where], where, me.dp, 0).wait_recv()

    part(x_ref.at[1 - me.half], mine, other, 0).start()
    part(x_ref.at[me.half], mine, me.dp + me.far, 1).start()
    part(x_ref.at[me.half], mine, me.dp + me.db, 2).start()
    part(x_ref.at[me.half], mine, me.dp + me.da, 3).start()
    yield
    arrived(other)
    relay(other, me.dp + me.far, 4)
    relay(other, me.dp + me.db, 5)
    relay(other, me.dp + me.da, 6)
    yield
    arrived(mine + me.da)
    relay(mine + me.da, me.dp + me.db, 7)
    yield
    arrived(mine + me.far)
    relay(mine + me.far, me.dp + me.db, 8)
    relay(mine + me.far, me.dp + me.da, 9)
    yield
    arrived(other + me.da)
    relay(other + me.da, me.dp + me.db, 10)
    yield
    arrived(other + me.far)
    relay(other + me.far, me.dp + me.db, 11)
    relay(other + me.far, me.dp + me.da, 12)
    yield
    arrived(mine + me.far + me.da)
    relay(mine + me.far + me.da, me.dp + me.db, 13)
    yield
    arrived(other + me.far + me.da)
    relay(other + me.far + me.da, me.dp + me.db, 14)
    yield
    for base in (mine, other, mine + me.far, other + me.far):
        arrived(base + me.db)
        yield
        arrived(base + me.da + me.db)
        yield
    for slot in range(15):
        part(out_ref.at[mine], mine, me.dp, slot).wait_send()


def swap_rows(me, x_ref, out_ref, send_sem, recv_sem):
    for r in range(1, 16):
        to = (me.dp + r) % 16
        me.copy(x_ref.at[to], out_ref.at[me.dp], send_sem.at[r], recv_sem.at[r], to).start()
    yield
    for r in range(1, 16):
        s = (me.dp + 16 - r) % 16
        me.copy(x_ref.at[s], out_ref.at[s], send_sem.at[r], recv_sem.at[r], me.dp).wait_recv()
    for r in range(1, 16):
        me.copy(x_ref.at[me.dp], out_ref.at[me.dp], send_sem.at[r], recv_sem.at[r], me.dp).wait_send()


def keep_own(src, staging, dst, sems):
    load = pltpu.make_async_copy(src, staging, sems.at[0])
    store = pltpu.make_async_copy(staging, dst, sems.at[1])
    load.start()

    def finish():
        load.wait()
        store.start()
        store.wait()

    return finish


def gather_first_kernel(w_ref, c_ref, g_ref, w_out, c_out, g_out, w_own, c_own, w_send, w_recv, c_send, c_recv, g_send, g_recv, copy_sem):
    me = Place()
    ends = [
        keep_own(w_ref.at[me.half], w_own, w_out.at[me.dp], copy_sem.at[0]),
        keep_own(c_ref, c_own, c_out.at[me.dp], copy_sem.at[1]),
    ]
    g_out[me.dp] = g_ref[me.dp]
    me.greet(everyone=True)
    run(
        gather_pairs(me, w_ref, w_out, w_send, w_recv),
        gather_line(me, c_ref, c_out, c_send, c_recv),
        swap_rows(me, g_ref, g_out, g_send, g_recv),
    )
    for end in ends:
        end()


def gather_first(weights, rows, gates, cid):
    hbm, vmem = pl.BlockSpec(memory_space=pl.ANY), pl.BlockSpec(memory_space=pltpu.VMEM)
    dma = pltpu.SemaphoreType.DMA
    return pl.pallas_call(
        gather_first_kernel,
        out_shape=[
            jax.ShapeDtypeStruct((16,) + weights.shape[1:], weights.dtype),
            jax.ShapeDtypeStruct((16,) + rows.shape, rows.dtype),
            jax.ShapeDtypeStruct(gates.shape, gates.dtype),
        ],
        in_specs=[hbm, hbm, vmem],
        out_specs=[hbm, hbm, vmem],
        scratch_shapes=[
            pltpu.VMEM(weights.shape[1:], weights.dtype),
            pltpu.VMEM(rows.shape, rows.dtype),
            dma((15,)),
            dma((16,)),
            dma((29,)),
            dma((16,)),
            dma((16,)),
            dma((16,)),
            dma((2, 2)),
        ],
        compiler_params=pltpu.CompilerParams(collective_id=cid, has_side_effects=True),
        name="gather_first",
    )(weights, rows, gates)


def gather_rows_kernel(x_ref, out_ref, own, send_sem, recv_sem, copy_sem):
    me = Place()
    end = keep_own(x_ref, own, out_ref.at[me.dp], copy_sem)
    me.greet(line=True, near=True)
    run(gather_line(me, x_ref, out_ref, send_sem, recv_sem))
    end()


def gather_dp(x, cid):
    hbm = pl.BlockSpec(memory_space=pl.ANY)
    dma = pltpu.SemaphoreType.DMA
    return pl.pallas_call(
        gather_rows_kernel,
        out_shape=jax.ShapeDtypeStruct((16,) + x.shape, x.dtype),
        in_specs=[hbm],
        out_specs=hbm,
        scratch_shapes=[pltpu.VMEM(x.shape, x.dtype), dma((29,)), dma((16,)), dma((2,))],
        compiler_params=pltpu.CompilerParams(collective_id=cid, has_side_effects=True),
        name="gather_dp",
    )(x)


def scatter_pairs(me, chunks, p_ref, out_ref, from_b, from_a, from_far, send_sem, recv_sem):
    rows = p_ref.shape[1] // chunks
    other = me.dp + me.pair
    bases = (me.dp, other, me.dp + me.far, other + me.far)
    items = [(j, k) for j in (2, 3, 1, 0) for k in range(chunks)]

    def at(k):
        return pl.ds(k * rows, rows)

    def copy(src, dst, slot, k, to):
        return me.copy(src, dst, send_sem.at[slot, k], recv_sem.at[slot, k], to)

    def send_b(g, j, k):
        return copy(p_ref.at[bases[j] + me.db + g * me.da, at(k)], from_b.at[g, j, at(k)], g * 4 + j, k, me.dp + me.db)

    def send_a(j, k):
        return copy(from_b.at[1, j, at(k)], from_a.at[j, at(k)], 8 + j, k, me.dp + me.da)

    def send_far(j, k):
        return copy(from_b.at[0, 2 + j, at(k)], from_far.at[j, at(k)], 12 + j, k, me.dp + me.far)

    def swap(k):
        return copy(from_b.at[0, 1, at(k)], out_ref.at[me.half, at(k)], 14, k, other)

    for j, k in items:
        send_b(1, j, k).start()
        send_b(0, j, k).start()
    yield

    def first(item):
        j, k = item
        send_b(1, j, k).wait_recv()
        add_rows(from_b.at[1, j, at(k)], (p_ref.at[bases[j] + me.da, at(k)], from_b.at[1, j, at(k)]), rows)
        send_a(j, k).start()

    def second(item):
        j, k = item
        send_b(0, j, k).wait_recv()
        send_a(j, k).wait_recv()
        terms = (p_ref.at[bases[j], at(k)], from_b.at[0, j, at(k)], from_a.at[j, at(k)])
        if j >= 2:
            add_rows(from_b.at[0, j, at(k)], terms, rows)
            send_far(j - 2, k).start()
        else:
            send_far(j, k).wait_recv()
            target = from_b.at[0, 1, at(k)] if j else out_ref.at[me.half, at(k)]
            add_rows(target, terms + (from_far.at[j, at(k)],), rows)
            if j:
                swap(k).start()

    yield from lagged(items, first, second, 2)
    for k in range(chunks):
        swap(k).wait_send()
        theirs = out_ref.at[1 - me.half, at(k)]
        copy(theirs, theirs, 14, k, other).wait_recv()
        for j in range(4):
            send_b(0, j, k).wait_send()
            send_b(1, j, k).wait_send()
            send_a(j, k).wait_send()
        send_far(0, k).wait_send()
        send_far(1, k).wait_send()


def sum_all(me, x_ref, out_ref, held, send_sem, recv_sem):
    out_ref[...] = x_ref[...]
    steps = ((me.dp, 1 - me.core), (me.dp + me.da, me.core), (me.dp + me.db, me.core), (me.dp + me.pair, me.core), (me.dp + me.far, me.core))
    yield
    for n, (to, core) in enumerate(steps):
        send = me.copy(held.at[0, n], held.at[1, n], send_sem.at[n], recv_sem.at[n], to, core)
        held[0, n] = out_ref[...]
        send.start()
        yield
        send.wait()
        out_ref[...] = held[0, n] + held[1, n]
        yield


def scatter_last_kernel(chunks, p_ref, x_ref, out_ref, sum_ref, from_b, from_a, from_far, held, send_sem, recv_sem, sum_send, sum_recv):
    me = Place()
    me.greet(near=True, chain=True, partner=True)
    run(
        scatter_pairs(me, chunks, p_ref, out_ref, from_b, from_a, from_far, send_sem, recv_sem),
        sum_all(me, x_ref, sum_ref, held, sum_send, sum_recv),
    )


def scatter_last(p, x, cid, chunks=2):
    _, rows, columns = p.shape
    vmem = pl.BlockSpec(memory_space=pltpu.VMEM)
    dma = pltpu.SemaphoreType.DMA
    return pl.pallas_call(
        functools.partial(scatter_last_kernel, chunks),
        out_shape=[jax.ShapeDtypeStruct((2, rows, columns), p.dtype), jax.ShapeDtypeStruct(x.shape, x.dtype)],
        in_specs=[vmem] * 2,
        out_specs=[vmem] * 2,
        scratch_shapes=[
            pltpu.VMEM((2, 4, rows, columns), p.dtype),
            pltpu.VMEM((4, rows, columns), p.dtype),
            pltpu.VMEM((2, rows, columns), p.dtype),
            pltpu.VMEM((2, 5) + x.shape, x.dtype),
            dma((15, chunks)),
            dma((15, chunks)),
            dma((5,)),
            dma((5,)),
        ],
        compiler_params=pltpu.CompilerParams(collective_id=cid, has_side_effects=True, vmem_limit_bytes=LIMIT),
        name="scatter_last",
    )(p, x)


def scatter_line(me, p_ref, out_ref, from_b, from_a, from_z, send_sem, recv_sem):
    rows = p_ref.shape[1]
    low = me.z < 2
    depth = jnp.where(low, me.z, 3 - me.z)
    away = jnp.where(low, 1, 0)
    items = [(t, jnp.where(low, t, 3 - t)) for t in (3, 2, 1, 0)]

    def copy(src, dst, slot, to):
        return me.copy(src, dst, send_sem.at[slot], recv_sem.at[slot], to)

    def send_b(g, z):
        return copy(p_ref.at[me.at_z(z) + me.db + g * me.da], from_b.at[g, z], g * 4 + z, me.dp + me.db)

    def send_a(z):
        return copy(from_b.at[1, z], from_a.at[z], 8 + z, me.dp + me.da)

    def send_z(z, up):
        return copy(from_b.at[0, z], from_z.at[up, z], 12 + 4 * up + z, me.dp - 4 + 8 * up)

    for _, z in items:
        send_b(1, z).start()
        send_b(0, z).start()
    yield

    def first(item):
        _, z = item
        send_b(1, z).wait_recv()
        add_rows(from_b.at[1, z], (p_ref.at[me.at_z(z) + me.da], from_b.at[1, z]), rows)
        send_a(z).start()

    def second(item):
        t, z = item
        up = away if t else 1 - away
        send_b(0, z).wait_recv()
        send_a(z).wait_recv()
        terms = (p_ref.at[me.at_z(z)], from_b.at[0, z], from_a.at[z])
        joins = (depth == 1) & (t != 1) if t < 2 else depth == 1

        def alone():
            add_rows(from_b.at[0, z], terms, rows)

        def join():
            send_z(z, up).wait_recv()
            add_rows(from_b.at[0, z], terms + (from_z.at[up, z],), rows)

        pl.when(joins)(join)
        pl.when(jnp.logical_not(joins))(alone)
        pl.when((depth < t) if t else (depth == 1))(lambda: send_z(z, up).start())

    yield from lagged(items, first, second, 1)
    here = from_b.at[0, me.z]
    pl.when(me.z > 0)(lambda: send_z(me.z, 1).wait_recv())
    pl.when(me.z < 3)(lambda: send_z(me.z, 0).wait_recv())
    pl.when(me.z == 0)(lambda: add_rows(out_ref, (here, from_z.at[0, me.z]), rows))
    pl.when(me.z == 3)(lambda: add_rows(out_ref, (here, from_z.at[1, me.z]), rows))
    pl.when(depth == 1)(lambda: add_rows(out_ref, (here, from_z.at[0, me.z], from_z.at[1, me.z]), rows))
    yield
    for z in range(4):
        send_b(0, z).wait_send()
        send_b(1, z).wait_send()
        send_a(z).wait_send()
        pl.when(me.z < z)(lambda: send_z(z, 1).wait_send())
        pl.when(me.z > z)(lambda: send_z(z, 0).wait_send())


def scatter_rows_kernel(number, *refs):
    p_refs, out_refs = refs[:number], refs[number : 2 * number]
    from_b, from_a, from_z, send_sem, recv_sem = refs[2 * number :]
    me = Place()
    me.greet(line=True, near=True)
    run(
        *(
            scatter_line(me, p_refs[i], out_refs[i], from_b.at[i], from_a.at[i], from_z.at[i], send_sem.at[i], recv_sem.at[i])
            for i in range(number)
        )
    )


def scatter_dp(arrays, cid):
    number = len(arrays)
    _, rows, columns = arrays[0].shape
    dtype = arrays[0].dtype
    vmem = pl.BlockSpec(memory_space=pltpu.VMEM)
    return pl.pallas_call(
        functools.partial(scatter_rows_kernel, number),
        out_shape=[jax.ShapeDtypeStruct((rows, columns), jnp.float32)] * number,
        in_specs=[vmem] * number,
        out_specs=[vmem] * number,
        scratch_shapes=[
            pltpu.VMEM((number, 2, 4, rows, columns), dtype),
            pltpu.VMEM((number, 4, rows, columns), dtype),
            pltpu.VMEM((number, 2, 4, rows, columns), dtype),
            pltpu.SemaphoreType.DMA((number, 20)),
            pltpu.SemaphoreType.DMA((number, 20)),
        ],
        compiler_params=pltpu.CompilerParams(collective_id=cid, has_side_effects=True, vmem_limit_bytes=LIMIT),
        name="scatter_dp",
    )(*arrays)


def join_cores_kernel(number, *refs):
    ins, outs = refs[:number], refs[number : 2 * number]
    send_sem, recv_sem, copy_sem = refs[2 * number :]
    me = Place()
    me.greet(partner=True)
    columns = ins[0].shape[1]
    cols = pl.ds(pl.multiple_of(me.core * columns, 128), columns)
    copies = []
    for i, (src, dst) in enumerate(zip(ins, outs)):
        copies.append(me.copy(src, dst.at[:, cols], send_sem.at[i], recv_sem.at[i], me.dp, 1 - me.core))
        copies.append(pltpu.make_async_copy(src, dst.at[:, cols], copy_sem.at[i]))
    for c in copies:
        c.start()
    for c in copies[1::2]:
        c.wait()
    other = pl.ds(pl.multiple_of((1 - me.core) * columns, 128), columns)
    for i, (src, dst) in enumerate(zip(ins, outs)):
        me.copy(src, dst.at[:, other], send_sem.at[i], recv_sem.at[i], me.dp, 1 - me.core).wait_recv()
        copies[2 * i].wait_send()


def join_cores(arrays, cid):
    number = len(arrays)
    rows, columns = arrays[0].shape
    hbm, vmem = pl.BlockSpec(memory_space=pl.ANY), pl.BlockSpec(memory_space=pltpu.VMEM)
    return pl.pallas_call(
        functools.partial(join_cores_kernel, number),
        out_shape=[jax.ShapeDtypeStruct((rows, 2 * columns), arrays[0].dtype)] * number,
        in_specs=[vmem] * number,
        out_specs=[hbm] * number,
        scratch_shapes=[pltpu.SemaphoreType.DMA((number,))] * 3,
        compiler_params=pltpu.CompilerParams(collective_id=cid, has_side_effects=True),
        name="join_cores",
    )(*arrays)


def sum_cores_kernel(number, *refs):
    ins, outs = refs[:number], refs[number : 2 * number]
    held, send_sem, recv_sem = refs[2 * number :]
    me = Place()
    me.greet(partner=True)
    rows, columns = outs[0].shape
    chunks = send_sem.shape[1]
    part = rows // chunks
    cols = pl.ds(pl.multiple_of(me.core * columns, 128), columns)
    other = pl.ds(pl.multiple_of((1 - me.core) * columns, 128), columns)

    def send(i, k):
        at = pl.ds(k * part, part)
        return me.copy(ins[i].at[at, other], held.at[i, at], send_sem.at[i, k], recv_sem.at[i, k], me.dp, 1 - me.core)

    every = [(i, k) for i in range(number) for k in range(chunks)]
    for i, k in every:
        send(i, k).start()
    for i, k in every:
        send(i, k).wait_recv()
        at = pl.ds(k * part, part)
        add_rows(outs[i].at[at], (ins[i].at[at, cols], held.at[i, at]), part, 64)
    for i, k in every:
        send(i, k).wait_send()


def sum_cores(arrays, cid, chunks=4):
    number = len(arrays)
    rows, columns = arrays[0].shape[0], arrays[0].shape[1] // 2
    vmem = pl.BlockSpec(memory_space=pltpu.VMEM)
    return pl.pallas_call(
        functools.partial(sum_cores_kernel, number),
        out_shape=[jax.ShapeDtypeStruct((rows, columns), arrays[0].dtype)] * number,
        in_specs=[vmem] * number,
        out_specs=[vmem] * number,
        scratch_shapes=[
            pltpu.VMEM((number, rows, columns), arrays[0].dtype),
            pltpu.SemaphoreType.DMA((number, chunks)),
            pltpu.SemaphoreType.DMA((number, chunks)),
        ],
        compiler_params=pltpu.CompilerParams(collective_id=cid, has_side_effects=True, vmem_limit_bytes=LIMIT),
        name="sum_cores",
    )(*arrays)


def per_device_any(
    tokens,
    cotangent,
    expert_ids,
    gate_values,
    w_query,
    w_key,
    w_value,
    w_out,
    w_gate,
    w_up,
    w_down,
    attn_gain,
    ffn_gain,
    query_gain,
    key_gain,
):
    contract = (((1,), (1,)), ((), ()))
    contract_rows = (((0,), (0,)), ((), ()))
    residual = tokens.astype(jnp.float32)
    model_width = residual.shape[1]
    inverse_one = rms_inverse(residual)
    seq_normed = gather_rows((residual * inverse_one * attn_gain).astype(jnp.bfloat16))
    full_query, full_key, full_value, full_out = (
        lax.all_gather(w_query, "dp", axis=0, tiled=True),
        lax.all_gather(w_key, "dp", axis=0, tiled=True),
        lax.all_gather(w_value, "dp", axis=0, tiled=True),
        lax.all_gather(w_out, "dp", axis=1, tiled=True),
    )
    seq_len = seq_normed.shape[0]
    head_dim = query_gain.shape[0]
    local_heads = full_query.shape[1] // head_dim
    local_kv = full_key.shape[1] // head_dim
    group_size = local_heads // local_kv
    attn_scale = head_dim ** (-0.5)
    cosine, sine_table = rotary_tables(seq_len, head_dim)
    query_raw = jnp.dot(seq_normed, full_query, preferred_element_type=jnp.float32).reshape(
        seq_len, local_heads, head_dim
    )
    key_raw = jnp.dot(seq_normed, full_key, preferred_element_type=jnp.float32).reshape(
        seq_len, local_kv, head_dim
    )
    value_low = (
        jnp.dot(seq_normed, full_value, preferred_element_type=jnp.float32)
        .astype(jnp.bfloat16)
        .reshape(seq_len, local_kv, head_dim)
    )
    query_inverse = rms_inverse(query_raw)
    key_inverse = rms_inverse(key_raw)
    query_low = (
        rotate(query_raw * query_inverse * query_gain, cosine, sine_table) * attn_scale
    ).astype(jnp.bfloat16)
    key_low = rotate(key_raw * key_inverse * key_gain, cosine, sine_table).astype(jnp.bfloat16)
    query_heads = query_low.reshape(seq_len, local_kv, group_size, head_dim).transpose(1, 0, 2, 3)
    key_heads = key_low.transpose(1, 0, 2)
    value_heads = value_low.transpose(1, 0, 2)
    mixed_heads, logsum = lax.map(head_forward, (query_heads, key_heads, value_heads))
    mixed_flat = mixed_heads.transpose(1, 0, 2, 3).reshape(seq_len, local_heads * head_dim)
    hidden = residual + scatter_rows(
        jnp.dot(mixed_flat, full_out, preferred_element_type=jnp.float32)
    )
    inverse_two = rms_inverse(hidden)
    seq_two = gather_rows((hidden * inverse_two * ffn_gain).astype(jnp.bfloat16))
    seq_grad = gather_rows(cotangent)
    experts = w_gate.shape[0]
    dp_rows = w_gate.shape[1]
    hidden_units = w_gate.shape[2]
    dp_count = lax.axis_size("dp")
    group = dp_count // experts
    routed_rows = seq_len * expert_ids.shape[1] * 9 // 8
    capacity = (routed_rows + experts * group - 1) // (experts * group) * group
    slot_table, gate_table = dispatch(expert_ids, gate_values, experts, capacity)
    blank_row = jnp.zeros((1, model_width), jnp.bfloat16)
    padded_in = jnp.concatenate([seq_two, blank_row], axis=0)
    padded_grad = jnp.concatenate([seq_grad, blank_row], axis=0)
    empty_rows = jnp.zeros((seq_len + 1, model_width), jnp.float32)
    piece_rows = capacity // group
    down_rows = jnp.transpose(w_down, (0, 2, 1))
    gate_mine, up_mine, down_mine = (
        lax.all_to_all(widen(w_gate, group), "dp", split_axis=0, concat_axis=1, tiled=True),
        lax.all_to_all(widen(w_up, group), "dp", split_axis=0, concat_axis=1, tiled=True),
        lax.all_to_all(widen(down_rows, group), "dp", split_axis=0, concat_axis=1, tiled=True),
    )
    gate_mine = gate_mine[0]
    up_mine = up_mine[0]
    down_mine = down_mine[0]
    blocks_in = padded_in[slot_table]
    grad_blocks = (padded_grad[slot_table].astype(jnp.float32) * gate_table[:, :, None]).astype(
        jnp.bfloat16
    )
    recv_in, recv_grad = (
        lax.all_to_all(
            blocks_in.reshape(dp_count, piece_rows, model_width),
            "dp",
            split_axis=0,
            concat_axis=0,
            tiled=True,
        ),
        lax.all_to_all(
            grad_blocks.reshape(dp_count, piece_rows, model_width),
            "dp",
            split_axis=0,
            concat_axis=0,
            tiled=True,
        ),
    )
    rows_in = recv_in.reshape(-1, model_width)
    rows_grad = recv_grad.reshape(-1, model_width)
    gate_pre = jnp.dot(rows_in, gate_mine, preferred_element_type=jnp.float32)
    up_pre = jnp.dot(rows_in, up_mine, preferred_element_type=jnp.float32)
    act_low = (jax.nn.silu(gate_pre) * up_pre).astype(jnp.bfloat16)
    expert_out = lax.dot_general(act_low, down_mine, contract, preferred_element_type=jnp.float32)
    grad_act = jnp.dot(rows_grad, down_mine, preferred_element_type=jnp.float32)
    sigmoid_gate = jax.nn.sigmoid(gate_pre)
    grad_gate = (grad_act * up_pre * sigmoid_gate * (1.0 + gate_pre * (1.0 - sigmoid_gate))).astype(
        jnp.bfloat16
    )
    grad_up = (grad_act * gate_pre * sigmoid_gate).astype(jnp.bfloat16)
    grad_input = lax.dot_general(
        grad_gate, gate_mine, contract, preferred_element_type=jnp.float32
    ) + lax.dot_general(grad_up, up_mine, contract, preferred_element_type=jnp.float32)
    back_out, back_grad = (
        lax.all_to_all(
            expert_out.reshape(dp_count, piece_rows, model_width).astype(jnp.bfloat16),
            "dp",
            split_axis=0,
            concat_axis=0,
            tiled=True,
        ).astype(jnp.float32),
        lax.all_to_all(
            grad_input.reshape(dp_count, piece_rows, model_width).astype(jnp.bfloat16),
            "dp",
            split_axis=0,
            concat_axis=0,
            tiled=True,
        ).astype(jnp.float32),
    )
    back_out = back_out.reshape(experts, capacity, model_width)
    back_grad = back_grad.reshape(experts * capacity, model_width)
    flat_slots = slot_table.reshape(-1)
    combined = empty_rows.at[flat_slots].add(
        (back_out * gate_table[:, :, None]).reshape(-1, model_width)
    )
    grad_acc = empty_rows.at[flat_slots].add(back_grad)
    grad_both = jnp.concatenate([grad_gate, grad_up], axis=1)
    grad_cols = jnp.concatenate(
        [
            lax.dot_general(rows_in, grad_both, contract_rows, preferred_element_type=jnp.float32),
            lax.dot_general(rows_grad, act_low, contract_rows, preferred_element_type=jnp.float32),
        ],
        axis=1,
    )
    returned = lax.all_to_all(
        grad_cols[None].astype(jnp.bfloat16), "dp", split_axis=1, concat_axis=0, tiled=True
    ).astype(jnp.float32)
    summed = jnp.sum(returned.reshape(experts, group, dp_rows, 3 * hidden_units), axis=1)
    grad_w_gate = summed[:, :, :hidden_units]
    grad_w_up = summed[:, :, hidden_units : 2 * hidden_units]
    grad_w_down = jnp.transpose(summed[:, :, 2 * hidden_units :], (0, 2, 1))
    output = (hidden + scatter_rows(combined[:seq_len])).astype(jnp.bfloat16)
    grad_two = scatter_rows(grad_acc[:seq_len])
    ffn_gain_part = jnp.sum(grad_two * hidden * inverse_two, axis=0)
    grad_hidden = cotangent.astype(jnp.float32) + norm_backward(
        grad_two, hidden, inverse_two, ffn_gain
    )
    grad_attn = gather_rows(grad_hidden.astype(jnp.bfloat16))
    grad_mixed = lax.dot_general(
        grad_attn, full_out, contract, preferred_element_type=jnp.float32
    ).astype(jnp.bfloat16)
    grad_mixed_heads = grad_mixed.reshape(seq_len, local_kv, group_size, head_dim).transpose(
        1, 0, 2, 3
    )
    grad_query_heads, grad_key_heads, grad_value_heads = lax.map(
        head_backward, (query_heads, key_heads, value_heads, logsum, grad_mixed_heads)
    )
    grad_query_rot = (
        grad_query_heads.transpose(1, 0, 2, 3).reshape(seq_len, local_heads, head_dim) * attn_scale
    )
    grad_query_norm = rotate_back(grad_query_rot, cosine, sine_table)
    query_gain_part = jnp.sum(grad_query_norm * query_raw * query_inverse, axis=(0, 1))
    grad_query_low = (
        norm_backward(grad_query_norm, query_raw, query_inverse, query_gain)
        .astype(jnp.bfloat16)
        .reshape(seq_len, local_heads * head_dim)
    )
    grad_key_norm = rotate_back(grad_key_heads.transpose(1, 0, 2), cosine, sine_table)
    key_gain_part = jnp.sum(grad_key_norm * key_raw * key_inverse, axis=(0, 1))
    grad_key_low = (
        norm_backward(grad_key_norm, key_raw, key_inverse, key_gain)
        .astype(jnp.bfloat16)
        .reshape(seq_len, local_kv * head_dim)
    )
    grad_value_low = (
        grad_value_heads.transpose(1, 0, 2)
        .reshape(seq_len, local_kv * head_dim)
        .astype(jnp.bfloat16)
    )
    grad_proj = jnp.concatenate([grad_query_low, grad_key_low, grad_value_low], axis=1)
    full_proj = jnp.concatenate([full_query, full_key, full_value], axis=1)
    grad_one = scatter_rows(
        lax.dot_general(grad_proj, full_proj, contract, preferred_element_type=jnp.float32)
    )
    first_part = jnp.einsum("sd,sf->df", seq_normed, grad_proj, preferred_element_type=jnp.float32)
    second = jnp.einsum("sd,sf->df", grad_attn, mixed_flat, preferred_element_type=jnp.float32)
    shares = lax.psum_scatter(
        jnp.concatenate([first_part, second], axis=1), "dp", scatter_dimension=0, tiled=True
    )
    query_cols = w_query.shape[1]
    key_cols = w_key.shape[1]
    grad_w_query = shares[:, :query_cols]
    grad_w_key = shares[:, query_cols : query_cols + key_cols]
    grad_w_value = shares[:, query_cols + key_cols : query_cols + 2 * key_cols]
    grad_w_out = jnp.transpose(shares[:, query_cols + 2 * key_cols :])
    attn_gain_part = jnp.sum(grad_one * residual * inverse_one, axis=0)
    grad_tokens = (grad_hidden + norm_backward(grad_one, residual, inverse_one, attn_gain)).astype(
        jnp.bfloat16
    )
    total_gains = lax.psum(
        (attn_gain_part, ffn_gain_part, query_gain_part, key_gain_part), ("dp", "tensor")
    )
    return (
        output,
        grad_tokens,
        grad_w_query,
        grad_w_key,
        grad_w_value,
        grad_w_out,
        grad_w_gate,
        grad_w_up,
        grad_w_down,
        total_gains[0],
        total_gains[1],
        total_gains[2],
        total_gains[3],
    )


def per_device_relay(
    tokens,
    cotangent,
    expert_ids,
    gate_values,
    w_query,
    w_key,
    w_value,
    w_out,
    w_gate,
    w_up,
    w_down,
    attn_gain,
    ffn_gain,
    query_gain,
    key_gain,
):
    dot = functools.partial(jnp.dot, preferred_element_type=jnp.float32)
    dot_t = functools.partial(lax.dot_general, dimension_numbers=(((1,), (1,)), ((), ())), preferred_element_type=jnp.float32)
    t_dot = functools.partial(lax.dot_general, dimension_numbers=(((0,), (0,)), ((), ())), preferred_element_type=jnp.float32)
    low = jnp.bfloat16
    rows, width = tokens.shape
    head_dim = query_gain.shape[0]
    experts = w_gate.shape[0]
    core = lax.axis_index("tensor")
    mine = lax.dynamic_slice_in_dim(expert_ids, core * rows, rows, 0)
    values = lax.dynamic_slice_in_dim(gate_values, core * rows, rows, 0)
    match = mine[None] == jnp.arange(experts, dtype=jnp.int32)[:, None, None]
    gates = jnp.sum(jnp.where(match, values[None], 0.0), axis=2)
    gates = jnp.broadcast_to(gates[:, None], (experts, 8, rows))

    q_cols, kv_cols = w_query.shape[1] // 2, w_key.shape[1] // 2
    w_out_rows = jnp.transpose(w_out)
    halves = jnp.stack(
        [
            jnp.concatenate([w[:, h * (w.shape[1] // 2) : (h + 1) * (w.shape[1] // 2)] for w in (w_query, w_key, w_value, w_out_rows)], axis=1)
            for h in range(2)
        ]
    )
    swap_weights = functools.partial(lax.all_to_all, axis_name="dp", split_axis=0, concat_axis=1, tiled=True)
    gate_mine, up_mine, down_mine = [swap_weights(w)[0] for w in (w_gate, w_up, jnp.transpose(w_down, (0, 2, 1)))]
    weights, rows_grad, gates = gather_first(halves, cotangent, gates, 1)
    weights, rows_grad, gates = weights.reshape(-1, weights.shape[2]), rows_grad.reshape(-1, width), gates[:, 0].reshape(-1, 1)
    proj_cols = q_cols + 2 * kv_cols
    w_proj, w_back = weights[:, :proj_cols], weights[:, proj_cols:]

    residual = tokens.astype(jnp.float32)
    inverse_one = rms_inverse(residual)
    seq_normed = gather_four((residual * inverse_one * attn_gain).astype(low), 4).reshape(-1, width)
    seq_len = 2 * rows
    group = q_cols // head_dim
    scale = head_dim ** (-0.5)
    cosine, sine_table = rotary_tables(seq_len, head_dim)
    proj = dot(seq_normed, w_proj)
    query_raw = proj[:, :q_cols].reshape(2, seq_len, group, head_dim)
    key_raw = proj[:, q_cols : q_cols + kv_cols].reshape(2, seq_len, 1, head_dim)
    value_low = proj[:, q_cols + kv_cols :].astype(low).reshape(2, seq_len, head_dim)
    query_inverse, key_inverse = rms_inverse(query_raw), rms_inverse(key_raw)
    query_low = (rotate(query_raw * query_inverse * query_gain, cosine, sine_table) * scale).astype(low)
    key_low = rotate(key_raw * key_inverse * key_gain, cosine, sine_table).astype(low)[:, :, 0]
    causal = jnp.arange(seq_len)[:, None] >= jnp.arange(seq_len)[None, :]
    scores = jnp.einsum("bqgd,bsd->bgqs", query_low, key_low, preferred_element_type=jnp.float32)
    exp_scores = jnp.where(causal, jnp.exp(scores), 0.0)
    probs = exp_scores / jnp.sum(exp_scores, axis=-1, keepdims=True)
    probs_low = probs.astype(low)
    mixed = jnp.einsum("bgqs,bsd->bqgd", probs_low, value_low, preferred_element_type=jnp.float32).astype(low).reshape(2 * seq_len, q_cols)
    hidden = residual + scatter_four(dot_t(mixed, w_back).astype(low).reshape(2, 2, rows, width), 5)
    inverse_two = rms_inverse(hidden)
    rows_in = gather_dp((hidden * inverse_two * ffn_gain).astype(low), 6).reshape(-1, width)
    gate_full, up_full, down_full = join_cores((gate_mine, up_mine, down_mine), 2)

    gate_pre = dot(rows_in, gate_full)
    up_pre = dot(rows_in, up_full)
    sigmoid_gate = jax.nn.sigmoid(gate_pre)
    act = (gate_pre * sigmoid_gate * up_pre).astype(low)
    expert_out = (dot_t(act, down_full) * gates).astype(low)
    grad_out = (rows_grad.astype(jnp.float32) * gates).astype(low)
    grad_act = dot(grad_out, down_full)
    grad_gate = (grad_act * up_pre * sigmoid_gate * (1.0 + gate_pre * (1.0 - sigmoid_gate))).astype(low)
    grad_up = (grad_act * gate_pre * sigmoid_gate).astype(low)
    grad_in = (dot_t(grad_gate, gate_full) + dot_t(grad_up, up_full)).astype(low)
    moe, grad_two = scatter_dp([v.reshape(-1, rows, width) for v in (expert_out, grad_in)], 7)
    w_gate_part = t_dot(rows_in, grad_gate).astype(low)
    w_up_part = t_dot(rows_in, grad_up).astype(low)
    w_down_part = t_dot(grad_out, act).astype(low)
    owned = sum_cores((w_gate_part, w_up_part, w_down_part), 8)
    swap_grads = functools.partial(lax.all_to_all, axis_name="dp", split_axis=0, concat_axis=0, tiled=True)
    grad_w_gate, grad_w_up, grad_w_down = [swap_grads(v.reshape(experts, rows, -1)).astype(jnp.float32) for v in owned]
    grad_w_down = jnp.transpose(grad_w_down, (0, 2, 1))

    output = (hidden + moe).astype(low)
    ffn_gain_part = jnp.sum(grad_two * hidden * inverse_two, axis=0)
    grad_hidden = cotangent.astype(jnp.float32) + norm_backward(grad_two, hidden, inverse_two, ffn_gain)
    grad_attn = gather_four(grad_hidden.astype(low), 9).reshape(-1, width)
    grad_mixed = dot(grad_attn, w_back).astype(low).reshape(2, seq_len, group, head_dim)
    grad_probs = jnp.einsum("bqgd,bsd->bgqs", grad_mixed, value_low, preferred_element_type=jnp.float32)
    delta_sum = jnp.sum(grad_probs * probs, axis=-1, keepdims=True)
    grad_scores = (probs * (grad_probs - delta_sum)).astype(low)
    grad_query = jnp.einsum("bgqs,bsd->bqgd", grad_scores, key_low, preferred_element_type=jnp.float32)
    grad_key = jnp.einsum("bgqs,bqgd->bsd", grad_scores, query_low, preferred_element_type=jnp.float32)
    grad_value = jnp.einsum("bgqs,bqgd->bsd", probs_low, grad_mixed, preferred_element_type=jnp.float32)
    grad_query_norm = rotate_back(grad_query * scale, cosine, sine_table)
    query_gain_part = jnp.sum(grad_query_norm * query_raw * query_inverse, axis=(0, 1, 2))
    grad_query_low = norm_backward(grad_query_norm, query_raw, query_inverse, query_gain).astype(low)
    grad_key_norm = rotate_back(grad_key[:, :, None], cosine, sine_table)
    key_gain_part = jnp.sum(grad_key_norm * key_raw * key_inverse, axis=(0, 1, 2))
    grad_key_low = norm_backward(grad_key_norm, key_raw, key_inverse, key_gain).astype(low)
    grad_proj = jnp.concatenate([v.astype(low).reshape(2 * seq_len, -1) for v in (grad_query_low, grad_key_low, grad_value)], axis=1)
    grad_one = scatter_four(dot_t(grad_proj, w_proj).astype(low).reshape(2, 2, rows, width), 10)
    w_parts = jnp.concatenate([t_dot(seq_normed, grad_proj), t_dot(grad_attn, mixed)], axis=1).astype(low)
    attn_gain_part = jnp.sum(grad_one * residual * inverse_one, axis=0)
    gains = jnp.concatenate([attn_gain_part, ffn_gain_part, query_gain_part, key_gain_part])
    gains = jnp.pad(gains, (0, -gains.shape[0] % 1024)).reshape(-1, 128)
    shares, totals = scatter_last(w_parts.reshape(-1, rows, w_parts.shape[1]), gains, 11)
    shares, totals = shares.astype(jnp.float32), totals.reshape(-1)
    stops = (0, q_cols, q_cols + kv_cols, proj_cols, proj_cols + q_cols)
    grads = [jnp.concatenate([shares[0, :, a:b], shares[1, :, a:b]], axis=1) for a, b in zip(stops, stops[1:])]
    grad_tokens = (grad_hidden + norm_backward(grad_one, residual, inverse_one, attn_gain)).astype(low)
    totals = jnp.split(totals, (width, 2 * width, 2 * width + head_dim, 2 * width + 2 * head_dim))[:4]
    return (output, grad_tokens, grads[0], grads[1], grads[2], jnp.transpose(grads[3]), grad_w_gate, grad_w_up, grad_w_down, *totals)


def solution(mesh):
    return jax.shard_map(
        per_device_relay if tuple(mesh.shape.values()) == (16, 2) else per_device_any,
        mesh=mesh,
        in_specs=(
            P(("dp", "tensor"), None),
            P(("dp", "tensor"), None),
            P("dp", None),
            P("dp", None),
            P("dp", "tensor"),
            P("dp", "tensor"),
            P("dp", "tensor"),
            P("tensor", "dp"),
            P(None, "dp", "tensor"),
            P(None, "dp", "tensor"),
            P(None, "tensor", "dp"),
            P(),
            P(),
            P(),
            P(),
        ),
        out_specs=(
            P(("dp", "tensor"), None),
            P(("dp", "tensor"), None),
            P("dp", "tensor"),
            P("dp", "tensor"),
            P("dp", "tensor"),
            P("tensor", "dp"),
            P(None, "dp", "tensor"),
            P(None, "dp", "tensor"),
            P(None, "tensor", "dp"),
            P(),
            P(),
            P(),
            P(),
        ),
        check_vma=False,
    )
```

```python
import functools

import jax
import jax.numpy as jnp
from jax import lax
from jax.experimental import pallas as pl
from jax.experimental.pallas import tpu as pltpu
from jax.sharding import PartitionSpec as P

epsilon = 1e-06
theta_base = 1000000.0


def rms_inverse(values):
    return lax.rsqrt(jnp.mean(values * values, axis=-1, keepdims=True) + epsilon)


def norm_backward(grad_in, values, inverse, gain_vec):
    scaled = grad_in * gain_vec
    inner_mean = jnp.mean(scaled * values, axis=-1, keepdims=True)
    return inverse * scaled - values * inverse**3 * inner_mean


def rotary_tables(seq_len, head_dim):
    half_dim = head_dim // 2
    frequency = theta_base ** (-jnp.arange(half_dim, dtype=jnp.float32) * 2.0 / head_dim)
    angles = jnp.arange(seq_len, dtype=jnp.float32)[:, None] * frequency[None, :]
    return (jnp.cos(angles)[:, None, :], jnp.sin(angles)[:, None, :])


def rotate(values, cosine, sine_table):
    half_dim = values.shape[-1] // 2
    first_part = values[..., :half_dim]
    second = values[..., half_dim:]
    return jnp.concatenate(
        [first_part * cosine - second * sine_table, second * cosine + first_part * sine_table],
        axis=-1,
    )


def rotate_back(grad_in, cosine, sine_table):
    half_dim = grad_in.shape[-1] // 2
    first_part = grad_in[..., :half_dim]
    second = grad_in[..., half_dim:]
    return jnp.concatenate(
        [first_part * cosine + second * sine_table, second * cosine - first_part * sine_table],
        axis=-1,
    )


def dispatch(expert_ids, gate_values, experts, capacity):
    seq_len = expert_ids.shape[0]
    is_match = expert_ids[:, :, None] == jnp.arange(experts, dtype=jnp.int32)[None, None, :]
    expert_hits = jnp.sum(is_match.astype(jnp.int32), axis=1)
    before = jnp.cumsum(expert_hits, axis=0) - expert_hits
    slot_ids = jnp.sum(jnp.where(is_match, before[:, None, :], 0), axis=2)
    token_index = jnp.broadcast_to(jnp.arange(seq_len, dtype=jnp.int32)[:, None], expert_ids.shape)
    slot_table = (
        jnp.full((experts, capacity), seq_len, jnp.int32).at[expert_ids, slot_ids].set(token_index)
    )
    gate_table = (
        jnp.zeros((experts, capacity), jnp.float32).at[expert_ids, slot_ids].set(gate_values)
    )
    return (slot_table, gate_table)


def head_forward(head_inputs):
    query_vals, key_vals, value_vals = head_inputs
    seq_len = key_vals.shape[0]
    block_rows = min(512, seq_len)
    key_positions = jnp.arange(seq_len)

    def one_block(row_start):
        scores = jnp.einsum("qgd,sd->gqs", query_vals, key_vals, preferred_element_type=jnp.float32)
        causal = (row_start + jnp.arange(block_rows))[:, None] >= key_positions[None, :]
        exp_scores = jnp.where(causal, jnp.exp(scores), 0.0)
        denominator = jnp.sum(exp_scores, axis=-1, keepdims=True)
        softmax_low = (exp_scores / denominator).astype(jnp.bfloat16)
        mixed_out = jnp.einsum(
            "gqs,sd->qgd", softmax_low, value_vals, preferred_element_type=jnp.float32
        )
        return (mixed_out.astype(jnp.bfloat16), jnp.log(denominator[..., 0]))

    block_starts = jnp.arange(seq_len // block_rows, dtype=jnp.int32) * block_rows
    mixed_out, logsum = lax.map(one_block, block_starts)
    return (mixed_out.reshape(seq_len, query_vals.shape[1], query_vals.shape[2]), logsum)


def head_backward(head_inputs):
    query_vals, key_vals, value_vals, logsum, grad_mixed = head_inputs
    seq_len = key_vals.shape[0]
    block_rows = min(512, seq_len)
    key_positions = jnp.arange(seq_len)

    def one_block(state_in, block_in):
        grad_key, grad_value = state_in
        row_start, block_logsum = block_in
        scores = jnp.einsum("qgd,sd->gqs", query_vals, key_vals, preferred_element_type=jnp.float32)
        causal = (row_start + jnp.arange(block_rows))[:, None] >= key_positions[None, :]
        softmax_vals = jnp.where(causal, jnp.exp(scores - block_logsum[..., None]), 0.0)
        grad_probs = jnp.einsum(
            "qgd,sd->gqs", grad_mixed, value_vals, preferred_element_type=jnp.float32
        )
        delta_sum = jnp.sum(grad_probs * softmax_vals, axis=-1, keepdims=True)
        grad_scores = (softmax_vals * (grad_probs - delta_sum)).astype(jnp.bfloat16)
        grad_query = jnp.einsum(
            "gqs,sd->qgd", grad_scores, key_vals, preferred_element_type=jnp.float32
        )
        grad_key = grad_key + jnp.einsum(
            "gqs,qgd->sd", grad_scores, query_vals, preferred_element_type=jnp.float32
        )
        grad_value = grad_value + jnp.einsum(
            "gqs,qgd->sd",
            softmax_vals.astype(jnp.bfloat16),
            grad_mixed,
            preferred_element_type=jnp.float32,
        )
        return ((grad_key, grad_value), grad_query)

    block_starts = jnp.arange(seq_len // block_rows, dtype=jnp.int32) * block_rows
    zero_rows = jnp.zeros(key_vals.shape, jnp.float32)
    (grad_key, grad_value), grad_query = lax.scan(
        one_block, (zero_rows, zero_rows), (block_starts, logsum)
    )
    return (grad_query.reshape(query_vals.shape), grad_key, grad_value)


def gather_rows(values):
    return lax.all_gather(values, "tensor", axis=0, tiled=True)


def scatter_rows(values):
    return lax.psum_scatter(
        values.astype(jnp.bfloat16), "tensor", scatter_dimension=0, tiled=True
    ).astype(jnp.float32)


def widen(stacked, group):
    experts = stacked.shape[0]
    spread = jnp.broadcast_to(stacked[:, None], (experts, group) + stacked.shape[1:])
    return spread.reshape((experts * group,) + stacked.shape[1:])


MESH = pl.DeviceIdType.MESH
LIMIT = 66_000_000


class Place:
    def __init__(self):
        self.dp = lax.axis_index("dp")
        self.core = lax.axis_index("tensor")
        x, y = self.dp % 2, (self.dp // 2) % 2
        self.z = self.dp // 4
        step_x, step_y = 1 - 2 * x, 2 * (1 - 2 * y)
        self.da = (1 - self.core) * step_x + self.core * step_y
        self.db = (1 - self.core) * step_y + self.core * step_x
        self.half = self.z % 2
        self.pair = 4 * (1 - 2 * self.half)
        self.far = 8 * (1 - 2 * (self.z // 2))

    def copy(self, src, dst, send_sem, recv_sem, to, core=None):
        return pltpu.make_async_remote_copy(
            src_ref=src,
            dst_ref=dst,
            send_sem=send_sem,
            recv_sem=recv_sem,
            device_id=(to, self.core if core is None else core),
            device_id_type=MESH,
        )

    def at_z(self, z):
        return self.dp + 4 * (z - self.z)

    def greet(self, line=False, near=False, chain=False, everyone=False, partner=False):
        barrier = pltpu.get_barrier_semaphore()
        count = 0

        def signal(to, core):
            pl.semaphore_signal(barrier, inc=1, device_id=(to, core), device_id_type=MESH)

        if everyone:
            for r in range(1, 16):
                signal((self.dp + r) % 16, self.core)
            count = count + 15
        else:
            if near:
                signal(self.dp + self.da, self.core)
                signal(self.dp + self.db, self.core)
                count = count + 2
            if chain:
                signal(self.dp + self.pair, self.core)
                count = count + 1
                if near:
                    signal(self.dp + self.far, self.core)
                    count = count + 1
            if line:
                pl.when(self.z > 0)(lambda: signal(self.dp - 4, self.core))
                pl.when(self.z < 3)(lambda: signal(self.dp + 4, self.core))
                count = count + jnp.where(self.z > 0, 1, 0) + jnp.where(self.z < 3, 1, 0)
        if partner:
            signal(self.dp, 1 - self.core)
            count = count + 1
        pl.semaphore_wait(barrier, count)


def add_rows(target, terms, rows, block=16):
    def body(i, _):
        at = pl.ds(pl.multiple_of(i * block, block), block)
        total = terms[0][at, :].astype(jnp.float32)
        for term in terms[1:]:
            total = total + term[at, :].astype(jnp.float32)
        target[at, :] = total.astype(target.dtype)
        return 0

    lax.fori_loop(0, rows // block, body, 0)


def gather_four_kernel(x_ref, out_ref, send_sem, recv_sem):
    me = Place()
    me.greet(chain=True, partner=True)
    mine, theirs = out_ref.at[me.half, me.core], out_ref.at[1 - me.half, me.core]
    across = me.copy(x_ref, mine, send_sem.at[0], recv_sem.at[0], me.dp + me.pair)
    across.start()
    beside = me.copy(x_ref, mine, send_sem.at[1], recv_sem.at[1], me.dp, 1 - me.core)
    beside.start()
    mine[...] = x_ref[...]
    across.wait_recv()
    relay = me.copy(theirs, theirs, send_sem.at[2], recv_sem.at[2], me.dp, 1 - me.core)
    relay.start()
    across.wait_send()
    beside.wait()
    relay.wait()


def gather_four(x, cid):
    rows, columns = x.shape
    vmem = pl.BlockSpec(memory_space=pltpu.VMEM)
    return pl.pallas_call(
        gather_four_kernel,
        out_shape=jax.ShapeDtypeStruct((2, 2, rows, columns), x.dtype),
        in_specs=[vmem],
        out_specs=vmem,
        scratch_shapes=[pltpu.SemaphoreType.DMA((3,)), pltpu.SemaphoreType.DMA((3,))],
        compiler_params=pltpu.CompilerParams(collective_id=cid, has_side_effects=True),
        name="gather_four",
    )(x)


def scatter_four_kernel(p_ref, out_ref, from_core, from_pair, send_sem, recv_sem):
    me = Place()
    rows = p_ref.shape[2]
    me.greet(chain=True, partner=True)

    def beside(h, slot):
        return me.copy(p_ref.at[h, 1 - me.core], from_core.at[slot], send_sem.at[slot], recv_sem.at[slot], me.dp, 1 - me.core)

    first, second = beside(1 - me.half, 0), beside(me.half, 1)
    first.start()
    second.start()
    first.wait_recv()
    add_rows(from_core.at[0], (p_ref.at[1 - me.half, me.core], from_core.at[0]), rows)
    across = me.copy(from_core.at[0], from_pair, send_sem.at[2], recv_sem.at[2], me.dp + me.pair)
    across.start()
    second.wait_recv()
    add_rows(from_core.at[1], (p_ref.at[me.half, me.core], from_core.at[1]), rows)
    across.wait_recv()
    add_rows(out_ref, (from_core.at[1], from_pair), rows)
    across.wait_send()
    first.wait_send()
    second.wait_send()


def scatter_four(p, cid):
    _, _, rows, columns = p.shape
    vmem = pl.BlockSpec(memory_space=pltpu.VMEM)
    return pl.pallas_call(
        scatter_four_kernel,
        out_shape=jax.ShapeDtypeStruct((rows, columns), jnp.float32),
        in_specs=[vmem],
        out_specs=vmem,
        scratch_shapes=[
            pltpu.VMEM((2, rows, columns), p.dtype),
            pltpu.VMEM((rows, columns), p.dtype),
            pltpu.SemaphoreType.DMA((3,)),
            pltpu.SemaphoreType.DMA((3,)),
        ],
        compiler_params=pltpu.CompilerParams(collective_id=cid, has_side_effects=True),
        name="scatter_four",
    )(p)


def run(*threads):
    threads = list(threads)
    while threads:
        for thread in list(threads):
            if next(thread, "end") == "end":
                threads.remove(thread)


def lagged(items, first, second, lag):
    for n in range(len(items) + lag):
        if n < len(items):
            first(items[n])
            yield
        if n >= lag:
            second(items[n - lag])
            yield


def gather_line(me, x_ref, out_ref, send_sem, recv_sem):
    def part(source, to, slot, own=False):
        return me.copy(x_ref if own else out_ref.at[source], out_ref.at[source], send_sem.at[slot], recv_sem.at[source], to)

    sides = ((-1, me.z < 3, 4), (1, me.z > 0, -4))

    def exists(d, side):
        return (me.z - d >= 0) if side == 0 else (me.z + d <= 3)

    def slot_z(d, side, j):
        return 4 + ((d - 1) * 2 + side) * 3 + j

    def slot_a(off):
        return 25 + off

    def pass_a(off):
        source = me.dp + me.da + 4 * off
        part(source, me.dp, slot_a(off)).wait_recv()
        part(source, me.dp + me.db, slot_a(off)).start()

    pl.when(me.z < 3)(lambda: part(me.dp, me.dp + 4, 0, True).start())
    pl.when(me.z > 0)(lambda: part(me.dp, me.dp - 4, 1, True).start())
    part(me.dp, me.dp + me.db, 3, True).start()
    part(me.dp, me.dp + me.da, 2, True).start()
    yield
    for d in range(1, 5):
        if d < 4:
            for side, (sign, forward, step) in enumerate(sides):
                source = me.dp + 4 * sign * d

                def arrive():
                    part(source, me.dp, slot_z(d, side, 0)).wait_recv()
                    pl.when(forward)(lambda: part(source, me.dp + step, slot_z(d, side, 0)).start())
                    part(source, me.dp + me.db, slot_z(d, side, 2)).start()
                    part(source, me.dp + me.da, slot_z(d, side, 1)).start()

                pl.when(exists(d, side))(arrive)
                yield
        if d == 1:
            pass_a(0)
            yield
        else:
            for side, (sign, *_) in enumerate(sides):
                pl.when(exists(d - 1, side))(lambda: pass_a(sign * (d - 1)))
                yield
    for z in range(4):
        for g in (0, 1):
            part(me.at_z(z) + me.db + g * me.da, me.dp, 0).wait_recv()
            yield

    def sent(slot):
        part(me.dp, me.dp, slot).wait_send()

    pl.when(me.z < 3)(lambda: sent(0))
    pl.when(me.z > 0)(lambda: sent(1))
    sent(2)
    sent(3)
    sent(slot_a(0))
    for d in range(1, 4):
        for side, (sign, forward, _) in enumerate(sides):

            def finish():
                pl.when(forward)(lambda: sent(slot_z(d, side, 0)))
                sent(slot_z(d, side, 1))
                sent(slot_z(d, side, 2))
                sent(slot_a(sign * d))

            pl.when(exists(d, side))(finish)


def gather_pairs(me, x_ref, out_ref, send_sem, recv_sem):
    mine, other = me.dp, me.dp + me.pair

    def part(src, where, to, slot):
        return me.copy(src, out_ref.at[where], send_sem.at[slot], recv_sem.at[where], to)

    def relay(where, to, slot):
        part(out_ref.at[where], where, to, slot).start()

    def arrived(where):
        part(out_ref.at[where], where, me.dp, 0).wait_recv()

    part(x_ref.at[1 - me.half], mine, other, 0).start()
    part(x_ref.at[me.half], mine, me.dp + me.far, 1).start()
    part(x_ref.at[me.half], mine, me.dp + me.db, 2).start()
    part(x_ref.at[me.half], mine, me.dp + me.da, 3).start()
    yield
    arrived(other)
    relay(other, me.dp + me.far, 4)
    relay(other, me.dp + me.db, 5)
    relay(other, me.dp + me.da, 6)
    yield
    arrived(mine + me.da)
    relay(mine + me.da, me.dp + me.db, 7)
    yield
    arrived(mine + me.far)
    relay(mine + me.far, me.dp + me.db, 8)
    relay(mine + me.far, me.dp + me.da, 9)
    yield
    arrived(other + me.da)
    relay(other + me.da, me.dp + me.db, 10)
    yield
    arrived(other + me.far)
    relay(other + me.far, me.dp + me.db, 11)
    relay(other + me.far, me.dp + me.da, 12)
    yield
    arrived(mine + me.far + me.da)
    relay(mine + me.far + me.da, me.dp + me.db, 13)
    yield
    arrived(other + me.far + me.da)
    relay(other + me.far + me.da, me.dp + me.db, 14)
    yield
    for base in (mine, other, mine + me.far, other + me.far):
        arrived(base + me.db)
        yield
        arrived(base + me.da + me.db)
        yield
    for slot in range(15):
        part(out_ref.at[mine], mine, me.dp, slot).wait_send()


def swap_rows(me, x_ref, out_ref, send_sem, recv_sem):
    for r in range(1, 16):
        to = (me.dp + r) % 16
        me.copy(x_ref.at[to], out_ref.at[me.dp], send_sem.at[r], recv_sem.at[r], to).start()
    yield
    for r in range(1, 16):
        s = (me.dp + 16 - r) % 16
        me.copy(x_ref.at[s], out_ref.at[s], send_sem.at[r], recv_sem.at[r], me.dp).wait_recv()
    for r in range(1, 16):
        me.copy(x_ref.at[me.dp], out_ref.at[me.dp], send_sem.at[r], recv_sem.at[r], me.dp).wait_send()


def keep_own(src, staging, dst, sems):
    load = pltpu.make_async_copy(src, staging, sems.at[0])
    store = pltpu.make_async_copy(staging, dst, sems.at[1])
    load.start()

    def finish():
        load.wait()
        store.start()
        store.wait()

    return finish


def gather_first_kernel(w_ref, c_ref, g_ref, w_out, c_out, g_out, w_own, c_own, w_send, w_recv, c_send, c_recv, g_send, g_recv, copy_sem):
    me = Place()
    ends = [
        keep_own(w_ref.at[me.half], w_own, w_out.at[me.dp], copy_sem.at[0]),
        keep_own(c_ref, c_own, c_out.at[me.dp], copy_sem.at[1]),
    ]
    g_out[me.dp] = g_ref[me.dp]
    me.greet(everyone=True)
    run(
        gather_pairs(me, w_ref, w_out, w_send, w_recv),
        gather_line(me, c_ref, c_out, c_send, c_recv),
        swap_rows(me, g_ref, g_out, g_send, g_recv),
    )
    for end in ends:
        end()


def gather_first(weights, rows, gates, cid):
    hbm, vmem = pl.BlockSpec(memory_space=pl.ANY), pl.BlockSpec(memory_space=pltpu.VMEM)
    dma = pltpu.SemaphoreType.DMA
    return pl.pallas_call(
        gather_first_kernel,
        out_shape=[
            jax.ShapeDtypeStruct((16,) + weights.shape[1:], weights.dtype),
            jax.ShapeDtypeStruct((16,) + rows.shape, rows.dtype),
            jax.ShapeDtypeStruct(gates.shape, gates.dtype),
        ],
        in_specs=[hbm, hbm, vmem],
        out_specs=[hbm, hbm, vmem],
        scratch_shapes=[
            pltpu.VMEM(weights.shape[1:], weights.dtype),
            pltpu.VMEM(rows.shape, rows.dtype),
            dma((15,)),
            dma((16,)),
            dma((29,)),
            dma((16,)),
            dma((16,)),
            dma((16,)),
            dma((2, 2)),
        ],
        compiler_params=pltpu.CompilerParams(collective_id=cid, has_side_effects=True),
        name="gather_first",
    )(weights, rows, gates)


def scatter_pairs(me, chunks, p_ref, out_ref, from_b, from_a, from_far, send_sem, recv_sem):
    rows = p_ref.shape[1] // chunks
    other = me.dp + me.pair
    bases = (me.dp, other, me.dp + me.far, other + me.far)
    items = [(j, k) for j in (2, 3, 1, 0) for k in range(chunks)]

    def at(k):
        return pl.ds(k * rows, rows)

    def copy(src, dst, slot, k, to):
        return me.copy(src, dst, send_sem.at[slot, k], recv_sem.at[slot, k], to)

    def send_b(g, j, k):
        return copy(p_ref.at[bases[j] + me.db + g * me.da, at(k)], from_b.at[g, j, at(k)], g * 4 + j, k, me.dp + me.db)

    def send_a(j, k):
        return copy(from_b.at[1, j, at(k)], from_a.at[j, at(k)], 8 + j, k, me.dp + me.da)

    def send_far(j, k):
        return copy(from_b.at[0, 2 + j, at(k)], from_far.at[j, at(k)], 12 + j, k, me.dp + me.far)

    def swap(k):
        return copy(from_b.at[0, 1, at(k)], out_ref.at[me.half, at(k)], 14, k, other)

    for j, k in items:
        send_b(1, j, k).start()
        send_b(0, j, k).start()
    yield

    def first(item):
        j, k = item
        send_b(1, j, k).wait_recv()
        add_rows(from_b.at[1, j, at(k)], (p_ref.at[bases[j] + me.da, at(k)], from_b.at[1, j, at(k)]), rows)
        send_a(j, k).start()

    def second(item):
        j, k = item
        send_b(0, j, k).wait_recv()
        send_a(j, k).wait_recv()
        terms = (p_ref.at[bases[j], at(k)], from_b.at[0, j, at(k)], from_a.at[j, at(k)])
        if j >= 2:
            add_rows(from_b.at[0, j, at(k)], terms, rows)
            send_far(j - 2, k).start()
        else:
            send_far(j, k).wait_recv()
            target = from_b.at[0, 1, at(k)] if j else out_ref.at[me.half, at(k)]
            add_rows(target, terms + (from_far.at[j, at(k)],), rows)
            if j:
                swap(k).start()

    yield from lagged(items, first, second, 2)
    for k in range(chunks):
        swap(k).wait_send()
        theirs = out_ref.at[1 - me.half, at(k)]
        copy(theirs, theirs, 14, k, other).wait_recv()
        for j in range(4):
            send_b(0, j, k).wait_send()
            send_b(1, j, k).wait_send()
            send_a(j, k).wait_send()
        send_far(0, k).wait_send()
        send_far(1, k).wait_send()


def sum_all(me, x_ref, out_ref, held, send_sem, recv_sem):
    out_ref[...] = x_ref[...]
    steps = ((me.dp, 1 - me.core), (me.dp + me.da, me.core), (me.dp + me.db, me.core), (me.dp + me.pair, me.core), (me.dp + me.far, me.core))
    yield
    for n, (to, core) in enumerate(steps):
        send = me.copy(held.at[0, n], held.at[1, n], send_sem.at[n], recv_sem.at[n], to, core)
        held[0, n] = out_ref[...]
        send.start()
        yield
        send.wait()
        out_ref[...] = held[0, n] + held[1, n]
        yield


def scatter_last_kernel(chunks, p_ref, x_ref, out_ref, sum_ref, from_b, from_a, from_far, held, send_sem, recv_sem, sum_send, sum_recv):
    me = Place()
    me.greet(near=True, chain=True, partner=True)
    run(
        scatter_pairs(me, chunks, p_ref, out_ref, from_b, from_a, from_far, send_sem, recv_sem),
        sum_all(me, x_ref, sum_ref, held, sum_send, sum_recv),
    )


def scatter_last(p, x, cid, chunks=2):
    _, rows, columns = p.shape
    vmem = pl.BlockSpec(memory_space=pltpu.VMEM)
    dma = pltpu.SemaphoreType.DMA
    return pl.pallas_call(
        functools.partial(scatter_last_kernel, chunks),
        out_shape=[jax.ShapeDtypeStruct((2, rows, columns), p.dtype), jax.ShapeDtypeStruct(x.shape, x.dtype)],
        in_specs=[vmem] * 2,
        out_specs=[vmem] * 2,
        scratch_shapes=[
            pltpu.VMEM((2, 4, rows, columns), p.dtype),
            pltpu.VMEM((4, rows, columns), p.dtype),
            pltpu.VMEM((2, rows, columns), p.dtype),
            pltpu.VMEM((2, 5) + x.shape, x.dtype),
            dma((15, chunks)),
            dma((15, chunks)),
            dma((5,)),
            dma((5,)),
        ],
        compiler_params=pltpu.CompilerParams(collective_id=cid, has_side_effects=True, vmem_limit_bytes=LIMIT),
        name="scatter_last",
    )(p, x)


def experts_kernel(
    x_ref, c_ref, g_ref, gate_ref, up_ref, down_ref,
    moe_ref, two_ref, gu_out, down_out, xg_ref,
    wgu, wd, ag, ggu, p, from_b, from_a, from_z, xb, cb,
    g_send, g_recv, b_send, b_recv, a_send, a_recv, z_send, z_recv, w_send, w_recv, load_sem, tile_sem, keep_sem,
):
    me = Place()
    rows, width = x_ref.shape
    hidden = wd.shape[1]
    half = hidden // 2
    low = me.z < 2
    depth = jnp.where(low, me.z, 3 - me.z)
    away = jnp.where(low, 1, 0)
    dot = functools.partial(jnp.dot, preferred_element_type=jnp.float32)
    dot_t = functools.partial(lax.dot_general, dimension_numbers=(((1,), (1,)), ((), ())), preferred_element_type=jnp.float32)
    t_dot = functools.partial(lax.dot_general, dimension_numbers=(((0,), (0,)), ((), ())), preferred_element_type=jnp.float32)
    upper, lower = pl.ds(rows, rows), pl.ds(0, rows)

    def z_of(m):
        t = jnp.where(m == 0, 1 - depth, jnp.where(m == 1, 2, jnp.where(m == 2, 3, depth)))
        return jnp.where(low, t, 3 - t)

    def block(n):
        return me.at_z(z_of(n // 2)) + (n % 2) * me.da

    def part(source, to, slot, own=False):
        return me.copy(x_ref if own else xg_ref.at[source], xg_ref.at[source], g_send.at[slot], g_recv.at[source], to)

    def onward(m):
        below = z_of(m) < me.z
        return jnp.logical_or(jnp.logical_and(below, me.z < 3), jnp.logical_and(jnp.logical_not(below), me.z > 0)), jnp.where(below, 4, -4)

    def arrive(m):
        source = me.at_z(z_of(m))
        part(source, me.dp, 0).wait_recv()
        goes, step = onward(m)
        pl.when(goes)(lambda: part(source, me.dp + step, 4 + 3 * m).start())
        part(source, me.dp + me.db, 6 + 3 * m).start()
        part(source, me.dp + me.da, 5 + 3 * m).start()

    def arrive_a(m):
        source = me.at_z(z_of(m)) + me.da
        part(source, me.dp, 0).wait_recv()
        part(source, me.dp + me.db, 13 + m).start()

    def loads(n):
        slot = n % 2
        copies = []
        for j, source in enumerate((block(n), block(n) + me.db)):
            at = pl.ds(j * rows, rows)
            copies.append(pltpu.make_async_copy(xg_ref.at[source], xb.at[slot, at], load_sem.at[slot, j]))
            copies.append(pltpu.make_async_copy(c_ref.at[source], cb.at[slot, at], load_sem.at[slot, 2 + j]))
        return copies

    def fetch(n):
        part(block(n) + me.db, me.dp, 0).wait_recv()
        for c in loads(n):
            c.start()

    def send_b(i, n):
        return me.copy(p.at[i, n, upper], from_b.at[i, n], b_send.at[i, n], b_recv.at[i, n], me.dp + me.db)

    def send_a(i, m):
        return me.copy(from_b.at[i, 2 * m + 1], from_a.at[i, m], a_send.at[i, m], a_recv.at[i, m], me.dp + me.da)

    def slot_z(z, up, at):
        return jnp.where(up == 1, z, jnp.where(z == at, 4, z))

    def send_z(i, m, up):
        z = z_of(m)
        slot = slot_z(z, up, me.z - 1)
        return me.copy(from_b.at[i, 2 * m], from_z.at[i, slot], z_send.at[i, m], z_recv.at[i, slot], me.dp - 4 + 8 * up)

    def wait_z(i, z, up):
        slot = slot_z(z, up, me.z)
        me.copy(from_z.at[i, slot], from_z.at[i, slot], z_send.at[i, 0], z_recv.at[i, slot], me.dp).wait_recv()
        return from_z.at[i, slot]

    def first(m):
        for i in range(2):
            n = 2 * m + 1
            send_b(i, n).wait_recv()
            add_rows(from_b.at[i, n], (p.at[i, n, lower], from_b.at[i, n]), rows)
            send_a(i, m).start()

    def second(m):
        for i in range(2):
            n = 2 * m
            send_b(i, n).wait_recv()
            send_a(i, m).wait_recv()
            terms = (p.at[i, n, lower], from_b.at[i, n], from_a.at[i, m])
            if m in (1, 2):
                pl.when(depth == 0)(lambda: add_rows(from_b.at[i, n], terms, rows))
                pl.when(depth == 1)(lambda: add_rows(from_b.at[i, n], terms + (wait_z(i, z_of(m), away),), rows))
                send_z(i, m, away).start()
            else:
                add_rows(from_b.at[i, n], terms, rows)
                if m == 0:
                    pl.when(depth == 0)(lambda: send_z(i, 0, away).start())

    own = p.at[1, 7, lower]
    load = pltpu.make_async_copy(x_ref, own, keep_sem.at[0])
    store = pltpu.make_async_copy(own, xg_ref.at[me.dp], keep_sem.at[1])
    load.start()

    def half_of(core):
        at = core * half
        return (
            wgu.at[:, pl.ds(pl.multiple_of(at, 128), half)],
            wgu.at[:, pl.ds(pl.multiple_of(hidden + at, 128), half)],
            wd.at[:, pl.ds(pl.multiple_of(at, 128), half)],
        )

    mine = (gate_ref, up_ref, down_ref)
    locals_ = [pltpu.make_async_copy(src, dst, keep_sem.at[2 + j]) for j, (src, dst) in enumerate(zip(mine, half_of(me.core)))]
    for c in locals_:
        c.start()
    me.greet(line=True, near=True, partner=True)
    pl.when(me.z < 3)(lambda: part(me.dp, me.dp + 4, 0, True).start())
    pl.when(me.z > 0)(lambda: part(me.dp, me.dp - 4, 1, True).start())
    part(me.dp, me.dp + me.db, 3, True).start()
    part(me.dp, me.dp + me.da, 2, True).start()
    shares = [
        me.copy(src, dst, w_send.at[j], w_recv.at[j], me.dp, 1 - me.core) for j, (src, dst) in enumerate(zip(mine, half_of(me.core)))
    ]
    for c in shares:
        c.start()
    load.wait()
    store.start()
    arrive_a(3)
    arrive(0)
    store.wait()
    for c in locals_:
        c.wait()
    for j, dst in enumerate(half_of(1 - me.core)):
        me.copy(dst, dst, w_send.at[j], w_recv.at[j], me.dp).wait_recv()
    fetch(0)

    tile = 256

    def step(n, _):
        slot = n % 2
        for c in loads(n):
            c.wait()
        gates = jnp.concatenate([g_ref[block(n)], g_ref[block(n) + me.db]], axis=0)

        def inner(j, _):
            at, at_up = pl.ds(pl.multiple_of(j * tile, tile), tile), pl.ds(pl.multiple_of(hidden + j * tile, tile), tile)
            gate, up, grad = dot(xb[slot], wgu[:, at]), dot(xb[slot], wgu[:, at_up]), dot(cb[slot], wd[:, at]) * gates
            sig = 1.0 / (1.0 + jnp.exp(-gate))
            act = gate * sig
            ag[n, :, at] = (act * up * gates).astype(ag.dtype)
            ggu[n, :, at] = (grad * up * sig * (1.0 + gate * (1.0 - sig))).astype(ggu.dtype)
            ggu[n, :, at_up] = (grad * act).astype(ggu.dtype)
            return 0

        lax.fori_loop(0, hidden // tile, inner, 0)

        def at_step(k, *calls):
            def go():
                for call, m in calls:
                    call(m)

            pl.when(n == k)(go)

        at_step(0, (arrive, 1), (arrive_a, 0))
        at_step(1, (arrive, 2))
        at_step(2, (arrive_a, 1))
        at_step(3, (arrive_a, 2))
        pl.when(n < 7)(lambda: fetch(n + 1))

        def outer(j, _):
            at = pl.ds(pl.multiple_of(j * 2 * tile, 2 * tile), 2 * tile)
            p[0, n, :, at] = dot_t(ag[n], wd[at, :]).astype(p.dtype)
            p[1, n, :, at] = dot_t(ggu[n], wgu[at, :]).astype(p.dtype)
            return 0

        lax.fori_loop(0, width // (2 * tile), outer, 0)
        send_b(0, n).start()
        send_b(1, n).start()
        at_step(4, (first, 0))
        at_step(6, (second, 0))
        at_step(7, (first, 1))
        return 0

    lax.fori_loop(0, 8, step, 0)

    def tiles(i):
        slot = i % 2
        cols = pl.ds(pl.multiple_of(i * tile, tile), tile)
        copies = []
        for which, src in enumerate((xg_ref, c_ref)):
            to = pl.ds(pl.multiple_of((2 * which + slot) * tile, tile), tile)

            def one(n, side, which=which, src=src, to=to):
                at = pl.ds(pl.multiple_of((2 * n + side) * rows, rows), rows)
                return pltpu.make_async_copy(src.at[block(n) + side * me.db, :, cols], wgu.at[at, to], tile_sem.at[which, slot, 2 * n + side])

            copies.append(one)
        return copies

    def each_tile(i, act):
        for one in tiles(i):

            def body(n, _):
                for side in (0, 1):
                    act(one(n, side))
                return 0

            lax.fori_loop(0, 8, body, 0)

    def outs(i):
        slot = i % 2
        at = pl.ds(pl.multiple_of(i * tile, tile), tile)
        return (
            pltpu.make_async_copy(xb.at[slot, :, pl.ds(0, 2 * hidden)], gu_out.at[at], load_sem.at[slot, 0]),
            pltpu.make_async_copy(cb.at[slot, :, pl.ds(0, hidden)], down_out.at[at], load_sem.at[slot, 1]),
        )

    each_tile(0, lambda c: c.start())

    def weight_step(i, _):
        slot = i % 2
        pl.when(i < 7)(lambda: each_tile(i + 1, lambda c: c.start()))
        each_tile(i, lambda c: c.wait())

        def free():
            for c in outs(i - 2):
                c.wait()

        pl.when(i >= 2)(free)
        x_tile = wgu[:, pl.ds(pl.multiple_of(slot * tile, tile), tile)]
        xb[slot, :, pl.ds(0, 2 * hidden)] = t_dot(x_tile, ggu[...].reshape(-1, 2 * hidden)).astype(xb.dtype)
        c_tile = wgu[:, pl.ds(pl.multiple_of((2 + slot) * tile, tile), tile)]
        cb[slot, :, pl.ds(0, hidden)] = t_dot(c_tile, ag[...].reshape(-1, hidden)).astype(cb.dtype)
        for c in outs(i):
            c.start()
        pl.when(i == 1)(lambda: second(1))
        pl.when(i == 2)(lambda: first(2))
        pl.when(i == 4)(lambda: second(2))
        pl.when(i == 5)(lambda: first(3))
        return 0

    lax.fori_loop(0, 8, weight_step, 0)
    second(3)

    def pass_back():
        for i in range(2):
            add_rows(from_b.at[i, 0], (from_b.at[i, 0], wait_z(i, z_of(0), 1 - away)), rows)
            send_z(i, 0, 1 - away).start()

    pl.when(depth == 1)(pass_back)
    for i, out_ref in enumerate((moe_ref, two_ref)):
        here = from_b.at[i, 6]
        pl.when(me.z == 0)(lambda: add_rows(out_ref, (here, wait_z(i, me.z, 0)), rows))
        pl.when(me.z == 3)(lambda: add_rows(out_ref, (here, wait_z(i, me.z, 1)), rows))
        pl.when(depth == 1)(lambda: add_rows(out_ref, (here, wait_z(i, me.z, 0), wait_z(i, me.z, 1)), rows))

    for i in (6, 7):
        for c in outs(i):
            c.wait()
    for c in shares:
        c.wait_send()
    pl.when(me.z < 3)(lambda: part(me.dp, me.dp, 0).wait_send())
    pl.when(me.z > 0)(lambda: part(me.dp, me.dp, 1).wait_send())
    part(me.dp, me.dp, 2).wait_send()
    part(me.dp, me.dp, 3).wait_send()
    for m in range(4):
        if m < 3:
            pl.when(onward(m)[0])(lambda: part(me.dp, me.dp, 4 + 3 * m).wait_send())
            part(me.dp, me.dp, 5 + 3 * m).wait_send()
            part(me.dp, me.dp, 6 + 3 * m).wait_send()
        part(me.dp, me.dp, 13 + m).wait_send()
        for i in range(2):
            send_b(i, 2 * m).wait_send()
            send_b(i, 2 * m + 1).wait_send()
            send_a(i, m).wait_send()
            if m < 3:
                send_z(i, m, away).wait_send()


def expert_layer(x, grads, gates, gate, up, down, cid):
    rows, width = x.shape
    half = gate.shape[1]
    hbm, vmem = pl.BlockSpec(memory_space=pl.ANY), pl.BlockSpec(memory_space=pltpu.VMEM)
    dma = pltpu.SemaphoreType.DMA
    dtype = x.dtype
    return pl.pallas_call(
        experts_kernel,
        out_shape=[
            jax.ShapeDtypeStruct((rows, width), jnp.float32),
            jax.ShapeDtypeStruct((rows, width), jnp.float32),
            jax.ShapeDtypeStruct((width, 4 * half), dtype),
            jax.ShapeDtypeStruct((width, 2 * half), dtype),
            jax.ShapeDtypeStruct((16, rows, width), dtype),
        ],
        in_specs=[hbm, hbm, vmem, hbm, hbm, hbm],
        out_specs=[vmem, vmem, hbm, hbm, hbm],
        scratch_shapes=[
            pltpu.VMEM((width, 4 * half), dtype),
            pltpu.VMEM((width, 2 * half), dtype),
            pltpu.VMEM((8, 2 * rows, 2 * half), dtype),
            pltpu.VMEM((8, 2 * rows, 4 * half), dtype),
            pltpu.VMEM((2, 8, 2 * rows, width), dtype),
            pltpu.VMEM((2, 8, rows, width), dtype),
            pltpu.VMEM((2, 4, rows, width), dtype),
            pltpu.VMEM((2, 5, rows, width), dtype),
            pltpu.VMEM((2, 2 * rows, width), dtype),
            pltpu.VMEM((2, 2 * rows, width), dtype),
            dma((17,)), dma((16,)),
            dma((2, 8)), dma((2, 8)),
            dma((2, 4)), dma((2, 4)),
            dma((2, 4)), dma((2, 5)),
            dma((3,)), dma((3,)),
            dma((2, 4)), dma((2, 2, 16)), dma((5,)),
        ],
        compiler_params=pltpu.CompilerParams(collective_id=cid, has_side_effects=True, vmem_limit_bytes=67_043_328),
        name="experts",
    )(x, grads, gates, gate, up, down)


def sum_cores_kernel(gu_ref, down_ref, gate_out, up_out, down_out, held, send_sem, recv_sem):
    me = Place()
    me.greet(partner=True)
    rows, half = gate_out.shape
    chunks = send_sem.shape[1]
    part = rows // chunks
    outs = (gate_out, up_out, down_out)

    def view(i, at, core):
        return (gu_ref, gu_ref, down_ref)[i].at[at, pl.ds(pl.multiple_of((2 * half if i == 1 else 0) + core * half, 128), half)]

    def send(i, k):
        at = pl.ds(k * part, part)
        return me.copy(view(i, at, 1 - me.core), held.at[i, at], send_sem.at[i, k], recv_sem.at[i, k], me.dp, 1 - me.core)

    every = [(i, k) for i in range(3) for k in range(chunks)]
    for i, k in every:
        send(i, k).start()
    for i, k in every:
        send(i, k).wait_recv()
        at = pl.ds(k * part, part)
        add_rows(outs[i].at[at], (view(i, at, me.core), held.at[i, at]), part, 64)
    for i, k in every:
        send(i, k).wait_send()


def sum_cores(gu, down, cid, chunks=4):
    rows, half = down.shape[0], down.shape[1] // 2
    vmem = pl.BlockSpec(memory_space=pltpu.VMEM)
    return pl.pallas_call(
        sum_cores_kernel,
        out_shape=[jax.ShapeDtypeStruct((rows, half), down.dtype)] * 3,
        in_specs=[vmem] * 2,
        out_specs=[vmem] * 3,
        scratch_shapes=[
            pltpu.VMEM((3, rows, half), down.dtype),
            pltpu.SemaphoreType.DMA((3, chunks)),
            pltpu.SemaphoreType.DMA((3, chunks)),
        ],
        compiler_params=pltpu.CompilerParams(collective_id=cid, has_side_effects=True, vmem_limit_bytes=LIMIT),
        name="sum_cores",
    )(gu, down)


def per_device_any(
    tokens,
    cotangent,
    expert_ids,
    gate_values,
    w_query,
    w_key,
    w_value,
    w_out,
    w_gate,
    w_up,
    w_down,
    attn_gain,
    ffn_gain,
    query_gain,
    key_gain,
):
    contract = (((1,), (1,)), ((), ()))
    contract_rows = (((0,), (0,)), ((), ()))
    residual = tokens.astype(jnp.float32)
    model_width = residual.shape[1]
    inverse_one = rms_inverse(residual)
    seq_normed = gather_rows((residual * inverse_one * attn_gain).astype(jnp.bfloat16))
    full_query, full_key, full_value, full_out = (
        lax.all_gather(w_query, "dp", axis=0, tiled=True),
        lax.all_gather(w_key, "dp", axis=0, tiled=True),
        lax.all_gather(w_value, "dp", axis=0, tiled=True),
        lax.all_gather(w_out, "dp", axis=1, tiled=True),
    )
    seq_len = seq_normed.shape[0]
    head_dim = query_gain.shape[0]
    local_heads = full_query.shape[1] // head_dim
    local_kv = full_key.shape[1] // head_dim
    group_size = local_heads // local_kv
    attn_scale = head_dim ** (-0.5)
    cosine, sine_table = rotary_tables(seq_len, head_dim)
    query_raw = jnp.dot(seq_normed, full_query, preferred_element_type=jnp.float32).reshape(
        seq_len, local_heads, head_dim
    )
    key_raw = jnp.dot(seq_normed, full_key, preferred_element_type=jnp.float32).reshape(
        seq_len, local_kv, head_dim
    )
    value_low = (
        jnp.dot(seq_normed, full_value, preferred_element_type=jnp.float32)
        .astype(jnp.bfloat16)
        .reshape(seq_len, local_kv, head_dim)
    )
    query_inverse = rms_inverse(query_raw)
    key_inverse = rms_inverse(key_raw)
    query_low = (
        rotate(query_raw * query_inverse * query_gain, cosine, sine_table) * attn_scale
    ).astype(jnp.bfloat16)
    key_low = rotate(key_raw * key_inverse * key_gain, cosine, sine_table).astype(jnp.bfloat16)
    query_heads = query_low.reshape(seq_len, local_kv, group_size, head_dim).transpose(1, 0, 2, 3)
    key_heads = key_low.transpose(1, 0, 2)
    value_heads = value_low.transpose(1, 0, 2)
    mixed_heads, logsum = lax.map(head_forward, (query_heads, key_heads, value_heads))
    mixed_flat = mixed_heads.transpose(1, 0, 2, 3).reshape(seq_len, local_heads * head_dim)
    hidden = residual + scatter_rows(
        jnp.dot(mixed_flat, full_out, preferred_element_type=jnp.float32)
    )
    inverse_two = rms_inverse(hidden)
    seq_two = gather_rows((hidden * inverse_two * ffn_gain).astype(jnp.bfloat16))
    seq_grad = gather_rows(cotangent)
    experts = w_gate.shape[0]
    dp_rows = w_gate.shape[1]
    hidden_units = w_gate.shape[2]
    dp_count = lax.axis_size("dp")
    group = dp_count // experts
    routed_rows = seq_len * expert_ids.shape[1] * 9 // 8
    capacity = (routed_rows + experts * group - 1) // (experts * group) * group
    slot_table, gate_table = dispatch(expert_ids, gate_values, experts, capacity)
    blank_row = jnp.zeros((1, model_width), jnp.bfloat16)
    padded_in = jnp.concatenate([seq_two, blank_row], axis=0)
    padded_grad = jnp.concatenate([seq_grad, blank_row], axis=0)
    empty_rows = jnp.zeros((seq_len + 1, model_width), jnp.float32)
    piece_rows = capacity // group
    down_rows = jnp.transpose(w_down, (0, 2, 1))
    gate_mine, up_mine, down_mine = (
        lax.all_to_all(widen(w_gate, group), "dp", split_axis=0, concat_axis=1, tiled=True),
        lax.all_to_all(widen(w_up, group), "dp", split_axis=0, concat_axis=1, tiled=True),
        lax.all_to_all(widen(down_rows, group), "dp", split_axis=0, concat_axis=1, tiled=True),
    )
    gate_mine = gate_mine[0]
    up_mine = up_mine[0]
    down_mine = down_mine[0]
    blocks_in = padded_in[slot_table]
    grad_blocks = (padded_grad[slot_table].astype(jnp.float32) * gate_table[:, :, None]).astype(
        jnp.bfloat16
    )
    recv_in, recv_grad = (
        lax.all_to_all(
            blocks_in.reshape(dp_count, piece_rows, model_width),
            "dp",
            split_axis=0,
            concat_axis=0,
            tiled=True,
        ),
        lax.all_to_all(
            grad_blocks.reshape(dp_count, piece_rows, model_width),
            "dp",
            split_axis=0,
            concat_axis=0,
            tiled=True,
        ),
    )
    rows_in = recv_in.reshape(-1, model_width)
    rows_grad = recv_grad.reshape(-1, model_width)
    gate_pre = jnp.dot(rows_in, gate_mine, preferred_element_type=jnp.float32)
    up_pre = jnp.dot(rows_in, up_mine, preferred_element_type=jnp.float32)
    act_low = (jax.nn.silu(gate_pre) * up_pre).astype(jnp.bfloat16)
    expert_out = lax.dot_general(act_low, down_mine, contract, preferred_element_type=jnp.float32)
    grad_act = jnp.dot(rows_grad, down_mine, preferred_element_type=jnp.float32)
    sigmoid_gate = jax.nn.sigmoid(gate_pre)
    grad_gate = (grad_act * up_pre * sigmoid_gate * (1.0 + gate_pre * (1.0 - sigmoid_gate))).astype(
        jnp.bfloat16
    )
    grad_up = (grad_act * gate_pre * sigmoid_gate).astype(jnp.bfloat16)
    grad_input = lax.dot_general(
        grad_gate, gate_mine, contract, preferred_element_type=jnp.float32
    ) + lax.dot_general(grad_up, up_mine, contract, preferred_element_type=jnp.float32)
    back_out, back_grad = (
        lax.all_to_all(
            expert_out.reshape(dp_count, piece_rows, model_width).astype(jnp.bfloat16),
            "dp",
            split_axis=0,
            concat_axis=0,
            tiled=True,
        ).astype(jnp.float32),
        lax.all_to_all(
            grad_input.reshape(dp_count, piece_rows, model_width).astype(jnp.bfloat16),
            "dp",
            split_axis=0,
            concat_axis=0,
            tiled=True,
        ).astype(jnp.float32),
    )
    back_out = back_out.reshape(experts, capacity, model_width)
    back_grad = back_grad.reshape(experts * capacity, model_width)
    flat_slots = slot_table.reshape(-1)
    combined = empty_rows.at[flat_slots].add(
        (back_out * gate_table[:, :, None]).reshape(-1, model_width)
    )
    grad_acc = empty_rows.at[flat_slots].add(back_grad)
    grad_both = jnp.concatenate([grad_gate, grad_up], axis=1)
    grad_cols = jnp.concatenate(
        [
            lax.dot_general(rows_in, grad_both, contract_rows, preferred_element_type=jnp.float32),
            lax.dot_general(rows_grad, act_low, contract_rows, preferred_element_type=jnp.float32),
        ],
        axis=1,
    )
    returned = lax.all_to_all(
        grad_cols[None].astype(jnp.bfloat16), "dp", split_axis=1, concat_axis=0, tiled=True
    ).astype(jnp.float32)
    summed = jnp.sum(returned.reshape(experts, group, dp_rows, 3 * hidden_units), axis=1)
    grad_w_gate = summed[:, :, :hidden_units]
    grad_w_up = summed[:, :, hidden_units : 2 * hidden_units]
    grad_w_down = jnp.transpose(summed[:, :, 2 * hidden_units :], (0, 2, 1))
    output = (hidden + scatter_rows(combined[:seq_len])).astype(jnp.bfloat16)
    grad_two = scatter_rows(grad_acc[:seq_len])
    ffn_gain_part = jnp.sum(grad_two * hidden * inverse_two, axis=0)
    grad_hidden = cotangent.astype(jnp.float32) + norm_backward(
        grad_two, hidden, inverse_two, ffn_gain
    )
    grad_attn = gather_rows(grad_hidden.astype(jnp.bfloat16))
    grad_mixed = lax.dot_general(
        grad_attn, full_out, contract, preferred_element_type=jnp.float32
    ).astype(jnp.bfloat16)
    grad_mixed_heads = grad_mixed.reshape(seq_len, local_kv, group_size, head_dim).transpose(
        1, 0, 2, 3
    )
    grad_query_heads, grad_key_heads, grad_value_heads = lax.map(
        head_backward, (query_heads, key_heads, value_heads, logsum, grad_mixed_heads)
    )
    grad_query_rot = (
        grad_query_heads.transpose(1, 0, 2, 3).reshape(seq_len, local_heads, head_dim) * attn_scale
    )
    grad_query_norm = rotate_back(grad_query_rot, cosine, sine_table)
    query_gain_part = jnp.sum(grad_query_norm * query_raw * query_inverse, axis=(0, 1))
    grad_query_low = (
        norm_backward(grad_query_norm, query_raw, query_inverse, query_gain)
        .astype(jnp.bfloat16)
        .reshape(seq_len, local_heads * head_dim)
    )
    grad_key_norm = rotate_back(grad_key_heads.transpose(1, 0, 2), cosine, sine_table)
    key_gain_part = jnp.sum(grad_key_norm * key_raw * key_inverse, axis=(0, 1))
    grad_key_low = (
        norm_backward(grad_key_norm, key_raw, key_inverse, key_gain)
        .astype(jnp.bfloat16)
        .reshape(seq_len, local_kv * head_dim)
    )
    grad_value_low = (
        grad_value_heads.transpose(1, 0, 2)
        .reshape(seq_len, local_kv * head_dim)
        .astype(jnp.bfloat16)
    )
    grad_proj = jnp.concatenate([grad_query_low, grad_key_low, grad_value_low], axis=1)
    full_proj = jnp.concatenate([full_query, full_key, full_value], axis=1)
    grad_one = scatter_rows(
        lax.dot_general(grad_proj, full_proj, contract, preferred_element_type=jnp.float32)
    )
    first_part = jnp.einsum("sd,sf->df", seq_normed, grad_proj, preferred_element_type=jnp.float32)
    second = jnp.einsum("sd,sf->df", grad_attn, mixed_flat, preferred_element_type=jnp.float32)
    shares = lax.psum_scatter(
        jnp.concatenate([first_part, second], axis=1), "dp", scatter_dimension=0, tiled=True
    )
    query_cols = w_query.shape[1]
    key_cols = w_key.shape[1]
    grad_w_query = shares[:, :query_cols]
    grad_w_key = shares[:, query_cols : query_cols + key_cols]
    grad_w_value = shares[:, query_cols + key_cols : query_cols + 2 * key_cols]
    grad_w_out = jnp.transpose(shares[:, query_cols + 2 * key_cols :])
    attn_gain_part = jnp.sum(grad_one * residual * inverse_one, axis=0)
    grad_tokens = (grad_hidden + norm_backward(grad_one, residual, inverse_one, attn_gain)).astype(
        jnp.bfloat16
    )
    total_gains = lax.psum(
        (attn_gain_part, ffn_gain_part, query_gain_part, key_gain_part), ("dp", "tensor")
    )
    return (
        output,
        grad_tokens,
        grad_w_query,
        grad_w_key,
        grad_w_value,
        grad_w_out,
        grad_w_gate,
        grad_w_up,
        grad_w_down,
        total_gains[0],
        total_gains[1],
        total_gains[2],
        total_gains[3],
    )


def per_device_relay(
    tokens,
    cotangent,
    expert_ids,
    gate_values,
    w_query,
    w_key,
    w_value,
    w_out,
    w_gate,
    w_up,
    w_down,
    attn_gain,
    ffn_gain,
    query_gain,
    key_gain,
):
    dot = functools.partial(jnp.dot, preferred_element_type=jnp.float32)
    dot_t = functools.partial(lax.dot_general, dimension_numbers=(((1,), (1,)), ((), ())), preferred_element_type=jnp.float32)
    t_dot = functools.partial(lax.dot_general, dimension_numbers=(((0,), (0,)), ((), ())), preferred_element_type=jnp.float32)
    low = jnp.bfloat16
    rows, width = tokens.shape
    head_dim = query_gain.shape[0]
    experts = w_gate.shape[0]
    core = lax.axis_index("tensor")
    mine = lax.dynamic_slice_in_dim(expert_ids, core * rows, rows, 0)
    values = lax.dynamic_slice_in_dim(gate_values, core * rows, rows, 0)
    match = mine[None] == jnp.arange(experts, dtype=jnp.int32)[:, None, None]
    gates = jnp.sum(jnp.where(match, values[None], 0.0), axis=2)
    gates = jnp.broadcast_to(gates[:, None], (experts, 8, rows))

    q_cols, kv_cols = w_query.shape[1] // 2, w_key.shape[1] // 2
    w_out_rows = jnp.transpose(w_out)
    halves = jnp.stack(
        [
            jnp.concatenate([w[:, h * (w.shape[1] // 2) : (h + 1) * (w.shape[1] // 2)] for w in (w_query, w_key, w_value, w_out_rows)], axis=1)
            for h in range(2)
        ]
    )
    swap_weights = functools.partial(lax.all_to_all, axis_name="dp", split_axis=0, concat_axis=1, tiled=True)
    gate_mine, up_mine, down_mine = [swap_weights(w)[0] for w in (w_gate, w_up, jnp.transpose(w_down, (0, 2, 1)))]
    weights, rows_grad, gates = gather_first(halves, cotangent, gates, 1)
    weights, gates = weights.reshape(-1, weights.shape[2]), gates[:, 0][:, :, None]
    proj_cols = q_cols + 2 * kv_cols
    w_proj, w_back = weights[:, :proj_cols], weights[:, proj_cols:]

    residual = tokens.astype(jnp.float32)
    inverse_one = rms_inverse(residual)
    seq_normed = gather_four((residual * inverse_one * attn_gain).astype(low), 4).reshape(-1, width)
    seq_len = 2 * rows
    group = q_cols // head_dim
    scale = head_dim ** (-0.5)
    cosine, sine_table = rotary_tables(seq_len, head_dim)
    proj = dot(seq_normed, w_proj)
    query_raw = proj[:, :q_cols].reshape(2, seq_len, group, head_dim)
    key_raw = proj[:, q_cols : q_cols + kv_cols].reshape(2, seq_len, 1, head_dim)
    value_low = proj[:, q_cols + kv_cols :].astype(low).reshape(2, seq_len, head_dim)
    query_inverse, key_inverse = rms_inverse(query_raw), rms_inverse(key_raw)
    query_low = (rotate(query_raw * query_inverse * query_gain, cosine, sine_table) * scale).astype(low)
    key_low = rotate(key_raw * key_inverse * key_gain, cosine, sine_table).astype(low)[:, :, 0]
    causal = jnp.arange(seq_len)[:, None] >= jnp.arange(seq_len)[None, :]
    scores = jnp.einsum("bqgd,bsd->bgqs", query_low, key_low, preferred_element_type=jnp.float32)
    exp_scores = jnp.where(causal, jnp.exp(scores), 0.0)
    probs = exp_scores / jnp.sum(exp_scores, axis=-1, keepdims=True)
    probs_low = probs.astype(low)
    mixed = jnp.einsum("bgqs,bsd->bqgd", probs_low, value_low, preferred_element_type=jnp.float32).astype(low).reshape(2 * seq_len, q_cols)
    hidden = residual + scatter_four(dot_t(mixed, w_back).astype(low).reshape(2, 2, rows, width), 5)
    inverse_two = rms_inverse(hidden)
    normed_two = (hidden * inverse_two * ffn_gain).astype(low)
    moe, grad_two, gu_part, down_part, _ = expert_layer(normed_two, rows_grad, gates, gate_mine, up_mine, down_mine, 2)
    owned = sum_cores(gu_part, down_part, 8)
    swap_grads = functools.partial(lax.all_to_all, axis_name="dp", split_axis=0, concat_axis=0, tiled=True)
    grad_w_gate, grad_w_up, grad_w_down = [swap_grads(v.reshape(experts, rows, -1)).astype(jnp.float32) for v in owned]
    grad_w_down = jnp.transpose(grad_w_down, (0, 2, 1))

    output = (hidden + moe).astype(low)
    ffn_gain_part = jnp.sum(grad_two * hidden * inverse_two, axis=0)
    grad_hidden = cotangent.astype(jnp.float32) + norm_backward(grad_two, hidden, inverse_two, ffn_gain)
    grad_attn = gather_four(grad_hidden.astype(low), 9).reshape(-1, width)
    grad_mixed = dot(grad_attn, w_back).astype(low).reshape(2, seq_len, group, head_dim)
    grad_probs = jnp.einsum("bqgd,bsd->bgqs", grad_mixed, value_low, preferred_element_type=jnp.float32)
    delta_sum = jnp.sum(grad_probs * probs, axis=-1, keepdims=True)
    grad_scores = (probs * (grad_probs - delta_sum)).astype(low)
    grad_query = jnp.einsum("bgqs,bsd->bqgd", grad_scores, key_low, preferred_element_type=jnp.float32)
    grad_key = jnp.einsum("bgqs,bqgd->bsd", grad_scores, query_low, preferred_element_type=jnp.float32)
    grad_value = jnp.einsum("bgqs,bqgd->bsd", probs_low, grad_mixed, preferred_element_type=jnp.float32)
    grad_query_norm = rotate_back(grad_query * scale, cosine, sine_table)
    query_gain_part = jnp.sum(grad_query_norm * query_raw * query_inverse, axis=(0, 1, 2))
    grad_query_low = norm_backward(grad_query_norm, query_raw, query_inverse, query_gain).astype(low)
    grad_key_norm = rotate_back(grad_key[:, :, None], cosine, sine_table)
    key_gain_part = jnp.sum(grad_key_norm * key_raw * key_inverse, axis=(0, 1, 2))
    grad_key_low = norm_backward(grad_key_norm, key_raw, key_inverse, key_gain).astype(low)
    grad_proj = jnp.concatenate([v.astype(low).reshape(2 * seq_len, -1) for v in (grad_query_low, grad_key_low, grad_value)], axis=1)
    grad_one = scatter_four(dot_t(grad_proj, w_proj).astype(low).reshape(2, 2, rows, width), 10)
    w_parts = jnp.concatenate([t_dot(seq_normed, grad_proj), t_dot(grad_attn, mixed)], axis=1).astype(low)
    attn_gain_part = jnp.sum(grad_one * residual * inverse_one, axis=0)
    gains = jnp.concatenate([attn_gain_part, ffn_gain_part, query_gain_part, key_gain_part])
    gains = jnp.pad(gains, (0, -gains.shape[0] % 1024)).reshape(-1, 128)
    shares, totals = scatter_last(w_parts.reshape(-1, rows, w_parts.shape[1]), gains, 11)
    shares, totals = shares.astype(jnp.float32), totals.reshape(-1)
    stops = (0, q_cols, q_cols + kv_cols, proj_cols, proj_cols + q_cols)
    grads = [jnp.concatenate([shares[0, :, a:b], shares[1, :, a:b]], axis=1) for a, b in zip(stops, stops[1:])]
    grad_tokens = (grad_hidden + norm_backward(grad_one, residual, inverse_one, attn_gain)).astype(low)
    totals = jnp.split(totals, (width, 2 * width, 2 * width + head_dim, 2 * width + 2 * head_dim))[:4]
    return (output, grad_tokens, grads[0], grads[1], grads[2], jnp.transpose(grads[3]), grad_w_gate, grad_w_up, grad_w_down, *totals)


def solution(mesh):
    return jax.shard_map(
        per_device_relay if tuple(mesh.shape.values()) == (16, 2) else per_device_any,
        mesh=mesh,
        in_specs=(
            P(("dp", "tensor"), None),
            P(("dp", "tensor"), None),
            P("dp", None),
            P("dp", None),
            P("dp", "tensor"),
            P("dp", "tensor"),
            P("dp", "tensor"),
            P("tensor", "dp"),
            P(None, "dp", "tensor"),
            P(None, "dp", "tensor"),
            P(None, "tensor", "dp"),
            P(),
            P(),
            P(),
            P(),
        ),
        out_specs=(
            P(("dp", "tensor"), None),
            P(("dp", "tensor"), None),
            P("dp", "tensor"),
            P("dp", "tensor"),
            P("dp", "tensor"),
            P("tensor", "dp"),
            P(None, "dp", "tensor"),
            P(None, "dp", "tensor"),
            P(None, "tensor", "dp"),
            P(),
            P(),
            P(),
            P(),
        ),
        check_vma=False,
    )
```

```python
import functools

import jax
import jax.numpy as jnp
from jax import lax
from jax.experimental import pallas as pl
from jax.experimental.pallas import tpu as pltpu
from jax.sharding import PartitionSpec as P

epsilon = 1e-06
theta_base = 1000000.0


def rms_inverse(values):
    return lax.rsqrt(jnp.mean(values * values, axis=-1, keepdims=True) + epsilon)


def norm_backward(grad_in, values, inverse, gain_vec):
    scaled = grad_in * gain_vec
    inner_mean = jnp.mean(scaled * values, axis=-1, keepdims=True)
    return inverse * scaled - values * inverse**3 * inner_mean


def rotary_tables(seq_len, head_dim):
    half_dim = head_dim // 2
    frequency = theta_base ** (-jnp.arange(half_dim, dtype=jnp.float32) * 2.0 / head_dim)
    angles = jnp.arange(seq_len, dtype=jnp.float32)[:, None] * frequency[None, :]
    return (jnp.cos(angles)[:, None, :], jnp.sin(angles)[:, None, :])


def rotate(values, cosine, sine_table):
    half_dim = values.shape[-1] // 2
    first_part = values[..., :half_dim]
    second = values[..., half_dim:]
    return jnp.concatenate(
        [first_part * cosine - second * sine_table, second * cosine + first_part * sine_table],
        axis=-1,
    )


def rotate_back(grad_in, cosine, sine_table):
    half_dim = grad_in.shape[-1] // 2
    first_part = grad_in[..., :half_dim]
    second = grad_in[..., half_dim:]
    return jnp.concatenate(
        [first_part * cosine + second * sine_table, second * cosine - first_part * sine_table],
        axis=-1,
    )


def dispatch(expert_ids, gate_values, experts, capacity):
    seq_len = expert_ids.shape[0]
    is_match = expert_ids[:, :, None] == jnp.arange(experts, dtype=jnp.int32)[None, None, :]
    expert_hits = jnp.sum(is_match.astype(jnp.int32), axis=1)
    before = jnp.cumsum(expert_hits, axis=0) - expert_hits
    slot_ids = jnp.sum(jnp.where(is_match, before[:, None, :], 0), axis=2)
    token_index = jnp.broadcast_to(jnp.arange(seq_len, dtype=jnp.int32)[:, None], expert_ids.shape)
    slot_table = (
        jnp.full((experts, capacity), seq_len, jnp.int32).at[expert_ids, slot_ids].set(token_index)
    )
    gate_table = (
        jnp.zeros((experts, capacity), jnp.float32).at[expert_ids, slot_ids].set(gate_values)
    )
    return (slot_table, gate_table)


def head_forward(head_inputs):
    query_vals, key_vals, value_vals = head_inputs
    seq_len = key_vals.shape[0]
    block_rows = min(512, seq_len)
    key_positions = jnp.arange(seq_len)

    def one_block(row_start):
        scores = jnp.einsum("qgd,sd->gqs", query_vals, key_vals, preferred_element_type=jnp.float32)
        causal = (row_start + jnp.arange(block_rows))[:, None] >= key_positions[None, :]
        exp_scores = jnp.where(causal, jnp.exp(scores), 0.0)
        denominator = jnp.sum(exp_scores, axis=-1, keepdims=True)
        softmax_low = (exp_scores / denominator).astype(jnp.bfloat16)
        mixed_out = jnp.einsum(
            "gqs,sd->qgd", softmax_low, value_vals, preferred_element_type=jnp.float32
        )
        return (mixed_out.astype(jnp.bfloat16), jnp.log(denominator[..., 0]))

    block_starts = jnp.arange(seq_len // block_rows, dtype=jnp.int32) * block_rows
    mixed_out, logsum = lax.map(one_block, block_starts)
    return (mixed_out.reshape(seq_len, query_vals.shape[1], query_vals.shape[2]), logsum)


def head_backward(head_inputs):
    query_vals, key_vals, value_vals, logsum, grad_mixed = head_inputs
    seq_len = key_vals.shape[0]
    block_rows = min(512, seq_len)
    key_positions = jnp.arange(seq_len)

    def one_block(state_in, block_in):
        grad_key, grad_value = state_in
        row_start, block_logsum = block_in
        scores = jnp.einsum("qgd,sd->gqs", query_vals, key_vals, preferred_element_type=jnp.float32)
        causal = (row_start + jnp.arange(block_rows))[:, None] >= key_positions[None, :]
        softmax_vals = jnp.where(causal, jnp.exp(scores - block_logsum[..., None]), 0.0)
        grad_probs = jnp.einsum(
            "qgd,sd->gqs", grad_mixed, value_vals, preferred_element_type=jnp.float32
        )
        delta_sum = jnp.sum(grad_probs * softmax_vals, axis=-1, keepdims=True)
        grad_scores = (softmax_vals * (grad_probs - delta_sum)).astype(jnp.bfloat16)
        grad_query = jnp.einsum(
            "gqs,sd->qgd", grad_scores, key_vals, preferred_element_type=jnp.float32
        )
        grad_key = grad_key + jnp.einsum(
            "gqs,qgd->sd", grad_scores, query_vals, preferred_element_type=jnp.float32
        )
        grad_value = grad_value + jnp.einsum(
            "gqs,qgd->sd",
            softmax_vals.astype(jnp.bfloat16),
            grad_mixed,
            preferred_element_type=jnp.float32,
        )
        return ((grad_key, grad_value), grad_query)

    block_starts = jnp.arange(seq_len // block_rows, dtype=jnp.int32) * block_rows
    zero_rows = jnp.zeros(key_vals.shape, jnp.float32)
    (grad_key, grad_value), grad_query = lax.scan(
        one_block, (zero_rows, zero_rows), (block_starts, logsum)
    )
    return (grad_query.reshape(query_vals.shape), grad_key, grad_value)


def gather_rows(values):
    return lax.all_gather(values, "tensor", axis=0, tiled=True)


def scatter_rows(values):
    return lax.psum_scatter(
        values.astype(jnp.bfloat16), "tensor", scatter_dimension=0, tiled=True
    ).astype(jnp.float32)


def widen(stacked, group):
    experts = stacked.shape[0]
    spread = jnp.broadcast_to(stacked[:, None], (experts, group) + stacked.shape[1:])
    return spread.reshape((experts * group,) + stacked.shape[1:])


MESH = pl.DeviceIdType.MESH
LIMIT = 66_000_000


class Place:
    def __init__(self):
        self.dp = lax.axis_index("dp")
        self.core = lax.axis_index("tensor")
        x, y = self.dp % 2, (self.dp // 2) % 2
        self.z = self.dp // 4
        step_x, step_y = 1 - 2 * x, 2 * (1 - 2 * y)
        self.da = (1 - self.core) * step_x + self.core * step_y
        self.db = (1 - self.core) * step_y + self.core * step_x
        self.half = self.z % 2
        self.pair = 4 * (1 - 2 * self.half)
        self.far = 8 * (1 - 2 * (self.z // 2))

    def copy(self, src, dst, send_sem, recv_sem, to, core=None):
        return pltpu.make_async_remote_copy(
            src_ref=src,
            dst_ref=dst,
            send_sem=send_sem,
            recv_sem=recv_sem,
            device_id=(to, self.core if core is None else core),
            device_id_type=MESH,
        )

    def at_z(self, z):
        return self.dp + 4 * (z - self.z)

    def greet(self, line=False, near=False, chain=False, everyone=False, partner=False):
        barrier = pltpu.get_barrier_semaphore()
        count = 0

        def signal(to, core):
            pl.semaphore_signal(barrier, inc=1, device_id=(to, core), device_id_type=MESH)

        if everyone:
            for r in range(1, 16):
                signal((self.dp + r) % 16, self.core)
            count = count + 15
        else:
            if near:
                signal(self.dp + self.da, self.core)
                signal(self.dp + self.db, self.core)
                count = count + 2
            if chain:
                signal(self.dp + self.pair, self.core)
                count = count + 1
                if near:
                    signal(self.dp + self.far, self.core)
                    count = count + 1
            if line:
                pl.when(self.z > 0)(lambda: signal(self.dp - 4, self.core))
                pl.when(self.z < 3)(lambda: signal(self.dp + 4, self.core))
                count = count + jnp.where(self.z > 0, 1, 0) + jnp.where(self.z < 3, 1, 0)
        if partner:
            signal(self.dp, 1 - self.core)
            count = count + 1
        pl.semaphore_wait(barrier, count)


def add_rows(target, terms, rows, block=16):
    def body(i, _):
        at = pl.ds(pl.multiple_of(i * block, block), block)
        total = terms[0][at, :].astype(jnp.float32)
        for term in terms[1:]:
            total = total + term[at, :].astype(jnp.float32)
        target[at, :] = total.astype(target.dtype)
        return 0

    lax.fori_loop(0, rows // block, body, 0)


def gather_four_kernel(x_ref, out_ref, send_sem, recv_sem):
    me = Place()
    me.greet(chain=True, partner=True)
    run(gather_four(me, x_ref, out_ref, send_sem, recv_sem))


def gather_pair_rows(x, cid):
    rows, columns = x.shape
    vmem = pl.BlockSpec(memory_space=pltpu.VMEM)
    return pl.pallas_call(
        gather_four_kernel,
        out_shape=jax.ShapeDtypeStruct((2, 2, rows, columns), x.dtype),
        in_specs=[vmem],
        out_specs=vmem,
        scratch_shapes=[pltpu.SemaphoreType.DMA((3,)), pltpu.SemaphoreType.DMA((3,))],
        compiler_params=pltpu.CompilerParams(collective_id=cid, has_side_effects=True),
        name="gather_four",
    )(x)


def scatter_four_kernel(p_ref, out_ref, from_core, from_pair, send_sem, recv_sem):
    me = Place()
    rows = p_ref.shape[2]
    me.greet(chain=True, partner=True)

    def beside(h, slot):
        return me.copy(p_ref.at[h, 1 - me.core], from_core.at[slot], send_sem.at[slot], recv_sem.at[slot], me.dp, 1 - me.core)

    first, second = beside(1 - me.half, 0), beside(me.half, 1)
    first.start()
    second.start()
    first.wait_recv()
    add_rows(from_core.at[0], (p_ref.at[1 - me.half, me.core], from_core.at[0]), rows)
    across = me.copy(from_core.at[0], from_pair, send_sem.at[2], recv_sem.at[2], me.dp + me.pair)
    across.start()
    second.wait_recv()
    add_rows(from_core.at[1], (p_ref.at[me.half, me.core], from_core.at[1]), rows)
    across.wait_recv()
    add_rows(out_ref, (from_core.at[1], from_pair), rows)
    across.wait_send()
    first.wait_send()
    second.wait_send()


def scatter_four(p, cid):
    _, _, rows, columns = p.shape
    vmem = pl.BlockSpec(memory_space=pltpu.VMEM)
    return pl.pallas_call(
        scatter_four_kernel,
        out_shape=jax.ShapeDtypeStruct((rows, columns), jnp.float32),
        in_specs=[vmem],
        out_specs=vmem,
        scratch_shapes=[
            pltpu.VMEM((2, rows, columns), p.dtype),
            pltpu.VMEM((rows, columns), p.dtype),
            pltpu.SemaphoreType.DMA((3,)),
            pltpu.SemaphoreType.DMA((3,)),
        ],
        compiler_params=pltpu.CompilerParams(collective_id=cid, has_side_effects=True),
        name="scatter_four",
    )(p)


def run(*threads):
    threads = list(threads)
    while threads:
        for thread in list(threads):
            if next(thread, "end") == "end":
                threads.remove(thread)


def lagged(items, first, second, lag):
    for n in range(len(items) + lag):
        if n < len(items):
            first(items[n])
            yield
        if n >= lag:
            second(items[n - lag])
            yield


def gather_line(me, x_ref, out_ref, send_sem, recv_sem):
    def part(source, to, slot, own=False):
        return me.copy(x_ref if own else out_ref.at[source], out_ref.at[source], send_sem.at[slot], recv_sem.at[source], to)

    sides = ((-1, me.z < 3, 4), (1, me.z > 0, -4))

    def exists(d, side):
        return (me.z - d >= 0) if side == 0 else (me.z + d <= 3)

    def slot_z(d, side, j):
        return 4 + ((d - 1) * 2 + side) * 3 + j

    def slot_a(off):
        return 25 + off

    def pass_a(off):
        source = me.dp + me.da + 4 * off
        part(source, me.dp, slot_a(off)).wait_recv()
        part(source, me.dp + me.db, slot_a(off)).start()

    pl.when(me.z < 3)(lambda: part(me.dp, me.dp + 4, 0, True).start())
    pl.when(me.z > 0)(lambda: part(me.dp, me.dp - 4, 1, True).start())
    part(me.dp, me.dp + me.db, 3, True).start()
    part(me.dp, me.dp + me.da, 2, True).start()
    yield
    for d in range(1, 5):
        if d < 4:
            for side, (sign, forward, step) in enumerate(sides):
                source = me.dp + 4 * sign * d

                def arrive():
                    part(source, me.dp, slot_z(d, side, 0)).wait_recv()
                    pl.when(forward)(lambda: part(source, me.dp + step, slot_z(d, side, 0)).start())
                    part(source, me.dp + me.db, slot_z(d, side, 2)).start()
                    part(source, me.dp + me.da, slot_z(d, side, 1)).start()

                pl.when(exists(d, side))(arrive)
                yield
        if d == 1:
            pass_a(0)
            yield
        else:
            for side, (sign, *_) in enumerate(sides):
                pl.when(exists(d - 1, side))(lambda: pass_a(sign * (d - 1)))
                yield
    for z in range(4):
        for g in (0, 1):
            part(me.at_z(z) + me.db + g * me.da, me.dp, 0).wait_recv()
            yield

    def sent(slot):
        part(me.dp, me.dp, slot).wait_send()

    pl.when(me.z < 3)(lambda: sent(0))
    pl.when(me.z > 0)(lambda: sent(1))
    sent(2)
    sent(3)
    sent(slot_a(0))
    for d in range(1, 4):
        for side, (sign, forward, _) in enumerate(sides):

            def finish():
                pl.when(forward)(lambda: sent(slot_z(d, side, 0)))
                sent(slot_z(d, side, 1))
                sent(slot_z(d, side, 2))
                sent(slot_a(sign * d))

            pl.when(exists(d, side))(finish)


def gather_pairs(me, x_ref, out_ref, send_sem, recv_sem):
    mine, other = me.dp, me.dp + me.pair

    def part(src, where, to, slot):
        return me.copy(src, out_ref.at[where], send_sem.at[slot], recv_sem.at[where], to)

    def relay(where, to, slot):
        part(out_ref.at[where], where, to, slot).start()

    def arrived(where):
        part(out_ref.at[where], where, me.dp, 0).wait_recv()

    part(x_ref.at[1 - me.half], mine, other, 0).start()
    part(x_ref.at[me.half], mine, me.dp + me.far, 1).start()
    part(x_ref.at[me.half], mine, me.dp + me.db, 2).start()
    part(x_ref.at[me.half], mine, me.dp + me.da, 3).start()
    yield
    arrived(other)
    relay(other, me.dp + me.far, 4)
    relay(other, me.dp + me.db, 5)
    relay(other, me.dp + me.da, 6)
    yield
    arrived(mine + me.da)
    relay(mine + me.da, me.dp + me.db, 7)
    yield
    arrived(mine + me.far)
    relay(mine + me.far, me.dp + me.db, 8)
    relay(mine + me.far, me.dp + me.da, 9)
    yield
    arrived(other + me.da)
    relay(other + me.da, me.dp + me.db, 10)
    yield
    arrived(other + me.far)
    relay(other + me.far, me.dp + me.db, 11)
    relay(other + me.far, me.dp + me.da, 12)
    yield
    arrived(mine + me.far + me.da)
    relay(mine + me.far + me.da, me.dp + me.db, 13)
    yield
    arrived(other + me.far + me.da)
    relay(other + me.far + me.da, me.dp + me.db, 14)
    yield
    for base in (mine, other, mine + me.far, other + me.far):
        arrived(base + me.db)
        yield
        arrived(base + me.da + me.db)
        yield
    for slot in range(15):
        part(out_ref.at[mine], mine, me.dp, slot).wait_send()


def swap_rows(me, x_ref, out_ref, send_sem, recv_sem):
    for r in range(1, 16):
        to = (me.dp + r) % 16
        me.copy(x_ref.at[to], out_ref.at[me.dp], send_sem.at[r], recv_sem.at[r], to).start()
    yield
    for r in range(1, 16):
        s = (me.dp + 16 - r) % 16
        me.copy(x_ref.at[s], out_ref.at[s], send_sem.at[r], recv_sem.at[r], me.dp).wait_recv()
    for r in range(1, 16):
        me.copy(x_ref.at[me.dp], out_ref.at[me.dp], send_sem.at[r], recv_sem.at[r], me.dp).wait_send()


def keep_own(src, staging, dst, sems):
    load = pltpu.make_async_copy(src, staging, sems.at[0])
    store = pltpu.make_async_copy(staging, dst, sems.at[1])
    load.start()

    def finish():
        load.wait()
        store.start()
        store.wait()

    return finish


def share_experts(me, ins, outs, send_sem, recv_sem):
    depth = ins[0].shape[1]

    def sends(r):
        to = (me.dp + r) % 16
        at = pl.ds(pl.multiple_of(me.dp * depth, depth), depth)
        pairs = ((ins[0].at[to], outs[0].at[at]), (ins[1].at[to], outs[1].at[at]), (ins[2].at[to], outs[2].at[:, at]))
        return [me.copy(src, dst, send_sem.at[r, j], recv_sem.at[r, j], to) for j, (src, dst) in enumerate(pairs)]

    for r in (8, 7, 9, 4, 12, 5, 11, 6, 10, 3, 13, 2, 14, 1, 15):
        for c in sends(r):
            c.start()
    yield
    for r in range(1, 16):
        at = pl.ds(pl.multiple_of((me.dp + 16 - r) % 16 * depth, depth), depth)
        for j, dst in enumerate((outs[0].at[at], outs[1].at[at], outs[2].at[:, at])):
            me.copy(dst, dst, send_sem.at[r, j], recv_sem.at[r, j], me.dp).wait_recv()
    for r in range(1, 16):
        for c in sends(r):
            c.wait_send()


def gather_four(me, x_ref, out_ref, send_sem, recv_sem):
    mine, theirs = out_ref.at[me.half, me.core], out_ref.at[1 - me.half, me.core]
    across = me.copy(x_ref, mine, send_sem.at[0], recv_sem.at[0], me.dp + me.pair)
    across.start()
    beside = me.copy(x_ref, mine, send_sem.at[1], recv_sem.at[1], me.dp, 1 - me.core)
    beside.start()
    mine[...] = x_ref[...]
    yield
    across.wait_recv()
    relay = me.copy(theirs, theirs, send_sem.at[2], recv_sem.at[2], me.dp, 1 - me.core)
    relay.start()
    yield
    across.wait_send()
    beside.wait()
    relay.wait()


def gather_first_kernel(
    w_ref, c_ref, g_ref, x_ref, gate_ref, up_ref, down_ref,
    w_out, c_out, g_out, x_out, gate_out, up_out, down_out,
    w_own, c_own, e_own, w_send, w_recv, c_send, c_recv, g_send, g_recv, x_send, x_recv, e_send, e_recv, copy_sem,
):
    me = Place()
    depth = gate_ref.shape[1]
    at = pl.ds(pl.multiple_of(me.dp * depth, depth), depth)
    ends = [
        keep_own(w_ref.at[me.half], w_own, w_out.at[me.dp], copy_sem.at[0]),
        keep_own(c_ref, c_own, c_out.at[me.dp], copy_sem.at[1]),
        keep_own(gate_ref.at[me.dp], e_own.at[0], gate_out.at[at], copy_sem.at[2]),
        keep_own(up_ref.at[me.dp], e_own.at[1], up_out.at[at], copy_sem.at[3]),
    ]
    flat = pltpu.make_async_copy(down_ref.at[me.dp], down_out.at[:, at], copy_sem.at[4, 0])
    flat.start()
    g_out[me.dp] = g_ref[me.dp]
    me.greet(everyone=True, partner=True)
    run(
        gather_four(me, x_ref, x_out, x_send, x_recv),
        gather_pairs(me, w_ref, w_out, w_send, w_recv),
        gather_line(me, c_ref, c_out, c_send, c_recv),
        swap_rows(me, g_ref, g_out, g_send, g_recv),
        share_experts(me, (gate_ref, up_ref, down_ref), (gate_out, up_out, down_out), e_send, e_recv),
    )
    for end in ends:
        end()
    flat.wait()


def gather_first(weights, rows, gates, normed, experts, cid):
    hbm, vmem = pl.BlockSpec(memory_space=pl.ANY), pl.BlockSpec(memory_space=pltpu.VMEM)
    dma = pltpu.SemaphoreType.DMA
    dtype = rows.dtype
    _, depth, hidden = experts[0].shape
    return pl.pallas_call(
        gather_first_kernel,
        out_shape=[
            jax.ShapeDtypeStruct((16,) + weights.shape[1:], dtype),
            jax.ShapeDtypeStruct((16,) + rows.shape, dtype),
            jax.ShapeDtypeStruct(gates.shape, gates.dtype),
            jax.ShapeDtypeStruct((2, 2) + normed.shape, dtype),
            jax.ShapeDtypeStruct((16 * depth, hidden), dtype),
            jax.ShapeDtypeStruct((16 * depth, hidden), dtype),
            jax.ShapeDtypeStruct((hidden, 16 * depth), dtype),
        ],
        in_specs=[hbm, hbm, vmem, vmem, hbm, hbm, hbm],
        out_specs=[hbm, hbm, vmem, vmem, hbm, hbm, hbm],
        scratch_shapes=[
            pltpu.VMEM(weights.shape[1:], dtype),
            pltpu.VMEM(rows.shape, dtype),
            pltpu.VMEM((2, depth, hidden), dtype),
            dma((15,)), dma((16,)),
            dma((29,)), dma((16,)),
            dma((16,)), dma((16,)),
            dma((3,)), dma((3,)),
            dma((16, 3)), dma((16, 3)),
            dma((5, 2)),
        ],
        compiler_params=pltpu.CompilerParams(collective_id=cid, has_side_effects=True),
        name="gather_first",
    )(weights, rows, gates, normed, *experts)


def scatter_pairs(me, chunks, p_ref, out_ref, from_b, from_a, from_far, send_sem, recv_sem):
    rows = p_ref.shape[1] // chunks
    other = me.dp + me.pair
    bases = (me.dp, other, me.dp + me.far, other + me.far)
    items = [(j, k) for j in (2, 3, 1, 0) for k in range(chunks)]

    def at(k):
        return pl.ds(k * rows, rows)

    def copy(src, dst, slot, k, to):
        return me.copy(src, dst, send_sem.at[slot, k], recv_sem.at[slot, k], to)

    def send_b(g, j, k):
        return copy(p_ref.at[bases[j] + me.db + g * me.da, at(k)], from_b.at[g, j, at(k)], g * 4 + j, k, me.dp + me.db)

    def send_a(j, k):
        return copy(from_b.at[1, j, at(k)], from_a.at[j, at(k)], 8 + j, k, me.dp + me.da)

    def send_far(j, k):
        return copy(from_b.at[0, 2 + j, at(k)], from_far.at[j, at(k)], 12 + j, k, me.dp + me.far)

    def swap(k):
        return copy(from_b.at[0, 1, at(k)], out_ref.at[me.half, at(k)], 14, k, other)

    for j, k in items:
        send_b(1, j, k).start()
        send_b(0, j, k).start()
    yield

    def first(item):
        j, k = item
        send_b(1, j, k).wait_recv()
        add_rows(from_b.at[1, j, at(k)], (p_ref.at[bases[j] + me.da, at(k)], from_b.at[1, j, at(k)]), rows)
        send_a(j, k).start()

    def second(item):
        j, k = item
        send_b(0, j, k).wait_recv()
        send_a(j, k).wait_recv()
        terms = (p_ref.at[bases[j], at(k)], from_b.at[0, j, at(k)], from_a.at[j, at(k)])
        if j >= 2:
            add_rows(from_b.at[0, j, at(k)], terms, rows)
            send_far(j - 2, k).start()
        else:
            send_far(j, k).wait_recv()
            target = from_b.at[0, 1, at(k)] if j else out_ref.at[me.half, at(k)]
            add_rows(target, terms + (from_far.at[j, at(k)],), rows)
            if j:
                swap(k).start()

    yield from lagged(items, first, second, 2)
    for k in range(chunks):
        swap(k).wait_send()
        theirs = out_ref.at[1 - me.half, at(k)]
        copy(theirs, theirs, 14, k, other).wait_recv()
        for j in range(4):
            send_b(0, j, k).wait_send()
            send_b(1, j, k).wait_send()
            send_a(j, k).wait_send()
        send_far(0, k).wait_send()
        send_far(1, k).wait_send()


def sum_all(me, x_ref, out_ref, held, send_sem, recv_sem):
    out_ref[...] = x_ref[...]
    steps = ((me.dp, 1 - me.core), (me.dp + me.da, me.core), (me.dp + me.db, me.core), (me.dp + me.pair, me.core), (me.dp + me.far, me.core))
    yield
    for n, (to, core) in enumerate(steps):
        send = me.copy(held.at[0, n], held.at[1, n], send_sem.at[n], recv_sem.at[n], to, core)
        held[0, n] = out_ref[...]
        send.start()
        yield
        send.wait()
        out_ref[...] = held[0, n] + held[1, n]
        yield


def return_experts(me, gu_ref, down_ref, outs, own, held, core_send, core_recv, send_sem, recv_sem, copy_sem):
    rows, half = outs[0].shape[1:]

    def views(d, core):
        at = pl.ds(pl.multiple_of(d * rows, rows), rows)
        starts = ((gu_ref, core * half), (gu_ref, 2 * half + core * half), (down_ref, core * half))
        return [ref.at[at, pl.ds(pl.multiple_of(start, 128), half)] for ref, start in starts]

    def beside(r):
        d = (me.dp + r) % 16
        return [
            me.copy(src, held.at[j, r], core_send.at[r, j], core_recv.at[r, j], me.dp, 1 - me.core)
            for j, src in enumerate(views(d, 1 - me.core))
        ]

    def loads(r):
        d = (me.dp + r) % 16
        return [pltpu.make_async_copy(src, own.at[j, r], copy_sem.at[r, j]) for j, src in enumerate(views(d, me.core))]

    def sends(r):
        d = (me.dp + r) % 16
        return [me.copy(held.at[j, r], outs[j].at[me.dp], send_sem.at[r, j], recv_sem.at[r, j], d) for j in range(3)]

    order = (8, 7, 9, 4, 12, 5, 11, 6, 10, 3, 13, 2, 14, 1, 15, 0)
    for r in order:
        for c in beside(r) + loads(r):
            c.start()
    yield
    keep = [pltpu.make_async_copy(held.at[j, 0], outs[j].at[me.dp], copy_sem.at[16, j]) for j in range(3)]
    for n, r in enumerate(order):
        for j, (arrives, load) in enumerate(zip(beside(r), loads(r))):
            arrives.wait_recv()
            load.wait()
            add_rows(held.at[j, r], (own.at[j, r], held.at[j, r]), rows, 64)
        for c in sends(r) if r else keep:
            c.start()
        if n % 2:
            yield
    for r in range(1, 16):
        s = (me.dp + 16 - r) % 16
        for j in range(3):
            dst = outs[j].at[s]
            me.copy(dst, dst, send_sem.at[r, j], recv_sem.at[r, j], me.dp).wait_recv()
    for c in keep:
        c.wait()
    for r in range(16):
        for c in beside(r) + (sends(r) if r else []):
            c.wait_send()


def scatter_last_kernel(
    chunks, p_ref, x_ref, gu_ref, down_ref, out_ref, sum_ref, gate_out, up_out, down_out,
    from_b, from_a, from_far, total, own, held, send_sem, recv_sem, sum_send, sum_recv, core_send, core_recv, e_send, e_recv, copy_sem,
):
    me = Place()
    me.greet(everyone=True, partner=True)
    run(
        return_experts(me, gu_ref, down_ref, (gate_out, up_out, down_out), own, held, core_send, core_recv, e_send, e_recv, copy_sem),
        scatter_pairs(me, chunks, p_ref, out_ref, from_b, from_a, from_far, send_sem, recv_sem),
        sum_all(me, x_ref, sum_ref, total, sum_send, sum_recv),
    )


def scatter_last(p, x, gu, down, cid, chunks=2):
    _, rows, columns = p.shape
    half = down.shape[1] // 2
    hbm, vmem = pl.BlockSpec(memory_space=pl.ANY), pl.BlockSpec(memory_space=pltpu.VMEM)
    dma = pltpu.SemaphoreType.DMA
    return pl.pallas_call(
        functools.partial(scatter_last_kernel, chunks),
        out_shape=[jax.ShapeDtypeStruct((2, rows, columns), p.dtype), jax.ShapeDtypeStruct(x.shape, x.dtype)]
        + [jax.ShapeDtypeStruct((16, rows, half), p.dtype)] * 3,
        in_specs=[vmem, vmem, hbm, hbm],
        out_specs=[vmem, vmem, hbm, hbm, hbm],
        scratch_shapes=[
            pltpu.VMEM((2, 4, rows, columns), p.dtype),
            pltpu.VMEM((4, rows, columns), p.dtype),
            pltpu.VMEM((2, rows, columns), p.dtype),
            pltpu.VMEM((2, 5) + x.shape, x.dtype),
            pltpu.VMEM((3, 16, rows, half), p.dtype),
            pltpu.VMEM((3, 16, rows, half), p.dtype),
            dma((15, chunks)), dma((15, chunks)),
            dma((5,)), dma((5,)),
            dma((16, 3)), dma((16, 3)),
            dma((16, 3)), dma((16, 3)),
            dma((17, 3)),
        ],
        compiler_params=pltpu.CompilerParams(collective_id=cid, has_side_effects=True, vmem_limit_bytes=LIMIT),
        name="scatter_last",
    )(p, x, gu, down)


def experts_kernel(
    x_ref, c_ref, g_ref, gate_ref, up_ref, down_ref,
    moe_ref, two_ref, gu_out, down_out, xg_ref,
    wgu, wd, ag, ggu, p, from_b, from_a, from_z, xb, cb,
    g_send, g_recv, b_send, b_recv, a_send, a_recv, z_send, z_recv, w_send, w_recv, load_sem, tile_sem, keep_sem,
):
    me = Place()
    rows, width = x_ref.shape
    hidden = wd.shape[0]
    half = hidden // 2
    low = me.z < 2
    depth = jnp.where(low, me.z, 3 - me.z)
    away = jnp.where(low, 1, 0)
    dot = functools.partial(jnp.dot, preferred_element_type=jnp.float32)
    dot_t = functools.partial(lax.dot_general, dimension_numbers=(((1,), (1,)), ((), ())), preferred_element_type=jnp.float32)
    t_dot = functools.partial(lax.dot_general, dimension_numbers=(((0,), (0,)), ((), ())), preferred_element_type=jnp.float32)
    upper, lower = pl.ds(rows, rows), pl.ds(0, rows)

    def z_of(m):
        t = jnp.where(m == 0, 1 - depth, jnp.where(m == 1, 2, jnp.where(m == 2, 3, depth)))
        return jnp.where(low, t, 3 - t)

    def block(n):
        return me.at_z(z_of(n // 2)) + (n % 2) * me.da

    def part(source, to, slot, own=False):
        return me.copy(x_ref if own else xg_ref.at[source], xg_ref.at[source], g_send.at[slot], g_recv.at[source], to)

    def onward(m):
        below = z_of(m) < me.z
        return jnp.logical_or(jnp.logical_and(below, me.z < 3), jnp.logical_and(jnp.logical_not(below), me.z > 0)), jnp.where(below, 4, -4)

    def arrive(m):
        source = me.at_z(z_of(m))
        part(source, me.dp, 0).wait_recv()
        goes, step = onward(m)
        pl.when(goes)(lambda: part(source, me.dp + step, 4 + 3 * m).start())
        part(source, me.dp + me.db, 6 + 3 * m).start()
        part(source, me.dp + me.da, 5 + 3 * m).start()

    def arrive_a(m):
        source = me.at_z(z_of(m)) + me.da
        part(source, me.dp, 0).wait_recv()
        part(source, me.dp + me.db, 13 + m).start()

    def loads(n):
        slot = n % 2
        copies = []
        for j, source in enumerate((block(n), block(n) + me.db)):
            at = pl.ds(j * rows, rows)
            copies.append(pltpu.make_async_copy(xg_ref.at[source], xb.at[slot, at], load_sem.at[slot, j]))
            copies.append(pltpu.make_async_copy(c_ref.at[source], cb.at[slot, at], load_sem.at[slot, 2 + j]))
        return copies

    def fetch(n):
        part(block(n) + me.db, me.dp, 0).wait_recv()
        for c in loads(n):
            c.start()

    def send_b(i, n):
        return me.copy(p.at[i, n, upper], from_b.at[i, n], b_send.at[i, n], b_recv.at[i, n], me.dp + me.db)

    def send_a(i, m):
        return me.copy(from_b.at[i, 2 * m + 1], from_a.at[i, m], a_send.at[i, m], a_recv.at[i, m], me.dp + me.da)

    def slot_z(z, up, at):
        return jnp.where(up == 1, z, jnp.where(z == at, 4, z))

    def send_z(i, m, up):
        z = z_of(m)
        slot = slot_z(z, up, me.z - 1)
        return me.copy(from_b.at[i, 2 * m], from_z.at[i, slot], z_send.at[i, m], z_recv.at[i, slot], me.dp - 4 + 8 * up)

    def wait_z(i, z, up):
        slot = slot_z(z, up, me.z)
        me.copy(from_z.at[i, slot], from_z.at[i, slot], z_send.at[i, 0], z_recv.at[i, slot], me.dp).wait_recv()
        return from_z.at[i, slot]

    def first(m):
        for i in range(2):
            n = 2 * m + 1
            send_b(i, n).wait_recv()
            add_rows(from_b.at[i, n], (p.at[i, n, lower], from_b.at[i, n]), rows)
            send_a(i, m).start()

    def second(m):
        for i in range(2):
            n = 2 * m
            send_b(i, n).wait_recv()
            send_a(i, m).wait_recv()
            terms = (p.at[i, n, lower], from_b.at[i, n], from_a.at[i, m])
            if m in (1, 2):
                pl.when(depth == 0)(lambda: add_rows(from_b.at[i, n], terms, rows))
                pl.when(depth == 1)(lambda: add_rows(from_b.at[i, n], terms + (wait_z(i, z_of(m), away),), rows))
                send_z(i, m, away).start()
            else:
                add_rows(from_b.at[i, n], terms, rows)
                if m == 0:
                    pl.when(depth == 0)(lambda: send_z(i, 0, away).start())

    own = p.at[1, 7, lower]
    load = pltpu.make_async_copy(x_ref, own, keep_sem.at[0])
    store = pltpu.make_async_copy(own, xg_ref.at[me.dp], keep_sem.at[1])
    load.start()

    def half_of(core):
        at = core * half
        return (
            wgu.at[:, pl.ds(pl.multiple_of(at, 128), half)],
            wgu.at[:, pl.ds(pl.multiple_of(hidden + at, 128), half)],
            wd.at[pl.ds(pl.multiple_of(at, 128), half)],
        )

    mine = (gate_ref, up_ref, down_ref)
    locals_ = [pltpu.make_async_copy(src, dst, keep_sem.at[2 + j]) for j, (src, dst) in enumerate(zip(mine, half_of(me.core)))]
    for c in locals_:
        c.start()
    me.greet(line=True, near=True, partner=True)
    pl.when(me.z < 3)(lambda: part(me.dp, me.dp + 4, 0, True).start())
    pl.when(me.z > 0)(lambda: part(me.dp, me.dp - 4, 1, True).start())
    part(me.dp, me.dp + me.db, 3, True).start()
    part(me.dp, me.dp + me.da, 2, True).start()
    shares = [
        me.copy(src, dst, w_send.at[j], w_recv.at[j], me.dp, 1 - me.core) for j, (src, dst) in enumerate(zip(mine, half_of(me.core)))
    ]
    for c in shares:
        c.start()
    load.wait()
    store.start()
    arrive_a(3)
    arrive(0)
    store.wait()
    for c in locals_:
        c.wait()
    for j, dst in enumerate(half_of(1 - me.core)):
        me.copy(dst, dst, w_send.at[j], w_recv.at[j], me.dp).wait_recv()
    fetch(0)

    tile = 256

    def step(n, _):
        slot = n % 2
        for c in loads(n):
            c.wait()
        gates = jnp.concatenate([g_ref[block(n)], g_ref[block(n) + me.db]], axis=0)

        def inner(j, _):
            at, at_up = pl.ds(pl.multiple_of(j * tile, tile), tile), pl.ds(pl.multiple_of(hidden + j * tile, tile), tile)
            gate, up, grad = dot(xb[slot], wgu[:, at]), dot(xb[slot], wgu[:, at_up]), dot_t(cb[slot], wd[at, :]) * gates
            sig = 1.0 / (1.0 + jnp.exp(-gate))
            act = gate * sig
            ag[n, :, at] = (act * up * gates).astype(ag.dtype)
            ggu[n, :, at] = (grad * up * sig * (1.0 + gate * (1.0 - sig))).astype(ggu.dtype)
            ggu[n, :, at_up] = (grad * act).astype(ggu.dtype)
            return 0

        lax.fori_loop(0, hidden // tile, inner, 0)

        def at_step(k, *calls):
            def go():
                for call, m in calls:
                    call(m)

            pl.when(n == k)(go)

        at_step(0, (arrive, 1), (arrive_a, 0))
        at_step(1, (arrive, 2))
        at_step(2, (arrive_a, 1))
        at_step(3, (arrive_a, 2))
        pl.when(n < 7)(lambda: fetch(n + 1))

        def outer(j, _):
            at = pl.ds(pl.multiple_of(j * 2 * tile, 2 * tile), 2 * tile)
            p[0, n, :, at] = dot(ag[n], wd[:, at]).astype(p.dtype)
            p[1, n, :, at] = dot_t(ggu[n], wgu[at, :]).astype(p.dtype)
            return 0

        lax.fori_loop(0, width // (2 * tile), outer, 0)
        send_b(0, n).start()
        send_b(1, n).start()
        at_step(4, (first, 0))
        at_step(6, (second, 0))
        at_step(7, (first, 1))
        return 0

    lax.fori_loop(0, 8, step, 0)

    def tiles(i):
        slot = i % 2
        cols = pl.ds(pl.multiple_of(i * tile, tile), tile)
        copies = []
        for which, src in enumerate((xg_ref, c_ref)):
            to = pl.ds(pl.multiple_of((2 * which + slot) * tile, tile), tile)

            def one(n, side, which=which, src=src, to=to):
                at = pl.ds(pl.multiple_of((2 * n + side) * rows, rows), rows)
                return pltpu.make_async_copy(src.at[block(n) + side * me.db, :, cols], wgu.at[at, to], tile_sem.at[which, slot, 2 * n + side])

            copies.append(one)
        return copies

    def each_tile(i, act):
        for one in tiles(i):

            def body(n, _):
                for side in (0, 1):
                    act(one(n, side))
                return 0

            lax.fori_loop(0, 8, body, 0)

    def outs(i):
        slot = i % 2
        at = pl.ds(pl.multiple_of(i * tile, tile), tile)
        return (
            pltpu.make_async_copy(xb.at[slot, :, pl.ds(0, 2 * hidden)], gu_out.at[at], load_sem.at[slot, 0]),
            pltpu.make_async_copy(cb.at[slot, :, pl.ds(0, hidden)], down_out.at[at], load_sem.at[slot, 1]),
        )

    each_tile(0, lambda c: c.start())

    def weight_step(i, _):
        slot = i % 2
        pl.when(i < 7)(lambda: each_tile(i + 1, lambda c: c.start()))
        each_tile(i, lambda c: c.wait())

        def free():
            for c in outs(i - 2):
                c.wait()

        pl.when(i >= 2)(free)
        x_tile = wgu[:, pl.ds(pl.multiple_of(slot * tile, tile), tile)]
        xb[slot, :, pl.ds(0, 2 * hidden)] = t_dot(x_tile, ggu[...].reshape(-1, 2 * hidden)).astype(xb.dtype)
        c_tile = wgu[:, pl.ds(pl.multiple_of((2 + slot) * tile, tile), tile)]
        cb[slot, :, pl.ds(0, hidden)] = t_dot(c_tile, ag[...].reshape(-1, hidden)).astype(cb.dtype)
        for c in outs(i):
            c.start()
        pl.when(i == 1)(lambda: second(1))
        pl.when(i == 2)(lambda: first(2))
        pl.when(i == 4)(lambda: second(2))
        pl.when(i == 5)(lambda: first(3))
        return 0

    lax.fori_loop(0, 8, weight_step, 0)
    second(3)

    def pass_back():
        for i in range(2):
            add_rows(from_b.at[i, 0], (from_b.at[i, 0], wait_z(i, z_of(0), 1 - away)), rows)
            send_z(i, 0, 1 - away).start()

    pl.when(depth == 1)(pass_back)
    for i, out_ref in enumerate((moe_ref, two_ref)):
        here = from_b.at[i, 6]
        pl.when(me.z == 0)(lambda: add_rows(out_ref, (here, wait_z(i, me.z, 0)), rows))
        pl.when(me.z == 3)(lambda: add_rows(out_ref, (here, wait_z(i, me.z, 1)), rows))
        pl.when(depth == 1)(lambda: add_rows(out_ref, (here, wait_z(i, me.z, 0), wait_z(i, me.z, 1)), rows))

    for i in (6, 7):
        for c in outs(i):
            c.wait()
    for c in shares:
        c.wait_send()
    pl.when(me.z < 3)(lambda: part(me.dp, me.dp, 0).wait_send())
    pl.when(me.z > 0)(lambda: part(me.dp, me.dp, 1).wait_send())
    part(me.dp, me.dp, 2).wait_send()
    part(me.dp, me.dp, 3).wait_send()
    for m in range(4):
        if m < 3:
            pl.when(onward(m)[0])(lambda: part(me.dp, me.dp, 4 + 3 * m).wait_send())
            part(me.dp, me.dp, 5 + 3 * m).wait_send()
            part(me.dp, me.dp, 6 + 3 * m).wait_send()
        part(me.dp, me.dp, 13 + m).wait_send()
        for i in range(2):
            send_b(i, 2 * m).wait_send()
            send_b(i, 2 * m + 1).wait_send()
            send_a(i, m).wait_send()
            if m < 3:
                send_z(i, m, away).wait_send()


def expert_layer(x, grads, gates, gate, up, down, cid):
    rows, width = x.shape
    half = gate.shape[1]
    hbm, vmem = pl.BlockSpec(memory_space=pl.ANY), pl.BlockSpec(memory_space=pltpu.VMEM)
    dma = pltpu.SemaphoreType.DMA
    dtype = x.dtype
    return pl.pallas_call(
        experts_kernel,
        out_shape=[
            jax.ShapeDtypeStruct((rows, width), jnp.float32),
            jax.ShapeDtypeStruct((rows, width), jnp.float32),
            jax.ShapeDtypeStruct((width, 4 * half), dtype),
            jax.ShapeDtypeStruct((width, 2 * half), dtype),
            jax.ShapeDtypeStruct((16, rows, width), dtype),
        ],
        in_specs=[hbm, hbm, vmem, hbm, hbm, hbm],
        out_specs=[vmem, vmem, hbm, hbm, hbm],
        scratch_shapes=[
            pltpu.VMEM((width, 4 * half), dtype),
            pltpu.VMEM((2 * half, width), dtype),
            pltpu.VMEM((8, 2 * rows, 2 * half), dtype),
            pltpu.VMEM((8, 2 * rows, 4 * half), dtype),
            pltpu.VMEM((2, 8, 2 * rows, width), dtype),
            pltpu.VMEM((2, 8, rows, width), dtype),
            pltpu.VMEM((2, 4, rows, width), dtype),
            pltpu.VMEM((2, 5, rows, width), dtype),
            pltpu.VMEM((2, 2 * rows, width), dtype),
            pltpu.VMEM((2, 2 * rows, width), dtype),
            dma((17,)), dma((16,)),
            dma((2, 8)), dma((2, 8)),
            dma((2, 4)), dma((2, 4)),
            dma((2, 4)), dma((2, 5)),
            dma((3,)), dma((3,)),
            dma((2, 4)), dma((2, 2, 16)), dma((5,)),
        ],
        compiler_params=pltpu.CompilerParams(collective_id=cid, has_side_effects=True, vmem_limit_bytes=67_043_328),
        name="experts",
    )(x, grads, gates, gate, up, down)


def per_device_any(
    tokens,
    cotangent,
    expert_ids,
    gate_values,
    w_query,
    w_key,
    w_value,
    w_out,
    w_gate,
    w_up,
    w_down,
    attn_gain,
    ffn_gain,
    query_gain,
    key_gain,
):
    contract = (((1,), (1,)), ((), ()))
    contract_rows = (((0,), (0,)), ((), ()))
    residual = tokens.astype(jnp.float32)
    model_width = residual.shape[1]
    inverse_one = rms_inverse(residual)
    seq_normed = gather_rows((residual * inverse_one * attn_gain).astype(jnp.bfloat16))
    full_query, full_key, full_value, full_out = (
        lax.all_gather(w_query, "dp", axis=0, tiled=True),
        lax.all_gather(w_key, "dp", axis=0, tiled=True),
        lax.all_gather(w_value, "dp", axis=0, tiled=True),
        lax.all_gather(w_out, "dp", axis=1, tiled=True),
    )
    seq_len = seq_normed.shape[0]
    head_dim = query_gain.shape[0]
    local_heads = full_query.shape[1] // head_dim
    local_kv = full_key.shape[1] // head_dim
    group_size = local_heads // local_kv
    attn_scale = head_dim ** (-0.5)
    cosine, sine_table = rotary_tables(seq_len, head_dim)
    query_raw = jnp.dot(seq_normed, full_query, preferred_element_type=jnp.float32).reshape(
        seq_len, local_heads, head_dim
    )
    key_raw = jnp.dot(seq_normed, full_key, preferred_element_type=jnp.float32).reshape(
        seq_len, local_kv, head_dim
    )
    value_low = (
        jnp.dot(seq_normed, full_value, preferred_element_type=jnp.float32)
        .astype(jnp.bfloat16)
        .reshape(seq_len, local_kv, head_dim)
    )
    query_inverse = rms_inverse(query_raw)
    key_inverse = rms_inverse(key_raw)
    query_low = (
        rotate(query_raw * query_inverse * query_gain, cosine, sine_table) * attn_scale
    ).astype(jnp.bfloat16)
    key_low = rotate(key_raw * key_inverse * key_gain, cosine, sine_table).astype(jnp.bfloat16)
    query_heads = query_low.reshape(seq_len, local_kv, group_size, head_dim).transpose(1, 0, 2, 3)
    key_heads = key_low.transpose(1, 0, 2)
    value_heads = value_low.transpose(1, 0, 2)
    mixed_heads, logsum = lax.map(head_forward, (query_heads, key_heads, value_heads))
    mixed_flat = mixed_heads.transpose(1, 0, 2, 3).reshape(seq_len, local_heads * head_dim)
    hidden = residual + scatter_rows(
        jnp.dot(mixed_flat, full_out, preferred_element_type=jnp.float32)
    )
    inverse_two = rms_inverse(hidden)
    seq_two = gather_rows((hidden * inverse_two * ffn_gain).astype(jnp.bfloat16))
    seq_grad = gather_rows(cotangent)
    experts = w_gate.shape[0]
    dp_rows = w_gate.shape[1]
    hidden_units = w_gate.shape[2]
    dp_count = lax.axis_size("dp")
    group = dp_count // experts
    routed_rows = seq_len * expert_ids.shape[1] * 9 // 8
    capacity = (routed_rows + experts * group - 1) // (experts * group) * group
    slot_table, gate_table = dispatch(expert_ids, gate_values, experts, capacity)
    blank_row = jnp.zeros((1, model_width), jnp.bfloat16)
    padded_in = jnp.concatenate([seq_two, blank_row], axis=0)
    padded_grad = jnp.concatenate([seq_grad, blank_row], axis=0)
    empty_rows = jnp.zeros((seq_len + 1, model_width), jnp.float32)
    piece_rows = capacity // group
    down_rows = jnp.transpose(w_down, (0, 2, 1))
    gate_mine, up_mine, down_mine = (
        lax.all_to_all(widen(w_gate, group), "dp", split_axis=0, concat_axis=1, tiled=True),
        lax.all_to_all(widen(w_up, group), "dp", split_axis=0, concat_axis=1, tiled=True),
        lax.all_to_all(widen(down_rows, group), "dp", split_axis=0, concat_axis=1, tiled=True),
    )
    gate_mine = gate_mine[0]
    up_mine = up_mine[0]
    down_mine = down_mine[0]
    blocks_in = padded_in[slot_table]
    grad_blocks = (padded_grad[slot_table].astype(jnp.float32) * gate_table[:, :, None]).astype(
        jnp.bfloat16
    )
    recv_in, recv_grad = (
        lax.all_to_all(
            blocks_in.reshape(dp_count, piece_rows, model_width),
            "dp",
            split_axis=0,
            concat_axis=0,
            tiled=True,
        ),
        lax.all_to_all(
            grad_blocks.reshape(dp_count, piece_rows, model_width),
            "dp",
            split_axis=0,
            concat_axis=0,
            tiled=True,
        ),
    )
    rows_in = recv_in.reshape(-1, model_width)
    rows_grad = recv_grad.reshape(-1, model_width)
    gate_pre = jnp.dot(rows_in, gate_mine, preferred_element_type=jnp.float32)
    up_pre = jnp.dot(rows_in, up_mine, preferred_element_type=jnp.float32)
    act_low = (jax.nn.silu(gate_pre) * up_pre).astype(jnp.bfloat16)
    expert_out = lax.dot_general(act_low, down_mine, contract, preferred_element_type=jnp.float32)
    grad_act = jnp.dot(rows_grad, down_mine, preferred_element_type=jnp.float32)
    sigmoid_gate = jax.nn.sigmoid(gate_pre)
    grad_gate = (grad_act * up_pre * sigmoid_gate * (1.0 + gate_pre * (1.0 - sigmoid_gate))).astype(
        jnp.bfloat16
    )
    grad_up = (grad_act * gate_pre * sigmoid_gate).astype(jnp.bfloat16)
    grad_input = lax.dot_general(
        grad_gate, gate_mine, contract, preferred_element_type=jnp.float32
    ) + lax.dot_general(grad_up, up_mine, contract, preferred_element_type=jnp.float32)
    back_out, back_grad = (
        lax.all_to_all(
            expert_out.reshape(dp_count, piece_rows, model_width).astype(jnp.bfloat16),
            "dp",
            split_axis=0,
            concat_axis=0,
            tiled=True,
        ).astype(jnp.float32),
        lax.all_to_all(
            grad_input.reshape(dp_count, piece_rows, model_width).astype(jnp.bfloat16),
            "dp",
            split_axis=0,
            concat_axis=0,
            tiled=True,
        ).astype(jnp.float32),
    )
    back_out = back_out.reshape(experts, capacity, model_width)
    back_grad = back_grad.reshape(experts * capacity, model_width)
    flat_slots = slot_table.reshape(-1)
    combined = empty_rows.at[flat_slots].add(
        (back_out * gate_table[:, :, None]).reshape(-1, model_width)
    )
    grad_acc = empty_rows.at[flat_slots].add(back_grad)
    grad_both = jnp.concatenate([grad_gate, grad_up], axis=1)
    grad_cols = jnp.concatenate(
        [
            lax.dot_general(rows_in, grad_both, contract_rows, preferred_element_type=jnp.float32),
            lax.dot_general(rows_grad, act_low, contract_rows, preferred_element_type=jnp.float32),
        ],
        axis=1,
    )
    returned = lax.all_to_all(
        grad_cols[None].astype(jnp.bfloat16), "dp", split_axis=1, concat_axis=0, tiled=True
    ).astype(jnp.float32)
    summed = jnp.sum(returned.reshape(experts, group, dp_rows, 3 * hidden_units), axis=1)
    grad_w_gate = summed[:, :, :hidden_units]
    grad_w_up = summed[:, :, hidden_units : 2 * hidden_units]
    grad_w_down = jnp.transpose(summed[:, :, 2 * hidden_units :], (0, 2, 1))
    output = (hidden + scatter_rows(combined[:seq_len])).astype(jnp.bfloat16)
    grad_two = scatter_rows(grad_acc[:seq_len])
    ffn_gain_part = jnp.sum(grad_two * hidden * inverse_two, axis=0)
    grad_hidden = cotangent.astype(jnp.float32) + norm_backward(
        grad_two, hidden, inverse_two, ffn_gain
    )
    grad_attn = gather_rows(grad_hidden.astype(jnp.bfloat16))
    grad_mixed = lax.dot_general(
        grad_attn, full_out, contract, preferred_element_type=jnp.float32
    ).astype(jnp.bfloat16)
    grad_mixed_heads = grad_mixed.reshape(seq_len, local_kv, group_size, head_dim).transpose(
        1, 0, 2, 3
    )
    grad_query_heads, grad_key_heads, grad_value_heads = lax.map(
        head_backward, (query_heads, key_heads, value_heads, logsum, grad_mixed_heads)
    )
    grad_query_rot = (
        grad_query_heads.transpose(1, 0, 2, 3).reshape(seq_len, local_heads, head_dim) * attn_scale
    )
    grad_query_norm = rotate_back(grad_query_rot, cosine, sine_table)
    query_gain_part = jnp.sum(grad_query_norm * query_raw * query_inverse, axis=(0, 1))
    grad_query_low = (
        norm_backward(grad_query_norm, query_raw, query_inverse, query_gain)
        .astype(jnp.bfloat16)
        .reshape(seq_len, local_heads * head_dim)
    )
    grad_key_norm = rotate_back(grad_key_heads.transpose(1, 0, 2), cosine, sine_table)
    key_gain_part = jnp.sum(grad_key_norm * key_raw * key_inverse, axis=(0, 1))
    grad_key_low = (
        norm_backward(grad_key_norm, key_raw, key_inverse, key_gain)
        .astype(jnp.bfloat16)
        .reshape(seq_len, local_kv * head_dim)
    )
    grad_value_low = (
        grad_value_heads.transpose(1, 0, 2)
        .reshape(seq_len, local_kv * head_dim)
        .astype(jnp.bfloat16)
    )
    grad_proj = jnp.concatenate([grad_query_low, grad_key_low, grad_value_low], axis=1)
    full_proj = jnp.concatenate([full_query, full_key, full_value], axis=1)
    grad_one = scatter_rows(
        lax.dot_general(grad_proj, full_proj, contract, preferred_element_type=jnp.float32)
    )
    first_part = jnp.einsum("sd,sf->df", seq_normed, grad_proj, preferred_element_type=jnp.float32)
    second = jnp.einsum("sd,sf->df", grad_attn, mixed_flat, preferred_element_type=jnp.float32)
    shares = lax.psum_scatter(
        jnp.concatenate([first_part, second], axis=1), "dp", scatter_dimension=0, tiled=True
    )
    query_cols = w_query.shape[1]
    key_cols = w_key.shape[1]
    grad_w_query = shares[:, :query_cols]
    grad_w_key = shares[:, query_cols : query_cols + key_cols]
    grad_w_value = shares[:, query_cols + key_cols : query_cols + 2 * key_cols]
    grad_w_out = jnp.transpose(shares[:, query_cols + 2 * key_cols :])
    attn_gain_part = jnp.sum(grad_one * residual * inverse_one, axis=0)
    grad_tokens = (grad_hidden + norm_backward(grad_one, residual, inverse_one, attn_gain)).astype(
        jnp.bfloat16
    )
    total_gains = lax.psum(
        (attn_gain_part, ffn_gain_part, query_gain_part, key_gain_part), ("dp", "tensor")
    )
    return (
        output,
        grad_tokens,
        grad_w_query,
        grad_w_key,
        grad_w_value,
        grad_w_out,
        grad_w_gate,
        grad_w_up,
        grad_w_down,
        total_gains[0],
        total_gains[1],
        total_gains[2],
        total_gains[3],
    )


def per_device_relay(
    tokens,
    cotangent,
    expert_ids,
    gate_values,
    w_query,
    w_key,
    w_value,
    w_out,
    w_gate,
    w_up,
    w_down,
    attn_gain,
    ffn_gain,
    query_gain,
    key_gain,
):
    dot = functools.partial(jnp.dot, preferred_element_type=jnp.float32)
    dot_t = functools.partial(lax.dot_general, dimension_numbers=(((1,), (1,)), ((), ())), preferred_element_type=jnp.float32)
    t_dot = functools.partial(lax.dot_general, dimension_numbers=(((0,), (0,)), ((), ())), preferred_element_type=jnp.float32)
    low = jnp.bfloat16
    rows, width = tokens.shape
    head_dim = query_gain.shape[0]
    experts = w_gate.shape[0]
    core = lax.axis_index("tensor")
    mine = lax.dynamic_slice_in_dim(expert_ids, core * rows, rows, 0)
    values = lax.dynamic_slice_in_dim(gate_values, core * rows, rows, 0)
    match = mine[None] == jnp.arange(experts, dtype=jnp.int32)[:, None, None]
    gates = jnp.sum(jnp.where(match, values[None], 0.0), axis=2)
    gates = jnp.broadcast_to(gates[:, None], (experts, 8, rows))

    q_cols, kv_cols = w_query.shape[1] // 2, w_key.shape[1] // 2
    w_out_rows = jnp.transpose(w_out)
    halves = jnp.stack(
        [
            jnp.concatenate([w[:, h * (w.shape[1] // 2) : (h + 1) * (w.shape[1] // 2)] for w in (w_query, w_key, w_value, w_out_rows)], axis=1)
            for h in range(2)
        ]
    )
    residual = tokens.astype(jnp.float32)
    inverse_one = rms_inverse(residual)
    normed_one = (residual * inverse_one * attn_gain).astype(low)
    weights, rows_grad, gates, seq_normed, *projections = gather_first(halves, cotangent, gates, normed_one, (w_gate, w_up, w_down), 1)
    weights, gates, seq_normed = weights.reshape(-1, weights.shape[2]), gates[:, 0][:, :, None], seq_normed.reshape(-1, width)
    proj_cols = q_cols + 2 * kv_cols
    w_proj, w_back = weights[:, :proj_cols], weights[:, proj_cols:]

    seq_len = 2 * rows
    group = q_cols // head_dim
    scale = head_dim ** (-0.5)
    cosine, sine_table = rotary_tables(seq_len, head_dim)
    proj = dot(seq_normed, w_proj)
    query_raw = proj[:, :q_cols].reshape(2, seq_len, group, head_dim)
    key_raw = proj[:, q_cols : q_cols + kv_cols].reshape(2, seq_len, 1, head_dim)
    value_low = proj[:, q_cols + kv_cols :].astype(low).reshape(2, seq_len, head_dim)
    query_inverse, key_inverse = rms_inverse(query_raw), rms_inverse(key_raw)
    query_low = (rotate(query_raw * query_inverse * query_gain, cosine, sine_table) * scale).astype(low)
    key_low = rotate(key_raw * key_inverse * key_gain, cosine, sine_table).astype(low)[:, :, 0]
    causal = jnp.arange(seq_len)[:, None] >= jnp.arange(seq_len)[None, :]
    scores = jnp.einsum("bqgd,bsd->bgqs", query_low, key_low, preferred_element_type=jnp.float32)
    exp_scores = jnp.where(causal, jnp.exp(scores), 0.0)
    probs = exp_scores / jnp.sum(exp_scores, axis=-1, keepdims=True)
    probs_low = probs.astype(low)
    mixed = jnp.einsum("bgqs,bsd->bqgd", probs_low, value_low, preferred_element_type=jnp.float32).astype(low).reshape(2 * seq_len, q_cols)
    hidden = residual + scatter_four(dot_t(mixed, w_back).astype(low).reshape(2, 2, rows, width), 5)
    inverse_two = rms_inverse(hidden)
    normed_two = (hidden * inverse_two * ffn_gain).astype(low)
    moe, grad_two, gu_part, down_part, _ = expert_layer(normed_two, rows_grad, gates, *projections, 2)
    output = (hidden + moe).astype(low)
    ffn_gain_part = jnp.sum(grad_two * hidden * inverse_two, axis=0)
    grad_hidden = cotangent.astype(jnp.float32) + norm_backward(grad_two, hidden, inverse_two, ffn_gain)
    grad_attn = gather_pair_rows(grad_hidden.astype(low), 9).reshape(-1, width)
    grad_mixed = dot(grad_attn, w_back).astype(low).reshape(2, seq_len, group, head_dim)
    grad_probs = jnp.einsum("bqgd,bsd->bgqs", grad_mixed, value_low, preferred_element_type=jnp.float32)
    delta_sum = jnp.sum(grad_probs * probs, axis=-1, keepdims=True)
    grad_scores = (probs * (grad_probs - delta_sum)).astype(low)
    grad_query = jnp.einsum("bgqs,bsd->bqgd", grad_scores, key_low, preferred_element_type=jnp.float32)
    grad_key = jnp.einsum("bgqs,bqgd->bsd", grad_scores, query_low, preferred_element_type=jnp.float32)
    grad_value = jnp.einsum("bgqs,bqgd->bsd", probs_low, grad_mixed, preferred_element_type=jnp.float32)
    grad_query_norm = rotate_back(grad_query * scale, cosine, sine_table)
    query_gain_part = jnp.sum(grad_query_norm * query_raw * query_inverse, axis=(0, 1, 2))
    grad_query_low = norm_backward(grad_query_norm, query_raw, query_inverse, query_gain).astype(low)
    grad_key_norm = rotate_back(grad_key[:, :, None], cosine, sine_table)
    key_gain_part = jnp.sum(grad_key_norm * key_raw * key_inverse, axis=(0, 1, 2))
    grad_key_low = norm_backward(grad_key_norm, key_raw, key_inverse, key_gain).astype(low)
    grad_proj = jnp.concatenate([v.astype(low).reshape(2 * seq_len, -1) for v in (grad_query_low, grad_key_low, grad_value)], axis=1)
    grad_one = scatter_four(dot_t(grad_proj, w_proj).astype(low).reshape(2, 2, rows, width), 10)
    w_parts = jnp.concatenate([t_dot(seq_normed, grad_proj), t_dot(grad_attn, mixed)], axis=1).astype(low)
    attn_gain_part = jnp.sum(grad_one * residual * inverse_one, axis=0)
    gains = jnp.concatenate([attn_gain_part, ffn_gain_part, query_gain_part, key_gain_part])
    gains = jnp.pad(gains, (0, -gains.shape[0] % 1024)).reshape(-1, 128)
    shares, totals, *grads_moe = scatter_last(w_parts.reshape(-1, rows, w_parts.shape[1]), gains, gu_part, down_part, 11)
    grad_w_gate, grad_w_up, grad_w_down = [v.astype(jnp.float32) for v in grads_moe]
    grad_w_down = jnp.transpose(grad_w_down, (0, 2, 1))
    shares, totals = shares.astype(jnp.float32), totals.reshape(-1)
    stops = (0, q_cols, q_cols + kv_cols, proj_cols, proj_cols + q_cols)
    grads = [jnp.concatenate([shares[0, :, a:b], shares[1, :, a:b]], axis=1) for a, b in zip(stops, stops[1:])]
    grad_tokens = (grad_hidden + norm_backward(grad_one, residual, inverse_one, attn_gain)).astype(low)
    totals = jnp.split(totals, (width, 2 * width, 2 * width + head_dim, 2 * width + 2 * head_dim))[:4]
    return (output, grad_tokens, grads[0], grads[1], grads[2], jnp.transpose(grads[3]), grad_w_gate, grad_w_up, grad_w_down, *totals)


def solution(mesh):
    return jax.shard_map(
        per_device_relay if tuple(mesh.shape.values()) == (16, 2) else per_device_any,
        mesh=mesh,
        in_specs=(
            P(("dp", "tensor"), None),
            P(("dp", "tensor"), None),
            P("dp", None),
            P("dp", None),
            P("dp", "tensor"),
            P("dp", "tensor"),
            P("dp", "tensor"),
            P("tensor", "dp"),
            P(None, "dp", "tensor"),
            P(None, "dp", "tensor"),
            P(None, "tensor", "dp"),
            P(),
            P(),
            P(),
            P(),
        ),
        out_specs=(
            P(("dp", "tensor"), None),
            P(("dp", "tensor"), None),
            P("dp", "tensor"),
            P("dp", "tensor"),
            P("dp", "tensor"),
            P("tensor", "dp"),
            P(None, "dp", "tensor"),
            P(None, "dp", "tensor"),
            P(None, "tensor", "dp"),
            P(),
            P(),
            P(),
            P(),
        ),
        check_vma=False,
    )
```

```python
import functools

import jax
import jax.numpy as jnp
from jax import lax
from jax.experimental import pallas as pl
from jax.experimental.pallas import tpu as pltpu
from jax.sharding import PartitionSpec as P

epsilon = 1e-06
theta_base = 1000000.0


def rms_inverse(values):
    return lax.rsqrt(jnp.mean(values * values, axis=-1, keepdims=True) + epsilon)


def norm_backward(grad_in, values, inverse, gain_vec):
    scaled = grad_in * gain_vec
    inner_mean = jnp.mean(scaled * values, axis=-1, keepdims=True)
    return inverse * scaled - values * inverse**3 * inner_mean


def rotary_tables(seq_len, head_dim):
    half_dim = head_dim // 2
    frequency = theta_base ** (-jnp.arange(half_dim, dtype=jnp.float32) * 2.0 / head_dim)
    angles = jnp.arange(seq_len, dtype=jnp.float32)[:, None] * frequency[None, :]
    return (jnp.cos(angles)[:, None, :], jnp.sin(angles)[:, None, :])


def rotate(values, cosine, sine_table):
    half_dim = values.shape[-1] // 2
    first_part = values[..., :half_dim]
    second = values[..., half_dim:]
    return jnp.concatenate(
        [first_part * cosine - second * sine_table, second * cosine + first_part * sine_table],
        axis=-1,
    )


def rotate_back(grad_in, cosine, sine_table):
    half_dim = grad_in.shape[-1] // 2
    first_part = grad_in[..., :half_dim]
    second = grad_in[..., half_dim:]
    return jnp.concatenate(
        [first_part * cosine + second * sine_table, second * cosine - first_part * sine_table],
        axis=-1,
    )


def dispatch(expert_ids, gate_values, experts, capacity):
    seq_len = expert_ids.shape[0]
    is_match = expert_ids[:, :, None] == jnp.arange(experts, dtype=jnp.int32)[None, None, :]
    expert_hits = jnp.sum(is_match.astype(jnp.int32), axis=1)
    before = jnp.cumsum(expert_hits, axis=0) - expert_hits
    slot_ids = jnp.sum(jnp.where(is_match, before[:, None, :], 0), axis=2)
    token_index = jnp.broadcast_to(jnp.arange(seq_len, dtype=jnp.int32)[:, None], expert_ids.shape)
    slot_table = (
        jnp.full((experts, capacity), seq_len, jnp.int32).at[expert_ids, slot_ids].set(token_index)
    )
    gate_table = (
        jnp.zeros((experts, capacity), jnp.float32).at[expert_ids, slot_ids].set(gate_values)
    )
    return (slot_table, gate_table)


def head_forward(head_inputs):
    query_vals, key_vals, value_vals = head_inputs
    seq_len = key_vals.shape[0]
    block_rows = min(512, seq_len)
    key_positions = jnp.arange(seq_len)

    def one_block(row_start):
        scores = jnp.einsum("qgd,sd->gqs", query_vals, key_vals, preferred_element_type=jnp.float32)
        causal = (row_start + jnp.arange(block_rows))[:, None] >= key_positions[None, :]
        exp_scores = jnp.where(causal, jnp.exp(scores), 0.0)
        denominator = jnp.sum(exp_scores, axis=-1, keepdims=True)
        softmax_low = (exp_scores / denominator).astype(jnp.bfloat16)
        mixed_out = jnp.einsum(
            "gqs,sd->qgd", softmax_low, value_vals, preferred_element_type=jnp.float32
        )
        return (mixed_out.astype(jnp.bfloat16), jnp.log(denominator[..., 0]))

    block_starts = jnp.arange(seq_len // block_rows, dtype=jnp.int32) * block_rows
    mixed_out, logsum = lax.map(one_block, block_starts)
    return (mixed_out.reshape(seq_len, query_vals.shape[1], query_vals.shape[2]), logsum)


def head_backward(head_inputs):
    query_vals, key_vals, value_vals, logsum, grad_mixed = head_inputs
    seq_len = key_vals.shape[0]
    block_rows = min(512, seq_len)
    key_positions = jnp.arange(seq_len)

    def one_block(state_in, block_in):
        grad_key, grad_value = state_in
        row_start, block_logsum = block_in
        scores = jnp.einsum("qgd,sd->gqs", query_vals, key_vals, preferred_element_type=jnp.float32)
        causal = (row_start + jnp.arange(block_rows))[:, None] >= key_positions[None, :]
        softmax_vals = jnp.where(causal, jnp.exp(scores - block_logsum[..., None]), 0.0)
        grad_probs = jnp.einsum(
            "qgd,sd->gqs", grad_mixed, value_vals, preferred_element_type=jnp.float32
        )
        delta_sum = jnp.sum(grad_probs * softmax_vals, axis=-1, keepdims=True)
        grad_scores = (softmax_vals * (grad_probs - delta_sum)).astype(jnp.bfloat16)
        grad_query = jnp.einsum(
            "gqs,sd->qgd", grad_scores, key_vals, preferred_element_type=jnp.float32
        )
        grad_key = grad_key + jnp.einsum(
            "gqs,qgd->sd", grad_scores, query_vals, preferred_element_type=jnp.float32
        )
        grad_value = grad_value + jnp.einsum(
            "gqs,qgd->sd",
            softmax_vals.astype(jnp.bfloat16),
            grad_mixed,
            preferred_element_type=jnp.float32,
        )
        return ((grad_key, grad_value), grad_query)

    block_starts = jnp.arange(seq_len // block_rows, dtype=jnp.int32) * block_rows
    zero_rows = jnp.zeros(key_vals.shape, jnp.float32)
    (grad_key, grad_value), grad_query = lax.scan(
        one_block, (zero_rows, zero_rows), (block_starts, logsum)
    )
    return (grad_query.reshape(query_vals.shape), grad_key, grad_value)


def gather_rows(values):
    return lax.all_gather(values, "tensor", axis=0, tiled=True)


def scatter_rows(values):
    return lax.psum_scatter(
        values.astype(jnp.bfloat16), "tensor", scatter_dimension=0, tiled=True
    ).astype(jnp.float32)


def widen(stacked, group):
    experts = stacked.shape[0]
    spread = jnp.broadcast_to(stacked[:, None], (experts, group) + stacked.shape[1:])
    return spread.reshape((experts * group,) + stacked.shape[1:])


MESH = pl.DeviceIdType.MESH
LIMIT = 66_000_000


class Place:
    def __init__(self):
        self.dp = lax.axis_index("dp")
        self.core = lax.axis_index("tensor")
        x, y = self.dp % 2, (self.dp // 2) % 2
        self.z = self.dp // 4
        step_x, step_y = 1 - 2 * x, 2 * (1 - 2 * y)
        self.da = (1 - self.core) * step_x + self.core * step_y
        self.db = (1 - self.core) * step_y + self.core * step_x
        self.half = self.z % 2
        self.pair = 4 * (1 - 2 * self.half)
        self.far = 8 * (1 - 2 * (self.z // 2))

    def copy(self, src, dst, send_sem, recv_sem, to, core=None):
        return pltpu.make_async_remote_copy(
            src_ref=src,
            dst_ref=dst,
            send_sem=send_sem,
            recv_sem=recv_sem,
            device_id=(to, self.core if core is None else core),
            device_id_type=MESH,
        )

    def at_z(self, z):
        return self.dp + 4 * (z - self.z)

    def z_of(self, m):
        low = self.z < 2
        depth = jnp.where(low, self.z, 3 - self.z)
        t = jnp.where(m == 0, depth, jnp.where(m == 1, 1 - depth, m))
        return jnp.where(low, t, 3 - t)

    def block(self, n):
        return self.at_z(self.z_of(n // 2)) + (n % 2) * self.da

    def greet(self, line=False, column=False, near=False, chain=False, everyone=False, partner=False):
        barrier = pltpu.get_barrier_semaphore()
        count = 0

        def signal(to, core):
            pl.semaphore_signal(barrier, inc=1, device_id=(to, core), device_id_type=MESH)

        if everyone:
            for r in range(1, 16):
                signal((self.dp + r) % 16, self.core)
            count = count + 15
        else:
            if near:
                signal(self.dp + self.da, self.core)
                signal(self.dp + self.db, self.core)
                count = count + 2
            if chain:
                signal(self.dp + self.pair, self.core)
                count = count + 1
                if near:
                    signal(self.dp + self.far, self.core)
                    count = count + 1
            if column:
                for r in range(1, 4):
                    signal((self.dp + 4 * r) % 16, self.core)
                count = count + 3
            if line:
                pl.when(self.z > 0)(lambda: signal(self.dp - 4, self.core))
                pl.when(self.z < 3)(lambda: signal(self.dp + 4, self.core))
                count = count + jnp.where(self.z > 0, 1, 0) + jnp.where(self.z < 3, 1, 0)
        if partner:
            signal(self.dp, 1 - self.core)
            count = count + 1
        pl.semaphore_wait(barrier, count)


def add_rows(target, terms, rows, block=16):
    def body(i, _):
        at = pl.ds(pl.multiple_of(i * block, block), block)
        total = terms[0][at, :].astype(jnp.float32)
        for term in terms[1:]:
            total = total + term[at, :].astype(jnp.float32)
        target[at, :] = total.astype(target.dtype)
        return 0

    lax.fori_loop(0, rows // block, body, 0)


def scatter_four_kernel(p_ref, out_ref, from_core, from_pair, send_sem, recv_sem):
    me = Place()
    rows = p_ref.shape[2]
    me.greet(chain=True, partner=True)

    def beside(h, slot):
        return me.copy(p_ref.at[h, 1 - me.core], from_core.at[slot], send_sem.at[slot], recv_sem.at[slot], me.dp, 1 - me.core)

    first, second = beside(1 - me.half, 0), beside(me.half, 1)
    first.start()
    second.start()
    first.wait_recv()
    add_rows(from_core.at[0], (p_ref.at[1 - me.half, me.core], from_core.at[0]), rows)
    across = me.copy(from_core.at[0], from_pair, send_sem.at[2], recv_sem.at[2], me.dp + me.pair)
    across.start()
    second.wait_recv()
    add_rows(from_core.at[1], (p_ref.at[me.half, me.core], from_core.at[1]), rows)
    across.wait_recv()
    add_rows(out_ref, (from_core.at[1], from_pair), rows)
    across.wait_send()
    first.wait_send()
    second.wait_send()


def scatter_four(p, cid):
    _, _, rows, columns = p.shape
    vmem = pl.BlockSpec(memory_space=pltpu.VMEM)
    return pl.pallas_call(
        scatter_four_kernel,
        out_shape=jax.ShapeDtypeStruct((rows, columns), jnp.float32),
        in_specs=[vmem],
        out_specs=vmem,
        scratch_shapes=[
            pltpu.VMEM((2, rows, columns), p.dtype),
            pltpu.VMEM((rows, columns), p.dtype),
            pltpu.SemaphoreType.DMA((3,)),
            pltpu.SemaphoreType.DMA((3,)),
        ],
        compiler_params=pltpu.CompilerParams(collective_id=cid, has_side_effects=True),
        name="scatter_four",
    )(p)


def run(*threads):
    threads = list(threads)
    while threads:
        for thread in list(threads):
            if next(thread, "end") == "end":
                threads.remove(thread)


def lagged(items, first, second, lag):
    for n in range(len(items) + lag):
        if n < len(items):
            first(items[n])
            yield
        if n >= lag:
            second(items[n - lag])
            yield


def gather_line(me, x_ref, out_ref, send_sem, recv_sem):
    def part(source, to, slot, own=False):
        return me.copy(x_ref if own else out_ref.at[source], out_ref.at[source], send_sem.at[slot], recv_sem.at[source], to)

    sides = ((-1, me.z < 3, 4), (1, me.z > 0, -4))

    def exists(d, side):
        return (me.z - d >= 0) if side == 0 else (me.z + d <= 3)

    def slot_z(d, side, j):
        return 4 + ((d - 1) * 2 + side) * 3 + j

    def slot_a(off):
        return 25 + off

    def pass_a(off):
        source = me.dp + me.da + 4 * off
        part(source, me.dp, slot_a(off)).wait_recv()
        part(source, me.dp + me.db, slot_a(off)).start()

    pl.when(me.z < 3)(lambda: part(me.dp, me.dp + 4, 0, True).start())
    pl.when(me.z > 0)(lambda: part(me.dp, me.dp - 4, 1, True).start())
    part(me.dp, me.dp + me.db, 3, True).start()
    part(me.dp, me.dp + me.da, 2, True).start()
    yield
    for d in range(1, 5):
        if d < 4:
            for side, (sign, forward, step) in enumerate(sides):
                source = me.dp + 4 * sign * d

                def arrive():
                    part(source, me.dp, slot_z(d, side, 0)).wait_recv()
                    pl.when(forward)(lambda: part(source, me.dp + step, slot_z(d, side, 0)).start())
                    part(source, me.dp + me.db, slot_z(d, side, 2)).start()
                    part(source, me.dp + me.da, slot_z(d, side, 1)).start()

                pl.when(exists(d, side))(arrive)
                yield
        if d == 1:
            pass_a(0)
            yield
        else:
            for side, (sign, *_) in enumerate(sides):
                pl.when(exists(d - 1, side))(lambda: pass_a(sign * (d - 1)))
                yield
    for z in range(4):
        for g in (0, 1):
            part(me.at_z(z) + me.db + g * me.da, me.dp, 0).wait_recv()
            yield

    def sent(slot):
        part(me.dp, me.dp, slot).wait_send()

    pl.when(me.z < 3)(lambda: sent(0))
    pl.when(me.z > 0)(lambda: sent(1))
    sent(2)
    sent(3)
    sent(slot_a(0))
    for d in range(1, 4):
        for side, (sign, forward, _) in enumerate(sides):

            def finish():
                pl.when(forward)(lambda: sent(slot_z(d, side, 0)))
                sent(slot_z(d, side, 1))
                sent(slot_z(d, side, 2))
                sent(slot_a(sign * d))

            pl.when(exists(d, side))(finish)


def gather_pairs(me, x_ref, out_ref, send_sem, recv_sem):
    mine, other = me.dp, me.dp + me.pair

    def part(src, where, to, slot):
        return me.copy(src, out_ref.at[where], send_sem.at[slot], recv_sem.at[where], to)

    def relay(where, to, slot):
        part(out_ref.at[where], where, to, slot).start()

    def arrived(where):
        part(out_ref.at[where], where, me.dp, 0).wait_recv()

    part(x_ref.at[1 - me.half], mine, other, 0).start()
    part(x_ref.at[me.half], mine, me.dp + me.far, 1).start()
    part(x_ref.at[me.half], mine, me.dp + me.db, 2).start()
    part(x_ref.at[me.half], mine, me.dp + me.da, 3).start()
    yield
    arrived(other)
    relay(other, me.dp + me.far, 4)
    relay(other, me.dp + me.db, 5)
    relay(other, me.dp + me.da, 6)
    yield
    arrived(mine + me.da)
    relay(mine + me.da, me.dp + me.db, 7)
    yield
    arrived(mine + me.far)
    relay(mine + me.far, me.dp + me.db, 8)
    relay(mine + me.far, me.dp + me.da, 9)
    yield
    arrived(other + me.da)
    relay(other + me.da, me.dp + me.db, 10)
    yield
    arrived(other + me.far)
    relay(other + me.far, me.dp + me.db, 11)
    relay(other + me.far, me.dp + me.da, 12)
    yield
    arrived(mine + me.far + me.da)
    relay(mine + me.far + me.da, me.dp + me.db, 13)
    yield
    arrived(other + me.far + me.da)
    relay(other + me.far + me.da, me.dp + me.db, 14)
    yield
    for base in (mine, other, mine + me.far, other + me.far):
        arrived(base + me.db)
        yield
        arrived(base + me.da + me.db)
        yield
    for slot in range(15):
        part(out_ref.at[mine], mine, me.dp, slot).wait_send()


def swap_rows(me, x_ref, out_ref, send_sem, recv_sem):
    for r in range(1, 16):
        to = (me.dp + r) % 16
        me.copy(x_ref.at[to], out_ref.at[me.dp], send_sem.at[r], recv_sem.at[r], to).start()
    yield
    for r in range(1, 16):
        s = (me.dp + 16 - r) % 16
        me.copy(x_ref.at[s], out_ref.at[s], send_sem.at[r], recv_sem.at[r], me.dp).wait_recv()
    for r in range(1, 16):
        me.copy(x_ref.at[me.dp], out_ref.at[me.dp], send_sem.at[r], recv_sem.at[r], me.dp).wait_send()


def keep_own(src, staging, dst, sems):
    load = pltpu.make_async_copy(src, staging, sems.at[0])
    store = pltpu.make_async_copy(staging, dst, sems.at[1])
    load.start()

    def finish():
        load.wait()
        store.start()
        store.wait()

    return finish


def share_experts(me, ins, outs, send_sem, recv_sem):
    depth = ins[0].shape[1]

    def sends(r):
        to = (me.dp + r) % 16
        at = pl.ds(pl.multiple_of(me.dp * depth, depth), depth)
        pairs = ((ins[0].at[to], outs[0].at[at]), (ins[1].at[to], outs[1].at[at]), (ins[2].at[to], outs[2].at[:, at]))
        return [me.copy(src, dst, send_sem.at[r, j], recv_sem.at[r, j], to) for j, (src, dst) in enumerate(pairs)]

    for r in (8, 7, 9, 4, 12, 5, 11, 6, 10, 3, 13, 2, 14, 1, 15):
        for c in sends(r):
            c.start()
        yield
    for r in range(1, 16):
        at = pl.ds(pl.multiple_of((me.dp + 16 - r) % 16 * depth, depth), depth)
        for j, dst in enumerate((outs[0].at[at], outs[1].at[at], outs[2].at[:, at])):
            me.copy(dst, dst, send_sem.at[r, j], recv_sem.at[r, j], me.dp).wait_recv()
    for r in range(1, 16):
        for c in sends(r):
            c.wait_send()


def gather_four(me, x_ref, out_ref, send_sem, recv_sem):
    mine, theirs = out_ref.at[me.half, me.core], out_ref.at[1 - me.half, me.core]
    across = me.copy(x_ref, mine, send_sem.at[0], recv_sem.at[0], me.dp + me.pair)
    across.start()
    beside = me.copy(x_ref, mine, send_sem.at[1], recv_sem.at[1], me.dp, 1 - me.core)
    beside.start()
    mine[...] = x_ref[...]
    yield
    across.wait_recv()
    relay = me.copy(theirs, theirs, send_sem.at[2], recv_sem.at[2], me.dp, 1 - me.core)
    relay.start()
    yield
    across.wait_send()
    beside.wait()
    relay.wait()


def gather_first_kernel(
    w_ref, c_ref, g_ref, x_ref, gate_ref, up_ref, down_ref,
    w_out, c_out, g_out, x_out, gate_out, up_out, down_out,
    w_own, c_own, e_own, w_send, w_recv, c_send, c_recv, g_send, g_recv, x_send, x_recv, e_send, e_recv, copy_sem,
):
    me = Place()
    depth = gate_ref.shape[1]
    at = pl.ds(pl.multiple_of(me.dp * depth, depth), depth)
    ends = [
        keep_own(w_ref.at[me.half], w_own, w_out.at[me.dp], copy_sem.at[0]),
        keep_own(c_ref, c_own, c_out.at[me.dp], copy_sem.at[1]),
        keep_own(gate_ref.at[me.dp], e_own.at[0], gate_out.at[at], copy_sem.at[2]),
        keep_own(up_ref.at[me.dp], e_own.at[1], up_out.at[at], copy_sem.at[3]),
    ]
    flat = pltpu.make_async_copy(down_ref.at[me.dp], down_out.at[:, at], copy_sem.at[4, 0])
    flat.start()
    g_out[me.dp] = g_ref[me.dp]
    me.greet(everyone=True, partner=True)
    run(
        gather_four(me, x_ref, x_out, x_send, x_recv),
        gather_pairs(me, w_ref, w_out, w_send, w_recv),
        gather_line(me, c_ref, c_out, c_send, c_recv),
        swap_rows(me, g_ref, g_out, g_send, g_recv),
        share_experts(me, (gate_ref, up_ref, down_ref), (gate_out, up_out, down_out), e_send, e_recv),
    )
    for end in ends:
        end()
    flat.wait()


def gather_first(weights, rows, gates, normed, experts, cid):
    hbm, vmem = pl.BlockSpec(memory_space=pl.ANY), pl.BlockSpec(memory_space=pltpu.VMEM)
    dma = pltpu.SemaphoreType.DMA
    dtype = rows.dtype
    _, depth, hidden = experts[0].shape
    return pl.pallas_call(
        gather_first_kernel,
        out_shape=[
            jax.ShapeDtypeStruct((16,) + weights.shape[1:], dtype),
            jax.ShapeDtypeStruct((16,) + rows.shape, dtype),
            jax.ShapeDtypeStruct(gates.shape, gates.dtype),
            jax.ShapeDtypeStruct((2, 2) + normed.shape, dtype),
            jax.ShapeDtypeStruct((16 * depth, hidden), dtype),
            jax.ShapeDtypeStruct((16 * depth, hidden), dtype),
            jax.ShapeDtypeStruct((hidden, 16 * depth), dtype),
        ],
        in_specs=[hbm, hbm, vmem, vmem, hbm, hbm, hbm],
        out_specs=[hbm, hbm, vmem, vmem, hbm, hbm, hbm],
        scratch_shapes=[
            pltpu.VMEM(weights.shape[1:], dtype),
            pltpu.VMEM(rows.shape, dtype),
            pltpu.VMEM((2, depth, hidden), dtype),
            dma((15,)), dma((16,)),
            dma((29,)), dma((16,)),
            dma((16,)), dma((16,)),
            dma((3,)), dma((3,)),
            dma((16, 3)), dma((16, 3)),
            dma((5, 2)),
        ],
        compiler_params=pltpu.CompilerParams(collective_id=cid, has_side_effects=True),
        name="gather_first",
    )(weights, rows, gates, normed, *experts)


def scatter_pairs(me, chunks, share, make, out_ref, from_b, from_a, from_far, send_sem, recv_sem):
    rows = from_a.shape[1] // chunks
    other = me.dp + me.pair
    bases = (me.dp, other, me.dp + me.far, other + me.far)
    items = [(j, k) for j in (2, 3, 1, 0) for k in range(chunks)]

    def at(k):
        return pl.ds(k * rows, rows)

    def copy(src, dst, slot, k, to):
        return me.copy(src, dst, send_sem.at[slot, k], recv_sem.at[slot, k], to)

    def send_b(g, j, k):
        return copy(share(bases[j] + me.db + g * me.da).at[at(k)], from_b.at[g, j, at(k)], g * 4 + j, k, me.dp + me.db)

    def send_a(j, k):
        return copy(from_b.at[1, j, at(k)], from_a.at[j, at(k)], 8 + j, k, me.dp + me.da)

    def send_far(j, k):
        return copy(from_b.at[0, 2 + j, at(k)], from_far.at[j, at(k)], 12 + j, k, me.dp + me.far)

    def swap(k):
        return copy(from_b.at[0, 1, at(k)], out_ref.at[me.half, at(k)], 14, k, other)

    for j in (2, 3, 1, 0):
        for g in (1, 0):
            make(bases[j] + me.db + g * me.da)
            for k in range(chunks):
                send_b(g, j, k).start()
        if j == 3:
            yield
    for j in (2, 3, 1, 0):
        make(bases[j] + me.da)
        make(bases[j])
        if j == 3:
            yield
    yield

    def first(item):
        j, k = item
        send_b(1, j, k).wait_recv()
        add_rows(from_b.at[1, j, at(k)], (share(bases[j] + me.da).at[at(k)], from_b.at[1, j, at(k)]), rows)
        send_a(j, k).start()

    def second(item):
        j, k = item
        send_b(0, j, k).wait_recv()
        send_a(j, k).wait_recv()
        terms = (share(bases[j]).at[at(k)], from_b.at[0, j, at(k)], from_a.at[j, at(k)])
        if j >= 2:
            add_rows(from_b.at[0, j, at(k)], terms, rows)
            send_far(j - 2, k).start()
        else:
            send_far(j, k).wait_recv()
            target = from_b.at[0, 1, at(k)] if j else out_ref.at[me.half, at(k)]
            add_rows(target, terms + (from_far.at[j, at(k)],), rows)
            if j:
                swap(k).start()

    yield from lagged(items, first, second, 2)
    for k in range(chunks):
        swap(k).wait_send()
        theirs = out_ref.at[1 - me.half, at(k)]
        copy(theirs, theirs, 14, k, other).wait_recv()
        for j in range(4):
            send_b(0, j, k).wait_send()
            send_b(1, j, k).wait_send()
            send_a(j, k).wait_send()
        send_far(0, k).wait_send()
        send_far(1, k).wait_send()


def sum_all(me, out_ref, held, send_sem, recv_sem):
    steps = ((me.dp, 1 - me.core), (me.dp + me.da, me.core), (me.dp + me.db, me.core), (me.dp + me.pair, me.core), (me.dp + me.far, me.core))
    yield
    for n, (to, core) in enumerate(steps):
        send = me.copy(held.at[0, n], held.at[1, n], send_sem.at[n], recv_sem.at[n], to, core)
        held[0, n] = out_ref[...]
        send.start()
        yield
        send.wait()
        out_ref[...] = held[0, n] + held[1, n]
        yield


def return_experts(me, gu_ref, down_ref, outs, own, held, core_send, core_recv, send_sem, recv_sem, copy_sem):
    rows, half = outs[0].shape[1:]

    def views(d, core):
        at = pl.ds(pl.multiple_of(d * rows, rows), rows)
        starts = ((gu_ref, core * half), (gu_ref, 2 * half + core * half), (down_ref, core * half))
        return [ref.at[at, pl.ds(pl.multiple_of(start, 128), half)] for ref, start in starts]

    def beside(r):
        d = (me.dp + r) % 16
        return [
            me.copy(src, held.at[j, r], core_send.at[r, j], core_recv.at[r, j], me.dp, 1 - me.core)
            for j, src in enumerate(views(d, 1 - me.core))
        ]

    order = (8, 7, 9, 4, 12, 5, 11, 6, 10, 3, 13, 2, 14, 1, 15, 0)

    def loads(n):
        d = (me.dp + order[n]) % 16
        return [pltpu.make_async_copy(src, own.at[j, n % 8], copy_sem.at[n % 8, j]) for j, src in enumerate(views(d, me.core))]

    def sends(r):
        d = (me.dp + r) % 16
        return [me.copy(held.at[j, r], outs[j].at[me.dp], send_sem.at[r, j], recv_sem.at[r, j], d) for j in range(3)]

    for r in order:
        for c in beside(r):
            c.start()
    for n in range(8):
        for c in loads(n):
            c.start()
    yield
    keep = [pltpu.make_async_copy(held.at[j, 0], outs[j].at[me.dp], copy_sem.at[16, j]) for j in range(3)]
    for n, r in enumerate(order):
        for j, (arrives, load) in enumerate(zip(beside(r), loads(n))):
            arrives.wait_recv()
            load.wait()
            add_rows(held.at[j, r], (own.at[j, n % 8], held.at[j, r]), rows, 64)
        for c in sends(r) if r else keep:
            c.start()
        if n < 8:
            for c in loads(n + 8):
                c.start()
        if n % 2:
            yield
    for r in range(1, 16):
        s = (me.dp + 16 - r) % 16
        for j in range(3):
            dst = outs[j].at[s]
            me.copy(dst, dst, send_sem.at[r, j], recv_sem.at[r, j], me.dp).wait_recv()
    for c in keep:
        c.wait()
    for r in range(16):
        for c in beside(r) + (sends(r) if r else []):
            c.wait_send()


def attention_back_kernel(
    chunks, head_dim,
    ga_ref, w_ref, seq_ref, raw_ref, low_ref, mixed_ref, rope_ref, gain_ref, unit_ref, x_ref, gu_ref, down_ref, share_ref,
    one_ref, moe_ref, out_ref, sum_ref, gate_out, up_out, down_out,
    w, ga, gmix, gproj, part, kept, dk, dv, gains, from_core, from_pair,
    pair_b, pair_a, pair_far, total, own, held,
    from_b, from_a, from_z, b_send, b_recv, a_send, a_recv, z_send, z_recv,
    four_send, four_recv, back_send, back_recv, pair_send, pair_recv, sum_send, sum_recv, core_send, core_recv, e_send, e_recv,
    copy_sem, load_sem,
):
    me = Place()
    rows, width = ga_ref.shape
    seq_len = 2 * rows
    q_cols = mixed_ref.shape[1]
    proj_cols = q_cols + 2 * head_dim
    group = q_cols // head_dim
    dot = functools.partial(jnp.dot, preferred_element_type=jnp.float32)
    dot_t = functools.partial(lax.dot_general, dimension_numbers=(((1,), (1,)), ((), ())), preferred_element_type=jnp.float32)
    t_dot = functools.partial(lax.dot_general, dimension_numbers=(((0,), (0,)), ((), ())), preferred_element_type=jnp.float32)
    load = pltpu.make_async_copy(w_ref, w, load_sem.at[8])
    load.start()
    keeps = [pltpu.make_async_copy(share_ref.at[n, pl.ds(0, rows)], kept.at[n], load_sem.at[n]) for n in range(8)]
    for c in keeps:
        c.start()
    me.greet(everyone=True, partner=True)

    def ga_at(h, core):
        return ga.at[pl.ds(pl.multiple_of((2 * h + core) * rows, rows), rows)]

    mine, theirs = ga_at(me.half, me.core), ga_at(1 - me.half, me.core)
    across = me.copy(ga_ref, mine, four_send.at[0], four_recv.at[0], me.dp + me.pair)
    beside = me.copy(ga_ref, mine, four_send.at[1], four_recv.at[1], me.dp, 1 - me.core)
    relay = me.copy(theirs, theirs, four_send.at[2], four_recv.at[2], me.dp, 1 - me.core)
    across.start()
    beside.start()
    mine[...] = ga_ref[...]
    scatter = ScatterRows(
        me, lambda n: share_ref.at[n, pl.ds(rows, rows)], lambda n: kept.at[n], from_b, from_a, from_z,
        (b_send, b_recv, a_send, a_recv, z_send, z_recv),
    )
    for m in (1, 2, 3, 0):
        scatter.send_b(2 * m + 1).start()
        scatter.send_b(2 * m).start()
    experts = return_experts(me, gu_ref, down_ref, (gate_out, up_out, down_out), own, held, core_send, core_recv, e_send, e_recv, copy_sem)
    next(experts)
    across.wait_recv()
    relay.start()
    across.wait_send()
    beside.wait()
    next(experts)
    relay.wait()
    load.wait()
    for c in keeps:
        c.wait()

    def mix(j, _):
        at = pl.ds(pl.multiple_of(j * 256, 256), 256)
        at_w = pl.ds(pl.multiple_of(proj_cols + j * 256, 256), 256)
        gmix[:, at] = dot(ga[...], w[:, at_w]).astype(gmix.dtype)
        return 0

    lax.fori_loop(0, q_cols // 256, mix, 0)
    next(experts)
    gains[...] = jnp.zeros_like(gains)
    turn = rope_ref[1]
    cosine = rope_ref[0]
    causal = lax.broadcasted_iota(jnp.int32, (seq_len, seq_len), 0) >= lax.broadcasted_iota(jnp.int32, (seq_len, seq_len), 1)
    k_at, v_at = pl.ds(q_cols, head_dim), pl.ds(q_cols + head_dim, head_dim)

    def back(grad, raw, which):
        grad = grad * cosine + pltpu.roll(grad, head_dim // 2, 1) * turn
        inverse = lax.rsqrt(jnp.mean(raw * raw, axis=-1, keepdims=True) + epsilon)
        gains[which] = gains[which] + jnp.sum(grad * (raw * inverse), axis=0, keepdims=True)
        scaled = grad * gain_ref[which]
        inner = jnp.mean(scaled * raw, axis=-1, keepdims=True)
        return inverse * scaled - raw * (inverse * inverse * inverse) * inner

    def head(n, _):
        at = pl.ds(pl.multiple_of(n // group * seq_len, seq_len), seq_len)
        cols = pl.ds(pl.multiple_of(n % group * head_dim, head_dim), head_dim)
        query, key, value, grad = low_ref[at, cols], low_ref[at, k_at], low_ref[at, v_at], gmix[at, cols]
        exp_scores = jnp.where(causal, jnp.exp(dot_t(query, key)), 0.0)
        probs = exp_scores / jnp.sum(exp_scores, axis=-1, keepdims=True)
        grad_probs = dot_t(grad, value)
        delta = jnp.sum(grad_probs * probs, axis=-1, keepdims=True)
        grad_scores = (probs * (grad_probs - delta)).astype(query.dtype)
        grad_query = dot(grad_scores, key) * head_dim ** (-0.5)
        grad_key = t_dot(grad_scores, query)
        grad_value = t_dot(probs.astype(query.dtype), grad)

        def begin():
            dk[...] = grad_key
            dv[...] = grad_value

        def more():
            dk[...] = dk[...] + grad_key
            dv[...] = dv[...] + grad_value

        pl.when(n % group == 0)(begin)
        pl.when(n % group != 0)(more)
        gproj[at, cols] = back(grad_query, raw_ref[at, cols], 0).astype(gproj.dtype)

        def close():
            gproj[at, k_at] = back(dk[...], raw_ref[at, k_at], 1).astype(gproj.dtype)
            gproj[at, v_at] = dv[...].astype(gproj.dtype)

        pl.when(n % group == group - 1)(close)
        return 0

    heads = 2 * group
    quarter = heads // 4
    for k in range(4):
        lax.fori_loop(k * quarter, (k + 1) * quarter, head, 0)
        next(experts)
        scatter.first((1, 2, 3, 0)[k])
        if k:
            scatter.second((1, 2, 3, 0)[k - 1])

    def project(j, _):
        at = pl.ds(pl.multiple_of(j * 256, 256), 256)
        part[:, at] = dot_t(gproj[...], w[at, pl.ds(0, proj_cols)]).astype(part.dtype)
        return 0

    lax.fori_loop(0, width // 256, project, 0)

    def part_at(h, core):
        return part.at[pl.ds(pl.multiple_of((2 * h + core) * rows, rows), rows)]

    def give(h, slot):
        return me.copy(part_at(h, 1 - me.core), from_core.at[slot], back_send.at[slot], back_recv.at[slot], me.dp, 1 - me.core)

    give(1 - me.half, 0).start()
    give(me.half, 1).start()
    other = me.dp + me.pair
    bases = (me.dp, other, me.dp + me.far, other + me.far)

    def weight_block(d):
        at = pl.ds(pl.multiple_of(d * rows, rows), rows)
        w[at, pl.ds(0, proj_cols)] = t_dot(seq_ref[:, at], gproj[...]).astype(w.dtype)
        w[at, pl.ds(proj_cols, q_cols)] = t_dot(ga[:, at], mixed_ref[...]).astype(w.dtype)

    pairs = scatter_pairs(me, chunks, lambda d: w.at[pl.ds(pl.multiple_of(d * rows, rows), rows)], weight_block, out_ref, pair_b, pair_a, pair_far, pair_send, pair_recv)
    next(pairs)
    give(1 - me.half, 0).wait_recv()
    add_rows(from_core.at[0], (part_at(1 - me.half, me.core), from_core.at[0]), rows)
    over = me.copy(from_core.at[0], from_pair, back_send.at[2], back_recv.at[2], me.dp + me.pair)
    over.start()
    give(me.half, 1).wait_recv()
    add_rows(from_core.at[1], (part_at(me.half, me.core), from_core.at[1]), rows)
    next(pairs)
    scatter.second(0)
    next(experts)
    next(pairs)
    over.wait_recv()
    add_rows(one_ref, (from_core.at[1], from_pair), rows)
    sum_ref[...] = x_ref[...]
    attn = jnp.sum(one_ref[...] * unit_ref[...], axis=0, keepdims=True)
    for j in range(width // 128):
        sum_ref[pl.ds(j, 1), :] = attn[:, j * 128 : (j + 1) * 128]
    for j in range(2):
        sum_ref[pl.ds(2 * width // 128 + j, 1), :] = gains[j]
    scatter.finish(moe_ref)
    run(pairs, experts, sum_all(me, sum_ref, total, sum_send, sum_recv))
    scatter.drain()
    give(0, 0).wait_send()
    give(0, 1).wait_send()
    over.wait_send()


def attention_back(grad_attn, weights, seq_normed, raw, low, mixed, rope, gain, unit, sums, gu, down, share, cid, chunks=2):
    rows, width = grad_attn.shape
    head_dim = rope.shape[-1]
    columns = weights.shape[1]
    half = down.shape[1] // 2
    hbm, vmem = pl.BlockSpec(memory_space=pl.ANY), pl.BlockSpec(memory_space=pltpu.VMEM)
    dma = pltpu.SemaphoreType.DMA
    dtype = weights.dtype
    proj_cols = raw.shape[1] + head_dim
    whole = jax.ShapeDtypeStruct((rows, width), jnp.float32)
    return pl.pallas_call(
        functools.partial(attention_back_kernel, chunks, head_dim),
        out_shape=[whole, whole, jax.ShapeDtypeStruct((2, rows, columns), dtype), jax.ShapeDtypeStruct(sums.shape, sums.dtype)]
        + [jax.ShapeDtypeStruct((16, rows, half), dtype)] * 3,
        in_specs=[vmem, hbm] + [vmem] * 8 + [hbm] * 3,
        out_specs=[vmem] * 4 + [hbm] * 3,
        scratch_shapes=[
            pltpu.VMEM(weights.shape, dtype),
            pltpu.VMEM((4 * rows, width), dtype),
            pltpu.VMEM(mixed.shape, dtype),
            pltpu.VMEM((4 * rows, proj_cols), dtype),
            pltpu.VMEM((4 * rows, width), dtype),
            pltpu.VMEM((8, rows, width), dtype),
            pltpu.VMEM((2 * rows, head_dim), jnp.float32),
            pltpu.VMEM((2 * rows, head_dim), jnp.float32),
            pltpu.VMEM((2, 1, head_dim), jnp.float32),
            pltpu.VMEM((2, rows, width), dtype),
            pltpu.VMEM((rows, width), dtype),
            pltpu.VMEM((2, 4, rows, columns), dtype),
            pltpu.VMEM((4, rows, columns), dtype),
            pltpu.VMEM((2, rows, columns), dtype),
            pltpu.VMEM((2, 5) + sums.shape, sums.dtype),
            pltpu.VMEM((3, 8, rows, half), dtype),
            pltpu.VMEM((3, 16, rows, half), dtype),
            *scatter_rows_scratch(rows, width, dtype),
            dma((3,)), dma((3,)),
            dma((3,)), dma((3,)),
            dma((15, chunks)), dma((15, chunks)),
            dma((5,)), dma((5,)),
            dma((16, 3)), dma((16, 3)),
            dma((16, 3)), dma((16, 3)),
            dma((17, 3)), dma((9,)),
        ],
        compiler_params=pltpu.CompilerParams(collective_id=cid, has_side_effects=True, vmem_limit_bytes=67_043_328),
        name="attention_back",
    )(grad_attn, weights, seq_normed, raw, low, mixed, rope, gain, unit, sums, gu, down, share)


class ScatterRows:
    def __init__(self, me, sent, kept, from_b, from_a, from_z, sems):
        self.me, self.sent, self.kept = me, sent, kept
        self.from_b, self.from_a, self.from_z = from_b, from_a, from_z
        self.b_send, self.b_recv, self.a_send, self.a_recv, self.z_send, self.z_recv = sems
        self.rows = from_b.shape[1]

    def send_b(self, n):
        me = self.me
        return me.copy(self.sent(n), self.from_b.at[n], self.b_send.at[n], self.b_recv.at[n], me.dp + me.db)

    def send_a(self, m):
        me = self.me
        return me.copy(self.from_b.at[2 * m + 1], self.from_a.at[m], self.a_send.at[m], self.a_recv.at[m], me.dp + me.da)

    def send_z(self, m):
        me = self.me
        return me.copy(self.from_b.at[2 * m], self.from_z.at[me.z], self.z_send.at[m], self.z_recv.at[me.z], me.at_z(me.z_of(m)))

    def first(self, m):
        n = 2 * m + 1
        self.send_b(n).wait_recv()
        add_rows(self.from_b.at[n], (self.kept(n), self.from_b.at[n]), self.rows)
        self.send_a(m).start()

    def second(self, m):
        n = 2 * m
        self.send_b(n).wait_recv()
        self.send_a(m).wait_recv()
        add_rows(self.from_b.at[n], (self.kept(n), self.from_b.at[n], self.from_a.at[m]), self.rows)
        pl.when(m > 0)(lambda: self.send_z(m).start())

    def advance(self, now, lags=(1, 2)):
        for lag, call in zip(lags, (self.first, self.second)):
            m = (now - 1 - lag) // 2
            due = jnp.logical_and((now - 1 - lag) % 2 == 0, jnp.logical_and(now > lag, m < 4))
            pl.when(due)(lambda: call(m))

    def finish(self, out_ref):
        me = self.me
        others = [(me.z + r) % 4 for r in range(1, 4)]
        for z in others:
            me.copy(self.from_z.at[z], self.from_z.at[z], self.z_send.at[0], self.z_recv.at[z], me.dp).wait_recv()
        add_rows(out_ref, (self.from_b.at[0],) + tuple(self.from_z.at[z] for z in others), self.rows)

    def drain(self):
        for m in range(4):
            self.send_b(2 * m).wait_send()
            self.send_b(2 * m + 1).wait_send()
            self.send_a(m).wait_send()
            if m:
                self.send_z(m).wait_send()


def scatter_rows_scratch(rows, columns, dtype):
    dma = pltpu.SemaphoreType.DMA
    return [
        pltpu.VMEM((8, rows, columns), dtype),
        pltpu.VMEM((4, rows, columns), dtype),
        pltpu.VMEM((4, rows, columns), dtype),
        dma((8,)), dma((8,)), dma((4,)), dma((4,)), dma((4,)), dma((4,)),
    ]


def experts_kernel(
    x_ref, c_ref, g_ref, gate_ref, up_ref, down_ref,
    share_ref, two_ref, gu_out, down_out, xg_ref,
    wgu, wd, ag, ggu, share, p, xb, cb, from_b, from_a, from_z, b_send, b_recv, a_send, a_recv, z_send, z_recv,
    g_send, g_recv, w_send, w_recv, load_sem, tile_sem, keep_sem, share_sem,
):
    me = Place()
    rows, width = x_ref.shape
    hidden = wd.shape[0]
    half = hidden // 2
    dot = functools.partial(jnp.dot, preferred_element_type=jnp.float32)
    dot_t = functools.partial(lax.dot_general, dimension_numbers=(((1,), (1,)), ((), ())), preferred_element_type=jnp.float32)
    t_dot = functools.partial(lax.dot_general, dimension_numbers=(((0,), (0,)), ((), ())), preferred_element_type=jnp.float32)
    upper, lower = pl.ds(rows, rows), pl.ds(0, rows)

    z_of, block = me.z_of, me.block

    def part(source, to, slot, own=False):
        return me.copy(x_ref if own else xg_ref.at[source], xg_ref.at[source], g_send.at[slot], g_recv.at[source], to)

    def arrive(m):
        source = me.at_z(z_of(m))
        part(source, me.dp, 0).wait_recv()
        part(source, me.dp + me.db, 3 + 2 * m).start()
        part(source, me.dp + me.da, 4 + 2 * m).start()

    def arrive_a(m):
        source = me.at_z(z_of(m)) + me.da
        part(source, me.dp, 0).wait_recv()
        part(source, me.dp + me.db, 11 + m).start()

    def loads(n):
        slot = n % 2
        copies = []
        for j, source in enumerate((block(n), block(n) + me.db)):
            at = pl.ds(j * rows, rows)
            copies.append(pltpu.make_async_copy(xg_ref.at[source], xb.at[slot, at], load_sem.at[slot, j]))
            copies.append(pltpu.make_async_copy(c_ref.at[source], cb.at[slot, at], load_sem.at[slot, 2 + j]))
        return copies

    def fetch(n):
        part(block(n) + me.db, me.dp, 0).wait_recv()
        for c in loads(n):
            c.start()

    scatter = ScatterRows(
        me, lambda n: p.at[n, upper], lambda n: p.at[n, lower], from_b, from_a, from_z, (b_send, b_recv, a_send, a_recv, z_send, z_recv)
    )

    def keep_share(n):
        return pltpu.make_async_copy(share.at[n % 2], share_ref.at[n], share_sem.at[n % 2])

    own = p.at[7, lower]
    load = pltpu.make_async_copy(x_ref, own, keep_sem.at[0])
    store = pltpu.make_async_copy(own, xg_ref.at[me.dp], keep_sem.at[1])
    load.start()

    def half_of(core):
        at = core * half
        return (
            wgu.at[:, pl.ds(pl.multiple_of(at, 128), half)],
            wgu.at[:, pl.ds(pl.multiple_of(hidden + at, 128), half)],
            wd.at[pl.ds(pl.multiple_of(at, 128), half)],
        )

    mine = (gate_ref, up_ref, down_ref)
    locals_ = [pltpu.make_async_copy(src, dst, keep_sem.at[2 + j]) for j, (src, dst) in enumerate(zip(mine, half_of(me.core)))]
    for c in locals_:
        c.start()
    me.greet(column=True, near=True, partner=True)
    for m in range(1, 4):
        part(me.dp, me.at_z(z_of(m)), m - 1, True).start()
    part(me.dp, me.dp + me.db, 3, True).start()
    part(me.dp, me.dp + me.da, 4, True).start()
    shares = [
        me.copy(src, dst, w_send.at[j], w_recv.at[j], me.dp, 1 - me.core) for j, (src, dst) in enumerate(zip(mine, half_of(me.core)))
    ]
    for c in shares:
        c.start()
    load.wait()
    store.start()
    arrive_a(0)
    store.wait()
    for c in locals_:
        c.wait()
    for j, dst in enumerate(half_of(1 - me.core)):
        me.copy(dst, dst, w_send.at[j], w_recv.at[j], me.dp).wait_recv()
    fetch(0)

    tile = 256

    def step(n, _):
        slot = n % 2
        for c in loads(n):
            c.wait()
        gates = jnp.concatenate([g_ref[block(n)], g_ref[block(n) + me.db]], axis=0)

        def inner(j, _):
            at, at_up = pl.ds(pl.multiple_of(j * tile, tile), tile), pl.ds(pl.multiple_of(hidden + j * tile, tile), tile)
            gate, up, grad = dot(xb[slot], wgu[:, at]), dot(xb[slot], wgu[:, at_up]), dot_t(cb[slot], wd[at, :]) * gates
            sig = 1.0 / (1.0 + jnp.exp(-gate))
            act = gate * sig
            ag[n, :, at] = (act * up * gates).astype(ag.dtype)
            ggu[n, :, at] = (grad * up * sig * (1.0 + gate * (1.0 - sig))).astype(ggu.dtype)
            ggu[n, :, at_up] = (grad * act).astype(ggu.dtype)
            return 0

        lax.fori_loop(0, hidden // tile, inner, 0)

        def at_step(k, *calls):
            def go():
                for call, m in calls:
                    call(m)

            pl.when(n == k)(go)

        at_step(0, (arrive, 1))
        at_step(1, (arrive, 2), (arrive_a, 1))
        at_step(2, (arrive, 3))
        at_step(3, (arrive_a, 2))
        at_step(4, (arrive_a, 3))
        pl.when(n < 7)(lambda: fetch(n + 1))

        pl.when(n >= 2)(lambda: keep_share(n - 2).wait())

        def outer(j, _):
            at = pl.ds(pl.multiple_of(j * 2 * tile, 2 * tile), 2 * tile)
            share[slot, :, at] = dot(ag[n], wd[:, at]).astype(p.dtype)
            p[n, :, at] = dot_t(ggu[n], wgu[at, :]).astype(p.dtype)
            return 0

        lax.fori_loop(0, width // (2 * tile), outer, 0)
        scatter.send_b(n).start()
        keep_share(n).start()
        scatter.advance(n)
        return 0

    lax.fori_loop(0, 8, step, 0)

    def tiles(i):
        slot = i % 2
        cols = pl.ds(pl.multiple_of(i * tile, tile), tile)
        copies = []
        for which, src in enumerate((xg_ref, c_ref)):
            to = pl.ds(pl.multiple_of((2 * which + slot) * tile, tile), tile)

            def one(n, side, which=which, src=src, to=to):
                at = pl.ds(pl.multiple_of((2 * n + side) * rows, rows), rows)
                return pltpu.make_async_copy(src.at[block(n) + side * me.db, :, cols], wgu.at[at, to], tile_sem.at[which, slot, 2 * n + side])

            copies.append(one)
        return copies

    def each_tile(i, act):
        for one in tiles(i):

            def body(n, _):
                for side in (0, 1):
                    act(one(n, side))
                return 0

            lax.fori_loop(0, 8, body, 0)

    def outs(i):
        slot = i % 2
        at = pl.ds(pl.multiple_of(i * tile, tile), tile)
        return (
            pltpu.make_async_copy(xb.at[slot, :, pl.ds(0, 2 * hidden)], gu_out.at[at], load_sem.at[slot, 0]),
            pltpu.make_async_copy(cb.at[slot, :, pl.ds(0, hidden)], down_out.at[at], load_sem.at[slot, 1]),
        )

    each_tile(0, lambda c: c.start())

    def weight_step(i, _):
        slot = i % 2
        pl.when(i < 7)(lambda: each_tile(i + 1, lambda c: c.start()))
        each_tile(i, lambda c: c.wait())

        def free():
            for c in outs(i - 2):
                c.wait()

        pl.when(i >= 2)(free)
        x_tile = wgu[:, pl.ds(pl.multiple_of(slot * tile, tile), tile)]
        xb[slot, :, pl.ds(0, 2 * hidden)] = t_dot(x_tile, ggu[...].reshape(-1, 2 * hidden)).astype(xb.dtype)
        c_tile = wgu[:, pl.ds(pl.multiple_of((2 + slot) * tile, tile), tile)]
        cb[slot, :, pl.ds(0, hidden)] = t_dot(c_tile, ag[...].reshape(-1, hidden)).astype(cb.dtype)
        for c in outs(i):
            c.start()
        scatter.advance(i + 8)
        return 0

    lax.fori_loop(0, 8, weight_step, 0)
    scatter.finish(two_ref)

    for i in (6, 7):
        for c in outs(i):
            c.wait()
    for c in shares:
        c.wait_send()
    for slot in range(15):
        part(me.dp, me.dp, slot).wait_send()
    scatter.drain()
    keep_share(6).wait()
    keep_share(7).wait()


def expert_layer(x, grads, gates, gate, up, down, cid):
    rows, width = x.shape
    half = gate.shape[1]
    hbm, vmem = pl.BlockSpec(memory_space=pl.ANY), pl.BlockSpec(memory_space=pltpu.VMEM)
    dma = pltpu.SemaphoreType.DMA
    dtype = x.dtype
    return pl.pallas_call(
        experts_kernel,
        out_shape=[
            jax.ShapeDtypeStruct((8, 2 * rows, width), dtype),
            jax.ShapeDtypeStruct((rows, width), jnp.float32),
            jax.ShapeDtypeStruct((width, 4 * half), dtype),
            jax.ShapeDtypeStruct((width, 2 * half), dtype),
            jax.ShapeDtypeStruct((16, rows, width), dtype),
        ],
        in_specs=[hbm, hbm, vmem, hbm, hbm, hbm],
        out_specs=[hbm, vmem, hbm, hbm, hbm],
        scratch_shapes=[
            pltpu.VMEM((width, 4 * half), dtype),
            pltpu.VMEM((2 * half, width), dtype),
            pltpu.VMEM((8, 2 * rows, 2 * half), dtype),
            pltpu.VMEM((8, 2 * rows, 4 * half), dtype),
            pltpu.VMEM((2, 2 * rows, width), dtype),
            pltpu.VMEM((8, 2 * rows, width), dtype),
            pltpu.VMEM((2, 2 * rows, width), dtype),
            pltpu.VMEM((2, 2 * rows, width), dtype),
            *scatter_rows_scratch(rows, width, dtype),
            dma((15,)), dma((16,)),
            dma((3,)), dma((3,)),
            dma((2, 4)), dma((2, 2, 16)), dma((5,)), dma((2,)),
        ],
        compiler_params=pltpu.CompilerParams(collective_id=cid, has_side_effects=True, vmem_limit_bytes=67_043_328),
        name="experts",
    )(x, grads, gates, gate, up, down)


def per_device_any(
    tokens,
    cotangent,
    expert_ids,
    gate_values,
    w_query,
    w_key,
    w_value,
    w_out,
    w_gate,
    w_up,
    w_down,
    attn_gain,
    ffn_gain,
    query_gain,
    key_gain,
):
    contract = (((1,), (1,)), ((), ()))
    contract_rows = (((0,), (0,)), ((), ()))
    residual = tokens.astype(jnp.float32)
    model_width = residual.shape[1]
    inverse_one = rms_inverse(residual)
    seq_normed = gather_rows((residual * inverse_one * attn_gain).astype(jnp.bfloat16))
    full_query, full_key, full_value, full_out = (
        lax.all_gather(w_query, "dp", axis=0, tiled=True),
        lax.all_gather(w_key, "dp", axis=0, tiled=True),
        lax.all_gather(w_value, "dp", axis=0, tiled=True),
        lax.all_gather(w_out, "dp", axis=1, tiled=True),
    )
    seq_len = seq_normed.shape[0]
    head_dim = query_gain.shape[0]
    local_heads = full_query.shape[1] // head_dim
    local_kv = full_key.shape[1] // head_dim
    group_size = local_heads // local_kv
    attn_scale = head_dim ** (-0.5)
    cosine, sine_table = rotary_tables(seq_len, head_dim)
    query_raw = jnp.dot(seq_normed, full_query, preferred_element_type=jnp.float32).reshape(
        seq_len, local_heads, head_dim
    )
    key_raw = jnp.dot(seq_normed, full_key, preferred_element_type=jnp.float32).reshape(
        seq_len, local_kv, head_dim
    )
    value_low = (
        jnp.dot(seq_normed, full_value, preferred_element_type=jnp.float32)
        .astype(jnp.bfloat16)
        .reshape(seq_len, local_kv, head_dim)
    )
    query_inverse = rms_inverse(query_raw)
    key_inverse = rms_inverse(key_raw)
    query_low = (
        rotate(query_raw * query_inverse * query_gain, cosine, sine_table) * attn_scale
    ).astype(jnp.bfloat16)
    key_low = rotate(key_raw * key_inverse * key_gain, cosine, sine_table).astype(jnp.bfloat16)
    query_heads = query_low.reshape(seq_len, local_kv, group_size, head_dim).transpose(1, 0, 2, 3)
    key_heads = key_low.transpose(1, 0, 2)
    value_heads = value_low.transpose(1, 0, 2)
    mixed_heads, logsum = lax.map(head_forward, (query_heads, key_heads, value_heads))
    mixed_flat = mixed_heads.transpose(1, 0, 2, 3).reshape(seq_len, local_heads * head_dim)
    hidden = residual + scatter_rows(
        jnp.dot(mixed_flat, full_out, preferred_element_type=jnp.float32)
    )
    inverse_two = rms_inverse(hidden)
    seq_two = gather_rows((hidden * inverse_two * ffn_gain).astype(jnp.bfloat16))
    seq_grad = gather_rows(cotangent)
    experts = w_gate.shape[0]
    dp_rows = w_gate.shape[1]
    hidden_units = w_gate.shape[2]
    dp_count = lax.axis_size("dp")
    group = dp_count // experts
    routed_rows = seq_len * expert_ids.shape[1] * 9 // 8
    capacity = (routed_rows + experts * group - 1) // (experts * group) * group
    slot_table, gate_table = dispatch(expert_ids, gate_values, experts, capacity)
    blank_row = jnp.zeros((1, model_width), jnp.bfloat16)
    padded_in = jnp.concatenate([seq_two, blank_row], axis=0)
    padded_grad = jnp.concatenate([seq_grad, blank_row], axis=0)
    empty_rows = jnp.zeros((seq_len + 1, model_width), jnp.float32)
    piece_rows = capacity // group
    down_rows = jnp.transpose(w_down, (0, 2, 1))
    gate_mine, up_mine, down_mine = (
        lax.all_to_all(widen(w_gate, group), "dp", split_axis=0, concat_axis=1, tiled=True),
        lax.all_to_all(widen(w_up, group), "dp", split_axis=0, concat_axis=1, tiled=True),
        lax.all_to_all(widen(down_rows, group), "dp", split_axis=0, concat_axis=1, tiled=True),
    )
    gate_mine = gate_mine[0]
    up_mine = up_mine[0]
    down_mine = down_mine[0]
    blocks_in = padded_in[slot_table]
    grad_blocks = (padded_grad[slot_table].astype(jnp.float32) * gate_table[:, :, None]).astype(
        jnp.bfloat16
    )
    recv_in, recv_grad = (
        lax.all_to_all(
            blocks_in.reshape(dp_count, piece_rows, model_width),
            "dp",
            split_axis=0,
            concat_axis=0,
            tiled=True,
        ),
        lax.all_to_all(
            grad_blocks.reshape(dp_count, piece_rows, model_width),
            "dp",
            split_axis=0,
            concat_axis=0,
            tiled=True,
        ),
    )
    rows_in = recv_in.reshape(-1, model_width)
    rows_grad = recv_grad.reshape(-1, model_width)
    gate_pre = jnp.dot(rows_in, gate_mine, preferred_element_type=jnp.float32)
    up_pre = jnp.dot(rows_in, up_mine, preferred_element_type=jnp.float32)
    act_low = (jax.nn.silu(gate_pre) * up_pre).astype(jnp.bfloat16)
    expert_out = lax.dot_general(act_low, down_mine, contract, preferred_element_type=jnp.float32)
    grad_act = jnp.dot(rows_grad, down_mine, preferred_element_type=jnp.float32)
    sigmoid_gate = jax.nn.sigmoid(gate_pre)
    grad_gate = (grad_act * up_pre * sigmoid_gate * (1.0 + gate_pre * (1.0 - sigmoid_gate))).astype(
        jnp.bfloat16
    )
    grad_up = (grad_act * gate_pre * sigmoid_gate).astype(jnp.bfloat16)
    grad_input = lax.dot_general(
        grad_gate, gate_mine, contract, preferred_element_type=jnp.float32
    ) + lax.dot_general(grad_up, up_mine, contract, preferred_element_type=jnp.float32)
    back_out, back_grad = (
        lax.all_to_all(
            expert_out.reshape(dp_count, piece_rows, model_width).astype(jnp.bfloat16),
            "dp",
            split_axis=0,
            concat_axis=0,
            tiled=True,
        ).astype(jnp.float32),
        lax.all_to_all(
            grad_input.reshape(dp_count, piece_rows, model_width).astype(jnp.bfloat16),
            "dp",
            split_axis=0,
            concat_axis=0,
            tiled=True,
        ).astype(jnp.float32),
    )
    back_out = back_out.reshape(experts, capacity, model_width)
    back_grad = back_grad.reshape(experts * capacity, model_width)
    flat_slots = slot_table.reshape(-1)
    combined = empty_rows.at[flat_slots].add(
        (back_out * gate_table[:, :, None]).reshape(-1, model_width)
    )
    grad_acc = empty_rows.at[flat_slots].add(back_grad)
    grad_both = jnp.concatenate([grad_gate, grad_up], axis=1)
    grad_cols = jnp.concatenate(
        [
            lax.dot_general(rows_in, grad_both, contract_rows, preferred_element_type=jnp.float32),
            lax.dot_general(rows_grad, act_low, contract_rows, preferred_element_type=jnp.float32),
        ],
        axis=1,
    )
    returned = lax.all_to_all(
        grad_cols[None].astype(jnp.bfloat16), "dp", split_axis=1, concat_axis=0, tiled=True
    ).astype(jnp.float32)
    summed = jnp.sum(returned.reshape(experts, group, dp_rows, 3 * hidden_units), axis=1)
    grad_w_gate = summed[:, :, :hidden_units]
    grad_w_up = summed[:, :, hidden_units : 2 * hidden_units]
    grad_w_down = jnp.transpose(summed[:, :, 2 * hidden_units :], (0, 2, 1))
    output = (hidden + scatter_rows(combined[:seq_len])).astype(jnp.bfloat16)
    grad_two = scatter_rows(grad_acc[:seq_len])
    ffn_gain_part = jnp.sum(grad_two * hidden * inverse_two, axis=0)
    grad_hidden = cotangent.astype(jnp.float32) + norm_backward(
        grad_two, hidden, inverse_two, ffn_gain
    )
    grad_attn = gather_rows(grad_hidden.astype(jnp.bfloat16))
    grad_mixed = lax.dot_general(
        grad_attn, full_out, contract, preferred_element_type=jnp.float32
    ).astype(jnp.bfloat16)
    grad_mixed_heads = grad_mixed.reshape(seq_len, local_kv, group_size, head_dim).transpose(
        1, 0, 2, 3
    )
    grad_query_heads, grad_key_heads, grad_value_heads = lax.map(
        head_backward, (query_heads, key_heads, value_heads, logsum, grad_mixed_heads)
    )
    grad_query_rot = (
        grad_query_heads.transpose(1, 0, 2, 3).reshape(seq_len, local_heads, head_dim) * attn_scale
    )
    grad_query_norm = rotate_back(grad_query_rot, cosine, sine_table)
    query_gain_part = jnp.sum(grad_query_norm * query_raw * query_inverse, axis=(0, 1))
    grad_query_low = (
        norm_backward(grad_query_norm, query_raw, query_inverse, query_gain)
        .astype(jnp.bfloat16)
        .reshape(seq_len, local_heads * head_dim)
    )
    grad_key_norm = rotate_back(grad_key_heads.transpose(1, 0, 2), cosine, sine_table)
    key_gain_part = jnp.sum(grad_key_norm * key_raw * key_inverse, axis=(0, 1))
    grad_key_low = (
        norm_backward(grad_key_norm, key_raw, key_inverse, key_gain)
        .astype(jnp.bfloat16)
        .reshape(seq_len, local_kv * head_dim)
    )
    grad_value_low = (
        grad_value_heads.transpose(1, 0, 2)
        .reshape(seq_len, local_kv * head_dim)
        .astype(jnp.bfloat16)
    )
    grad_proj = jnp.concatenate([grad_query_low, grad_key_low, grad_value_low], axis=1)
    full_proj = jnp.concatenate([full_query, full_key, full_value], axis=1)
    grad_one = scatter_rows(
        lax.dot_general(grad_proj, full_proj, contract, preferred_element_type=jnp.float32)
    )
    first_part = jnp.einsum("sd,sf->df", seq_normed, grad_proj, preferred_element_type=jnp.float32)
    second = jnp.einsum("sd,sf->df", grad_attn, mixed_flat, preferred_element_type=jnp.float32)
    shares = lax.psum_scatter(
        jnp.concatenate([first_part, second], axis=1), "dp", scatter_dimension=0, tiled=True
    )
    query_cols = w_query.shape[1]
    key_cols = w_key.shape[1]
    grad_w_query = shares[:, :query_cols]
    grad_w_key = shares[:, query_cols : query_cols + key_cols]
    grad_w_value = shares[:, query_cols + key_cols : query_cols + 2 * key_cols]
    grad_w_out = jnp.transpose(shares[:, query_cols + 2 * key_cols :])
    attn_gain_part = jnp.sum(grad_one * residual * inverse_one, axis=0)
    grad_tokens = (grad_hidden + norm_backward(grad_one, residual, inverse_one, attn_gain)).astype(
        jnp.bfloat16
    )
    total_gains = lax.psum(
        (attn_gain_part, ffn_gain_part, query_gain_part, key_gain_part), ("dp", "tensor")
    )
    return (
        output,
        grad_tokens,
        grad_w_query,
        grad_w_key,
        grad_w_value,
        grad_w_out,
        grad_w_gate,
        grad_w_up,
        grad_w_down,
        total_gains[0],
        total_gains[1],
        total_gains[2],
        total_gains[3],
    )


def per_device_relay(
    tokens,
    cotangent,
    expert_ids,
    gate_values,
    w_query,
    w_key,
    w_value,
    w_out,
    w_gate,
    w_up,
    w_down,
    attn_gain,
    ffn_gain,
    query_gain,
    key_gain,
):
    dot = functools.partial(jnp.dot, preferred_element_type=jnp.float32)
    dot_t = functools.partial(lax.dot_general, dimension_numbers=(((1,), (1,)), ((), ())), preferred_element_type=jnp.float32)
    t_dot = functools.partial(lax.dot_general, dimension_numbers=(((0,), (0,)), ((), ())), preferred_element_type=jnp.float32)
    low = jnp.bfloat16
    rows, width = tokens.shape
    head_dim = query_gain.shape[0]
    experts = w_gate.shape[0]
    core = lax.axis_index("tensor")
    mine = lax.dynamic_slice_in_dim(expert_ids, core * rows, rows, 0)
    values = lax.dynamic_slice_in_dim(gate_values, core * rows, rows, 0)
    match = mine[None] == jnp.arange(experts, dtype=jnp.int32)[:, None, None]
    gates = jnp.sum(jnp.where(match, values[None], 0.0), axis=2)
    gates = jnp.broadcast_to(gates[:, None], (experts, 8, rows))

    q_cols, kv_cols = w_query.shape[1] // 2, w_key.shape[1] // 2
    w_out_rows = jnp.transpose(w_out)
    halves = jnp.stack(
        [
            jnp.concatenate([w[:, h * (w.shape[1] // 2) : (h + 1) * (w.shape[1] // 2)] for w in (w_query, w_key, w_value, w_out_rows)], axis=1)
            for h in range(2)
        ]
    )
    residual = tokens.astype(jnp.float32)
    inverse_one = rms_inverse(residual)
    normed_one = (residual * inverse_one * attn_gain).astype(low)
    weights, rows_grad, gates, seq_normed, *projections = gather_first(halves, cotangent, gates, normed_one, (w_gate, w_up, w_down), 1)
    weights, gates, seq_normed = weights.reshape(-1, weights.shape[2]), gates[:, 0][:, :, None], seq_normed.reshape(-1, width)
    proj_cols = q_cols + 2 * kv_cols
    w_proj, w_back = weights[:, :proj_cols], weights[:, proj_cols:]

    seq_len = 2 * rows
    group = q_cols // head_dim
    scale = head_dim ** (-0.5)
    cosine, sine_table = rotary_tables(seq_len, head_dim)
    proj = dot(seq_normed, w_proj)
    query_raw = proj[:, :q_cols].reshape(2, seq_len, group, head_dim)
    key_raw = proj[:, q_cols : q_cols + kv_cols].reshape(2, seq_len, 1, head_dim)
    value_low = proj[:, q_cols + kv_cols :].astype(low).reshape(2, seq_len, head_dim)
    query_inverse, key_inverse = rms_inverse(query_raw), rms_inverse(key_raw)
    query_low = (rotate(query_raw * query_inverse * query_gain, cosine, sine_table) * scale).astype(low)
    key_low = rotate(key_raw * key_inverse * key_gain, cosine, sine_table).astype(low)[:, :, 0]
    causal = jnp.arange(seq_len)[:, None] >= jnp.arange(seq_len)[None, :]
    scores = jnp.einsum("bqgd,bsd->bgqs", query_low, key_low, preferred_element_type=jnp.float32)
    exp_scores = jnp.where(causal, jnp.exp(scores), 0.0)
    probs = exp_scores / jnp.sum(exp_scores, axis=-1, keepdims=True)
    probs_low = probs.astype(low)
    mixed = jnp.einsum("bgqs,bsd->bqgd", probs_low, value_low, preferred_element_type=jnp.float32).astype(low).reshape(2 * seq_len, q_cols)
    hidden = residual + scatter_four(dot_t(mixed, w_back).astype(low).reshape(2, 2, rows, width), 5)
    inverse_two = rms_inverse(hidden)
    normed_two = (hidden * inverse_two * ffn_gain).astype(low)
    share, grad_two, gu_part, down_part, _ = expert_layer(normed_two, rows_grad, gates, *projections, 2)
    ffn_gain_part = jnp.sum(grad_two * hidden * inverse_two, axis=0)
    grad_hidden = cotangent.astype(jnp.float32) + norm_backward(grad_two, hidden, inverse_two, ffn_gain)
    gains = jnp.pad(ffn_gain_part, (width, 1024)).reshape(-1, 128)
    raw = proj[:, : q_cols + kv_cols]
    lows = jnp.concatenate([v.reshape(2 * seq_len, -1) for v in (query_low, key_low, value_low)], axis=1)
    rope = jnp.stack([jnp.concatenate([v, w], axis=1) for v, w in ((cosine[:, 0], cosine[:, 0]), (sine_table[:, 0], -sine_table[:, 0]))])
    gain = jnp.stack([query_gain, key_gain])[:, None]
    grad_one, moe, shares, totals, *grads_moe = attention_back(
        grad_hidden.astype(low), weights, seq_normed, raw, lows, mixed, rope, gain, residual * inverse_one, gains, gu_part, down_part, share, 9
    )
    output = (hidden + moe).astype(low)
    grad_w_gate, grad_w_up, grad_w_down = [v.astype(jnp.float32) for v in grads_moe]
    grad_w_down = jnp.transpose(grad_w_down, (0, 2, 1))
    shares, totals = shares.astype(jnp.float32), totals.reshape(-1)
    stops = (0, q_cols, q_cols + kv_cols, proj_cols, proj_cols + q_cols)
    grads = [jnp.concatenate([shares[0, :, a:b], shares[1, :, a:b]], axis=1) for a, b in zip(stops, stops[1:])]
    grad_tokens = (grad_hidden + norm_backward(grad_one, residual, inverse_one, attn_gain)).astype(low)
    totals = jnp.split(totals, (width, 2 * width, 2 * width + head_dim, 2 * width + 2 * head_dim))[:4]
    return (output, grad_tokens, grads[0], grads[1], grads[2], jnp.transpose(grads[3]), grad_w_gate, grad_w_up, grad_w_down, *totals)


def solution(mesh):
    return jax.shard_map(
        per_device_relay if tuple(mesh.shape.values()) == (16, 2) else per_device_any,
        mesh=mesh,
        in_specs=(
            P(("dp", "tensor"), None),
            P(("dp", "tensor"), None),
            P("dp", None),
            P("dp", None),
            P("dp", "tensor"),
            P("dp", "tensor"),
            P("dp", "tensor"),
            P("tensor", "dp"),
            P(None, "dp", "tensor"),
            P(None, "dp", "tensor"),
            P(None, "tensor", "dp"),
            P(),
            P(),
            P(),
            P(),
        ),
        out_specs=(
            P(("dp", "tensor"), None),
            P(("dp", "tensor"), None),
            P("dp", "tensor"),
            P("dp", "tensor"),
            P("dp", "tensor"),
            P("tensor", "dp"),
            P(None, "dp", "tensor"),
            P(None, "dp", "tensor"),
            P(None, "tensor", "dp"),
            P(),
            P(),
            P(),
            P(),
        ),
        check_vma=False,
    )
```

```python
import functools

import jax
import jax.numpy as jnp
from jax import lax
from jax.experimental import pallas as pl
from jax.experimental.pallas import tpu as pltpu
from jax.sharding import PartitionSpec as P

epsilon = 1e-06
theta_base = 1000000.0


def rms_inverse(values):
    return lax.rsqrt(jnp.mean(values * values, axis=-1, keepdims=True) + epsilon)


def norm_backward(grad_in, values, inverse, gain_vec):
    scaled = grad_in * gain_vec
    inner_mean = jnp.mean(scaled * values, axis=-1, keepdims=True)
    return inverse * scaled - values * inverse**3 * inner_mean


def rotary_tables(seq_len, head_dim):
    half_dim = head_dim // 2
    frequency = theta_base ** (-jnp.arange(half_dim, dtype=jnp.float32) * 2.0 / head_dim)
    angles = jnp.arange(seq_len, dtype=jnp.float32)[:, None] * frequency[None, :]
    return (jnp.cos(angles)[:, None, :], jnp.sin(angles)[:, None, :])


def rotate(values, cosine, sine_table):
    half_dim = values.shape[-1] // 2
    first_part = values[..., :half_dim]
    second = values[..., half_dim:]
    return jnp.concatenate(
        [first_part * cosine - second * sine_table, second * cosine + first_part * sine_table],
        axis=-1,
    )


def rotate_back(grad_in, cosine, sine_table):
    half_dim = grad_in.shape[-1] // 2
    first_part = grad_in[..., :half_dim]
    second = grad_in[..., half_dim:]
    return jnp.concatenate(
        [first_part * cosine + second * sine_table, second * cosine - first_part * sine_table],
        axis=-1,
    )


def dispatch(expert_ids, gate_values, experts, capacity):
    seq_len = expert_ids.shape[0]
    is_match = expert_ids[:, :, None] == jnp.arange(experts, dtype=jnp.int32)[None, None, :]
    expert_hits = jnp.sum(is_match.astype(jnp.int32), axis=1)
    before = jnp.cumsum(expert_hits, axis=0) - expert_hits
    slot_ids = jnp.sum(jnp.where(is_match, before[:, None, :], 0), axis=2)
    token_index = jnp.broadcast_to(jnp.arange(seq_len, dtype=jnp.int32)[:, None], expert_ids.shape)
    slot_table = (
        jnp.full((experts, capacity), seq_len, jnp.int32).at[expert_ids, slot_ids].set(token_index)
    )
    gate_table = (
        jnp.zeros((experts, capacity), jnp.float32).at[expert_ids, slot_ids].set(gate_values)
    )
    return (slot_table, gate_table)


def head_forward(head_inputs):
    query_vals, key_vals, value_vals = head_inputs
    seq_len = key_vals.shape[0]
    block_rows = min(512, seq_len)
    key_positions = jnp.arange(seq_len)

    def one_block(row_start):
        scores = jnp.einsum("qgd,sd->gqs", query_vals, key_vals, preferred_element_type=jnp.float32)
        causal = (row_start + jnp.arange(block_rows))[:, None] >= key_positions[None, :]
        exp_scores = jnp.where(causal, jnp.exp(scores), 0.0)
        denominator = jnp.sum(exp_scores, axis=-1, keepdims=True)
        softmax_low = (exp_scores / denominator).astype(jnp.bfloat16)
        mixed_out = jnp.einsum(
            "gqs,sd->qgd", softmax_low, value_vals, preferred_element_type=jnp.float32
        )
        return (mixed_out.astype(jnp.bfloat16), jnp.log(denominator[..., 0]))

    block_starts = jnp.arange(seq_len // block_rows, dtype=jnp.int32) * block_rows
    mixed_out, logsum = lax.map(one_block, block_starts)
    return (mixed_out.reshape(seq_len, query_vals.shape[1], query_vals.shape[2]), logsum)


def head_backward(head_inputs):
    query_vals, key_vals, value_vals, logsum, grad_mixed = head_inputs
    seq_len = key_vals.shape[0]
    block_rows = min(512, seq_len)
    key_positions = jnp.arange(seq_len)

    def one_block(state_in, block_in):
        grad_key, grad_value = state_in
        row_start, block_logsum = block_in
        scores = jnp.einsum("qgd,sd->gqs", query_vals, key_vals, preferred_element_type=jnp.float32)
        causal = (row_start + jnp.arange(block_rows))[:, None] >= key_positions[None, :]
        softmax_vals = jnp.where(causal, jnp.exp(scores - block_logsum[..., None]), 0.0)
        grad_probs = jnp.einsum(
            "qgd,sd->gqs", grad_mixed, value_vals, preferred_element_type=jnp.float32
        )
        delta_sum = jnp.sum(grad_probs * softmax_vals, axis=-1, keepdims=True)
        grad_scores = (softmax_vals * (grad_probs - delta_sum)).astype(jnp.bfloat16)
        grad_query = jnp.einsum(
            "gqs,sd->qgd", grad_scores, key_vals, preferred_element_type=jnp.float32
        )
        grad_key = grad_key + jnp.einsum(
            "gqs,qgd->sd", grad_scores, query_vals, preferred_element_type=jnp.float32
        )
        grad_value = grad_value + jnp.einsum(
            "gqs,qgd->sd",
            softmax_vals.astype(jnp.bfloat16),
            grad_mixed,
            preferred_element_type=jnp.float32,
        )
        return ((grad_key, grad_value), grad_query)

    block_starts = jnp.arange(seq_len // block_rows, dtype=jnp.int32) * block_rows
    zero_rows = jnp.zeros(key_vals.shape, jnp.float32)
    (grad_key, grad_value), grad_query = lax.scan(
        one_block, (zero_rows, zero_rows), (block_starts, logsum)
    )
    return (grad_query.reshape(query_vals.shape), grad_key, grad_value)


def gather_rows(values):
    return lax.all_gather(values, "tensor", axis=0, tiled=True)


def scatter_rows(values):
    return lax.psum_scatter(
        values.astype(jnp.bfloat16), "tensor", scatter_dimension=0, tiled=True
    ).astype(jnp.float32)


def widen(stacked, group):
    experts = stacked.shape[0]
    spread = jnp.broadcast_to(stacked[:, None], (experts, group) + stacked.shape[1:])
    return spread.reshape((experts * group,) + stacked.shape[1:])


MESH = pl.DeviceIdType.MESH
LIMIT = 66_000_000


class Place:
    def __init__(self):
        self.dp = lax.axis_index("dp")
        self.core = lax.axis_index("tensor")
        x, y = self.dp % 2, (self.dp // 2) % 2
        self.z = self.dp // 4
        step_x, step_y = 1 - 2 * x, 2 * (1 - 2 * y)
        self.da = (1 - self.core) * step_x + self.core * step_y
        self.db = (1 - self.core) * step_y + self.core * step_x
        self.half = self.z % 2
        self.pair = 4 * (1 - 2 * self.half)
        self.far = 8 * (1 - 2 * (self.z // 2))

    def copy(self, src, dst, send_sem, recv_sem, to, core=None):
        return pltpu.make_async_remote_copy(
            src_ref=src,
            dst_ref=dst,
            send_sem=send_sem,
            recv_sem=recv_sem,
            device_id=(to, self.core if core is None else core),
            device_id_type=MESH,
        )

    def at_z(self, z):
        return self.dp + 4 * (z - self.z)

    def z_of(self, m):
        low = self.z < 2
        depth = jnp.where(low, self.z, 3 - self.z)
        t = jnp.where(m == 0, depth, jnp.where(m == 1, 1 - depth, m))
        return jnp.where(low, t, 3 - t)

    def block(self, n):
        return self.at_z(self.z_of(n // 2)) + (n % 2) * self.da

    def greet(self, line=False, column=False, near=False, chain=False, everyone=False, partner=False):
        barrier = pltpu.get_barrier_semaphore()
        count = 0

        def signal(to, core):
            pl.semaphore_signal(barrier, inc=1, device_id=(to, core), device_id_type=MESH)

        if everyone:
            for r in range(1, 16):
                signal((self.dp + r) % 16, self.core)
            count = count + 15
        else:
            if near:
                signal(self.dp + self.da, self.core)
                signal(self.dp + self.db, self.core)
                count = count + 2
            if chain:
                signal(self.dp + self.pair, self.core)
                count = count + 1
                if near:
                    signal(self.dp + self.far, self.core)
                    count = count + 1
            if column:
                for r in range(1, 4):
                    signal((self.dp + 4 * r) % 16, self.core)
                count = count + 3
            if line:
                pl.when(self.z > 0)(lambda: signal(self.dp - 4, self.core))
                pl.when(self.z < 3)(lambda: signal(self.dp + 4, self.core))
                count = count + jnp.where(self.z > 0, 1, 0) + jnp.where(self.z < 3, 1, 0)
        if partner:
            signal(self.dp, 1 - self.core)
            count = count + 1
        pl.semaphore_wait(barrier, count)


def add_rows(target, terms, rows, block=16):
    def body(i, _):
        at = pl.ds(pl.multiple_of(i * block, block), block)
        total = terms[0][at, :].astype(jnp.float32)
        for term in terms[1:]:
            total = total + term[at, :].astype(jnp.float32)
        target[at, :] = total.astype(target.dtype)
        return 0

    lax.fori_loop(0, rows // block, body, 0)


def run(*threads):
    threads = list(threads)
    while threads:
        for thread in list(threads):
            if next(thread, "end") == "end":
                threads.remove(thread)


class Threads:
    def __init__(self, *threads):
        self.threads = list(threads)

    def step(self, times=1):
        for _ in range(times):
            for thread in list(self.threads):
                if next(thread, "end") == "end":
                    self.threads.remove(thread)

    def finish(self):
        while self.threads:
            self.step()


def lagged(items, first, second, lag):
    for n in range(len(items) + lag):
        if n < len(items):
            first(items[n])
            yield
        if n >= lag:
            second(items[n - lag])
            yield


def gather_line(me, x_ref, out_ref, send_sem, recv_sem):
    def part(source, to, slot, own=False):
        return me.copy(x_ref if own else out_ref.at[source], out_ref.at[source], send_sem.at[slot], recv_sem.at[source], to)

    sides = ((-1, me.z < 3, 4), (1, me.z > 0, -4))

    def exists(d, side):
        return (me.z - d >= 0) if side == 0 else (me.z + d <= 3)

    def slot_z(d, side, j):
        return 4 + ((d - 1) * 2 + side) * 3 + j

    def slot_a(off):
        return 25 + off

    def pass_a(off):
        source = me.dp + me.da + 4 * off
        part(source, me.dp, slot_a(off)).wait_recv()
        part(source, me.dp + me.db, slot_a(off)).start()

    pl.when(me.z < 3)(lambda: part(me.dp, me.dp + 4, 0, True).start())
    pl.when(me.z > 0)(lambda: part(me.dp, me.dp - 4, 1, True).start())
    part(me.dp, me.dp + me.db, 3, True).start()
    part(me.dp, me.dp + me.da, 2, True).start()
    yield
    for d in range(1, 5):
        if d < 4:
            for side, (sign, forward, step) in enumerate(sides):
                source = me.dp + 4 * sign * d

                def arrive():
                    part(source, me.dp, slot_z(d, side, 0)).wait_recv()
                    pl.when(forward)(lambda: part(source, me.dp + step, slot_z(d, side, 0)).start())
                    part(source, me.dp + me.db, slot_z(d, side, 2)).start()
                    part(source, me.dp + me.da, slot_z(d, side, 1)).start()

                pl.when(exists(d, side))(arrive)
                yield
        if d == 1:
            pass_a(0)
            yield
        else:
            for side, (sign, *_) in enumerate(sides):
                pl.when(exists(d - 1, side))(lambda: pass_a(sign * (d - 1)))
                yield
    for z in range(4):
        for g in (0, 1):
            part(me.at_z(z) + me.db + g * me.da, me.dp, 0).wait_recv()
            yield

    def sent(slot):
        part(me.dp, me.dp, slot).wait_send()

    pl.when(me.z < 3)(lambda: sent(0))
    pl.when(me.z > 0)(lambda: sent(1))
    sent(2)
    sent(3)
    sent(slot_a(0))
    for d in range(1, 4):
        for side, (sign, forward, _) in enumerate(sides):

            def finish():
                pl.when(forward)(lambda: sent(slot_z(d, side, 0)))
                sent(slot_z(d, side, 1))
                sent(slot_z(d, side, 2))
                sent(slot_a(sign * d))

            pl.when(exists(d, side))(finish)


def gather_pairs(me, x_ref, out_ref, send_sem, recv_sem):
    mine, other = me.dp, me.dp + me.pair

    def part(src, where, to, slot):
        return me.copy(src, out_ref.at[where], send_sem.at[slot], recv_sem.at[where], to)

    def relay(where, to, slot):
        part(out_ref.at[where], where, to, slot).start()

    def arrived(where):
        part(out_ref.at[where], where, me.dp, 0).wait_recv()

    part(x_ref.at[1 - me.half], mine, other, 0).start()
    part(x_ref.at[me.half], mine, me.dp + me.far, 1).start()
    part(x_ref.at[me.half], mine, me.dp + me.db, 2).start()
    part(x_ref.at[me.half], mine, me.dp + me.da, 3).start()
    yield
    arrived(other)
    relay(other, me.dp + me.far, 4)
    relay(other, me.dp + me.db, 5)
    relay(other, me.dp + me.da, 6)
    yield
    arrived(mine + me.da)
    relay(mine + me.da, me.dp + me.db, 7)
    yield
    arrived(mine + me.far)
    relay(mine + me.far, me.dp + me.db, 8)
    relay(mine + me.far, me.dp + me.da, 9)
    yield
    arrived(other + me.da)
    relay(other + me.da, me.dp + me.db, 10)
    yield
    arrived(other + me.far)
    relay(other + me.far, me.dp + me.db, 11)
    relay(other + me.far, me.dp + me.da, 12)
    yield
    arrived(mine + me.far + me.da)
    relay(mine + me.far + me.da, me.dp + me.db, 13)
    yield
    arrived(other + me.far + me.da)
    relay(other + me.far + me.da, me.dp + me.db, 14)
    yield
    for base in (mine, other, mine + me.far, other + me.far):
        arrived(base + me.db)
        yield
        arrived(base + me.da + me.db)
        yield
    for slot in range(15):
        part(out_ref.at[mine], mine, me.dp, slot).wait_send()


def swap_rows(me, x_ref, out_ref, send_sem, recv_sem):
    for r in range(1, 16):
        to = (me.dp + r) % 16
        me.copy(x_ref.at[to], out_ref.at[me.dp], send_sem.at[r], recv_sem.at[r], to).start()
    yield
    for r in range(1, 16):
        s = (me.dp + 16 - r) % 16
        me.copy(x_ref.at[s], out_ref.at[s], send_sem.at[r], recv_sem.at[r], me.dp).wait_recv()
    for r in range(1, 16):
        me.copy(x_ref.at[me.dp], out_ref.at[me.dp], send_sem.at[r], recv_sem.at[r], me.dp).wait_send()


def keep_own(src, staging, dst, sems):
    load = pltpu.make_async_copy(src, staging, sems.at[0])
    store = pltpu.make_async_copy(staging, dst, sems.at[1])
    load.start()

    def finish():
        load.wait()
        store.start()
        store.wait()

    return finish


def share_experts(me, ins, outs, send_sem, recv_sem):
    depth = ins[0].shape[1]

    def sends(r):
        to = (me.dp + r) % 16
        at = pl.ds(pl.multiple_of(me.dp * depth, depth), depth)
        pairs = ((ins[0].at[to], outs[0].at[at]), (ins[1].at[to], outs[1].at[at]), (ins[2].at[to], outs[2].at[:, at]))
        return [me.copy(src, dst, send_sem.at[r, j], recv_sem.at[r, j], to) for j, (src, dst) in enumerate(pairs)]

    for r in (8, 7, 9, 4, 12, 5, 11, 6, 10, 3, 13, 2, 14, 1, 15):
        for c in sends(r):
            c.start()
        yield
    for r in range(1, 16):
        at = pl.ds(pl.multiple_of((me.dp + 16 - r) % 16 * depth, depth), depth)
        for j, dst in enumerate((outs[0].at[at], outs[1].at[at], outs[2].at[:, at])):
            me.copy(dst, dst, send_sem.at[r, j], recv_sem.at[r, j], me.dp).wait_recv()
    for r in range(1, 16):
        for c in sends(r):
            c.wait_send()


def gather_four(me, x_ref, out_ref, send_sem, recv_sem):
    mine, theirs = out_ref.at[me.half, me.core], out_ref.at[1 - me.half, me.core]
    across = me.copy(x_ref, mine, send_sem.at[0], recv_sem.at[0], me.dp + me.pair)
    across.start()
    beside = me.copy(x_ref, mine, send_sem.at[1], recv_sem.at[1], me.dp, 1 - me.core)
    beside.start()
    mine[...] = x_ref[...]
    yield
    across.wait_recv()
    relay = me.copy(theirs, theirs, send_sem.at[2], recv_sem.at[2], me.dp, 1 - me.core)
    relay.start()
    yield
    across.wait_send()
    beside.wait()
    relay.wait()


def attention_first_kernel(
    head_dim, start,
    w_ref, c_ref, g_ref, x_ref, rope_ref, gain_ref, gate_ref, up_ref, down_ref,
    w_out, c_out, g_out, seq, raw, low, mixed, sum_ref, gate_out, up_out, down_out,
    w, c_own, e_own, part, from_core, from_pair,
    w_send, w_recv, c_send, c_recv, g_send, g_recv, x_send, x_recv, e_send, e_recv, back_send, back_recv, copy_sem,
):
    me = Place()
    rows, width = x_ref.shape
    seq_len = 2 * rows
    q_cols = mixed.shape[1]
    proj_cols = q_cols + 2 * head_dim
    group = q_cols // head_dim
    depth = gate_ref.shape[1]
    dot = functools.partial(jnp.dot, preferred_element_type=jnp.float32)
    dot_t = functools.partial(lax.dot_general, dimension_numbers=(((1,), (1,)), ((), ())), preferred_element_type=jnp.float32)
    at_mine = pl.ds(pl.multiple_of(me.dp * depth, depth), depth)
    ends = [
        keep_own(c_ref, c_own, c_out.at[me.dp], copy_sem.at[1]),
        keep_own(gate_ref.at[me.dp], e_own.at[0], gate_out.at[at_mine], copy_sem.at[2]),
        keep_own(up_ref.at[me.dp], e_own.at[1], up_out.at[at_mine], copy_sem.at[3]),
    ]
    flat = pltpu.make_async_copy(down_ref.at[me.dp], down_out.at[:, at_mine], copy_sem.at[4, 0])
    flat.start()
    kept = pltpu.make_async_copy(w_ref.at[me.half], w.at[me.dp], copy_sem.at[0, 0])
    kept.start()
    g_out[me.dp] = g_ref[me.dp]
    me.greet(everyone=True, partner=True)
    beside = Threads(
        swap_rows(me, g_ref, g_out, g_send, g_recv),
        share_experts(me, (gate_ref, up_ref, down_ref), (gate_out, up_out, down_out), e_send, e_recv),
    )
    needed = Threads(gather_four(me, x_ref, seq, x_send, x_recv), gather_pairs(me, w_ref, w, w_send, w_recv))
    rounds = 0
    while needed.threads:
        needed.step()
        if rounds == start:
            beside.threads.insert(0, gather_line(me, c_ref, c_out, c_send, c_recv))
        beside.step()
        rounds += 1
    kept.wait()
    store = pltpu.make_async_copy(w, w_out, copy_sem.at[0, 1])
    store.start()
    weights = w.reshape(16 * rows, w.shape[2])

    def row_block(ref, h, core):
        return ref.at[pl.ds(pl.multiple_of((2 * h + core) * rows, rows), rows)]

    seqs = seq.reshape(4 * rows, width)
    q_part, k_part = pl.ds(0, q_cols), pl.ds(q_cols, 2 * head_dim)

    def project(j, _):
        at = pl.ds(pl.multiple_of(j * 256, 256), 256)
        raw[:, at] = dot(seqs[...], weights[:, at])
        return 0

    lax.fori_loop(0, q_cols // 256, project, 0)
    keys = dot(seqs[...], weights[:, k_part])
    raw[:, pl.ds(q_cols, head_dim)] = keys[:, :head_dim]
    low[:, pl.ds(q_cols + head_dim, head_dim)] = keys[:, head_dim:].astype(low.dtype)
    beside.step()
    cosine, turn = rope_ref[0], rope_ref[1]

    def turned(at, cols, which, scale):
        values = raw[at, cols]
        values = values * lax.rsqrt(jnp.mean(values * values, axis=-1, keepdims=True) + epsilon) * gain_ref[which]
        return ((values * cosine - pltpu.roll(values, head_dim // 2, 1) * turn) * scale).astype(low.dtype)

    k_at, v_at = pl.ds(q_cols, head_dim), pl.ds(q_cols + head_dim, head_dim)
    for b in range(2):
        at = pl.ds(b * seq_len, seq_len)
        low[at, k_at] = turned(at, k_at, 1, 1.0)
    causal = lax.broadcasted_iota(jnp.int32, (seq_len, seq_len), 0) >= lax.broadcasted_iota(jnp.int32, (seq_len, seq_len), 1)

    def head(n, _):
        at = pl.ds(pl.multiple_of(n // group * seq_len, seq_len), seq_len)
        cols = pl.ds(pl.multiple_of(n % group * head_dim, head_dim), head_dim)
        query = turned(at, cols, 0, head_dim ** (-0.5))
        low[at, cols] = query
        exp_scores = jnp.where(causal, jnp.exp(dot_t(query, low[at, k_at])), 0.0)
        probs = exp_scores / jnp.sum(exp_scores, axis=-1, keepdims=True)
        mixed[at, cols] = dot(probs.astype(low.dtype), low[at, v_at]).astype(mixed.dtype)
        return 0

    quarter = group // 2
    for k in range(4):
        lax.fori_loop(k * quarter, (k + 1) * quarter, head, 0)
        beside.step()

    def project_back(j, _):
        at = pl.ds(pl.multiple_of(j * 256, 256), 256)
        part[:, at] = dot_t(mixed[...], weights[at, pl.ds(proj_cols, q_cols)]).astype(part.dtype)
        return 0

    lax.fori_loop(0, width // 256, project_back, 0)

    def give(h, slot):
        return me.copy(row_block(part, h, 1 - me.core), from_core.at[slot], back_send.at[slot], back_recv.at[slot], me.dp, 1 - me.core)

    give(1 - me.half, 0).start()
    give(me.half, 1).start()
    beside.step()
    give(1 - me.half, 0).wait_recv()
    add_rows(from_core.at[0], (row_block(part, 1 - me.half, me.core), from_core.at[0]), rows)
    over = me.copy(from_core.at[0], from_pair, back_send.at[2], back_recv.at[2], me.dp + me.pair)
    over.start()
    give(me.half, 1).wait_recv()
    add_rows(from_core.at[1], (row_block(part, me.half, me.core), from_core.at[1]), rows)
    beside.step()
    over.wait_recv()
    add_rows(sum_ref, (from_core.at[1], from_pair), rows)
    beside.finish()
    for end in ends:
        end()
    flat.wait()
    store.wait()
    give(0, 0).wait_send()
    give(0, 1).wait_send()
    over.wait_send()


def attention_first(weights, rows, gates, normed, rope, gain, experts, cid, start=4):
    hbm, vmem = pl.BlockSpec(memory_space=pl.ANY), pl.BlockSpec(memory_space=pltpu.VMEM)
    dma = pltpu.SemaphoreType.DMA
    dtype = rows.dtype
    _, depth, hidden = experts[0].shape
    block, width = rows.shape
    head_dim = rope.shape[-1]
    columns = weights.shape[2]
    q_cols = (columns - 2 * head_dim) // 2
    return pl.pallas_call(
        functools.partial(attention_first_kernel, head_dim, start),
        out_shape=[
            jax.ShapeDtypeStruct((16,) + weights.shape[1:], dtype),
            jax.ShapeDtypeStruct((16, block, width), dtype),
            jax.ShapeDtypeStruct(gates.shape, gates.dtype),
            jax.ShapeDtypeStruct((2, 2, block, width), dtype),
            jax.ShapeDtypeStruct((4 * block, q_cols + head_dim), jnp.float32),
            jax.ShapeDtypeStruct((4 * block, q_cols + 2 * head_dim), dtype),
            jax.ShapeDtypeStruct((4 * block, q_cols), dtype),
            jax.ShapeDtypeStruct((block, width), jnp.float32),
            jax.ShapeDtypeStruct((16 * depth, hidden), dtype),
            jax.ShapeDtypeStruct((16 * depth, hidden), dtype),
            jax.ShapeDtypeStruct((hidden, 16 * depth), dtype),
        ],
        in_specs=[hbm, hbm, vmem, vmem, vmem, vmem, hbm, hbm, hbm],
        out_specs=[hbm, hbm] + [vmem] * 6 + [hbm] * 3,
        scratch_shapes=[
            pltpu.VMEM((16,) + weights.shape[1:], dtype),
            pltpu.VMEM((block, width), dtype),
            pltpu.VMEM((2, depth, hidden), dtype),
            pltpu.VMEM((4 * block, width), dtype),
            pltpu.VMEM((2, block, width), dtype),
            pltpu.VMEM((block, width), dtype),
            dma((15,)), dma((16,)),
            dma((29,)), dma((16,)),
            dma((16,)), dma((16,)),
            dma((3,)), dma((3,)),
            dma((16, 3)), dma((16, 3)),
            dma((3,)), dma((3,)),
            dma((5, 2)),
        ],
        compiler_params=pltpu.CompilerParams(collective_id=cid, has_side_effects=True, vmem_limit_bytes=67_043_328),
        name="attention_first",
    )(weights, rows, gates, normed, rope, gain, *experts)


def scatter_pairs(me, chunks, share, make, out_ref, from_b, from_a, from_far, send_sem, recv_sem):
    rows = from_a.shape[1] // chunks
    other = me.dp + me.pair
    bases = (me.dp, other, me.dp + me.far, other + me.far)
    items = [(j, k) for j in (2, 3, 1, 0) for k in range(chunks)]

    def at(k):
        return pl.ds(k * rows, rows)

    def copy(src, dst, slot, k, to):
        return me.copy(src, dst, send_sem.at[slot, k], recv_sem.at[slot, k], to)

    def send_b(g, j, k):
        return copy(share(bases[j] + me.db + g * me.da).at[at(k)], from_b.at[g, j, at(k)], g * 4 + j, k, me.dp + me.db)

    def send_a(j, k):
        return copy(from_b.at[1, j, at(k)], from_a.at[j, at(k)], 8 + j, k, me.dp + me.da)

    def send_far(j, k):
        return copy(from_b.at[0, 2 + j, at(k)], from_far.at[j, at(k)], 12 + j, k, me.dp + me.far)

    def swap(k):
        return copy(from_b.at[0, 1, at(k)], out_ref.at[me.half, at(k)], 14, k, other)

    for j in (2, 3, 1, 0):
        for g in (1, 0):
            make(bases[j] + me.db + g * me.da)
            for k in range(chunks):
                send_b(g, j, k).start()
        if j == 3:
            yield
    for j in (2, 3, 1, 0):
        make(bases[j] + me.da)
        make(bases[j])
        if j == 3:
            yield
    yield

    def first(item):
        j, k = item
        send_b(1, j, k).wait_recv()
        add_rows(from_b.at[1, j, at(k)], (share(bases[j] + me.da).at[at(k)], from_b.at[1, j, at(k)]), rows)
        send_a(j, k).start()

    def second(item):
        j, k = item
        send_b(0, j, k).wait_recv()
        send_a(j, k).wait_recv()
        terms = (share(bases[j]).at[at(k)], from_b.at[0, j, at(k)], from_a.at[j, at(k)])
        if j >= 2:
            add_rows(from_b.at[0, j, at(k)], terms, rows)
            send_far(j - 2, k).start()
        else:
            send_far(j, k).wait_recv()
            target = from_b.at[0, 1, at(k)] if j else out_ref.at[me.half, at(k)]
            add_rows(target, terms + (from_far.at[j, at(k)],), rows)
            if j:
                swap(k).start()

    yield from lagged(items, first, second, 2)
    for k in range(chunks):
        swap(k).wait_send()
        theirs = out_ref.at[1 - me.half, at(k)]
        copy(theirs, theirs, 14, k, other).wait_recv()
        for j in range(4):
            send_b(0, j, k).wait_send()
            send_b(1, j, k).wait_send()
            send_a(j, k).wait_send()
        send_far(0, k).wait_send()
        send_far(1, k).wait_send()


def sum_all(me, out_ref, held, send_sem, recv_sem):
    steps = ((me.dp, 1 - me.core), (me.dp + me.da, me.core), (me.dp + me.db, me.core), (me.dp + me.pair, me.core), (me.dp + me.far, me.core))
    yield
    for n, (to, core) in enumerate(steps):
        send = me.copy(held.at[0, n], held.at[1, n], send_sem.at[n], recv_sem.at[n], to, core)
        held[0, n] = out_ref[...]
        send.start()
        yield
        send.wait()
        out_ref[...] = held[0, n] + held[1, n]
        yield


def return_experts(me, gu_ref, down_ref, outs, own, held, core_send, core_recv, send_sem, recv_sem, copy_sem):
    rows, half = outs[0].shape[1:]

    def views(d, core):
        at = pl.ds(pl.multiple_of(d * rows, rows), rows)
        starts = ((gu_ref, core * half), (gu_ref, 2 * half + core * half), (down_ref, core * half))
        return [ref.at[at, pl.ds(pl.multiple_of(start, 128), half)] for ref, start in starts]

    def beside(r):
        d = (me.dp + r) % 16
        return [
            me.copy(src, held.at[j, r], core_send.at[r, j], core_recv.at[r, j], me.dp, 1 - me.core)
            for j, src in enumerate(views(d, 1 - me.core))
        ]

    order = (8, 7, 9, 4, 12, 5, 11, 6, 10, 3, 13, 2, 14, 1, 15, 0)

    def loads(n):
        d = (me.dp + order[n]) % 16
        return [pltpu.make_async_copy(src, own.at[j, n % 8], copy_sem.at[n % 8, j]) for j, src in enumerate(views(d, me.core))]

    def sends(r):
        d = (me.dp + r) % 16
        return [me.copy(held.at[j, r], outs[j].at[me.dp], send_sem.at[r, j], recv_sem.at[r, j], d) for j in range(3)]

    for r in order:
        for c in beside(r):
            c.start()
    for n in range(8):
        for c in loads(n):
            c.start()
    yield
    keep = [pltpu.make_async_copy(held.at[j, 0], outs[j].at[me.dp], copy_sem.at[16, j]) for j in range(3)]
    for n, r in enumerate(order):
        for j, (arrives, load) in enumerate(zip(beside(r), loads(n))):
            arrives.wait_recv()
            load.wait()
            add_rows(held.at[j, r], (own.at[j, n % 8], held.at[j, r]), rows, 64)
        for c in sends(r) if r else keep:
            c.start()
        if n < 8:
            for c in loads(n + 8):
                c.start()
        if n % 2:
            yield
    for r in range(1, 16):
        s = (me.dp + 16 - r) % 16
        for j in range(3):
            dst = outs[j].at[s]
            me.copy(dst, dst, send_sem.at[r, j], recv_sem.at[r, j], me.dp).wait_recv()
    for c in keep:
        c.wait()
    for r in range(16):
        for c in beside(r) + (sends(r) if r else []):
            c.wait_send()


def attention_back_kernel(
    chunks, head_dim,
    ga_ref, w_ref, seq_ref, raw_ref, low_ref, mixed_ref, rope_ref, gain_ref, unit_ref, x_ref, gu_ref, down_ref, share_ref,
    one_ref, moe_ref, out_ref, sum_ref, gate_out, up_out, down_out,
    w, ga, gmix, gproj, part, kept, dk, dv, gains, from_core, from_pair,
    pair_b, pair_a, pair_far, total, own, held,
    from_b, from_a, from_z, b_send, b_recv, a_send, a_recv, z_send, z_recv,
    four_send, four_recv, back_send, back_recv, pair_send, pair_recv, sum_send, sum_recv, core_send, core_recv, e_send, e_recv,
    copy_sem, load_sem,
):
    me = Place()
    rows, width = ga_ref.shape
    seq_len = 2 * rows
    q_cols = mixed_ref.shape[1]
    proj_cols = q_cols + 2 * head_dim
    group = q_cols // head_dim
    dot = functools.partial(jnp.dot, preferred_element_type=jnp.float32)
    dot_t = functools.partial(lax.dot_general, dimension_numbers=(((1,), (1,)), ((), ())), preferred_element_type=jnp.float32)
    t_dot = functools.partial(lax.dot_general, dimension_numbers=(((0,), (0,)), ((), ())), preferred_element_type=jnp.float32)
    load = pltpu.make_async_copy(w_ref, w, load_sem.at[8])
    load.start()
    keeps = [pltpu.make_async_copy(share_ref.at[n, pl.ds(0, rows)], kept.at[n], load_sem.at[n]) for n in range(8)]
    for c in keeps:
        c.start()
    me.greet(everyone=True, partner=True)

    def ga_at(h, core):
        return ga.at[pl.ds(pl.multiple_of((2 * h + core) * rows, rows), rows)]

    mine, theirs = ga_at(me.half, me.core), ga_at(1 - me.half, me.core)
    across = me.copy(ga_ref, mine, four_send.at[0], four_recv.at[0], me.dp + me.pair)
    beside = me.copy(ga_ref, mine, four_send.at[1], four_recv.at[1], me.dp, 1 - me.core)
    relay = me.copy(theirs, theirs, four_send.at[2], four_recv.at[2], me.dp, 1 - me.core)
    across.start()
    beside.start()
    mine[...] = ga_ref[...]
    scatter = ScatterRows(
        me, lambda n: share_ref.at[n, pl.ds(rows, rows)], lambda n: kept.at[n], from_b, from_a, from_z,
        (b_send, b_recv, a_send, a_recv, z_send, z_recv),
    )
    for m in (1, 2, 3, 0):
        scatter.send_b(2 * m + 1).start()
        scatter.send_b(2 * m).start()
    experts = return_experts(me, gu_ref, down_ref, (gate_out, up_out, down_out), own, held, core_send, core_recv, e_send, e_recv, copy_sem)
    next(experts)
    across.wait_recv()
    relay.start()
    across.wait_send()
    beside.wait()
    next(experts)
    relay.wait()
    load.wait()
    for c in keeps:
        c.wait()

    def mix(j, _):
        at = pl.ds(pl.multiple_of(j * 256, 256), 256)
        at_w = pl.ds(pl.multiple_of(proj_cols + j * 256, 256), 256)
        gmix[:, at] = dot(ga[...], w[:, at_w]).astype(gmix.dtype)
        return 0

    lax.fori_loop(0, q_cols // 256, mix, 0)
    next(experts)
    gains[...] = jnp.zeros_like(gains)
    turn = rope_ref[1]
    cosine = rope_ref[0]
    causal = lax.broadcasted_iota(jnp.int32, (seq_len, seq_len), 0) >= lax.broadcasted_iota(jnp.int32, (seq_len, seq_len), 1)
    k_at, v_at = pl.ds(q_cols, head_dim), pl.ds(q_cols + head_dim, head_dim)

    def back(grad, raw, which):
        grad = grad * cosine + pltpu.roll(grad, head_dim // 2, 1) * turn
        inverse = lax.rsqrt(jnp.mean(raw * raw, axis=-1, keepdims=True) + epsilon)
        gains[which] = gains[which] + jnp.sum(grad * (raw * inverse), axis=0, keepdims=True)
        scaled = grad * gain_ref[which]
        inner = jnp.mean(scaled * raw, axis=-1, keepdims=True)
        return inverse * scaled - raw * (inverse * inverse * inverse) * inner

    def head(n, _):
        at = pl.ds(pl.multiple_of(n // group * seq_len, seq_len), seq_len)
        cols = pl.ds(pl.multiple_of(n % group * head_dim, head_dim), head_dim)
        query, key, value, grad = low_ref[at, cols], low_ref[at, k_at], low_ref[at, v_at], gmix[at, cols]
        exp_scores = jnp.where(causal, jnp.exp(dot_t(query, key)), 0.0)
        probs = exp_scores / jnp.sum(exp_scores, axis=-1, keepdims=True)
        grad_probs = dot_t(grad, value)
        delta = jnp.sum(grad_probs * probs, axis=-1, keepdims=True)
        grad_scores = (probs * (grad_probs - delta)).astype(query.dtype)
        grad_query = dot(grad_scores, key) * head_dim ** (-0.5)
        grad_key = t_dot(grad_scores, query)
        grad_value = t_dot(probs.astype(query.dtype), grad)

        def begin():
            dk[...] = grad_key
            dv[...] = grad_value

        def more():
            dk[...] = dk[...] + grad_key
            dv[...] = dv[...] + grad_value

        pl.when(n % group == 0)(begin)
        pl.when(n % group != 0)(more)
        gproj[at, cols] = back(grad_query, raw_ref[at, cols], 0).astype(gproj.dtype)

        def close():
            gproj[at, k_at] = back(dk[...], raw_ref[at, k_at], 1).astype(gproj.dtype)
            gproj[at, v_at] = dv[...].astype(gproj.dtype)

        pl.when(n % group == group - 1)(close)
        return 0

    heads = 2 * group
    quarter = heads // 4
    for k in range(4):
        lax.fori_loop(k * quarter, (k + 1) * quarter, head, 0)
        next(experts)
        scatter.first((1, 2, 3, 0)[k])
        if k:
            scatter.second((1, 2, 3, 0)[k - 1])

    def project(j, _):
        at = pl.ds(pl.multiple_of(j * 256, 256), 256)
        part[:, at] = dot_t(gproj[...], w[at, pl.ds(0, proj_cols)]).astype(part.dtype)
        return 0

    lax.fori_loop(0, width // 256, project, 0)

    def part_at(h, core):
        return part.at[pl.ds(pl.multiple_of((2 * h + core) * rows, rows), rows)]

    def give(h, slot):
        return me.copy(part_at(h, 1 - me.core), from_core.at[slot], back_send.at[slot], back_recv.at[slot], me.dp, 1 - me.core)

    give(1 - me.half, 0).start()
    give(me.half, 1).start()
    other = me.dp + me.pair
    bases = (me.dp, other, me.dp + me.far, other + me.far)

    def weight_block(d):
        at = pl.ds(pl.multiple_of(d * rows, rows), rows)
        w[at, pl.ds(0, proj_cols)] = t_dot(seq_ref[:, at], gproj[...]).astype(w.dtype)
        w[at, pl.ds(proj_cols, q_cols)] = t_dot(ga[:, at], mixed_ref[...]).astype(w.dtype)

    pairs = scatter_pairs(me, chunks, lambda d: w.at[pl.ds(pl.multiple_of(d * rows, rows), rows)], weight_block, out_ref, pair_b, pair_a, pair_far, pair_send, pair_recv)
    next(pairs)
    give(1 - me.half, 0).wait_recv()
    add_rows(from_core.at[0], (part_at(1 - me.half, me.core), from_core.at[0]), rows)
    over = me.copy(from_core.at[0], from_pair, back_send.at[2], back_recv.at[2], me.dp + me.pair)
    over.start()
    give(me.half, 1).wait_recv()
    add_rows(from_core.at[1], (part_at(me.half, me.core), from_core.at[1]), rows)
    next(pairs)
    scatter.second(0)
    next(experts)
    next(pairs)
    over.wait_recv()
    add_rows(one_ref, (from_core.at[1], from_pair), rows)
    sum_ref[...] = x_ref[...]
    attn = jnp.sum(one_ref[...] * unit_ref[...], axis=0, keepdims=True)
    for j in range(width // 128):
        sum_ref[pl.ds(j, 1), :] = attn[:, j * 128 : (j + 1) * 128]
    for j in range(2):
        sum_ref[pl.ds(2 * width // 128 + j, 1), :] = gains[j]
    scatter.finish(moe_ref)
    run(pairs, experts, sum_all(me, sum_ref, total, sum_send, sum_recv))
    scatter.drain()
    give(0, 0).wait_send()
    give(0, 1).wait_send()
    over.wait_send()


def attention_back(grad_attn, weights, seq_normed, raw, low, mixed, rope, gain, unit, sums, gu, down, share, cid, chunks=2):
    rows, width = grad_attn.shape
    head_dim = rope.shape[-1]
    columns = weights.shape[1]
    half = down.shape[1] // 2
    hbm, vmem = pl.BlockSpec(memory_space=pl.ANY), pl.BlockSpec(memory_space=pltpu.VMEM)
    dma = pltpu.SemaphoreType.DMA
    dtype = weights.dtype
    proj_cols = raw.shape[1] + head_dim
    whole = jax.ShapeDtypeStruct((rows, width), jnp.float32)
    return pl.pallas_call(
        functools.partial(attention_back_kernel, chunks, head_dim),
        out_shape=[whole, whole, jax.ShapeDtypeStruct((2, rows, columns), dtype), jax.ShapeDtypeStruct(sums.shape, sums.dtype)]
        + [jax.ShapeDtypeStruct((16, rows, half), dtype)] * 3,
        in_specs=[vmem, hbm] + [vmem] * 8 + [hbm] * 3,
        out_specs=[vmem] * 4 + [hbm] * 3,
        scratch_shapes=[
            pltpu.VMEM(weights.shape, dtype),
            pltpu.VMEM((4 * rows, width), dtype),
            pltpu.VMEM(mixed.shape, dtype),
            pltpu.VMEM((4 * rows, proj_cols), dtype),
            pltpu.VMEM((4 * rows, width), dtype),
            pltpu.VMEM((8, rows, width), dtype),
            pltpu.VMEM((2 * rows, head_dim), jnp.float32),
            pltpu.VMEM((2 * rows, head_dim), jnp.float32),
            pltpu.VMEM((2, 1, head_dim), jnp.float32),
            pltpu.VMEM((2, rows, width), dtype),
            pltpu.VMEM((rows, width), dtype),
            pltpu.VMEM((2, 4, rows, columns), dtype),
            pltpu.VMEM((4, rows, columns), dtype),
            pltpu.VMEM((2, rows, columns), dtype),
            pltpu.VMEM((2, 5) + sums.shape, sums.dtype),
            pltpu.VMEM((3, 8, rows, half), dtype),
            pltpu.VMEM((3, 16, rows, half), dtype),
            *scatter_rows_scratch(rows, width, dtype),
            dma((3,)), dma((3,)),
            dma((3,)), dma((3,)),
            dma((15, chunks)), dma((15, chunks)),
            dma((5,)), dma((5,)),
            dma((16, 3)), dma((16, 3)),
            dma((16, 3)), dma((16, 3)),
            dma((17, 3)), dma((9,)),
        ],
        compiler_params=pltpu.CompilerParams(collective_id=cid, has_side_effects=True, vmem_limit_bytes=67_043_328),
        name="attention_back",
    )(grad_attn, weights, seq_normed, raw, low, mixed, rope, gain, unit, sums, gu, down, share)


class ScatterRows:
    def __init__(self, me, sent, kept, from_b, from_a, from_z, sems):
        self.me, self.sent, self.kept = me, sent, kept
        self.from_b, self.from_a, self.from_z = from_b, from_a, from_z
        self.b_send, self.b_recv, self.a_send, self.a_recv, self.z_send, self.z_recv = sems
        self.rows = from_b.shape[1]

    def send_b(self, n):
        me = self.me
        return me.copy(self.sent(n), self.from_b.at[n], self.b_send.at[n], self.b_recv.at[n], me.dp + me.db)

    def send_a(self, m):
        me = self.me
        return me.copy(self.from_b.at[2 * m + 1], self.from_a.at[m], self.a_send.at[m], self.a_recv.at[m], me.dp + me.da)

    def send_z(self, m):
        me = self.me
        return me.copy(self.from_b.at[2 * m], self.from_z.at[me.z], self.z_send.at[m], self.z_recv.at[me.z], me.at_z(me.z_of(m)))

    def first(self, m):
        n = 2 * m + 1
        self.send_b(n).wait_recv()
        add_rows(self.from_b.at[n], (self.kept(n), self.from_b.at[n]), self.rows)
        self.send_a(m).start()

    def second(self, m):
        n = 2 * m
        self.send_b(n).wait_recv()
        self.send_a(m).wait_recv()
        add_rows(self.from_b.at[n], (self.kept(n), self.from_b.at[n], self.from_a.at[m]), self.rows)
        pl.when(m > 0)(lambda: self.send_z(m).start())

    def advance(self, now, lags=(1, 2)):
        for lag, call in zip(lags, (self.first, self.second)):
            m = (now - 1 - lag) // 2
            due = jnp.logical_and((now - 1 - lag) % 2 == 0, jnp.logical_and(now > lag, m < 4))
            pl.when(due)(lambda: call(m))

    def finish(self, out_ref):
        me = self.me
        others = [(me.z + r) % 4 for r in range(1, 4)]
        for z in others:
            me.copy(self.from_z.at[z], self.from_z.at[z], self.z_send.at[0], self.z_recv.at[z], me.dp).wait_recv()
        add_rows(out_ref, (self.from_b.at[0],) + tuple(self.from_z.at[z] for z in others), self.rows)

    def drain(self):
        for m in range(4):
            self.send_b(2 * m).wait_send()
            self.send_b(2 * m + 1).wait_send()
            self.send_a(m).wait_send()
            if m:
                self.send_z(m).wait_send()


def scatter_rows_scratch(rows, columns, dtype):
    dma = pltpu.SemaphoreType.DMA
    return [
        pltpu.VMEM((8, rows, columns), dtype),
        pltpu.VMEM((4, rows, columns), dtype),
        pltpu.VMEM((4, rows, columns), dtype),
        dma((8,)), dma((8,)), dma((4,)), dma((4,)), dma((4,)), dma((4,)),
    ]


def experts_kernel(
    x_ref, c_ref, g_ref, gate_ref, up_ref, down_ref,
    share_ref, two_ref, gu_out, down_out, xg_ref,
    wgu, wd, ag, ggu, share, p, xb, cb, from_b, from_a, from_z, b_send, b_recv, a_send, a_recv, z_send, z_recv,
    g_send, g_recv, w_send, w_recv, load_sem, tile_sem, keep_sem, share_sem,
):
    me = Place()
    rows, width = x_ref.shape
    hidden = wd.shape[0]
    half = hidden // 2
    dot = functools.partial(jnp.dot, preferred_element_type=jnp.float32)
    dot_t = functools.partial(lax.dot_general, dimension_numbers=(((1,), (1,)), ((), ())), preferred_element_type=jnp.float32)
    t_dot = functools.partial(lax.dot_general, dimension_numbers=(((0,), (0,)), ((), ())), preferred_element_type=jnp.float32)
    upper, lower = pl.ds(rows, rows), pl.ds(0, rows)

    z_of, block = me.z_of, me.block

    def part(source, to, slot, own=False):
        return me.copy(x_ref if own else xg_ref.at[source], xg_ref.at[source], g_send.at[slot], g_recv.at[source], to)

    def arrive(m):
        source = me.at_z(z_of(m))
        part(source, me.dp, 0).wait_recv()
        part(source, me.dp + me.db, 3 + 2 * m).start()
        part(source, me.dp + me.da, 4 + 2 * m).start()

    def arrive_a(m):
        source = me.at_z(z_of(m)) + me.da
        part(source, me.dp, 0).wait_recv()
        part(source, me.dp + me.db, 11 + m).start()

    def loads(n):
        slot = n % 2
        copies = []
        for j, source in enumerate((block(n), block(n) + me.db)):
            at = pl.ds(j * rows, rows)
            copies.append(pltpu.make_async_copy(xg_ref.at[source], xb.at[slot, at], load_sem.at[slot, j]))
            copies.append(pltpu.make_async_copy(c_ref.at[source], cb.at[slot, at], load_sem.at[slot, 2 + j]))
        return copies

    def fetch(n):
        part(block(n) + me.db, me.dp, 0).wait_recv()
        for c in loads(n):
            c.start()

    scatter = ScatterRows(
        me, lambda n: p.at[n, upper], lambda n: p.at[n, lower], from_b, from_a, from_z, (b_send, b_recv, a_send, a_recv, z_send, z_recv)
    )

    def keep_share(n):
        return pltpu.make_async_copy(share.at[n % 2], share_ref.at[n], share_sem.at[n % 2])

    own = p.at[7, lower]
    load = pltpu.make_async_copy(x_ref, own, keep_sem.at[0])
    store = pltpu.make_async_copy(own, xg_ref.at[me.dp], keep_sem.at[1])
    load.start()

    def half_of(core):
        at = core * half
        return (
            wgu.at[:, pl.ds(pl.multiple_of(at, 128), half)],
            wgu.at[:, pl.ds(pl.multiple_of(hidden + at, 128), half)],
            wd.at[pl.ds(pl.multiple_of(at, 128), half)],
        )

    mine = (gate_ref, up_ref, down_ref)
    locals_ = [pltpu.make_async_copy(src, dst, keep_sem.at[2 + j]) for j, (src, dst) in enumerate(zip(mine, half_of(me.core)))]
    for c in locals_:
        c.start()
    me.greet(column=True, near=True, partner=True)
    for m in range(1, 4):
        part(me.dp, me.at_z(z_of(m)), m - 1, True).start()
    part(me.dp, me.dp + me.db, 3, True).start()
    part(me.dp, me.dp + me.da, 4, True).start()
    shares = [
        me.copy(src, dst, w_send.at[j], w_recv.at[j], me.dp, 1 - me.core) for j, (src, dst) in enumerate(zip(mine, half_of(me.core)))
    ]
    for c in shares:
        c.start()
    load.wait()
    store.start()
    arrive_a(0)
    store.wait()
    for c in locals_:
        c.wait()
    for j, dst in enumerate(half_of(1 - me.core)):
        me.copy(dst, dst, w_send.at[j], w_recv.at[j], me.dp).wait_recv()
    fetch(0)

    tile = 256

    def step(n, _):
        slot = n % 2
        for c in loads(n):
            c.wait()
        gates = jnp.concatenate([g_ref[block(n)], g_ref[block(n) + me.db]], axis=0)

        def inner(j, _):
            at, at_up = pl.ds(pl.multiple_of(j * tile, tile), tile), pl.ds(pl.multiple_of(hidden + j * tile, tile), tile)
            gate, up, grad = dot(xb[slot], wgu[:, at]), dot(xb[slot], wgu[:, at_up]), dot_t(cb[slot], wd[at, :]) * gates
            sig = 1.0 / (1.0 + jnp.exp(-gate))
            act = gate * sig
            ag[n, :, at] = (act * up * gates).astype(ag.dtype)
            ggu[n, :, at] = (grad * up * sig * (1.0 + gate * (1.0 - sig))).astype(ggu.dtype)
            ggu[n, :, at_up] = (grad * act).astype(ggu.dtype)
            return 0

        lax.fori_loop(0, hidden // tile, inner, 0)

        def at_step(k, *calls):
            def go():
                for call, m in calls:
                    call(m)

            pl.when(n == k)(go)

        at_step(0, (arrive, 1))
        at_step(1, (arrive, 2), (arrive_a, 1))
        at_step(2, (arrive, 3))
        at_step(3, (arrive_a, 2))
        at_step(4, (arrive_a, 3))
        pl.when(n < 7)(lambda: fetch(n + 1))

        pl.when(n >= 2)(lambda: keep_share(n - 2).wait())

        def outer(j, _):
            at = pl.ds(pl.multiple_of(j * 2 * tile, 2 * tile), 2 * tile)
            share[slot, :, at] = dot(ag[n], wd[:, at]).astype(p.dtype)
            p[n, :, at] = dot_t(ggu[n], wgu[at, :]).astype(p.dtype)
            return 0

        lax.fori_loop(0, width // (2 * tile), outer, 0)
        scatter.send_b(n).start()
        keep_share(n).start()
        scatter.advance(n)
        return 0

    lax.fori_loop(0, 8, step, 0)

    def tiles(i):
        slot = i % 2
        cols = pl.ds(pl.multiple_of(i * tile, tile), tile)
        copies = []
        for which, src in enumerate((xg_ref, c_ref)):
            to = pl.ds(pl.multiple_of((2 * which + slot) * tile, tile), tile)

            def one(n, side, which=which, src=src, to=to):
                at = pl.ds(pl.multiple_of((2 * n + side) * rows, rows), rows)
                return pltpu.make_async_copy(src.at[block(n) + side * me.db, :, cols], wgu.at[at, to], tile_sem.at[which, slot, 2 * n + side])

            copies.append(one)
        return copies

    def each_tile(i, act):
        for one in tiles(i):

            def body(n, _):
                for side in (0, 1):
                    act(one(n, side))
                return 0

            lax.fori_loop(0, 8, body, 0)

    def outs(i):
        slot = i % 2
        at = pl.ds(pl.multiple_of(i * tile, tile), tile)
        return (
            pltpu.make_async_copy(xb.at[slot, :, pl.ds(0, 2 * hidden)], gu_out.at[at], load_sem.at[slot, 0]),
            pltpu.make_async_copy(cb.at[slot, :, pl.ds(0, hidden)], down_out.at[at], load_sem.at[slot, 1]),
        )

    each_tile(0, lambda c: c.start())

    def weight_step(i, _):
        slot = i % 2
        pl.when(i < 7)(lambda: each_tile(i + 1, lambda c: c.start()))
        each_tile(i, lambda c: c.wait())

        def free():
            for c in outs(i - 2):
                c.wait()

        pl.when(i >= 2)(free)
        x_tile = wgu[:, pl.ds(pl.multiple_of(slot * tile, tile), tile)]
        xb[slot, :, pl.ds(0, 2 * hidden)] = t_dot(x_tile, ggu[...].reshape(-1, 2 * hidden)).astype(xb.dtype)
        c_tile = wgu[:, pl.ds(pl.multiple_of((2 + slot) * tile, tile), tile)]
        cb[slot, :, pl.ds(0, hidden)] = t_dot(c_tile, ag[...].reshape(-1, hidden)).astype(cb.dtype)
        for c in outs(i):
            c.start()
        scatter.advance(i + 8)
        return 0

    lax.fori_loop(0, 8, weight_step, 0)
    scatter.finish(two_ref)

    for i in (6, 7):
        for c in outs(i):
            c.wait()
    for c in shares:
        c.wait_send()
    for slot in range(15):
        part(me.dp, me.dp, slot).wait_send()
    scatter.drain()
    keep_share(6).wait()
    keep_share(7).wait()


def expert_layer(x, grads, gates, gate, up, down, cid):
    rows, width = x.shape
    half = gate.shape[1]
    hbm, vmem = pl.BlockSpec(memory_space=pl.ANY), pl.BlockSpec(memory_space=pltpu.VMEM)
    dma = pltpu.SemaphoreType.DMA
    dtype = x.dtype
    return pl.pallas_call(
        experts_kernel,
        out_shape=[
            jax.ShapeDtypeStruct((8, 2 * rows, width), dtype),
            jax.ShapeDtypeStruct((rows, width), jnp.float32),
            jax.ShapeDtypeStruct((width, 4 * half), dtype),
            jax.ShapeDtypeStruct((width, 2 * half), dtype),
            jax.ShapeDtypeStruct((16, rows, width), dtype),
        ],
        in_specs=[hbm, hbm, vmem, hbm, hbm, hbm],
        out_specs=[hbm, vmem, hbm, hbm, hbm],
        scratch_shapes=[
            pltpu.VMEM((width, 4 * half), dtype),
            pltpu.VMEM((2 * half, width), dtype),
            pltpu.VMEM((8, 2 * rows, 2 * half), dtype),
            pltpu.VMEM((8, 2 * rows, 4 * half), dtype),
            pltpu.VMEM((2, 2 * rows, width), dtype),
            pltpu.VMEM((8, 2 * rows, width), dtype),
            pltpu.VMEM((2, 2 * rows, width), dtype),
            pltpu.VMEM((2, 2 * rows, width), dtype),
            *scatter_rows_scratch(rows, width, dtype),
            dma((15,)), dma((16,)),
            dma((3,)), dma((3,)),
            dma((2, 4)), dma((2, 2, 16)), dma((5,)), dma((2,)),
        ],
        compiler_params=pltpu.CompilerParams(collective_id=cid, has_side_effects=True, vmem_limit_bytes=67_043_328),
        name="experts",
    )(x, grads, gates, gate, up, down)


def per_device_any(
    tokens,
    cotangent,
    expert_ids,
    gate_values,
    w_query,
    w_key,
    w_value,
    w_out,
    w_gate,
    w_up,
    w_down,
    attn_gain,
    ffn_gain,
    query_gain,
    key_gain,
):
    contract = (((1,), (1,)), ((), ()))
    contract_rows = (((0,), (0,)), ((), ()))
    residual = tokens.astype(jnp.float32)
    model_width = residual.shape[1]
    inverse_one = rms_inverse(residual)
    seq_normed = gather_rows((residual * inverse_one * attn_gain).astype(jnp.bfloat16))
    full_query, full_key, full_value, full_out = (
        lax.all_gather(w_query, "dp", axis=0, tiled=True),
        lax.all_gather(w_key, "dp", axis=0, tiled=True),
        lax.all_gather(w_value, "dp", axis=0, tiled=True),
        lax.all_gather(w_out, "dp", axis=1, tiled=True),
    )
    seq_len = seq_normed.shape[0]
    head_dim = query_gain.shape[0]
    local_heads = full_query.shape[1] // head_dim
    local_kv = full_key.shape[1] // head_dim
    group_size = local_heads // local_kv
    attn_scale = head_dim ** (-0.5)
    cosine, sine_table = rotary_tables(seq_len, head_dim)
    query_raw = jnp.dot(seq_normed, full_query, preferred_element_type=jnp.float32).reshape(
        seq_len, local_heads, head_dim
    )
    key_raw = jnp.dot(seq_normed, full_key, preferred_element_type=jnp.float32).reshape(
        seq_len, local_kv, head_dim
    )
    value_low = (
        jnp.dot(seq_normed, full_value, preferred_element_type=jnp.float32)
        .astype(jnp.bfloat16)
        .reshape(seq_len, local_kv, head_dim)
    )
    query_inverse = rms_inverse(query_raw)
    key_inverse = rms_inverse(key_raw)
    query_low = (
        rotate(query_raw * query_inverse * query_gain, cosine, sine_table) * attn_scale
    ).astype(jnp.bfloat16)
    key_low = rotate(key_raw * key_inverse * key_gain, cosine, sine_table).astype(jnp.bfloat16)
    query_heads = query_low.reshape(seq_len, local_kv, group_size, head_dim).transpose(1, 0, 2, 3)
    key_heads = key_low.transpose(1, 0, 2)
    value_heads = value_low.transpose(1, 0, 2)
    mixed_heads, logsum = lax.map(head_forward, (query_heads, key_heads, value_heads))
    mixed_flat = mixed_heads.transpose(1, 0, 2, 3).reshape(seq_len, local_heads * head_dim)
    hidden = residual + scatter_rows(
        jnp.dot(mixed_flat, full_out, preferred_element_type=jnp.float32)
    )
    inverse_two = rms_inverse(hidden)
    seq_two = gather_rows((hidden * inverse_two * ffn_gain).astype(jnp.bfloat16))
    seq_grad = gather_rows(cotangent)
    experts = w_gate.shape[0]
    dp_rows = w_gate.shape[1]
    hidden_units = w_gate.shape[2]
    dp_count = lax.axis_size("dp")
    group = dp_count // experts
    routed_rows = seq_len * expert_ids.shape[1] * 9 // 8
    capacity = (routed_rows + experts * group - 1) // (experts * group) * group
    slot_table, gate_table = dispatch(expert_ids, gate_values, experts, capacity)
    blank_row = jnp.zeros((1, model_width), jnp.bfloat16)
    padded_in = jnp.concatenate([seq_two, blank_row], axis=0)
    padded_grad = jnp.concatenate([seq_grad, blank_row], axis=0)
    empty_rows = jnp.zeros((seq_len + 1, model_width), jnp.float32)
    piece_rows = capacity // group
    down_rows = jnp.transpose(w_down, (0, 2, 1))
    gate_mine, up_mine, down_mine = (
        lax.all_to_all(widen(w_gate, group), "dp", split_axis=0, concat_axis=1, tiled=True),
        lax.all_to_all(widen(w_up, group), "dp", split_axis=0, concat_axis=1, tiled=True),
        lax.all_to_all(widen(down_rows, group), "dp", split_axis=0, concat_axis=1, tiled=True),
    )
    gate_mine = gate_mine[0]
    up_mine = up_mine[0]
    down_mine = down_mine[0]
    blocks_in = padded_in[slot_table]
    grad_blocks = (padded_grad[slot_table].astype(jnp.float32) * gate_table[:, :, None]).astype(
        jnp.bfloat16
    )
    recv_in, recv_grad = (
        lax.all_to_all(
            blocks_in.reshape(dp_count, piece_rows, model_width),
            "dp",
            split_axis=0,
            concat_axis=0,
            tiled=True,
        ),
        lax.all_to_all(
            grad_blocks.reshape(dp_count, piece_rows, model_width),
            "dp",
            split_axis=0,
            concat_axis=0,
            tiled=True,
        ),
    )
    rows_in = recv_in.reshape(-1, model_width)
    rows_grad = recv_grad.reshape(-1, model_width)
    gate_pre = jnp.dot(rows_in, gate_mine, preferred_element_type=jnp.float32)
    up_pre = jnp.dot(rows_in, up_mine, preferred_element_type=jnp.float32)
    act_low = (jax.nn.silu(gate_pre) * up_pre).astype(jnp.bfloat16)
    expert_out = lax.dot_general(act_low, down_mine, contract, preferred_element_type=jnp.float32)
    grad_act = jnp.dot(rows_grad, down_mine, preferred_element_type=jnp.float32)
    sigmoid_gate = jax.nn.sigmoid(gate_pre)
    grad_gate = (grad_act * up_pre * sigmoid_gate * (1.0 + gate_pre * (1.0 - sigmoid_gate))).astype(
        jnp.bfloat16
    )
    grad_up = (grad_act * gate_pre * sigmoid_gate).astype(jnp.bfloat16)
    grad_input = lax.dot_general(
        grad_gate, gate_mine, contract, preferred_element_type=jnp.float32
    ) + lax.dot_general(grad_up, up_mine, contract, preferred_element_type=jnp.float32)
    back_out, back_grad = (
        lax.all_to_all(
            expert_out.reshape(dp_count, piece_rows, model_width).astype(jnp.bfloat16),
            "dp",
            split_axis=0,
            concat_axis=0,
            tiled=True,
        ).astype(jnp.float32),
        lax.all_to_all(
            grad_input.reshape(dp_count, piece_rows, model_width).astype(jnp.bfloat16),
            "dp",
            split_axis=0,
            concat_axis=0,
            tiled=True,
        ).astype(jnp.float32),
    )
    back_out = back_out.reshape(experts, capacity, model_width)
    back_grad = back_grad.reshape(experts * capacity, model_width)
    flat_slots = slot_table.reshape(-1)
    combined = empty_rows.at[flat_slots].add(
        (back_out * gate_table[:, :, None]).reshape(-1, model_width)
    )
    grad_acc = empty_rows.at[flat_slots].add(back_grad)
    grad_both = jnp.concatenate([grad_gate, grad_up], axis=1)
    grad_cols = jnp.concatenate(
        [
            lax.dot_general(rows_in, grad_both, contract_rows, preferred_element_type=jnp.float32),
            lax.dot_general(rows_grad, act_low, contract_rows, preferred_element_type=jnp.float32),
        ],
        axis=1,
    )
    returned = lax.all_to_all(
        grad_cols[None].astype(jnp.bfloat16), "dp", split_axis=1, concat_axis=0, tiled=True
    ).astype(jnp.float32)
    summed = jnp.sum(returned.reshape(experts, group, dp_rows, 3 * hidden_units), axis=1)
    grad_w_gate = summed[:, :, :hidden_units]
    grad_w_up = summed[:, :, hidden_units : 2 * hidden_units]
    grad_w_down = jnp.transpose(summed[:, :, 2 * hidden_units :], (0, 2, 1))
    output = (hidden + scatter_rows(combined[:seq_len])).astype(jnp.bfloat16)
    grad_two = scatter_rows(grad_acc[:seq_len])
    ffn_gain_part = jnp.sum(grad_two * hidden * inverse_two, axis=0)
    grad_hidden = cotangent.astype(jnp.float32) + norm_backward(
        grad_two, hidden, inverse_two, ffn_gain
    )
    grad_attn = gather_rows(grad_hidden.astype(jnp.bfloat16))
    grad_mixed = lax.dot_general(
        grad_attn, full_out, contract, preferred_element_type=jnp.float32
    ).astype(jnp.bfloat16)
    grad_mixed_heads = grad_mixed.reshape(seq_len, local_kv, group_size, head_dim).transpose(
        1, 0, 2, 3
    )
    grad_query_heads, grad_key_heads, grad_value_heads = lax.map(
        head_backward, (query_heads, key_heads, value_heads, logsum, grad_mixed_heads)
    )
    grad_query_rot = (
        grad_query_heads.transpose(1, 0, 2, 3).reshape(seq_len, local_heads, head_dim) * attn_scale
    )
    grad_query_norm = rotate_back(grad_query_rot, cosine, sine_table)
    query_gain_part = jnp.sum(grad_query_norm * query_raw * query_inverse, axis=(0, 1))
    grad_query_low = (
        norm_backward(grad_query_norm, query_raw, query_inverse, query_gain)
        .astype(jnp.bfloat16)
        .reshape(seq_len, local_heads * head_dim)
    )
    grad_key_norm = rotate_back(grad_key_heads.transpose(1, 0, 2), cosine, sine_table)
    key_gain_part = jnp.sum(grad_key_norm * key_raw * key_inverse, axis=(0, 1))
    grad_key_low = (
        norm_backward(grad_key_norm, key_raw, key_inverse, key_gain)
        .astype(jnp.bfloat16)
        .reshape(seq_len, local_kv * head_dim)
    )
    grad_value_low = (
        grad_value_heads.transpose(1, 0, 2)
        .reshape(seq_len, local_kv * head_dim)
        .astype(jnp.bfloat16)
    )
    grad_proj = jnp.concatenate([grad_query_low, grad_key_low, grad_value_low], axis=1)
    full_proj = jnp.concatenate([full_query, full_key, full_value], axis=1)
    grad_one = scatter_rows(
        lax.dot_general(grad_proj, full_proj, contract, preferred_element_type=jnp.float32)
    )
    first_part = jnp.einsum("sd,sf->df", seq_normed, grad_proj, preferred_element_type=jnp.float32)
    second = jnp.einsum("sd,sf->df", grad_attn, mixed_flat, preferred_element_type=jnp.float32)
    shares = lax.psum_scatter(
        jnp.concatenate([first_part, second], axis=1), "dp", scatter_dimension=0, tiled=True
    )
    query_cols = w_query.shape[1]
    key_cols = w_key.shape[1]
    grad_w_query = shares[:, :query_cols]
    grad_w_key = shares[:, query_cols : query_cols + key_cols]
    grad_w_value = shares[:, query_cols + key_cols : query_cols + 2 * key_cols]
    grad_w_out = jnp.transpose(shares[:, query_cols + 2 * key_cols :])
    attn_gain_part = jnp.sum(grad_one * residual * inverse_one, axis=0)
    grad_tokens = (grad_hidden + norm_backward(grad_one, residual, inverse_one, attn_gain)).astype(
        jnp.bfloat16
    )
    total_gains = lax.psum(
        (attn_gain_part, ffn_gain_part, query_gain_part, key_gain_part), ("dp", "tensor")
    )
    return (
        output,
        grad_tokens,
        grad_w_query,
        grad_w_key,
        grad_w_value,
        grad_w_out,
        grad_w_gate,
        grad_w_up,
        grad_w_down,
        total_gains[0],
        total_gains[1],
        total_gains[2],
        total_gains[3],
    )


def per_device_relay(
    tokens,
    cotangent,
    expert_ids,
    gate_values,
    w_query,
    w_key,
    w_value,
    w_out,
    w_gate,
    w_up,
    w_down,
    attn_gain,
    ffn_gain,
    query_gain,
    key_gain,
):
    dot = functools.partial(jnp.dot, preferred_element_type=jnp.float32)
    dot_t = functools.partial(lax.dot_general, dimension_numbers=(((1,), (1,)), ((), ())), preferred_element_type=jnp.float32)
    t_dot = functools.partial(lax.dot_general, dimension_numbers=(((0,), (0,)), ((), ())), preferred_element_type=jnp.float32)
    low = jnp.bfloat16
    rows, width = tokens.shape
    head_dim = query_gain.shape[0]
    experts = w_gate.shape[0]
    core = lax.axis_index("tensor")
    mine = lax.dynamic_slice_in_dim(expert_ids, core * rows, rows, 0)
    values = lax.dynamic_slice_in_dim(gate_values, core * rows, rows, 0)
    match = mine[None] == jnp.arange(experts, dtype=jnp.int32)[:, None, None]
    gates = jnp.sum(jnp.where(match, values[None], 0.0), axis=2)
    gates = jnp.broadcast_to(gates[:, None], (experts, 8, rows))

    q_cols, kv_cols = w_query.shape[1] // 2, w_key.shape[1] // 2
    w_out_rows = jnp.transpose(w_out)
    halves = jnp.stack(
        [
            jnp.concatenate([w[:, h * (w.shape[1] // 2) : (h + 1) * (w.shape[1] // 2)] for w in (w_query, w_key, w_value, w_out_rows)], axis=1)
            for h in range(2)
        ]
    )
    residual = tokens.astype(jnp.float32)
    inverse_one = rms_inverse(residual)
    normed_one = (residual * inverse_one * attn_gain).astype(low)
    cosine, sine_table = rotary_tables(2 * rows, head_dim)
    rope = jnp.stack([jnp.concatenate([v, w], axis=1) for v, w in ((cosine[:, 0], cosine[:, 0]), (sine_table[:, 0], -sine_table[:, 0]))])
    gain = jnp.stack([query_gain, key_gain])[:, None]
    weights, rows_grad, gates, seq_normed, raw, lows, mixed, attended, *projections = attention_first(
        halves, cotangent, gates, normed_one, rope, gain, (w_gate, w_up, w_down), 1
    )
    weights, gates, seq_normed = weights.reshape(-1, weights.shape[2]), gates[:, 0][:, :, None], seq_normed.reshape(-1, width)
    proj_cols = q_cols + 2 * kv_cols
    hidden = residual + attended
    inverse_two = rms_inverse(hidden)
    normed_two = (hidden * inverse_two * ffn_gain).astype(low)
    share, grad_two, gu_part, down_part, _ = expert_layer(normed_two, rows_grad, gates, *projections, 2)
    ffn_gain_part = jnp.sum(grad_two * hidden * inverse_two, axis=0)
    grad_hidden = cotangent.astype(jnp.float32) + norm_backward(grad_two, hidden, inverse_two, ffn_gain)
    gains = jnp.pad(ffn_gain_part, (width, 1024)).reshape(-1, 128)
    grad_one, moe, shares, totals, *grads_moe = attention_back(
        grad_hidden.astype(low), weights, seq_normed, raw, lows, mixed, rope, gain, residual * inverse_one, gains, gu_part, down_part, share, 9
    )
    output = (hidden + moe).astype(low)
    grad_w_gate, grad_w_up, grad_w_down = [v.astype(jnp.float32) for v in grads_moe]
    grad_w_down = jnp.transpose(grad_w_down, (0, 2, 1))
    shares, totals = shares.astype(jnp.float32), totals.reshape(-1)
    stops = (0, q_cols, q_cols + kv_cols, proj_cols, proj_cols + q_cols)
    grads = [jnp.concatenate([shares[0, :, a:b], shares[1, :, a:b]], axis=1) for a, b in zip(stops, stops[1:])]
    grad_tokens = (grad_hidden + norm_backward(grad_one, residual, inverse_one, attn_gain)).astype(low)
    totals = jnp.split(totals, (width, 2 * width, 2 * width + head_dim, 2 * width + 2 * head_dim))[:4]
    return (output, grad_tokens, grads[0], grads[1], grads[2], jnp.transpose(grads[3]), grad_w_gate, grad_w_up, grad_w_down, *totals)


def solution(mesh):
    return jax.shard_map(
        per_device_relay if tuple(mesh.shape.values()) == (16, 2) else per_device_any,
        mesh=mesh,
        in_specs=(
            P(("dp", "tensor"), None),
            P(("dp", "tensor"), None),
            P("dp", None),
            P("dp", None),
            P("dp", "tensor"),
            P("dp", "tensor"),
            P("dp", "tensor"),
            P("tensor", "dp"),
            P(None, "dp", "tensor"),
            P(None, "dp", "tensor"),
            P(None, "tensor", "dp"),
            P(),
            P(),
            P(),
            P(),
        ),
        out_specs=(
            P(("dp", "tensor"), None),
            P(("dp", "tensor"), None),
            P("dp", "tensor"),
            P("dp", "tensor"),
            P("dp", "tensor"),
            P("tensor", "dp"),
            P(None, "dp", "tensor"),
            P(None, "dp", "tensor"),
            P(None, "tensor", "dp"),
            P(),
            P(),
            P(),
            P(),
        ),
        check_vma=False,
    )
```

```python
import functools

import jax
import jax.numpy as jnp
from jax import lax
from jax.experimental import pallas as pl
from jax.experimental.pallas import tpu as pltpu
from jax.sharding import PartitionSpec as P

epsilon = 1e-06
theta_base = 1000000.0


def rms_inverse(values):
    return lax.rsqrt(jnp.mean(values * values, axis=-1, keepdims=True) + epsilon)


def norm_backward(grad_in, values, inverse, gain_vec):
    scaled = grad_in * gain_vec
    inner_mean = jnp.mean(scaled * values, axis=-1, keepdims=True)
    return inverse * scaled - values * inverse**3 * inner_mean


def rotary_tables(seq_len, head_dim):
    half_dim = head_dim // 2
    frequency = theta_base ** (-jnp.arange(half_dim, dtype=jnp.float32) * 2.0 / head_dim)
    angles = jnp.arange(seq_len, dtype=jnp.float32)[:, None] * frequency[None, :]
    return (jnp.cos(angles)[:, None, :], jnp.sin(angles)[:, None, :])


def rotate(values, cosine, sine_table):
    half_dim = values.shape[-1] // 2
    first_part = values[..., :half_dim]
    second = values[..., half_dim:]
    return jnp.concatenate(
        [first_part * cosine - second * sine_table, second * cosine + first_part * sine_table],
        axis=-1,
    )


def rotate_back(grad_in, cosine, sine_table):
    half_dim = grad_in.shape[-1] // 2
    first_part = grad_in[..., :half_dim]
    second = grad_in[..., half_dim:]
    return jnp.concatenate(
        [first_part * cosine + second * sine_table, second * cosine - first_part * sine_table],
        axis=-1,
    )


def dispatch(expert_ids, gate_values, experts, capacity):
    seq_len = expert_ids.shape[0]
    is_match = expert_ids[:, :, None] == jnp.arange(experts, dtype=jnp.int32)[None, None, :]
    expert_hits = jnp.sum(is_match.astype(jnp.int32), axis=1)
    before = jnp.cumsum(expert_hits, axis=0) - expert_hits
    slot_ids = jnp.sum(jnp.where(is_match, before[:, None, :], 0), axis=2)
    token_index = jnp.broadcast_to(jnp.arange(seq_len, dtype=jnp.int32)[:, None], expert_ids.shape)
    slot_table = (
        jnp.full((experts, capacity), seq_len, jnp.int32).at[expert_ids, slot_ids].set(token_index)
    )
    gate_table = (
        jnp.zeros((experts, capacity), jnp.float32).at[expert_ids, slot_ids].set(gate_values)
    )
    return (slot_table, gate_table)


def head_forward(head_inputs):
    query_vals, key_vals, value_vals = head_inputs
    seq_len = key_vals.shape[0]
    block_rows = min(512, seq_len)
    key_positions = jnp.arange(seq_len)

    def one_block(row_start):
        scores = jnp.einsum("qgd,sd->gqs", query_vals, key_vals, preferred_element_type=jnp.float32)
        causal = (row_start + jnp.arange(block_rows))[:, None] >= key_positions[None, :]
        exp_scores = jnp.where(causal, jnp.exp(scores), 0.0)
        denominator = jnp.sum(exp_scores, axis=-1, keepdims=True)
        softmax_low = (exp_scores / denominator).astype(jnp.bfloat16)
        mixed_out = jnp.einsum(
            "gqs,sd->qgd", softmax_low, value_vals, preferred_element_type=jnp.float32
        )
        return (mixed_out.astype(jnp.bfloat16), jnp.log(denominator[..., 0]))

    block_starts = jnp.arange(seq_len // block_rows, dtype=jnp.int32) * block_rows
    mixed_out, logsum = lax.map(one_block, block_starts)
    return (mixed_out.reshape(seq_len, query_vals.shape[1], query_vals.shape[2]), logsum)


def head_backward(head_inputs):
    query_vals, key_vals, value_vals, logsum, grad_mixed = head_inputs
    seq_len = key_vals.shape[0]
    block_rows = min(512, seq_len)
    key_positions = jnp.arange(seq_len)

    def one_block(state_in, block_in):
        grad_key, grad_value = state_in
        row_start, block_logsum = block_in
        scores = jnp.einsum("qgd,sd->gqs", query_vals, key_vals, preferred_element_type=jnp.float32)
        causal = (row_start + jnp.arange(block_rows))[:, None] >= key_positions[None, :]
        softmax_vals = jnp.where(causal, jnp.exp(scores - block_logsum[..., None]), 0.0)
        grad_probs = jnp.einsum(
            "qgd,sd->gqs", grad_mixed, value_vals, preferred_element_type=jnp.float32
        )
        delta_sum = jnp.sum(grad_probs * softmax_vals, axis=-1, keepdims=True)
        grad_scores = (softmax_vals * (grad_probs - delta_sum)).astype(jnp.bfloat16)
        grad_query = jnp.einsum(
            "gqs,sd->qgd", grad_scores, key_vals, preferred_element_type=jnp.float32
        )
        grad_key = grad_key + jnp.einsum(
            "gqs,qgd->sd", grad_scores, query_vals, preferred_element_type=jnp.float32
        )
        grad_value = grad_value + jnp.einsum(
            "gqs,qgd->sd",
            softmax_vals.astype(jnp.bfloat16),
            grad_mixed,
            preferred_element_type=jnp.float32,
        )
        return ((grad_key, grad_value), grad_query)

    block_starts = jnp.arange(seq_len // block_rows, dtype=jnp.int32) * block_rows
    zero_rows = jnp.zeros(key_vals.shape, jnp.float32)
    (grad_key, grad_value), grad_query = lax.scan(
        one_block, (zero_rows, zero_rows), (block_starts, logsum)
    )
    return (grad_query.reshape(query_vals.shape), grad_key, grad_value)


def gather_rows(values):
    return lax.all_gather(values, "tensor", axis=0, tiled=True)


def scatter_rows(values):
    return lax.psum_scatter(
        values.astype(jnp.bfloat16), "tensor", scatter_dimension=0, tiled=True
    ).astype(jnp.float32)


def widen(stacked, group):
    experts = stacked.shape[0]
    spread = jnp.broadcast_to(stacked[:, None], (experts, group) + stacked.shape[1:])
    return spread.reshape((experts * group,) + stacked.shape[1:])


MESH = pl.DeviceIdType.MESH
LIMIT = 66_000_000


class Place:
    def __init__(self):
        self.dp = lax.axis_index("dp")
        self.core = lax.axis_index("tensor")
        x, y = self.dp % 2, (self.dp // 2) % 2
        self.z = self.dp // 4
        step_x, step_y = 1 - 2 * x, 2 * (1 - 2 * y)
        self.da = (1 - self.core) * step_x + self.core * step_y
        self.db = (1 - self.core) * step_y + self.core * step_x
        self.half = self.z % 2
        self.pair = 4 * (1 - 2 * self.half)
        self.far = 8 * (1 - 2 * (self.z // 2))

    def copy(self, src, dst, send_sem, recv_sem, to, core=None):
        return pltpu.make_async_remote_copy(
            src_ref=src,
            dst_ref=dst,
            send_sem=send_sem,
            recv_sem=recv_sem,
            device_id=(to, self.core if core is None else core),
            device_id_type=MESH,
        )

    def at_z(self, z):
        return self.dp + 4 * (z - self.z)

    def z_of(self, m):
        low = self.z < 2
        depth = jnp.where(low, self.z, 3 - self.z)
        t = jnp.where(m == 0, depth, jnp.where(m == 1, 1 - depth, m))
        return jnp.where(low, t, 3 - t)

    def block(self, n):
        return self.at_z(self.z_of(n // 2)) + (n % 2) * self.da

    def greet(self, line=False, column=False, near=False, chain=False, everyone=False, partner=False):
        barrier = pltpu.get_barrier_semaphore()
        count = 0

        def signal(to, core):
            pl.semaphore_signal(barrier, inc=1, device_id=(to, core), device_id_type=MESH)

        if everyone:
            for r in range(1, 16):
                signal((self.dp + r) % 16, self.core)
            count = count + 15
        else:
            if near:
                signal(self.dp + self.da, self.core)
                signal(self.dp + self.db, self.core)
                count = count + 2
            if chain:
                signal(self.dp + self.pair, self.core)
                count = count + 1
                if near:
                    signal(self.dp + self.far, self.core)
                    count = count + 1
            if column:
                for r in range(1, 4):
                    signal((self.dp + 4 * r) % 16, self.core)
                count = count + 3
            if line:
                pl.when(self.z > 0)(lambda: signal(self.dp - 4, self.core))
                pl.when(self.z < 3)(lambda: signal(self.dp + 4, self.core))
                count = count + jnp.where(self.z > 0, 1, 0) + jnp.where(self.z < 3, 1, 0)
        if partner:
            signal(self.dp, 1 - self.core)
            count = count + 1
        pl.semaphore_wait(barrier, count)


def add_rows(target, terms, rows, block=16):
    def body(i, _):
        at = pl.ds(pl.multiple_of(i * block, block), block)
        total = terms[0][at, :].astype(jnp.float32)
        for term in terms[1:]:
            total = total + term[at, :].astype(jnp.float32)
        target[at, :] = total.astype(target.dtype)
        return 0

    lax.fori_loop(0, rows // block, body, 0)


def run(*threads):
    threads = list(threads)
    while threads:
        for thread in list(threads):
            if next(thread, "end") == "end":
                threads.remove(thread)


class Threads:
    def __init__(self, *threads):
        self.threads = list(threads)

    def step(self, times=1):
        for _ in range(times):
            for thread in list(self.threads):
                if next(thread, "end") == "end":
                    self.threads.remove(thread)

    def finish(self):
        while self.threads:
            self.step()


def lagged(items, first, second, lag):
    for n in range(len(items) + lag):
        if n < len(items):
            first(items[n])
            yield
        if n >= lag:
            second(items[n - lag])
            yield


def gather_line(me, x_ref, out_ref, send_sem, recv_sem):
    def part(source, to, slot, own=False):
        return me.copy(x_ref if own else out_ref.at[source], out_ref.at[source], send_sem.at[slot], recv_sem.at[source], to)

    sides = ((-1, me.z < 3, 4), (1, me.z > 0, -4))

    def exists(d, side):
        return (me.z - d >= 0) if side == 0 else (me.z + d <= 3)

    def slot_z(d, side, j):
        return 4 + ((d - 1) * 2 + side) * 3 + j

    def slot_a(off):
        return 25 + off

    def pass_a(off):
        source = me.dp + me.da + 4 * off
        part(source, me.dp, slot_a(off)).wait_recv()
        part(source, me.dp + me.db, slot_a(off)).start()

    pl.when(me.z < 3)(lambda: part(me.dp, me.dp + 4, 0, True).start())
    pl.when(me.z > 0)(lambda: part(me.dp, me.dp - 4, 1, True).start())
    part(me.dp, me.dp + me.db, 3, True).start()
    part(me.dp, me.dp + me.da, 2, True).start()
    yield
    for d in range(1, 5):
        if d < 4:
            for side, (sign, forward, step) in enumerate(sides):
                source = me.dp + 4 * sign * d

                def arrive():
                    part(source, me.dp, slot_z(d, side, 0)).wait_recv()
                    pl.when(forward)(lambda: part(source, me.dp + step, slot_z(d, side, 0)).start())
                    part(source, me.dp + me.db, slot_z(d, side, 2)).start()
                    part(source, me.dp + me.da, slot_z(d, side, 1)).start()

                pl.when(exists(d, side))(arrive)
                yield
        if d == 1:
            pass_a(0)
            yield
        else:
            for side, (sign, *_) in enumerate(sides):
                pl.when(exists(d - 1, side))(lambda: pass_a(sign * (d - 1)))
                yield
    for z in range(4):
        for g in (0, 1):
            part(me.at_z(z) + me.db + g * me.da, me.dp, 0).wait_recv()
            yield

    def sent(slot):
        part(me.dp, me.dp, slot).wait_send()

    pl.when(me.z < 3)(lambda: sent(0))
    pl.when(me.z > 0)(lambda: sent(1))
    sent(2)
    sent(3)
    sent(slot_a(0))
    for d in range(1, 4):
        for side, (sign, forward, _) in enumerate(sides):

            def finish():
                pl.when(forward)(lambda: sent(slot_z(d, side, 0)))
                sent(slot_z(d, side, 1))
                sent(slot_z(d, side, 2))
                sent(slot_a(sign * d))

            pl.when(exists(d, side))(finish)


def gather_pairs(me, x_ref, out_ref, send_sem, recv_sem):
    mine, other = me.dp, me.dp + me.pair

    def part(src, where, to, slot):
        return me.copy(src, out_ref.at[where], send_sem.at[slot], recv_sem.at[where], to)

    def relay(where, to, slot):
        part(out_ref.at[where], where, to, slot).start()

    def arrived(where):
        part(out_ref.at[where], where, me.dp, 0).wait_recv()

    part(x_ref.at[1 - me.half], mine, other, 0).start()
    part(x_ref.at[me.half], mine, me.dp + me.far, 1).start()
    part(x_ref.at[me.half], mine, me.dp + me.db, 2).start()
    part(x_ref.at[me.half], mine, me.dp + me.da, 3).start()
    yield
    arrived(other)
    relay(other, me.dp + me.far, 4)
    relay(other, me.dp + me.db, 5)
    relay(other, me.dp + me.da, 6)
    yield
    arrived(mine + me.da)
    relay(mine + me.da, me.dp + me.db, 7)
    yield
    arrived(mine + me.far)
    relay(mine + me.far, me.dp + me.db, 8)
    relay(mine + me.far, me.dp + me.da, 9)
    yield
    arrived(other + me.da)
    relay(other + me.da, me.dp + me.db, 10)
    yield
    arrived(other + me.far)
    relay(other + me.far, me.dp + me.db, 11)
    relay(other + me.far, me.dp + me.da, 12)
    yield
    arrived(mine + me.far + me.da)
    relay(mine + me.far + me.da, me.dp + me.db, 13)
    yield
    arrived(other + me.far + me.da)
    relay(other + me.far + me.da, me.dp + me.db, 14)
    yield
    for base in (mine, other, mine + me.far, other + me.far):
        arrived(base + me.db)
        yield
        arrived(base + me.da + me.db)
        yield
    for slot in range(15):
        part(out_ref.at[mine], mine, me.dp, slot).wait_send()


def swap_rows(me, x_ref, out_ref, send_sem, recv_sem):
    for r in range(1, 16):
        to = (me.dp + r) % 16
        me.copy(x_ref.at[to], out_ref.at[me.dp], send_sem.at[r], recv_sem.at[r], to).start()
    yield
    for r in range(1, 16):
        s = (me.dp + 16 - r) % 16
        me.copy(x_ref.at[s], out_ref.at[s], send_sem.at[r], recv_sem.at[r], me.dp).wait_recv()
    for r in range(1, 16):
        me.copy(x_ref.at[me.dp], out_ref.at[me.dp], send_sem.at[r], recv_sem.at[r], me.dp).wait_send()


def keep_own(src, staging, dst, sems):
    load = pltpu.make_async_copy(src, staging, sems.at[0])
    store = pltpu.make_async_copy(staging, dst, sems.at[1])
    load.start()

    def finish():
        load.wait()
        store.start()
        store.wait()

    return finish


def share_experts(me, ins, outs, send_sem, recv_sem):
    depth = ins[0].shape[1]

    def sends(r):
        to = (me.dp + r) % 16
        at = pl.ds(pl.multiple_of(me.dp * depth, depth), depth)
        pairs = ((ins[0].at[to], outs[0].at[at]), (ins[1].at[to], outs[1].at[at]), (ins[2].at[to], outs[2].at[:, at]))
        return [me.copy(src, dst, send_sem.at[r, j], recv_sem.at[r, j], to) for j, (src, dst) in enumerate(pairs)]

    for r in (8, 7, 9, 4, 12, 5, 11, 6, 10, 3, 13, 2, 14, 1, 15):
        for c in sends(r):
            c.start()
        yield
    for r in range(1, 16):
        at = pl.ds(pl.multiple_of((me.dp + 16 - r) % 16 * depth, depth), depth)
        for j, dst in enumerate((outs[0].at[at], outs[1].at[at], outs[2].at[:, at])):
            me.copy(dst, dst, send_sem.at[r, j], recv_sem.at[r, j], me.dp).wait_recv()
    for r in range(1, 16):
        for c in sends(r):
            c.wait_send()


def gather_four(me, x_ref, out_ref, send_sem, recv_sem):
    mine, theirs = out_ref.at[me.half, me.core], out_ref.at[1 - me.half, me.core]
    across = me.copy(x_ref, mine, send_sem.at[0], recv_sem.at[0], me.dp + me.pair)
    across.start()
    beside = me.copy(x_ref, mine, send_sem.at[1], recv_sem.at[1], me.dp, 1 - me.core)
    beside.start()
    mine[...] = x_ref[...]
    yield
    across.wait_recv()
    relay = me.copy(theirs, theirs, send_sem.at[2], recv_sem.at[2], me.dp, 1 - me.core)
    relay.start()
    yield
    across.wait_send()
    beside.wait()
    relay.wait()


def attention_first_kernel(
    head_dim, start,
    w_ref, c_ref, g_ref, x_ref, rope_ref, gain_ref, gate_ref, up_ref, down_ref,
    w_out, c_out, g_out, seq, raw, low, mixed, sum_ref, gate_out, up_out, down_out,
    w, c_own, e_own, part, from_core, from_pair,
    w_send, w_recv, c_send, c_recv, g_send, g_recv, x_send, x_recv, e_send, e_recv, back_send, back_recv, copy_sem,
):
    me = Place()
    rows, width = x_ref.shape
    seq_len = 2 * rows
    q_cols = mixed.shape[1]
    proj_cols = q_cols + 2 * head_dim
    group = q_cols // head_dim
    depth = gate_ref.shape[1]
    dot = functools.partial(jnp.dot, preferred_element_type=jnp.float32)
    dot_t = functools.partial(lax.dot_general, dimension_numbers=(((1,), (1,)), ((), ())), preferred_element_type=jnp.float32)
    at_mine = pl.ds(pl.multiple_of(me.dp * depth, depth), depth)
    ends = [
        keep_own(c_ref, c_own, c_out.at[me.dp], copy_sem.at[1]),
        keep_own(gate_ref.at[me.dp], e_own.at[0], gate_out.at[at_mine], copy_sem.at[2]),
        keep_own(up_ref.at[me.dp], e_own.at[1], up_out.at[at_mine], copy_sem.at[3]),
    ]
    flat = pltpu.make_async_copy(down_ref.at[me.dp], down_out.at[:, at_mine], copy_sem.at[4, 0])
    flat.start()
    kept = pltpu.make_async_copy(w_ref.at[me.half], w.at[me.dp], copy_sem.at[0, 0])
    kept.start()
    g_out[me.dp] = g_ref[me.dp]
    me.greet(everyone=True, partner=True)
    beside = Threads(
        swap_rows(me, g_ref, g_out, g_send, g_recv),
        share_experts(me, (gate_ref, up_ref, down_ref), (gate_out, up_out, down_out), e_send, e_recv),
    )
    needed = Threads(gather_four(me, x_ref, seq, x_send, x_recv), gather_pairs(me, w_ref, w, w_send, w_recv))
    rounds = 0
    while needed.threads:
        needed.step()
        if rounds == start:
            beside.threads.insert(0, gather_line(me, c_ref, c_out, c_send, c_recv))
        beside.step()
        rounds += 1
    kept.wait()
    store = pltpu.make_async_copy(w, w_out, copy_sem.at[0, 1])
    store.start()
    weights = w.reshape(16 * rows, w.shape[2])

    def row_block(ref, h, core):
        return ref.at[pl.ds(pl.multiple_of((2 * h + core) * rows, rows), rows)]

    seqs = seq.reshape(4 * rows, width)
    q_part, k_part = pl.ds(0, q_cols), pl.ds(q_cols, 2 * head_dim)

    def project(j, _):
        at = pl.ds(pl.multiple_of(j * 256, 256), 256)
        raw[:, at] = dot(seqs[...], weights[:, at])
        return 0

    lax.fori_loop(0, q_cols // 256, project, 0)
    keys = dot(seqs[...], weights[:, k_part])
    raw[:, pl.ds(q_cols, head_dim)] = keys[:, :head_dim]
    low[:, pl.ds(q_cols + head_dim, head_dim)] = keys[:, head_dim:].astype(low.dtype)
    beside.step()
    cosine, turn = rope_ref[0], rope_ref[1]

    def turned(at, cols, which, scale):
        values = raw[at, cols]
        values = values * lax.rsqrt(jnp.mean(values * values, axis=-1, keepdims=True) + epsilon) * gain_ref[which]
        return ((values * cosine - pltpu.roll(values, head_dim // 2, 1) * turn) * scale).astype(low.dtype)

    k_at, v_at = pl.ds(q_cols, head_dim), pl.ds(q_cols + head_dim, head_dim)
    for b in range(2):
        at = pl.ds(b * seq_len, seq_len)
        low[at, k_at] = turned(at, k_at, 1, 1.0)
    causal = lax.broadcasted_iota(jnp.int32, (seq_len, seq_len), 0) >= lax.broadcasted_iota(jnp.int32, (seq_len, seq_len), 1)

    def head(n, _):
        at = pl.ds(pl.multiple_of(n // group * seq_len, seq_len), seq_len)
        cols = pl.ds(pl.multiple_of(n % group * head_dim, head_dim), head_dim)
        query = turned(at, cols, 0, head_dim ** (-0.5))
        low[at, cols] = query
        exp_scores = jnp.where(causal, jnp.exp(dot_t(query, low[at, k_at])), 0.0)
        probs = exp_scores / jnp.sum(exp_scores, axis=-1, keepdims=True)
        mixed[at, cols] = dot(probs.astype(low.dtype), low[at, v_at]).astype(mixed.dtype)
        return 0

    quarter = group // 2
    for k in range(4):
        lax.fori_loop(k * quarter, (k + 1) * quarter, head, 0)
        beside.step()

    def project_back(j, _):
        at = pl.ds(pl.multiple_of(j * 256, 256), 256)
        part[:, at] = dot_t(mixed[...], weights[at, pl.ds(proj_cols, q_cols)]).astype(part.dtype)
        return 0

    lax.fori_loop(0, width // 256, project_back, 0)

    def give(h, slot):
        return me.copy(row_block(part, h, 1 - me.core), from_core.at[slot], back_send.at[slot], back_recv.at[slot], me.dp, 1 - me.core)

    give(1 - me.half, 0).start()
    give(me.half, 1).start()
    beside.step()
    give(1 - me.half, 0).wait_recv()
    add_rows(from_core.at[0], (row_block(part, 1 - me.half, me.core), from_core.at[0]), rows)
    over = me.copy(from_core.at[0], from_pair, back_send.at[2], back_recv.at[2], me.dp + me.pair)
    over.start()
    give(me.half, 1).wait_recv()
    add_rows(from_core.at[1], (row_block(part, me.half, me.core), from_core.at[1]), rows)
    beside.step()
    over.wait_recv()
    add_rows(sum_ref, (from_core.at[1], from_pair), rows)
    beside.finish()
    for end in ends:
        end()
    flat.wait()
    store.wait()
    give(0, 0).wait_send()
    give(0, 1).wait_send()
    over.wait_send()


def attention_first(weights, rows, gates, normed, rope, gain, experts, cid, start=14):
    hbm, vmem = pl.BlockSpec(memory_space=pl.ANY), pl.BlockSpec(memory_space=pltpu.VMEM)
    dma = pltpu.SemaphoreType.DMA
    dtype = rows.dtype
    _, depth, hidden = experts[0].shape
    block, width = rows.shape
    head_dim = rope.shape[-1]
    columns = weights.shape[2]
    q_cols = (columns - 2 * head_dim) // 2
    return pl.pallas_call(
        functools.partial(attention_first_kernel, head_dim, start),
        out_shape=[
            jax.ShapeDtypeStruct((16,) + weights.shape[1:], dtype),
            jax.ShapeDtypeStruct((16, block, width), dtype),
            jax.ShapeDtypeStruct(gates.shape, gates.dtype),
            jax.ShapeDtypeStruct((2, 2, block, width), dtype),
            jax.ShapeDtypeStruct((4 * block, q_cols + head_dim), jnp.float32),
            jax.ShapeDtypeStruct((4 * block, q_cols + 2 * head_dim), dtype),
            jax.ShapeDtypeStruct((4 * block, q_cols), dtype),
            jax.ShapeDtypeStruct((block, width), jnp.float32),
            jax.ShapeDtypeStruct((16 * depth, hidden), dtype),
            jax.ShapeDtypeStruct((16 * depth, hidden), dtype),
            jax.ShapeDtypeStruct((hidden, 16 * depth), dtype),
        ],
        in_specs=[hbm, hbm, vmem, vmem, vmem, vmem, hbm, hbm, hbm],
        out_specs=[hbm, hbm] + [vmem] * 6 + [hbm] * 3,
        scratch_shapes=[
            pltpu.VMEM((16,) + weights.shape[1:], dtype),
            pltpu.VMEM((block, width), dtype),
            pltpu.VMEM((2, depth, hidden), dtype),
            pltpu.VMEM((4 * block, width), dtype),
            pltpu.VMEM((2, block, width), dtype),
            pltpu.VMEM((block, width), dtype),
            dma((15,)), dma((16,)),
            dma((29,)), dma((16,)),
            dma((16,)), dma((16,)),
            dma((3,)), dma((3,)),
            dma((16, 3)), dma((16, 3)),
            dma((3,)), dma((3,)),
            dma((5, 2)),
        ],
        compiler_params=pltpu.CompilerParams(collective_id=cid, has_side_effects=True, vmem_limit_bytes=67_043_328),
        name="attention_first",
    )(weights, rows, gates, normed, rope, gain, *experts)


def scatter_pairs(me, chunks, share, make, out_ref, from_b, from_a, from_far, send_sem, recv_sem):
    rows = from_a.shape[1] // chunks
    other = me.dp + me.pair
    bases = (me.dp, other, me.dp + me.far, other + me.far)
    items = [(j, k) for j in (2, 3, 1, 0) for k in range(chunks)]

    def at(k):
        return pl.ds(k * rows, rows)

    def copy(src, dst, slot, k, to):
        return me.copy(src, dst, send_sem.at[slot, k], recv_sem.at[slot, k], to)

    def send_b(g, j, k):
        return copy(share(bases[j] + me.db + g * me.da).at[at(k)], from_b.at[g, j, at(k)], g * 4 + j, k, me.dp + me.db)

    def send_a(j, k):
        return copy(from_b.at[1, j, at(k)], from_a.at[j, at(k)], 8 + j, k, me.dp + me.da)

    def send_far(j, k):
        return copy(from_b.at[0, 2 + j, at(k)], from_far.at[j, at(k)], 12 + j, k, me.dp + me.far)

    def swap(k):
        return copy(from_b.at[0, 1, at(k)], out_ref.at[me.half, at(k)], 14, k, other)

    for j in (2, 3, 1, 0):
        for g in (1, 0):
            make(bases[j] + me.db + g * me.da)
            for k in range(chunks):
                send_b(g, j, k).start()
        if j == 3:
            yield
    for j in (2, 3, 1, 0):
        make(bases[j] + me.da)
        make(bases[j])
        if j == 3:
            yield
    yield

    def first(item):
        j, k = item
        send_b(1, j, k).wait_recv()
        add_rows(from_b.at[1, j, at(k)], (share(bases[j] + me.da).at[at(k)], from_b.at[1, j, at(k)]), rows)
        send_a(j, k).start()

    def second(item):
        j, k = item
        send_b(0, j, k).wait_recv()
        send_a(j, k).wait_recv()
        terms = (share(bases[j]).at[at(k)], from_b.at[0, j, at(k)], from_a.at[j, at(k)])
        if j >= 2:
            add_rows(from_b.at[0, j, at(k)], terms, rows)
            send_far(j - 2, k).start()
        else:
            send_far(j, k).wait_recv()
            target = from_b.at[0, 1, at(k)] if j else out_ref.at[me.half, at(k)]
            add_rows(target, terms + (from_far.at[j, at(k)],), rows)
            if j:
                swap(k).start()

    yield from lagged(items, first, second, 2)
    for k in range(chunks):
        swap(k).wait_send()
        theirs = out_ref.at[1 - me.half, at(k)]
        copy(theirs, theirs, 14, k, other).wait_recv()
        for j in range(4):
            send_b(0, j, k).wait_send()
            send_b(1, j, k).wait_send()
            send_a(j, k).wait_send()
        send_far(0, k).wait_send()
        send_far(1, k).wait_send()


def sum_all(me, out_ref, held, send_sem, recv_sem):
    steps = ((me.dp, 1 - me.core), (me.dp + me.da, me.core), (me.dp + me.db, me.core), (me.dp + me.pair, me.core), (me.dp + me.far, me.core))
    yield
    for n, (to, core) in enumerate(steps):
        send = me.copy(held.at[0, n], held.at[1, n], send_sem.at[n], recv_sem.at[n], to, core)
        held[0, n] = out_ref[...]
        send.start()
        yield
        send.wait()
        out_ref[...] = held[0, n] + held[1, n]
        yield


def return_experts(me, gu_ref, down_ref, outs, own, held, core_send, core_recv, send_sem, recv_sem, copy_sem):
    rows, half = outs[0].shape[1:]

    def views(d, core):
        at = pl.ds(pl.multiple_of(d * rows, rows), rows)
        starts = ((gu_ref, core * half), (gu_ref, 2 * half + core * half), (down_ref, core * half))
        return [ref.at[at, pl.ds(pl.multiple_of(start, 128), half)] for ref, start in starts]

    def beside(r):
        d = (me.dp + r) % 16
        return [
            me.copy(src, held.at[j, r], core_send.at[r, j], core_recv.at[r, j], me.dp, 1 - me.core)
            for j, src in enumerate(views(d, 1 - me.core))
        ]

    order = (8, 7, 9, 4, 12, 5, 11, 6, 10, 3, 13, 2, 14, 1, 15, 0)

    def loads(n):
        d = (me.dp + order[n]) % 16
        return [pltpu.make_async_copy(src, own.at[j, n % 8], copy_sem.at[n % 8, j]) for j, src in enumerate(views(d, me.core))]

    def sends(r):
        d = (me.dp + r) % 16
        return [me.copy(held.at[j, r], outs[j].at[me.dp], send_sem.at[r, j], recv_sem.at[r, j], d) for j in range(3)]

    for r in order:
        for c in beside(r):
            c.start()
    for n in range(8):
        for c in loads(n):
            c.start()
    yield
    keep = [pltpu.make_async_copy(held.at[j, 0], outs[j].at[me.dp], copy_sem.at[16, j]) for j in range(3)]
    for n, r in enumerate(order):
        for j, (arrives, load) in enumerate(zip(beside(r), loads(n))):
            arrives.wait_recv()
            load.wait()
            add_rows(held.at[j, r], (own.at[j, n % 8], held.at[j, r]), rows, 64)
        for c in sends(r) if r else keep:
            c.start()
        if n < 8:
            for c in loads(n + 8):
                c.start()
        if n % 2:
            yield
    for r in range(1, 16):
        s = (me.dp + 16 - r) % 16
        for j in range(3):
            dst = outs[j].at[s]
            me.copy(dst, dst, send_sem.at[r, j], recv_sem.at[r, j], me.dp).wait_recv()
    for c in keep:
        c.wait()
    for r in range(16):
        for c in beside(r) + (sends(r) if r else []):
            c.wait_send()


def attention_back_kernel(
    chunks, head_dim,
    ga_ref, w_ref, seq_ref, raw_ref, low_ref, mixed_ref, rope_ref, gain_ref, unit_ref, x_ref, gu_ref, down_ref, share_ref,
    one_ref, moe_ref, out_ref, sum_ref, gate_out, up_out, down_out,
    w, ga, gmix, gproj, part, kept, dk, dv, gains, from_core, from_pair,
    pair_b, pair_a, pair_far, total, own, held,
    from_b, from_a, from_z, b_send, b_recv, a_send, a_recv, z_send, z_recv,
    four_send, four_recv, back_send, back_recv, pair_send, pair_recv, sum_send, sum_recv, core_send, core_recv, e_send, e_recv,
    copy_sem, load_sem,
):
    me = Place()
    rows, width = ga_ref.shape
    seq_len = 2 * rows
    q_cols = mixed_ref.shape[1]
    proj_cols = q_cols + 2 * head_dim
    group = q_cols // head_dim
    dot = functools.partial(jnp.dot, preferred_element_type=jnp.float32)
    dot_t = functools.partial(lax.dot_general, dimension_numbers=(((1,), (1,)), ((), ())), preferred_element_type=jnp.float32)
    t_dot = functools.partial(lax.dot_general, dimension_numbers=(((0,), (0,)), ((), ())), preferred_element_type=jnp.float32)
    load = pltpu.make_async_copy(w_ref, w, load_sem.at[8])
    load.start()
    keeps = [pltpu.make_async_copy(share_ref.at[n, pl.ds(0, rows)], kept.at[n], load_sem.at[n]) for n in range(8)]
    for c in keeps:
        c.start()
    me.greet(everyone=True, partner=True)

    def ga_at(h, core):
        return ga.at[pl.ds(pl.multiple_of((2 * h + core) * rows, rows), rows)]

    mine, theirs = ga_at(me.half, me.core), ga_at(1 - me.half, me.core)
    across = me.copy(ga_ref, mine, four_send.at[0], four_recv.at[0], me.dp + me.pair)
    beside = me.copy(ga_ref, mine, four_send.at[1], four_recv.at[1], me.dp, 1 - me.core)
    relay = me.copy(theirs, theirs, four_send.at[2], four_recv.at[2], me.dp, 1 - me.core)
    across.start()
    beside.start()
    mine[...] = ga_ref[...]
    scatter = ScatterRows(
        me, lambda n: share_ref.at[n, pl.ds(rows, rows)], lambda n: kept.at[n], from_b, from_a, from_z,
        (b_send, b_recv, a_send, a_recv, z_send, z_recv),
    )
    for m in (1, 2, 3, 0):
        scatter.send_b(2 * m + 1).start()
        scatter.send_b(2 * m).start()
    experts = return_experts(me, gu_ref, down_ref, (gate_out, up_out, down_out), own, held, core_send, core_recv, e_send, e_recv, copy_sem)
    for _ in range(9):
        next(experts)
    across.wait_recv()
    relay.start()
    across.wait_send()
    beside.wait()
    relay.wait()
    load.wait()
    for c in keeps:
        c.wait()

    def mix(j, _):
        at = pl.ds(pl.multiple_of(j * 256, 256), 256)
        at_w = pl.ds(pl.multiple_of(proj_cols + j * 256, 256), 256)
        gmix[:, at] = dot(ga[...], w[:, at_w]).astype(gmix.dtype)
        return 0

    lax.fori_loop(0, q_cols // 256, mix, 0)
    gains[...] = jnp.zeros_like(gains)
    turn = rope_ref[1]
    cosine = rope_ref[0]
    causal = lax.broadcasted_iota(jnp.int32, (seq_len, seq_len), 0) >= lax.broadcasted_iota(jnp.int32, (seq_len, seq_len), 1)
    k_at, v_at = pl.ds(q_cols, head_dim), pl.ds(q_cols + head_dim, head_dim)

    def back(grad, raw, which):
        grad = grad * cosine + pltpu.roll(grad, head_dim // 2, 1) * turn
        inverse = lax.rsqrt(jnp.mean(raw * raw, axis=-1, keepdims=True) + epsilon)
        gains[which] = gains[which] + jnp.sum(grad * (raw * inverse), axis=0, keepdims=True)
        scaled = grad * gain_ref[which]
        inner = jnp.mean(scaled * raw, axis=-1, keepdims=True)
        return inverse * scaled - raw * (inverse * inverse * inverse) * inner

    def head(n, _):
        at = pl.ds(pl.multiple_of(n // group * seq_len, seq_len), seq_len)
        cols = pl.ds(pl.multiple_of(n % group * head_dim, head_dim), head_dim)
        query, key, value, grad = low_ref[at, cols], low_ref[at, k_at], low_ref[at, v_at], gmix[at, cols]
        exp_scores = jnp.where(causal, jnp.exp(dot_t(query, key)), 0.0)
        probs = exp_scores / jnp.sum(exp_scores, axis=-1, keepdims=True)
        grad_probs = dot_t(grad, value)
        delta = jnp.sum(grad_probs * probs, axis=-1, keepdims=True)
        grad_scores = (probs * (grad_probs - delta)).astype(query.dtype)
        grad_query = dot(grad_scores, key) * head_dim ** (-0.5)
        grad_key = t_dot(grad_scores, query)
        grad_value = t_dot(probs.astype(query.dtype), grad)

        def begin():
            dk[...] = grad_key
            dv[...] = grad_value

        def more():
            dk[...] = dk[...] + grad_key
            dv[...] = dv[...] + grad_value

        pl.when(n % group == 0)(begin)
        pl.when(n % group != 0)(more)
        gproj[at, cols] = back(grad_query, raw_ref[at, cols], 0).astype(gproj.dtype)

        def close():
            gproj[at, k_at] = back(dk[...], raw_ref[at, k_at], 1).astype(gproj.dtype)
            gproj[at, v_at] = dv[...].astype(gproj.dtype)

        pl.when(n % group == group - 1)(close)
        return 0

    heads = 2 * group
    quarter = heads // 4
    for k in range(4):
        lax.fori_loop(k * quarter, (k + 1) * quarter, head, 0)
        scatter.first((1, 2, 3, 0)[k])
        if k:
            scatter.second((1, 2, 3, 0)[k - 1])

    def project(j, _):
        at = pl.ds(pl.multiple_of(j * 256, 256), 256)
        part[:, at] = dot_t(gproj[...], w[at, pl.ds(0, proj_cols)]).astype(part.dtype)
        return 0

    lax.fori_loop(0, width // 256, project, 0)

    def part_at(h, core):
        return part.at[pl.ds(pl.multiple_of((2 * h + core) * rows, rows), rows)]

    def give(h, slot):
        return me.copy(part_at(h, 1 - me.core), from_core.at[slot], back_send.at[slot], back_recv.at[slot], me.dp, 1 - me.core)

    give(1 - me.half, 0).start()
    give(me.half, 1).start()
    other = me.dp + me.pair
    bases = (me.dp, other, me.dp + me.far, other + me.far)

    def weight_block(d):
        at = pl.ds(pl.multiple_of(d * rows, rows), rows)
        w[at, pl.ds(0, proj_cols)] = t_dot(seq_ref[:, at], gproj[...]).astype(w.dtype)
        w[at, pl.ds(proj_cols, q_cols)] = t_dot(ga[:, at], mixed_ref[...]).astype(w.dtype)

    pairs = scatter_pairs(me, chunks, lambda d: w.at[pl.ds(pl.multiple_of(d * rows, rows), rows)], weight_block, out_ref, pair_b, pair_a, pair_far, pair_send, pair_recv)
    next(pairs)
    give(1 - me.half, 0).wait_recv()
    add_rows(from_core.at[0], (part_at(1 - me.half, me.core), from_core.at[0]), rows)
    over = me.copy(from_core.at[0], from_pair, back_send.at[2], back_recv.at[2], me.dp + me.pair)
    over.start()
    give(me.half, 1).wait_recv()
    add_rows(from_core.at[1], (part_at(me.half, me.core), from_core.at[1]), rows)
    next(pairs)
    scatter.second(0)
    next(pairs)
    over.wait_recv()
    add_rows(one_ref, (from_core.at[1], from_pair), rows)
    sum_ref[...] = x_ref[...]
    attn = jnp.sum(one_ref[...] * unit_ref[...], axis=0, keepdims=True)
    for j in range(width // 128):
        sum_ref[pl.ds(j, 1), :] = attn[:, j * 128 : (j + 1) * 128]
    for j in range(2):
        sum_ref[pl.ds(2 * width // 128 + j, 1), :] = gains[j]
    scatter.finish(moe_ref)
    run(pairs, experts, sum_all(me, sum_ref, total, sum_send, sum_recv))
    scatter.drain()
    give(0, 0).wait_send()
    give(0, 1).wait_send()
    over.wait_send()


def attention_back(grad_attn, weights, seq_normed, raw, low, mixed, rope, gain, unit, sums, gu, down, share, cid, chunks=2):
    rows, width = grad_attn.shape
    head_dim = rope.shape[-1]
    columns = weights.shape[1]
    half = down.shape[1] // 2
    hbm, vmem = pl.BlockSpec(memory_space=pl.ANY), pl.BlockSpec(memory_space=pltpu.VMEM)
    dma = pltpu.SemaphoreType.DMA
    dtype = weights.dtype
    proj_cols = raw.shape[1] + head_dim
    whole = jax.ShapeDtypeStruct((rows, width), jnp.float32)
    return pl.pallas_call(
        functools.partial(attention_back_kernel, chunks, head_dim),
        out_shape=[whole, whole, jax.ShapeDtypeStruct((2, rows, columns), dtype), jax.ShapeDtypeStruct(sums.shape, sums.dtype)]
        + [jax.ShapeDtypeStruct((16, rows, half), dtype)] * 3,
        in_specs=[vmem, hbm] + [vmem] * 8 + [hbm] * 3,
        out_specs=[vmem] * 4 + [hbm] * 3,
        scratch_shapes=[
            pltpu.VMEM(weights.shape, dtype),
            pltpu.VMEM((4 * rows, width), dtype),
            pltpu.VMEM(mixed.shape, dtype),
            pltpu.VMEM((4 * rows, proj_cols), dtype),
            pltpu.VMEM((4 * rows, width), dtype),
            pltpu.VMEM((8, rows, width), dtype),
            pltpu.VMEM((2 * rows, head_dim), jnp.float32),
            pltpu.VMEM((2 * rows, head_dim), jnp.float32),
            pltpu.VMEM((2, 1, head_dim), jnp.float32),
            pltpu.VMEM((2, rows, width), dtype),
            pltpu.VMEM((rows, width), dtype),
            pltpu.VMEM((2, 4, rows, columns), dtype),
            pltpu.VMEM((4, rows, columns), dtype),
            pltpu.VMEM((2, rows, columns), dtype),
            pltpu.VMEM((2, 5) + sums.shape, sums.dtype),
            pltpu.VMEM((3, 8, rows, half), dtype),
            pltpu.VMEM((3, 16, rows, half), dtype),
            *scatter_rows_scratch(rows, width, dtype),
            dma((3,)), dma((3,)),
            dma((3,)), dma((3,)),
            dma((15, chunks)), dma((15, chunks)),
            dma((5,)), dma((5,)),
            dma((16, 3)), dma((16, 3)),
            dma((16, 3)), dma((16, 3)),
            dma((17, 3)), dma((9,)),
        ],
        compiler_params=pltpu.CompilerParams(collective_id=cid, has_side_effects=True, vmem_limit_bytes=67_043_328),
        name="attention_back",
    )(grad_attn, weights, seq_normed, raw, low, mixed, rope, gain, unit, sums, gu, down, share)


class ScatterRows:
    def __init__(self, me, sent, kept, from_b, from_a, from_z, sems):
        self.me, self.sent, self.kept = me, sent, kept
        self.from_b, self.from_a, self.from_z = from_b, from_a, from_z
        self.b_send, self.b_recv, self.a_send, self.a_recv, self.z_send, self.z_recv = sems
        self.rows = from_b.shape[1]

    def send_b(self, n):
        me = self.me
        return me.copy(self.sent(n), self.from_b.at[n], self.b_send.at[n], self.b_recv.at[n], me.dp + me.db)

    def send_a(self, m):
        me = self.me
        return me.copy(self.from_b.at[2 * m + 1], self.from_a.at[m], self.a_send.at[m], self.a_recv.at[m], me.dp + me.da)

    def send_z(self, m):
        me = self.me
        return me.copy(self.from_b.at[2 * m], self.from_z.at[me.z], self.z_send.at[m], self.z_recv.at[me.z], me.at_z(me.z_of(m)))

    def first(self, m):
        n = 2 * m + 1
        self.send_b(n).wait_recv()
        add_rows(self.from_b.at[n], (self.kept(n), self.from_b.at[n]), self.rows)
        self.send_a(m).start()

    def second(self, m):
        n = 2 * m
        self.send_b(n).wait_recv()
        self.send_a(m).wait_recv()
        add_rows(self.from_b.at[n], (self.kept(n), self.from_b.at[n], self.from_a.at[m]), self.rows)
        pl.when(m > 0)(lambda: self.send_z(m).start())

    def advance(self, now, lags=(1, 2)):
        for lag, call in zip(lags, (self.first, self.second)):
            m = (now - 1 - lag) // 2
            due = jnp.logical_and((now - 1 - lag) % 2 == 0, jnp.logical_and(now > lag, m < 4))
            pl.when(due)(lambda: call(m))

    def finish(self, out_ref):
        me = self.me
        others = [(me.z + r) % 4 for r in range(1, 4)]
        for z in others:
            me.copy(self.from_z.at[z], self.from_z.at[z], self.z_send.at[0], self.z_recv.at[z], me.dp).wait_recv()
        add_rows(out_ref, (self.from_b.at[0],) + tuple(self.from_z.at[z] for z in others), self.rows)

    def drain(self):
        for m in range(4):
            self.send_b(2 * m).wait_send()
            self.send_b(2 * m + 1).wait_send()
            self.send_a(m).wait_send()
            if m:
                self.send_z(m).wait_send()


def scatter_rows_scratch(rows, columns, dtype):
    dma = pltpu.SemaphoreType.DMA
    return [
        pltpu.VMEM((8, rows, columns), dtype),
        pltpu.VMEM((4, rows, columns), dtype),
        pltpu.VMEM((4, rows, columns), dtype),
        dma((8,)), dma((8,)), dma((4,)), dma((4,)), dma((4,)), dma((4,)),
    ]


def experts_kernel(
    x_ref, c_ref, g_ref, gate_ref, up_ref, down_ref,
    share_ref, two_ref, gu_out, down_out, xg_ref,
    wgu, wd, ag, ggu, share, p, xb, cb, from_b, from_a, from_z, b_send, b_recv, a_send, a_recv, z_send, z_recv,
    g_send, g_recv, w_send, w_recv, load_sem, tile_sem, keep_sem, share_sem,
):
    me = Place()
    rows, width = x_ref.shape
    hidden = wd.shape[0]
    half = hidden // 2
    dot = functools.partial(jnp.dot, preferred_element_type=jnp.float32)
    dot_t = functools.partial(lax.dot_general, dimension_numbers=(((1,), (1,)), ((), ())), preferred_element_type=jnp.float32)
    t_dot = functools.partial(lax.dot_general, dimension_numbers=(((0,), (0,)), ((), ())), preferred_element_type=jnp.float32)
    upper, lower = pl.ds(rows, rows), pl.ds(0, rows)

    z_of, block = me.z_of, me.block

    def part(source, to, slot, own=False):
        return me.copy(x_ref if own else xg_ref.at[source], xg_ref.at[source], g_send.at[slot], g_recv.at[source], to)

    def arrive(m):
        source = me.at_z(z_of(m))
        part(source, me.dp, 0).wait_recv()
        part(source, me.dp + me.db, 3 + 2 * m).start()
        part(source, me.dp + me.da, 4 + 2 * m).start()

    def arrive_a(m):
        source = me.at_z(z_of(m)) + me.da
        part(source, me.dp, 0).wait_recv()
        part(source, me.dp + me.db, 11 + m).start()

    def loads(n):
        slot = n % 2
        copies = []
        for j, source in enumerate((block(n), block(n) + me.db)):
            at = pl.ds(j * rows, rows)
            copies.append(pltpu.make_async_copy(xg_ref.at[source], xb.at[slot, at], load_sem.at[slot, j]))
            copies.append(pltpu.make_async_copy(c_ref.at[source], cb.at[slot, at], load_sem.at[slot, 2 + j]))
        return copies

    def fetch(n):
        part(block(n) + me.db, me.dp, 0).wait_recv()
        for c in loads(n):
            c.start()

    scatter = ScatterRows(
        me, lambda n: p.at[n, upper], lambda n: p.at[n, lower], from_b, from_a, from_z, (b_send, b_recv, a_send, a_recv, z_send, z_recv)
    )

    def keep_share(n):
        return pltpu.make_async_copy(share.at[n % 2], share_ref.at[n], share_sem.at[n % 2])

    own = p.at[7, lower]
    load = pltpu.make_async_copy(x_ref, own, keep_sem.at[0])
    store = pltpu.make_async_copy(own, xg_ref.at[me.dp], keep_sem.at[1])
    load.start()

    def half_of(core):
        at = core * half
        return (
            wgu.at[:, pl.ds(pl.multiple_of(at, 128), half)],
            wgu.at[:, pl.ds(pl.multiple_of(hidden + at, 128), half)],
            wd.at[pl.ds(pl.multiple_of(at, 128), half)],
        )

    mine = (gate_ref, up_ref, down_ref)
    locals_ = [pltpu.make_async_copy(src, dst, keep_sem.at[2 + j]) for j, (src, dst) in enumerate(zip(mine, half_of(me.core)))]
    for c in locals_:
        c.start()
    me.greet(column=True, near=True, partner=True)
    for m in range(1, 4):
        part(me.dp, me.at_z(z_of(m)), m - 1, True).start()
    part(me.dp, me.dp + me.db, 3, True).start()
    part(me.dp, me.dp + me.da, 4, True).start()
    shares = [
        me.copy(src, dst, w_send.at[j], w_recv.at[j], me.dp, 1 - me.core) for j, (src, dst) in enumerate(zip(mine, half_of(me.core)))
    ]
    for c in shares:
        c.start()
    load.wait()
    store.start()
    arrive_a(0)
    store.wait()
    for c in locals_:
        c.wait()
    for j, dst in enumerate(half_of(1 - me.core)):
        me.copy(dst, dst, w_send.at[j], w_recv.at[j], me.dp).wait_recv()
    fetch(0)

    tile = 256

    def step(n, _):
        slot = n % 2
        for c in loads(n):
            c.wait()
        gates = jnp.concatenate([g_ref[block(n)], g_ref[block(n) + me.db]], axis=0)

        def inner(j, _):
            at, at_up = pl.ds(pl.multiple_of(j * tile, tile), tile), pl.ds(pl.multiple_of(hidden + j * tile, tile), tile)
            gate, up, grad = dot(xb[slot], wgu[:, at]), dot(xb[slot], wgu[:, at_up]), dot_t(cb[slot], wd[at, :]) * gates
            sig = 1.0 / (1.0 + jnp.exp(-gate))
            act = gate * sig
            ag[n, :, at] = (act * up * gates).astype(ag.dtype)
            ggu[n, :, at] = (grad * up * sig * (1.0 + gate * (1.0 - sig))).astype(ggu.dtype)
            ggu[n, :, at_up] = (grad * act).astype(ggu.dtype)
            return 0

        lax.fori_loop(0, hidden // tile, inner, 0)

        def at_step(k, *calls):
            def go():
                for call, m in calls:
                    call(m)

            pl.when(n == k)(go)

        at_step(0, (arrive, 1))
        at_step(1, (arrive, 2), (arrive_a, 1))
        at_step(2, (arrive, 3))
        at_step(3, (arrive_a, 2))
        at_step(4, (arrive_a, 3))
        pl.when(n < 7)(lambda: fetch(n + 1))

        pl.when(n >= 2)(lambda: keep_share(n - 2).wait())

        def outer(j, _):
            at = pl.ds(pl.multiple_of(j * 2 * tile, 2 * tile), 2 * tile)
            share[slot, :, at] = dot(ag[n], wd[:, at]).astype(p.dtype)
            p[n, :, at] = dot_t(ggu[n], wgu[at, :]).astype(p.dtype)
            return 0

        lax.fori_loop(0, width // (2 * tile), outer, 0)
        scatter.send_b(n).start()
        keep_share(n).start()
        scatter.advance(n)
        return 0

    lax.fori_loop(0, 8, step, 0)

    def tiles(i):
        slot = i % 2
        cols = pl.ds(pl.multiple_of(i * tile, tile), tile)
        copies = []
        for which, src in enumerate((xg_ref, c_ref)):
            to = pl.ds(pl.multiple_of((2 * which + slot) * tile, tile), tile)

            def one(n, side, which=which, src=src, to=to):
                at = pl.ds(pl.multiple_of((2 * n + side) * rows, rows), rows)
                return pltpu.make_async_copy(src.at[block(n) + side * me.db, :, cols], wgu.at[at, to], tile_sem.at[which, slot, 2 * n + side])

            copies.append(one)
        return copies

    def each_tile(i, act):
        for one in tiles(i):

            def body(n, _):
                for side in (0, 1):
                    act(one(n, side))
                return 0

            lax.fori_loop(0, 8, body, 0)

    def outs(i):
        slot = i % 2
        at = pl.ds(pl.multiple_of(i * tile, tile), tile)
        return (
            pltpu.make_async_copy(xb.at[slot, :, pl.ds(0, 2 * hidden)], gu_out.at[at], load_sem.at[slot, 0]),
            pltpu.make_async_copy(cb.at[slot, :, pl.ds(0, hidden)], down_out.at[at], load_sem.at[slot, 1]),
        )

    each_tile(0, lambda c: c.start())

    def weight_step(i, _):
        slot = i % 2
        pl.when(i < 7)(lambda: each_tile(i + 1, lambda c: c.start()))
        each_tile(i, lambda c: c.wait())

        def free():
            for c in outs(i - 2):
                c.wait()

        pl.when(i >= 2)(free)
        x_tile = wgu[:, pl.ds(pl.multiple_of(slot * tile, tile), tile)]
        xb[slot, :, pl.ds(0, 2 * hidden)] = t_dot(x_tile, ggu[...].reshape(-1, 2 * hidden)).astype(xb.dtype)
        c_tile = wgu[:, pl.ds(pl.multiple_of((2 + slot) * tile, tile), tile)]
        cb[slot, :, pl.ds(0, hidden)] = t_dot(c_tile, ag[...].reshape(-1, hidden)).astype(cb.dtype)
        for c in outs(i):
            c.start()
        scatter.advance(i + 8)
        return 0

    lax.fori_loop(0, 8, weight_step, 0)
    scatter.finish(two_ref)

    for i in (6, 7):
        for c in outs(i):
            c.wait()
    for c in shares:
        c.wait_send()
    for slot in range(15):
        part(me.dp, me.dp, slot).wait_send()
    scatter.drain()
    keep_share(6).wait()
    keep_share(7).wait()


def expert_layer(x, grads, gates, gate, up, down, cid):
    rows, width = x.shape
    half = gate.shape[1]
    hbm, vmem = pl.BlockSpec(memory_space=pl.ANY), pl.BlockSpec(memory_space=pltpu.VMEM)
    dma = pltpu.SemaphoreType.DMA
    dtype = x.dtype
    return pl.pallas_call(
        experts_kernel,
        out_shape=[
            jax.ShapeDtypeStruct((8, 2 * rows, width), dtype),
            jax.ShapeDtypeStruct((rows, width), jnp.float32),
            jax.ShapeDtypeStruct((width, 4 * half), dtype),
            jax.ShapeDtypeStruct((width, 2 * half), dtype),
            jax.ShapeDtypeStruct((16, rows, width), dtype),
        ],
        in_specs=[hbm, hbm, vmem, hbm, hbm, hbm],
        out_specs=[hbm, vmem, hbm, hbm, hbm],
        scratch_shapes=[
            pltpu.VMEM((width, 4 * half), dtype),
            pltpu.VMEM((2 * half, width), dtype),
            pltpu.VMEM((8, 2 * rows, 2 * half), dtype),
            pltpu.VMEM((8, 2 * rows, 4 * half), dtype),
            pltpu.VMEM((2, 2 * rows, width), dtype),
            pltpu.VMEM((8, 2 * rows, width), dtype),
            pltpu.VMEM((2, 2 * rows, width), dtype),
            pltpu.VMEM((2, 2 * rows, width), dtype),
            *scatter_rows_scratch(rows, width, dtype),
            dma((15,)), dma((16,)),
            dma((3,)), dma((3,)),
            dma((2, 4)), dma((2, 2, 16)), dma((5,)), dma((2,)),
        ],
        compiler_params=pltpu.CompilerParams(collective_id=cid, has_side_effects=True, vmem_limit_bytes=67_043_328),
        name="experts",
    )(x, grads, gates, gate, up, down)


def per_device_any(
    tokens,
    cotangent,
    expert_ids,
    gate_values,
    w_query,
    w_key,
    w_value,
    w_out,
    w_gate,
    w_up,
    w_down,
    attn_gain,
    ffn_gain,
    query_gain,
    key_gain,
):
    contract = (((1,), (1,)), ((), ()))
    contract_rows = (((0,), (0,)), ((), ()))
    residual = tokens.astype(jnp.float32)
    model_width = residual.shape[1]
    inverse_one = rms_inverse(residual)
    seq_normed = gather_rows((residual * inverse_one * attn_gain).astype(jnp.bfloat16))
    full_query, full_key, full_value, full_out = (
        lax.all_gather(w_query, "dp", axis=0, tiled=True),
        lax.all_gather(w_key, "dp", axis=0, tiled=True),
        lax.all_gather(w_value, "dp", axis=0, tiled=True),
        lax.all_gather(w_out, "dp", axis=1, tiled=True),
    )
    seq_len = seq_normed.shape[0]
    head_dim = query_gain.shape[0]
    local_heads = full_query.shape[1] // head_dim
    local_kv = full_key.shape[1] // head_dim
    group_size = local_heads // local_kv
    attn_scale = head_dim ** (-0.5)
    cosine, sine_table = rotary_tables(seq_len, head_dim)
    query_raw = jnp.dot(seq_normed, full_query, preferred_element_type=jnp.float32).reshape(
        seq_len, local_heads, head_dim
    )
    key_raw = jnp.dot(seq_normed, full_key, preferred_element_type=jnp.float32).reshape(
        seq_len, local_kv, head_dim
    )
    value_low = (
        jnp.dot(seq_normed, full_value, preferred_element_type=jnp.float32)
        .astype(jnp.bfloat16)
        .reshape(seq_len, local_kv, head_dim)
    )
    query_inverse = rms_inverse(query_raw)
    key_inverse = rms_inverse(key_raw)
    query_low = (
        rotate(query_raw * query_inverse * query_gain, cosine, sine_table) * attn_scale
    ).astype(jnp.bfloat16)
    key_low = rotate(key_raw * key_inverse * key_gain, cosine, sine_table).astype(jnp.bfloat16)
    query_heads = query_low.reshape(seq_len, local_kv, group_size, head_dim).transpose(1, 0, 2, 3)
    key_heads = key_low.transpose(1, 0, 2)
    value_heads = value_low.transpose(1, 0, 2)
    mixed_heads, logsum = lax.map(head_forward, (query_heads, key_heads, value_heads))
    mixed_flat = mixed_heads.transpose(1, 0, 2, 3).reshape(seq_len, local_heads * head_dim)
    hidden = residual + scatter_rows(
        jnp.dot(mixed_flat, full_out, preferred_element_type=jnp.float32)
    )
    inverse_two = rms_inverse(hidden)
    seq_two = gather_rows((hidden * inverse_two * ffn_gain).astype(jnp.bfloat16))
    seq_grad = gather_rows(cotangent)
    experts = w_gate.shape[0]
    dp_rows = w_gate.shape[1]
    hidden_units = w_gate.shape[2]
    dp_count = lax.axis_size("dp")
    group = dp_count // experts
    routed_rows = seq_len * expert_ids.shape[1] * 9 // 8
    capacity = (routed_rows + experts * group - 1) // (experts * group) * group
    slot_table, gate_table = dispatch(expert_ids, gate_values, experts, capacity)
    blank_row = jnp.zeros((1, model_width), jnp.bfloat16)
    padded_in = jnp.concatenate([seq_two, blank_row], axis=0)
    padded_grad = jnp.concatenate([seq_grad, blank_row], axis=0)
    empty_rows = jnp.zeros((seq_len + 1, model_width), jnp.float32)
    piece_rows = capacity // group
    down_rows = jnp.transpose(w_down, (0, 2, 1))
    gate_mine, up_mine, down_mine = (
        lax.all_to_all(widen(w_gate, group), "dp", split_axis=0, concat_axis=1, tiled=True),
        lax.all_to_all(widen(w_up, group), "dp", split_axis=0, concat_axis=1, tiled=True),
        lax.all_to_all(widen(down_rows, group), "dp", split_axis=0, concat_axis=1, tiled=True),
    )
    gate_mine = gate_mine[0]
    up_mine = up_mine[0]
    down_mine = down_mine[0]
    blocks_in = padded_in[slot_table]
    grad_blocks = (padded_grad[slot_table].astype(jnp.float32) * gate_table[:, :, None]).astype(
        jnp.bfloat16
    )
    recv_in, recv_grad = (
        lax.all_to_all(
            blocks_in.reshape(dp_count, piece_rows, model_width),
            "dp",
            split_axis=0,
            concat_axis=0,
            tiled=True,
        ),
        lax.all_to_all(
            grad_blocks.reshape(dp_count, piece_rows, model_width),
            "dp",
            split_axis=0,
            concat_axis=0,
            tiled=True,
        ),
    )
    rows_in = recv_in.reshape(-1, model_width)
    rows_grad = recv_grad.reshape(-1, model_width)
    gate_pre = jnp.dot(rows_in, gate_mine, preferred_element_type=jnp.float32)
    up_pre = jnp.dot(rows_in, up_mine, preferred_element_type=jnp.float32)
    act_low = (jax.nn.silu(gate_pre) * up_pre).astype(jnp.bfloat16)
    expert_out = lax.dot_general(act_low, down_mine, contract, preferred_element_type=jnp.float32)
    grad_act = jnp.dot(rows_grad, down_mine, preferred_element_type=jnp.float32)
    sigmoid_gate = jax.nn.sigmoid(gate_pre)
    grad_gate = (grad_act * up_pre * sigmoid_gate * (1.0 + gate_pre * (1.0 - sigmoid_gate))).astype(
        jnp.bfloat16
    )
    grad_up = (grad_act * gate_pre * sigmoid_gate).astype(jnp.bfloat16)
    grad_input = lax.dot_general(
        grad_gate, gate_mine, contract, preferred_element_type=jnp.float32
    ) + lax.dot_general(grad_up, up_mine, contract, preferred_element_type=jnp.float32)
    back_out, back_grad = (
        lax.all_to_all(
            expert_out.reshape(dp_count, piece_rows, model_width).astype(jnp.bfloat16),
            "dp",
            split_axis=0,
            concat_axis=0,
            tiled=True,
        ).astype(jnp.float32),
        lax.all_to_all(
            grad_input.reshape(dp_count, piece_rows, model_width).astype(jnp.bfloat16),
            "dp",
            split_axis=0,
            concat_axis=0,
            tiled=True,
        ).astype(jnp.float32),
    )
    back_out = back_out.reshape(experts, capacity, model_width)
    back_grad = back_grad.reshape(experts * capacity, model_width)
    flat_slots = slot_table.reshape(-1)
    combined = empty_rows.at[flat_slots].add(
        (back_out * gate_table[:, :, None]).reshape(-1, model_width)
    )
    grad_acc = empty_rows.at[flat_slots].add(back_grad)
    grad_both = jnp.concatenate([grad_gate, grad_up], axis=1)
    grad_cols = jnp.concatenate(
        [
            lax.dot_general(rows_in, grad_both, contract_rows, preferred_element_type=jnp.float32),
            lax.dot_general(rows_grad, act_low, contract_rows, preferred_element_type=jnp.float32),
        ],
        axis=1,
    )
    returned = lax.all_to_all(
        grad_cols[None].astype(jnp.bfloat16), "dp", split_axis=1, concat_axis=0, tiled=True
    ).astype(jnp.float32)
    summed = jnp.sum(returned.reshape(experts, group, dp_rows, 3 * hidden_units), axis=1)
    grad_w_gate = summed[:, :, :hidden_units]
    grad_w_up = summed[:, :, hidden_units : 2 * hidden_units]
    grad_w_down = jnp.transpose(summed[:, :, 2 * hidden_units :], (0, 2, 1))
    output = (hidden + scatter_rows(combined[:seq_len])).astype(jnp.bfloat16)
    grad_two = scatter_rows(grad_acc[:seq_len])
    ffn_gain_part = jnp.sum(grad_two * hidden * inverse_two, axis=0)
    grad_hidden = cotangent.astype(jnp.float32) + norm_backward(
        grad_two, hidden, inverse_two, ffn_gain
    )
    grad_attn = gather_rows(grad_hidden.astype(jnp.bfloat16))
    grad_mixed = lax.dot_general(
        grad_attn, full_out, contract, preferred_element_type=jnp.float32
    ).astype(jnp.bfloat16)
    grad_mixed_heads = grad_mixed.reshape(seq_len, local_kv, group_size, head_dim).transpose(
        1, 0, 2, 3
    )
    grad_query_heads, grad_key_heads, grad_value_heads = lax.map(
        head_backward, (query_heads, key_heads, value_heads, logsum, grad_mixed_heads)
    )
    grad_query_rot = (
        grad_query_heads.transpose(1, 0, 2, 3).reshape(seq_len, local_heads, head_dim) * attn_scale
    )
    grad_query_norm = rotate_back(grad_query_rot, cosine, sine_table)
    query_gain_part = jnp.sum(grad_query_norm * query_raw * query_inverse, axis=(0, 1))
    grad_query_low = (
        norm_backward(grad_query_norm, query_raw, query_inverse, query_gain)
        .astype(jnp.bfloat16)
        .reshape(seq_len, local_heads * head_dim)
    )
    grad_key_norm = rotate_back(grad_key_heads.transpose(1, 0, 2), cosine, sine_table)
    key_gain_part = jnp.sum(grad_key_norm * key_raw * key_inverse, axis=(0, 1))
    grad_key_low = (
        norm_backward(grad_key_norm, key_raw, key_inverse, key_gain)
        .astype(jnp.bfloat16)
        .reshape(seq_len, local_kv * head_dim)
    )
    grad_value_low = (
        grad_value_heads.transpose(1, 0, 2)
        .reshape(seq_len, local_kv * head_dim)
        .astype(jnp.bfloat16)
    )
    grad_proj = jnp.concatenate([grad_query_low, grad_key_low, grad_value_low], axis=1)
    full_proj = jnp.concatenate([full_query, full_key, full_value], axis=1)
    grad_one = scatter_rows(
        lax.dot_general(grad_proj, full_proj, contract, preferred_element_type=jnp.float32)
    )
    first_part = jnp.einsum("sd,sf->df", seq_normed, grad_proj, preferred_element_type=jnp.float32)
    second = jnp.einsum("sd,sf->df", grad_attn, mixed_flat, preferred_element_type=jnp.float32)
    shares = lax.psum_scatter(
        jnp.concatenate([first_part, second], axis=1), "dp", scatter_dimension=0, tiled=True
    )
    query_cols = w_query.shape[1]
    key_cols = w_key.shape[1]
    grad_w_query = shares[:, :query_cols]
    grad_w_key = shares[:, query_cols : query_cols + key_cols]
    grad_w_value = shares[:, query_cols + key_cols : query_cols + 2 * key_cols]
    grad_w_out = jnp.transpose(shares[:, query_cols + 2 * key_cols :])
    attn_gain_part = jnp.sum(grad_one * residual * inverse_one, axis=0)
    grad_tokens = (grad_hidden + norm_backward(grad_one, residual, inverse_one, attn_gain)).astype(
        jnp.bfloat16
    )
    total_gains = lax.psum(
        (attn_gain_part, ffn_gain_part, query_gain_part, key_gain_part), ("dp", "tensor")
    )
    return (
        output,
        grad_tokens,
        grad_w_query,
        grad_w_key,
        grad_w_value,
        grad_w_out,
        grad_w_gate,
        grad_w_up,
        grad_w_down,
        total_gains[0],
        total_gains[1],
        total_gains[2],
        total_gains[3],
    )


def per_device_relay(
    tokens,
    cotangent,
    expert_ids,
    gate_values,
    w_query,
    w_key,
    w_value,
    w_out,
    w_gate,
    w_up,
    w_down,
    attn_gain,
    ffn_gain,
    query_gain,
    key_gain,
):
    dot = functools.partial(jnp.dot, preferred_element_type=jnp.float32)
    dot_t = functools.partial(lax.dot_general, dimension_numbers=(((1,), (1,)), ((), ())), preferred_element_type=jnp.float32)
    t_dot = functools.partial(lax.dot_general, dimension_numbers=(((0,), (0,)), ((), ())), preferred_element_type=jnp.float32)
    low = jnp.bfloat16
    rows, width = tokens.shape
    head_dim = query_gain.shape[0]
    experts = w_gate.shape[0]
    core = lax.axis_index("tensor")
    mine = lax.dynamic_slice_in_dim(expert_ids, core * rows, rows, 0)
    values = lax.dynamic_slice_in_dim(gate_values, core * rows, rows, 0)
    match = mine[None] == jnp.arange(experts, dtype=jnp.int32)[:, None, None]
    gates = jnp.sum(jnp.where(match, values[None], 0.0), axis=2)
    gates = jnp.broadcast_to(gates[:, None], (experts, 8, rows))

    q_cols, kv_cols = w_query.shape[1] // 2, w_key.shape[1] // 2
    w_out_rows = jnp.transpose(w_out)
    halves = jnp.stack(
        [
            jnp.concatenate([w[:, h * (w.shape[1] // 2) : (h + 1) * (w.shape[1] // 2)] for w in (w_query, w_key, w_value, w_out_rows)], axis=1)
            for h in range(2)
        ]
    )
    residual = tokens.astype(jnp.float32)
    inverse_one = rms_inverse(residual)
    normed_one = (residual * inverse_one * attn_gain).astype(low)
    cosine, sine_table = rotary_tables(2 * rows, head_dim)
    rope = jnp.stack([jnp.concatenate([v, w], axis=1) for v, w in ((cosine[:, 0], cosine[:, 0]), (sine_table[:, 0], -sine_table[:, 0]))])
    gain = jnp.stack([query_gain, key_gain])[:, None]
    weights, rows_grad, gates, seq_normed, raw, lows, mixed, attended, *projections = attention_first(
        halves, cotangent, gates, normed_one, rope, gain, (w_gate, w_up, w_down), 1
    )
    weights, gates, seq_normed = weights.reshape(-1, weights.shape[2]), gates[:, 0][:, :, None], seq_normed.reshape(-1, width)
    proj_cols = q_cols + 2 * kv_cols
    hidden = residual + attended
    inverse_two = rms_inverse(hidden)
    normed_two = (hidden * inverse_two * ffn_gain).astype(low)
    share, grad_two, gu_part, down_part, _ = expert_layer(normed_two, rows_grad, gates, *projections, 2)
    ffn_gain_part = jnp.sum(grad_two * hidden * inverse_two, axis=0)
    grad_hidden = cotangent.astype(jnp.float32) + norm_backward(grad_two, hidden, inverse_two, ffn_gain)
    gains = jnp.pad(ffn_gain_part, (width, 1024)).reshape(-1, 128)
    grad_one, moe, shares, totals, *grads_moe = attention_back(
        grad_hidden.astype(low), weights, seq_normed, raw, lows, mixed, rope, gain, residual * inverse_one, gains, gu_part, down_part, share, 9
    )
    output = (hidden + moe).astype(low)
    grad_w_gate, grad_w_up, grad_w_down = [v.astype(jnp.float32) for v in grads_moe]
    grad_w_down = jnp.transpose(grad_w_down, (0, 2, 1))
    shares, totals = shares.astype(jnp.float32), totals.reshape(-1)
    stops = (0, q_cols, q_cols + kv_cols, proj_cols, proj_cols + q_cols)
    grads = [jnp.concatenate([shares[0, :, a:b], shares[1, :, a:b]], axis=1) for a, b in zip(stops, stops[1:])]
    grad_tokens = (grad_hidden + norm_backward(grad_one, residual, inverse_one, attn_gain)).astype(low)
    totals = jnp.split(totals, (width, 2 * width, 2 * width + head_dim, 2 * width + 2 * head_dim))[:4]
    return (output, grad_tokens, grads[0], grads[1], grads[2], jnp.transpose(grads[3]), grad_w_gate, grad_w_up, grad_w_down, *totals)


def solution(mesh):
    return jax.shard_map(
        per_device_relay if tuple(mesh.shape.values()) == (16, 2) else per_device_any,
        mesh=mesh,
        in_specs=(
            P(("dp", "tensor"), None),
            P(("dp", "tensor"), None),
            P("dp", None),
            P("dp", None),
            P("dp", "tensor"),
            P("dp", "tensor"),
            P("dp", "tensor"),
            P("tensor", "dp"),
            P(None, "dp", "tensor"),
            P(None, "dp", "tensor"),
            P(None, "tensor", "dp"),
            P(),
            P(),
            P(),
            P(),
        ),
        out_specs=(
            P(("dp", "tensor"), None),
            P(("dp", "tensor"), None),
            P("dp", "tensor"),
            P("dp", "tensor"),
            P("dp", "tensor"),
            P("tensor", "dp"),
            P(None, "dp", "tensor"),
            P(None, "dp", "tensor"),
            P(None, "tensor", "dp"),
            P(),
            P(),
            P(),
            P(),
        ),
        check_vma=False,
    )
```

```python
import functools

import jax
import jax.numpy as jnp
from jax import lax
from jax.experimental import pallas as pl
from jax.experimental.pallas import tpu as pltpu
from jax.sharding import PartitionSpec as P

epsilon = 1e-06
theta_base = 1000000.0


def rms_inverse(values):
    return lax.rsqrt(jnp.mean(values * values, axis=-1, keepdims=True) + epsilon)


def norm_backward(grad_in, values, inverse, gain_vec):
    scaled = grad_in * gain_vec
    inner_mean = jnp.mean(scaled * values, axis=-1, keepdims=True)
    return inverse * scaled - values * inverse**3 * inner_mean


def rotary_tables(seq_len, head_dim):
    half_dim = head_dim // 2
    frequency = theta_base ** (-jnp.arange(half_dim, dtype=jnp.float32) * 2.0 / head_dim)
    angles = jnp.arange(seq_len, dtype=jnp.float32)[:, None] * frequency[None, :]
    return (jnp.cos(angles)[:, None, :], jnp.sin(angles)[:, None, :])


def rotate(values, cosine, sine_table):
    half_dim = values.shape[-1] // 2
    first_part = values[..., :half_dim]
    second = values[..., half_dim:]
    return jnp.concatenate(
        [first_part * cosine - second * sine_table, second * cosine + first_part * sine_table],
        axis=-1,
    )


def rotate_back(grad_in, cosine, sine_table):
    half_dim = grad_in.shape[-1] // 2
    first_part = grad_in[..., :half_dim]
    second = grad_in[..., half_dim:]
    return jnp.concatenate(
        [first_part * cosine + second * sine_table, second * cosine - first_part * sine_table],
        axis=-1,
    )


def dispatch(expert_ids, gate_values, experts, capacity):
    seq_len = expert_ids.shape[0]
    is_match = expert_ids[:, :, None] == jnp.arange(experts, dtype=jnp.int32)[None, None, :]
    expert_hits = jnp.sum(is_match.astype(jnp.int32), axis=1)
    before = jnp.cumsum(expert_hits, axis=0) - expert_hits
    slot_ids = jnp.sum(jnp.where(is_match, before[:, None, :], 0), axis=2)
    token_index = jnp.broadcast_to(jnp.arange(seq_len, dtype=jnp.int32)[:, None], expert_ids.shape)
    slot_table = (
        jnp.full((experts, capacity), seq_len, jnp.int32).at[expert_ids, slot_ids].set(token_index)
    )
    gate_table = (
        jnp.zeros((experts, capacity), jnp.float32).at[expert_ids, slot_ids].set(gate_values)
    )
    return (slot_table, gate_table)


def head_forward(head_inputs):
    query_vals, key_vals, value_vals = head_inputs
    seq_len = key_vals.shape[0]
    block_rows = min(512, seq_len)
    key_positions = jnp.arange(seq_len)

    def one_block(row_start):
        scores = jnp.einsum("qgd,sd->gqs", query_vals, key_vals, preferred_element_type=jnp.float32)
        causal = (row_start + jnp.arange(block_rows))[:, None] >= key_positions[None, :]
        exp_scores = jnp.where(causal, jnp.exp(scores), 0.0)
        denominator = jnp.sum(exp_scores, axis=-1, keepdims=True)
        softmax_low = (exp_scores / denominator).astype(jnp.bfloat16)
        mixed_out = jnp.einsum(
            "gqs,sd->qgd", softmax_low, value_vals, preferred_element_type=jnp.float32
        )
        return (mixed_out.astype(jnp.bfloat16), jnp.log(denominator[..., 0]))

    block_starts = jnp.arange(seq_len // block_rows, dtype=jnp.int32) * block_rows
    mixed_out, logsum = lax.map(one_block, block_starts)
    return (mixed_out.reshape(seq_len, query_vals.shape[1], query_vals.shape[2]), logsum)


def head_backward(head_inputs):
    query_vals, key_vals, value_vals, logsum, grad_mixed = head_inputs
    seq_len = key_vals.shape[0]
    block_rows = min(512, seq_len)
    key_positions = jnp.arange(seq_len)

    def one_block(state_in, block_in):
        grad_key, grad_value = state_in
        row_start, block_logsum = block_in
        scores = jnp.einsum("qgd,sd->gqs", query_vals, key_vals, preferred_element_type=jnp.float32)
        causal = (row_start + jnp.arange(block_rows))[:, None] >= key_positions[None, :]
        softmax_vals = jnp.where(causal, jnp.exp(scores - block_logsum[..., None]), 0.0)
        grad_probs = jnp.einsum(
            "qgd,sd->gqs", grad_mixed, value_vals, preferred_element_type=jnp.float32
        )
        delta_sum = jnp.sum(grad_probs * softmax_vals, axis=-1, keepdims=True)
        grad_scores = (softmax_vals * (grad_probs - delta_sum)).astype(jnp.bfloat16)
        grad_query = jnp.einsum(
            "gqs,sd->qgd", grad_scores, key_vals, preferred_element_type=jnp.float32
        )
        grad_key = grad_key + jnp.einsum(
            "gqs,qgd->sd", grad_scores, query_vals, preferred_element_type=jnp.float32
        )
        grad_value = grad_value + jnp.einsum(
            "gqs,qgd->sd",
            softmax_vals.astype(jnp.bfloat16),
            grad_mixed,
            preferred_element_type=jnp.float32,
        )
        return ((grad_key, grad_value), grad_query)

    block_starts = jnp.arange(seq_len // block_rows, dtype=jnp.int32) * block_rows
    zero_rows = jnp.zeros(key_vals.shape, jnp.float32)
    (grad_key, grad_value), grad_query = lax.scan(
        one_block, (zero_rows, zero_rows), (block_starts, logsum)
    )
    return (grad_query.reshape(query_vals.shape), grad_key, grad_value)


def gather_rows(values):
    return lax.all_gather(values, "tensor", axis=0, tiled=True)


def scatter_rows(values):
    return lax.psum_scatter(
        values.astype(jnp.bfloat16), "tensor", scatter_dimension=0, tiled=True
    ).astype(jnp.float32)


def widen(stacked, group):
    experts = stacked.shape[0]
    spread = jnp.broadcast_to(stacked[:, None], (experts, group) + stacked.shape[1:])
    return spread.reshape((experts * group,) + stacked.shape[1:])


MESH = pl.DeviceIdType.MESH
LIMIT = 66_000_000


class Place:
    def __init__(self):
        self.dp = lax.axis_index("dp")
        self.core = lax.axis_index("tensor")
        x, y = self.dp % 2, (self.dp // 2) % 2
        self.z = self.dp // 4
        step_x, step_y = 1 - 2 * x, 2 * (1 - 2 * y)
        self.da = (1 - self.core) * step_x + self.core * step_y
        self.db = (1 - self.core) * step_y + self.core * step_x
        self.half = self.z % 2
        self.pair = 4 * (1 - 2 * self.half)
        self.far = 8 * (1 - 2 * (self.z // 2))

    def copy(self, src, dst, send_sem, recv_sem, to, core=None):
        return pltpu.make_async_remote_copy(
            src_ref=src,
            dst_ref=dst,
            send_sem=send_sem,
            recv_sem=recv_sem,
            device_id=(to, self.core if core is None else core),
            device_id_type=MESH,
        )

    def at_z(self, z):
        return self.dp + 4 * (z - self.z)

    def z_of(self, m):
        low = self.z < 2
        depth = jnp.where(low, self.z, 3 - self.z)
        t = jnp.where(m == 0, depth, jnp.where(m == 1, 1 - depth, m))
        return jnp.where(low, t, 3 - t)

    def block(self, n):
        return self.at_z(self.z_of(n // 2)) + (n % 2) * self.da

    def greet(self, line=False, column=False, near=False, chain=False, everyone=False, partner=False):
        barrier = pltpu.get_barrier_semaphore()
        count = 0

        def signal(to, core):
            pl.semaphore_signal(barrier, inc=1, device_id=(to, core), device_id_type=MESH)

        if everyone:
            for r in range(1, 16):
                signal((self.dp + r) % 16, self.core)
            count = count + 15
        else:
            if near:
                signal(self.dp + self.da, self.core)
                signal(self.dp + self.db, self.core)
                count = count + 2
            if chain:
                signal(self.dp + self.pair, self.core)
                count = count + 1
                if near:
                    signal(self.dp + self.far, self.core)
                    count = count + 1
            if column:
                for r in range(1, 4):
                    signal((self.dp + 4 * r) % 16, self.core)
                count = count + 3
            if line:
                pl.when(self.z > 0)(lambda: signal(self.dp - 4, self.core))
                pl.when(self.z < 3)(lambda: signal(self.dp + 4, self.core))
                count = count + jnp.where(self.z > 0, 1, 0) + jnp.where(self.z < 3, 1, 0)
        if partner:
            signal(self.dp, 1 - self.core)
            count = count + 1
        pl.semaphore_wait(barrier, count)


def each_rows(rows, body, start=None, block=16):
    def go(i, carried):
        return body(pl.ds(pl.multiple_of(i * block, block), block), carried)

    return lax.fori_loop(0, rows // block, go, 0 if start is None else start)


def add_rows(target, terms, rows, block=16):
    def body(i, _):
        at = pl.ds(pl.multiple_of(i * block, block), block)
        total = terms[0][at, :].astype(jnp.float32)
        for term in terms[1:]:
            total = total + term[at, :].astype(jnp.float32)
        target[at, :] = total.astype(target.dtype)
        return 0

    lax.fori_loop(0, rows // block, body, 0)


def run(*threads):
    threads = list(threads)
    while threads:
        for thread in list(threads):
            if next(thread, "end") == "end":
                threads.remove(thread)


class Threads:
    def __init__(self, *threads):
        self.threads = list(threads)

    def step(self, times=1):
        for _ in range(times):
            for thread in list(self.threads):
                if next(thread, "end") == "end":
                    self.threads.remove(thread)

    def finish(self):
        while self.threads:
            self.step()


def lagged(items, first, second, lag):
    for n in range(len(items) + lag):
        if n < len(items):
            first(items[n])
            yield
        if n >= lag:
            second(items[n - lag])
            yield


def gather_line(me, x_ref, out_ref, send_sem, recv_sem):
    def part(source, to, slot, own=False):
        return me.copy(x_ref if own else out_ref.at[source], out_ref.at[source], send_sem.at[slot], recv_sem.at[source], to)

    sides = ((-1, me.z < 3, 4), (1, me.z > 0, -4))

    def exists(d, side):
        return (me.z - d >= 0) if side == 0 else (me.z + d <= 3)

    def slot_z(d, side, j):
        return 4 + ((d - 1) * 2 + side) * 3 + j

    def slot_a(off):
        return 25 + off

    def pass_a(off):
        source = me.dp + me.da + 4 * off
        part(source, me.dp, slot_a(off)).wait_recv()
        part(source, me.dp + me.db, slot_a(off)).start()

    pl.when(me.z < 3)(lambda: part(me.dp, me.dp + 4, 0, True).start())
    pl.when(me.z > 0)(lambda: part(me.dp, me.dp - 4, 1, True).start())
    part(me.dp, me.dp + me.db, 3, True).start()
    part(me.dp, me.dp + me.da, 2, True).start()
    yield
    for d in range(1, 5):
        if d < 4:
            for side, (sign, forward, step) in enumerate(sides):
                source = me.dp + 4 * sign * d

                def arrive():
                    part(source, me.dp, slot_z(d, side, 0)).wait_recv()
                    pl.when(forward)(lambda: part(source, me.dp + step, slot_z(d, side, 0)).start())
                    part(source, me.dp + me.db, slot_z(d, side, 2)).start()
                    part(source, me.dp + me.da, slot_z(d, side, 1)).start()

                pl.when(exists(d, side))(arrive)
                yield
        if d == 1:
            pass_a(0)
            yield
        else:
            for side, (sign, *_) in enumerate(sides):
                pl.when(exists(d - 1, side))(lambda: pass_a(sign * (d - 1)))
                yield
    for z in range(4):
        for g in (0, 1):
            part(me.at_z(z) + me.db + g * me.da, me.dp, 0).wait_recv()
            yield

    def sent(slot):
        part(me.dp, me.dp, slot).wait_send()

    pl.when(me.z < 3)(lambda: sent(0))
    pl.when(me.z > 0)(lambda: sent(1))
    sent(2)
    sent(3)
    sent(slot_a(0))
    for d in range(1, 4):
        for side, (sign, forward, _) in enumerate(sides):

            def finish():
                pl.when(forward)(lambda: sent(slot_z(d, side, 0)))
                sent(slot_z(d, side, 1))
                sent(slot_z(d, side, 2))
                sent(slot_a(sign * d))

            pl.when(exists(d, side))(finish)


def gather_pairs(me, x_ref, out_ref, send_sem, recv_sem):
    mine, other = me.dp, me.dp + me.pair
    chunks = send_sem.shape[1]
    rows = x_ref.shape[1] // chunks

    def part(src, where, to, slot, k):
        at = pl.ds(k * rows, rows)
        return me.copy(src.at[at], out_ref.at[where, at], send_sem.at[slot, k], recv_sem.at[where, k], to)

    def step(where, *relays):
        for k in range(chunks):
            part(out_ref.at[where], where, me.dp, 0, k).wait_recv()
            for to, slot in relays:
                part(out_ref.at[where], where, to, slot, k).start()

    far, db, da = me.dp + me.far, me.dp + me.db, me.dp + me.da
    for k in range(chunks):
        part(x_ref.at[1 - me.half], mine, other, 0, k).start()
        part(x_ref.at[me.half], mine, far, 1, k).start()
        part(x_ref.at[me.half], mine, db, 2, k).start()
        part(x_ref.at[me.half], mine, da, 3, k).start()
    yield
    step(other, (far, 4), (db, 5), (da, 6))
    yield
    step(mine + me.da, (db, 7))
    yield
    step(mine + me.far, (db, 8), (da, 9))
    yield
    step(other + me.da, (db, 10))
    yield
    step(other + me.far, (db, 11), (da, 12))
    yield
    step(mine + me.far + me.da, (db, 13))
    yield
    step(other + me.far + me.da, (db, 14))
    yield
    for base in (mine, other, mine + me.far, other + me.far):
        step(base + me.db)
        yield
        step(base + me.da + me.db)
        yield
    for slot in range(15):
        for k in range(chunks):
            part(out_ref.at[mine], mine, me.dp, slot, k).wait_send()


def swap_rows(me, x_ref, out_ref, send_sem, recv_sem):
    for r in range(1, 16):
        to = (me.dp + r) % 16
        me.copy(x_ref.at[to], out_ref.at[me.dp], send_sem.at[r], recv_sem.at[r], to).start()
    yield
    for r in range(1, 16):
        s = (me.dp + 16 - r) % 16
        me.copy(x_ref.at[s], out_ref.at[s], send_sem.at[r], recv_sem.at[r], me.dp).wait_recv()
    for r in range(1, 16):
        me.copy(x_ref.at[me.dp], out_ref.at[me.dp], send_sem.at[r], recv_sem.at[r], me.dp).wait_send()


def keep_own(src, staging, dst, sems):
    load = pltpu.make_async_copy(src, staging, sems.at[0])
    store = pltpu.make_async_copy(staging, dst, sems.at[1])
    load.start()

    def finish():
        load.wait()
        store.start()
        store.wait()

    return finish


def share_experts(me, ins, outs, send_sem, recv_sem):
    depth = ins[0].shape[1]

    def sends(r):
        to = (me.dp + r) % 16
        at = pl.ds(pl.multiple_of(me.dp * depth, depth), depth)
        pairs = ((ins[0].at[to], outs[0].at[at]), (ins[1].at[to], outs[1].at[at]), (ins[2].at[to], outs[2].at[:, at]))
        return [me.copy(src, dst, send_sem.at[r, j], recv_sem.at[r, j], to) for j, (src, dst) in enumerate(pairs)]

    for r in (8, 7, 9, 4, 12, 5, 11, 6, 10, 3, 13, 2, 14, 1, 15):
        for c in sends(r):
            c.start()
        yield
    for r in range(1, 16):
        at = pl.ds(pl.multiple_of((me.dp + 16 - r) % 16 * depth, depth), depth)
        for j, dst in enumerate((outs[0].at[at], outs[1].at[at], outs[2].at[:, at])):
            me.copy(dst, dst, send_sem.at[r, j], recv_sem.at[r, j], me.dp).wait_recv()
    for r in range(1, 16):
        for c in sends(r):
            c.wait_send()


def gather_four(me, x_ref, out_ref, send_sem, recv_sem):
    mine, theirs = out_ref.at[me.half, me.core], out_ref.at[1 - me.half, me.core]
    across = me.copy(x_ref, mine, send_sem.at[0], recv_sem.at[0], me.dp + me.pair)
    across.start()
    beside = me.copy(x_ref, mine, send_sem.at[1], recv_sem.at[1], me.dp, 1 - me.core)
    beside.start()
    mine[...] = x_ref[...]
    yield
    across.wait_recv()
    relay = me.copy(theirs, theirs, send_sem.at[2], recv_sem.at[2], me.dp, 1 - me.core)
    relay.start()
    yield
    across.wait_send()
    beside.wait()
    relay.wait()


def attention_first_kernel(
    head_dim, start,
    w_ref, c_ref, g_ref, x_ref, rope_ref, gain_ref, tokens_ref, ffn_ref, gate_ref, up_ref, down_ref,
    w_out, c_out, g_out, seq, raw, low, mixed, hidden_ref, normed_ref, gate_out, up_out, down_out,
    w, c_own, e_own, part, from_core, from_pair,
    w_send, w_recv, c_send, c_recv, g_send, g_recv, x_send, x_recv, e_send, e_recv, back_send, back_recv, copy_sem,
):
    me = Place()
    rows, width = x_ref.shape
    seq_len = 2 * rows
    q_cols = mixed.shape[1]
    proj_cols = q_cols + 2 * head_dim
    group = q_cols // head_dim
    depth = gate_ref.shape[1]
    dot = functools.partial(jnp.dot, preferred_element_type=jnp.float32)
    dot_t = functools.partial(lax.dot_general, dimension_numbers=(((1,), (1,)), ((), ())), preferred_element_type=jnp.float32)
    at_mine = pl.ds(pl.multiple_of(me.dp * depth, depth), depth)
    ends = [
        keep_own(c_ref, c_own, c_out.at[me.dp], copy_sem.at[1]),
        keep_own(gate_ref.at[me.dp], e_own.at[0], gate_out.at[at_mine], copy_sem.at[2]),
        keep_own(up_ref.at[me.dp], e_own.at[1], up_out.at[at_mine], copy_sem.at[3]),
    ]
    flat = pltpu.make_async_copy(down_ref.at[me.dp], down_out.at[:, at_mine], copy_sem.at[4, 0])
    flat.start()
    kept = pltpu.make_async_copy(w_ref.at[me.half], w.at[me.dp], copy_sem.at[0, 0])
    kept.start()
    g_out[me.dp] = g_ref[me.dp]
    me.greet(everyone=True, partner=True)
    beside = Threads(
        swap_rows(me, g_ref, g_out, g_send, g_recv),
        share_experts(me, (gate_ref, up_ref, down_ref), (gate_out, up_out, down_out), e_send, e_recv),
    )
    needed = Threads(gather_four(me, x_ref, seq, x_send, x_recv), gather_pairs(me, w_ref, w, w_send, w_recv))
    rounds = 0
    while needed.threads:
        needed.step()
        if rounds == start:
            beside.threads.insert(0, gather_line(me, c_ref, c_out, c_send, c_recv))
        beside.step()
        rounds += 1
    kept.wait()
    store = pltpu.make_async_copy(w, w_out, copy_sem.at[0, 1])
    store.start()
    weights = w.reshape(16 * rows, w.shape[2])

    def row_block(ref, h, core):
        return ref.at[pl.ds(pl.multiple_of((2 * h + core) * rows, rows), rows)]

    seqs = seq.reshape(4 * rows, width)
    q_part, k_part = pl.ds(0, q_cols), pl.ds(q_cols, 2 * head_dim)

    def project(j, _):
        at = pl.ds(pl.multiple_of(j * 256, 256), 256)
        raw[:, at] = dot(seqs[...], weights[:, at])
        return 0

    lax.fori_loop(0, q_cols // 256, project, 0)
    keys = dot(seqs[...], weights[:, k_part])
    raw[:, pl.ds(q_cols, head_dim)] = keys[:, :head_dim]
    low[:, pl.ds(q_cols + head_dim, head_dim)] = keys[:, head_dim:].astype(low.dtype)
    beside.step()
    cosine, turn = rope_ref[0], rope_ref[1]

    def turned(at, cols, which, scale):
        values = raw[at, cols]
        values = values * lax.rsqrt(jnp.mean(values * values, axis=-1, keepdims=True) + epsilon) * gain_ref[which]
        return ((values * cosine - pltpu.roll(values, head_dim // 2, 1) * turn) * scale).astype(low.dtype)

    k_at, v_at = pl.ds(q_cols, head_dim), pl.ds(q_cols + head_dim, head_dim)
    for b in range(2):
        at = pl.ds(b * seq_len, seq_len)
        low[at, k_at] = turned(at, k_at, 1, 1.0)
    causal = lax.broadcasted_iota(jnp.int32, (seq_len, seq_len), 0) >= lax.broadcasted_iota(jnp.int32, (seq_len, seq_len), 1)

    def head(n, _):
        at = pl.ds(pl.multiple_of(n // group * seq_len, seq_len), seq_len)
        cols = pl.ds(pl.multiple_of(n % group * head_dim, head_dim), head_dim)
        query = turned(at, cols, 0, head_dim ** (-0.5))
        low[at, cols] = query
        exp_scores = jnp.where(causal, jnp.exp(dot_t(query, low[at, k_at])), 0.0)
        probs = exp_scores / jnp.sum(exp_scores, axis=-1, keepdims=True)
        mixed[at, cols] = dot(probs.astype(low.dtype), low[at, v_at]).astype(mixed.dtype)
        return 0

    quarter = group // 2
    for k in range(4):
        lax.fori_loop(k * quarter, (k + 1) * quarter, head, 0)
        beside.step()

    def project_back(j, _):
        at = pl.ds(pl.multiple_of(j * 256, 256), 256)
        part[:, at] = dot_t(mixed[...], weights[at, pl.ds(proj_cols, q_cols)]).astype(part.dtype)
        return 0

    lax.fori_loop(0, width // 256, project_back, 0)

    def give(h, slot):
        return me.copy(row_block(part, h, 1 - me.core), from_core.at[slot], back_send.at[slot], back_recv.at[slot], me.dp, 1 - me.core)

    give(1 - me.half, 0).start()
    give(me.half, 1).start()
    beside.step()
    give(1 - me.half, 0).wait_recv()
    add_rows(from_core.at[0], (row_block(part, 1 - me.half, me.core), from_core.at[0]), rows)
    over = me.copy(from_core.at[0], from_pair, back_send.at[2], back_recv.at[2], me.dp + me.pair)
    over.start()
    give(me.half, 1).wait_recv()
    add_rows(from_core.at[1], (row_block(part, me.half, me.core), from_core.at[1]), rows)
    beside.step()
    over.wait_recv()

    def close(at, _):
        hidden = tokens_ref[at, :].astype(jnp.float32) + (from_core[1, at, :].astype(jnp.float32) + from_pair[at, :].astype(jnp.float32))
        hidden_ref[at, :] = hidden
        normed_ref[at, :] = (hidden * rms_inverse(hidden) * ffn_ref[...]).astype(normed_ref.dtype)
        return 0

    each_rows(rows, close)
    beside.finish()
    for end in ends:
        end()
    flat.wait()
    store.wait()
    give(0, 0).wait_send()
    give(0, 1).wait_send()
    over.wait_send()


def attention_first(weights, rows, gates, normed, rope, gain, tokens, ffn_gain, experts, cid, start=14):
    hbm, vmem = pl.BlockSpec(memory_space=pl.ANY), pl.BlockSpec(memory_space=pltpu.VMEM)
    dma = pltpu.SemaphoreType.DMA
    dtype = rows.dtype
    _, depth, hidden = experts[0].shape
    block, width = rows.shape
    head_dim = rope.shape[-1]
    columns = weights.shape[2]
    q_cols = (columns - 2 * head_dim) // 2
    return pl.pallas_call(
        functools.partial(attention_first_kernel, head_dim, start),
        out_shape=[
            jax.ShapeDtypeStruct((16,) + weights.shape[1:], dtype),
            jax.ShapeDtypeStruct((16, block, width), dtype),
            jax.ShapeDtypeStruct(gates.shape, gates.dtype),
            jax.ShapeDtypeStruct((2, 2, block, width), dtype),
            jax.ShapeDtypeStruct((4 * block, q_cols + head_dim), jnp.float32),
            jax.ShapeDtypeStruct((4 * block, q_cols + 2 * head_dim), dtype),
            jax.ShapeDtypeStruct((4 * block, q_cols), dtype),
            jax.ShapeDtypeStruct((block, width), jnp.float32),
            jax.ShapeDtypeStruct((block, width), dtype),
            jax.ShapeDtypeStruct((16 * depth, hidden), dtype),
            jax.ShapeDtypeStruct((16 * depth, hidden), dtype),
            jax.ShapeDtypeStruct((hidden, 16 * depth), dtype),
        ],
        in_specs=[hbm, hbm] + [vmem] * 6 + [hbm] * 3,
        out_specs=[hbm, hbm] + [vmem] * 7 + [hbm] * 3,
        scratch_shapes=[
            pltpu.VMEM((16,) + weights.shape[1:], dtype),
            pltpu.VMEM((block, width), dtype),
            pltpu.VMEM((2, depth, hidden), dtype),
            pltpu.VMEM((4 * block, width), dtype),
            pltpu.VMEM((2, block, width), dtype),
            pltpu.VMEM((block, width), dtype),
            dma((15, 2)), dma((16, 2)),
            dma((29,)), dma((16,)),
            dma((16,)), dma((16,)),
            dma((3,)), dma((3,)),
            dma((16, 3)), dma((16, 3)),
            dma((3,)), dma((3,)),
            dma((5, 2)),
        ],
        compiler_params=pltpu.CompilerParams(collective_id=cid, has_side_effects=True, vmem_limit_bytes=67_043_328),
        name="attention_first",
    )(weights, rows, gates, normed, rope, gain, tokens, ffn_gain, *experts)


def scatter_pairs(me, chunks, share, make, out_ref, from_b, from_a, from_far, send_sem, recv_sem):
    rows = from_a.shape[1] // chunks
    other = me.dp + me.pair
    bases = (me.dp, other, me.dp + me.far, other + me.far)
    items = [(j, k) for j in (2, 3, 1, 0) for k in range(chunks)]

    def at(k):
        return pl.ds(k * rows, rows)

    def copy(src, dst, slot, k, to):
        return me.copy(src, dst, send_sem.at[slot, k], recv_sem.at[slot, k], to)

    def send_b(g, j, k):
        return copy(share(bases[j] + me.db + g * me.da).at[at(k)], from_b.at[g, j, at(k)], g * 4 + j, k, me.dp + me.db)

    def send_a(j, k):
        return copy(from_b.at[1, j, at(k)], from_a.at[j, at(k)], 8 + j, k, me.dp + me.da)

    def send_far(j, k):
        return copy(from_b.at[0, 2 + j, at(k)], from_far.at[j, at(k)], 12 + j, k, me.dp + me.far)

    def swap(k):
        return copy(from_b.at[0, 1, at(k)], out_ref.at[me.half, at(k)], 14, k, other)

    for j in (2, 3, 1, 0):
        for g in (1, 0):
            make(bases[j] + me.db + g * me.da)
            for k in range(chunks):
                send_b(g, j, k).start()
        if j == 3:
            yield
    for j in (2, 3, 1, 0):
        make(bases[j] + me.da)
        make(bases[j])
        if j == 3:
            yield
    yield

    def first(item):
        j, k = item
        send_b(1, j, k).wait_recv()
        add_rows(from_b.at[1, j, at(k)], (share(bases[j] + me.da).at[at(k)], from_b.at[1, j, at(k)]), rows)
        send_a(j, k).start()

    def second(item):
        j, k = item
        send_b(0, j, k).wait_recv()
        send_a(j, k).wait_recv()
        terms = (share(bases[j]).at[at(k)], from_b.at[0, j, at(k)], from_a.at[j, at(k)])
        if j >= 2:
            add_rows(from_b.at[0, j, at(k)], terms, rows)
            send_far(j - 2, k).start()
        else:
            send_far(j, k).wait_recv()
            target = from_b.at[0, 1, at(k)] if j else out_ref.at[me.half, at(k)]
            add_rows(target, terms + (from_far.at[j, at(k)],), rows)
            if j:
                swap(k).start()

    yield from lagged(items, first, second, 2)
    for k in range(chunks):
        swap(k).wait_send()
        theirs = out_ref.at[1 - me.half, at(k)]
        copy(theirs, theirs, 14, k, other).wait_recv()
        for j in range(4):
            send_b(0, j, k).wait_send()
            send_b(1, j, k).wait_send()
            send_a(j, k).wait_send()
        send_far(0, k).wait_send()
        send_far(1, k).wait_send()


def sum_all(me, out_ref, held, send_sem, recv_sem):
    steps = ((me.dp, 1 - me.core), (me.dp + me.da, me.core), (me.dp + me.db, me.core), (me.dp + me.pair, me.core), (me.dp + me.far, me.core))
    yield
    for n, (to, core) in enumerate(steps):
        send = me.copy(held.at[0, n], held.at[1, n], send_sem.at[n], recv_sem.at[n], to, core)
        held[0, n] = out_ref[...]
        send.start()
        yield
        send.wait()
        out_ref[...] = held[0, n] + held[1, n]
        yield


def return_experts(me, gu_ref, down_ref, outs, own, held, core_send, core_recv, send_sem, recv_sem, copy_sem):
    rows, half = outs[0].shape[1:]

    def views(d, core):
        at = pl.ds(pl.multiple_of(d * rows, rows), rows)
        starts = ((gu_ref, core * half), (gu_ref, 2 * half + core * half), (down_ref, core * half))
        return [ref.at[at, pl.ds(pl.multiple_of(start, 128), half)] for ref, start in starts]

    def beside(r):
        d = (me.dp + r) % 16
        return [
            me.copy(src, held.at[j, r], core_send.at[r, j], core_recv.at[r, j], me.dp, 1 - me.core)
            for j, src in enumerate(views(d, 1 - me.core))
        ]

    order = (8, 7, 9, 4, 12, 5, 11, 6, 10, 3, 13, 2, 14, 1, 15, 0)

    def loads(n):
        d = (me.dp + order[n]) % 16
        return [pltpu.make_async_copy(src, own.at[j, n % 8], copy_sem.at[n % 8, j]) for j, src in enumerate(views(d, me.core))]

    def sends(r):
        d = (me.dp + r) % 16
        return [me.copy(held.at[j, r], outs[j].at[me.dp], send_sem.at[r, j], recv_sem.at[r, j], d) for j in range(3)]

    for r in order:
        for c in beside(r):
            c.start()
    for n in range(8):
        for c in loads(n):
            c.start()
    yield
    keep = [pltpu.make_async_copy(held.at[j, 0], outs[j].at[me.dp], copy_sem.at[16, j]) for j in range(3)]
    for n, r in enumerate(order):
        for j, (arrives, load) in enumerate(zip(beside(r), loads(n))):
            arrives.wait_recv()
            load.wait()
            add_rows(held.at[j, r], (own.at[j, n % 8], held.at[j, r]), rows, 64)
        for c in sends(r) if r else keep:
            c.start()
        if n < 8:
            for c in loads(n + 8):
                c.start()
        if n % 2:
            yield
    for r in range(1, 16):
        s = (me.dp + 16 - r) % 16
        for j in range(3):
            dst = outs[j].at[s]
            me.copy(dst, dst, send_sem.at[r, j], recv_sem.at[r, j], me.dp).wait_recv()
    for c in keep:
        c.wait()
    for r in range(16):
        for c in beside(r) + (sends(r) if r else []):
            c.wait_send()


def attention_back_kernel(
    chunks, head_dim,
    tokens_ref, grad_ref, hidden_ref, two_ref, norms_ref, w_ref, seq_ref, raw_ref, low_ref, mixed_ref, rope_ref, gain_ref, gu_ref, down_ref, share_ref,
    output_ref, grad_tokens_ref, query_out, key_out, value_out, back_out, sum_ref, gate_out, up_out, down_out,
    grad_hidden, out_ref, w, ga, gmix, gproj, part, kept, dk, dv, gains, from_core, from_pair,
    pair_b, pair_a, pair_far, total, own, held,
    from_b, from_a, from_z, b_send, b_recv, a_send, a_recv, z_send, z_recv,
    four_send, four_recv, back_send, back_recv, pair_send, pair_recv, sum_send, sum_recv, core_send, core_recv, e_send, e_recv,
    copy_sem, load_sem,
):
    me = Place()
    rows, width = tokens_ref.shape
    seq_len = 2 * rows
    q_cols = mixed_ref.shape[1]
    proj_cols = q_cols + 2 * head_dim
    group = q_cols // head_dim
    dot = functools.partial(jnp.dot, preferred_element_type=jnp.float32)
    dot_t = functools.partial(lax.dot_general, dimension_numbers=(((1,), (1,)), ((), ())), preferred_element_type=jnp.float32)
    t_dot = functools.partial(lax.dot_general, dimension_numbers=(((0,), (0,)), ((), ())), preferred_element_type=jnp.float32)
    load = pltpu.make_async_copy(w_ref, w, load_sem.at[8])
    load.start()
    keeps = [pltpu.make_async_copy(share_ref.at[n, pl.ds(0, rows)], kept.at[n], load_sem.at[n]) for n in range(8)]
    for c in keeps:
        c.start()
    me.greet(everyone=True, partner=True)

    def ga_at(h, core):
        return ga.at[pl.ds(pl.multiple_of((2 * h + core) * rows, rows), rows)]

    mine, theirs = ga_at(me.half, me.core), ga_at(1 - me.half, me.core)
    attn_gain, ffn_gain = norms_ref[0], norms_ref[1]

    def norm_back(grad, values, gain):
        inverse = rms_inverse(values)
        return norm_backward(grad, values, inverse, gain), grad * values * inverse

    def open_rows(at, total):
        grad, term = norm_back(two_ref[at, :], hidden_ref[at, :], ffn_gain)
        grad = grad_ref[at, :].astype(jnp.float32) + grad
        grad_hidden[at, :] = grad
        mine[at, :] = grad.astype(ga.dtype)
        return total + term

    ffn_part = jnp.sum(each_rows(rows, open_rows, jnp.zeros((16, width), jnp.float32)), axis=0, keepdims=True)
    across = me.copy(mine, mine, four_send.at[0], four_recv.at[0], me.dp + me.pair)
    beside = me.copy(mine, mine, four_send.at[1], four_recv.at[1], me.dp, 1 - me.core)
    relay = me.copy(theirs, theirs, four_send.at[2], four_recv.at[2], me.dp, 1 - me.core)
    across.start()
    beside.start()
    scatter = ScatterRows(
        me, lambda n: share_ref.at[n, pl.ds(rows, rows)], lambda n: kept.at[n], from_b, from_a, from_z,
        (b_send, b_recv, a_send, a_recv, z_send, z_recv),
    )
    for m in (1, 2, 3, 0):
        scatter.send_b(2 * m + 1).start()
        scatter.send_b(2 * m).start()
    experts = return_experts(me, gu_ref, down_ref, (gate_out, up_out, down_out), own, held, core_send, core_recv, e_send, e_recv, copy_sem)
    for _ in range(9):
        next(experts)
    across.wait_recv()
    relay.start()
    across.wait_send()
    beside.wait()
    relay.wait()
    load.wait()
    for c in keeps:
        c.wait()

    def mix(j, _):
        at = pl.ds(pl.multiple_of(j * 256, 256), 256)
        at_w = pl.ds(pl.multiple_of(proj_cols + j * 256, 256), 256)
        gmix[:, at] = dot(ga[...], w[:, at_w]).astype(gmix.dtype)
        return 0

    lax.fori_loop(0, q_cols // 256, mix, 0)
    gains[...] = jnp.zeros_like(gains)
    turn = rope_ref[1]
    cosine = rope_ref[0]
    causal = lax.broadcasted_iota(jnp.int32, (seq_len, seq_len), 0) >= lax.broadcasted_iota(jnp.int32, (seq_len, seq_len), 1)
    k_at, v_at = pl.ds(q_cols, head_dim), pl.ds(q_cols + head_dim, head_dim)

    def back(grad, raw, which):
        grad = grad * cosine + pltpu.roll(grad, head_dim // 2, 1) * turn
        inverse = lax.rsqrt(jnp.mean(raw * raw, axis=-1, keepdims=True) + epsilon)
        gains[which] = gains[which] + jnp.sum(grad * (raw * inverse), axis=0, keepdims=True)
        scaled = grad * gain_ref[which]
        inner = jnp.mean(scaled * raw, axis=-1, keepdims=True)
        return inverse * scaled - raw * (inverse * inverse * inverse) * inner

    def head(n, _):
        at = pl.ds(pl.multiple_of(n // group * seq_len, seq_len), seq_len)
        cols = pl.ds(pl.multiple_of(n % group * head_dim, head_dim), head_dim)
        query, key, value, grad = low_ref[at, cols], low_ref[at, k_at], low_ref[at, v_at], gmix[at, cols]
        exp_scores = jnp.where(causal, jnp.exp(dot_t(query, key)), 0.0)
        probs = exp_scores / jnp.sum(exp_scores, axis=-1, keepdims=True)
        grad_probs = dot_t(grad, value)
        delta = jnp.sum(grad_probs * probs, axis=-1, keepdims=True)
        grad_scores = (probs * (grad_probs - delta)).astype(query.dtype)
        grad_query = dot(grad_scores, key) * head_dim ** (-0.5)
        grad_key = t_dot(grad_scores, query)
        grad_value = t_dot(probs.astype(query.dtype), grad)

        def begin():
            dk[...] = grad_key
            dv[...] = grad_value

        def more():
            dk[...] = dk[...] + grad_key
            dv[...] = dv[...] + grad_value

        pl.when(n % group == 0)(begin)
        pl.when(n % group != 0)(more)
        gproj[at, cols] = back(grad_query, raw_ref[at, cols], 0).astype(gproj.dtype)

        def close():
            gproj[at, k_at] = back(dk[...], raw_ref[at, k_at], 1).astype(gproj.dtype)
            gproj[at, v_at] = dv[...].astype(gproj.dtype)

        pl.when(n % group == group - 1)(close)
        return 0

    heads = 2 * group
    quarter = heads // 4
    for k in range(4):
        lax.fori_loop(k * quarter, (k + 1) * quarter, head, 0)
        scatter.first((1, 2, 3, 0)[k])
        if k:
            scatter.second((1, 2, 3, 0)[k - 1])

    def project(j, _):
        at = pl.ds(pl.multiple_of(j * 256, 256), 256)
        part[:, at] = dot_t(gproj[...], w[at, pl.ds(0, proj_cols)]).astype(part.dtype)
        return 0

    lax.fori_loop(0, width // 256, project, 0)

    def part_at(h, core):
        return part.at[pl.ds(pl.multiple_of((2 * h + core) * rows, rows), rows)]

    def give(h, slot):
        return me.copy(part_at(h, 1 - me.core), from_core.at[slot], back_send.at[slot], back_recv.at[slot], me.dp, 1 - me.core)

    give(1 - me.half, 0).start()
    give(me.half, 1).start()
    other = me.dp + me.pair
    bases = (me.dp, other, me.dp + me.far, other + me.far)

    def weight_block(d):
        at = pl.ds(pl.multiple_of(d * rows, rows), rows)
        w[at, pl.ds(0, proj_cols)] = t_dot(seq_ref[:, at], gproj[...]).astype(w.dtype)
        w[at, pl.ds(proj_cols, q_cols)] = t_dot(ga[:, at], mixed_ref[...]).astype(w.dtype)

    pairs = scatter_pairs(me, chunks, lambda d: w.at[pl.ds(pl.multiple_of(d * rows, rows), rows)], weight_block, out_ref, pair_b, pair_a, pair_far, pair_send, pair_recv)
    next(pairs)
    give(1 - me.half, 0).wait_recv()
    add_rows(from_core.at[0], (part_at(1 - me.half, me.core), from_core.at[0]), rows)
    over = me.copy(from_core.at[0], from_pair, back_send.at[2], back_recv.at[2], me.dp + me.pair)
    over.start()
    give(me.half, 1).wait_recv()
    add_rows(from_core.at[1], (part_at(me.half, me.core), from_core.at[1]), rows)
    next(pairs)
    scatter.second(0)
    next(pairs)
    over.wait_recv()

    def close_rows(at, total):
        grad = from_core[1, at, :].astype(jnp.float32) + from_pair[at, :].astype(jnp.float32)
        back_part, term = norm_back(grad, tokens_ref[at, :].astype(jnp.float32), attn_gain)
        grad_tokens_ref[at, :] = (grad_hidden[at, :] + back_part).astype(grad_tokens_ref.dtype)
        return total + term

    attn_part = jnp.sum(each_rows(rows, close_rows, jnp.zeros((16, width), jnp.float32)), axis=0, keepdims=True)
    sum_ref[...] = jnp.zeros_like(sum_ref)
    for j in range(width // 128):
        sum_ref[pl.ds(j, 1), :] = attn_part[:, j * 128 : (j + 1) * 128]
        sum_ref[pl.ds(width // 128 + j, 1), :] = ffn_part[:, j * 128 : (j + 1) * 128]
    for j in range(2):
        sum_ref[pl.ds(2 * width // 128 + j, 1), :] = gains[j]
    scatter.finish(output_ref, hidden_ref)
    run(pairs, experts, sum_all(me, sum_ref, total, sum_send, sum_recv))

    def widen_rows(at, _):
        start = 0
        for target in (query_out, key_out, value_out, back_out):
            size = target.shape[1] // 2
            for h in range(2):
                target[at, h * size : (h + 1) * size] = out_ref[h, at, start : start + size].astype(jnp.float32)
            start += size
        return 0

    each_rows(rows, widen_rows)
    scatter.drain()
    give(0, 0).wait_send()
    give(0, 1).wait_send()
    over.wait_send()


def attention_back(tokens, cotangent, hidden, grad_two, norms, weights, seq_normed, raw, low, mixed, rope, gain, gu, down, share, cid, chunks=4):
    rows, width = tokens.shape
    head_dim = rope.shape[-1]
    columns = weights.shape[1]
    half = down.shape[1] // 2
    hbm, vmem = pl.BlockSpec(memory_space=pl.ANY), pl.BlockSpec(memory_space=pltpu.VMEM)
    dma = pltpu.SemaphoreType.DMA
    dtype = weights.dtype
    proj_cols = raw.shape[1] + head_dim
    q_cols = mixed.shape[1]
    whole = jax.ShapeDtypeStruct((rows, width), dtype)
    grads = [jax.ShapeDtypeStruct((rows, 2 * size), jnp.float32) for size in (q_cols, head_dim, head_dim, q_cols)]
    sums = jax.ShapeDtypeStruct((-(-(2 * width + 2 * head_dim) // 1024) * 8, 128), jnp.float32)
    return pl.pallas_call(
        functools.partial(attention_back_kernel, chunks, head_dim),
        out_shape=[whole, whole, *grads, sums]
        + [jax.ShapeDtypeStruct((16, rows, half), dtype)] * 3,
        in_specs=[vmem] * 5 + [hbm] + [vmem] * 6 + [hbm] * 3,
        out_specs=[vmem] * 7 + [hbm] * 3,
        scratch_shapes=[
            pltpu.VMEM((rows, width), jnp.float32),
            pltpu.VMEM((2, rows, columns), dtype),
            pltpu.VMEM(weights.shape, dtype),
            pltpu.VMEM((4 * rows, width), dtype),
            pltpu.VMEM(mixed.shape, dtype),
            pltpu.VMEM((4 * rows, proj_cols), dtype),
            pltpu.VMEM((4 * rows, width), dtype),
            pltpu.VMEM((8, rows, width), dtype),
            pltpu.VMEM((2 * rows, head_dim), jnp.float32),
            pltpu.VMEM((2 * rows, head_dim), jnp.float32),
            pltpu.VMEM((2, 1, head_dim), jnp.float32),
            pltpu.VMEM((2, rows, width), dtype),
            pltpu.VMEM((rows, width), dtype),
            pltpu.VMEM((2, 4, rows, columns), dtype),
            pltpu.VMEM((4, rows, columns), dtype),
            pltpu.VMEM((2, rows, columns), dtype),
            pltpu.VMEM((2, 5) + sums.shape, sums.dtype),
            pltpu.VMEM((3, 8, rows, half), dtype),
            pltpu.VMEM((3, 16, rows, half), dtype),
            *scatter_rows_scratch(rows, width, dtype),
            dma((3,)), dma((3,)),
            dma((3,)), dma((3,)),
            dma((15, chunks)), dma((15, chunks)),
            dma((5,)), dma((5,)),
            dma((16, 3)), dma((16, 3)),
            dma((16, 3)), dma((16, 3)),
            dma((17, 3)), dma((9,)),
        ],
        compiler_params=pltpu.CompilerParams(collective_id=cid, has_side_effects=True, vmem_limit_bytes=67_043_328),
        name="attention_back",
    )(tokens, cotangent, hidden, grad_two, norms, weights, seq_normed, raw, low, mixed, rope, gain, gu, down, share)


class ScatterRows:
    def __init__(self, me, sent, kept, from_b, from_a, from_z, sems):
        self.me, self.sent, self.kept = me, sent, kept
        self.from_b, self.from_a, self.from_z = from_b, from_a, from_z
        self.b_send, self.b_recv, self.a_send, self.a_recv, self.z_send, self.z_recv = sems
        self.rows = from_b.shape[1]

    def send_b(self, n):
        me = self.me
        return me.copy(self.sent(n), self.from_b.at[n], self.b_send.at[n], self.b_recv.at[n], me.dp + me.db)

    def send_a(self, m):
        me = self.me
        return me.copy(self.from_b.at[2 * m + 1], self.from_a.at[m], self.a_send.at[m], self.a_recv.at[m], me.dp + me.da)

    def send_z(self, m):
        me = self.me
        return me.copy(self.from_b.at[2 * m], self.from_z.at[me.z], self.z_send.at[m], self.z_recv.at[me.z], me.at_z(me.z_of(m)))

    def first(self, m):
        n = 2 * m + 1
        self.send_b(n).wait_recv()
        add_rows(self.from_b.at[n], (self.kept(n), self.from_b.at[n]), self.rows)
        self.send_a(m).start()

    def second(self, m):
        n = 2 * m
        self.send_b(n).wait_recv()
        self.send_a(m).wait_recv()
        add_rows(self.from_b.at[n], (self.kept(n), self.from_b.at[n], self.from_a.at[m]), self.rows)
        pl.when(m > 0)(lambda: self.send_z(m).start())

    def advance(self, now, lags=(1, 2)):
        for lag, call in zip(lags, (self.first, self.second)):
            m = (now - 1 - lag) // 2
            due = jnp.logical_and((now - 1 - lag) % 2 == 0, jnp.logical_and(now > lag, m < 4))
            pl.when(due)(lambda: call(m))

    def finish(self, out_ref, *more):
        me = self.me
        others = [(me.z + r) % 4 for r in range(1, 4)]
        for z in others:
            me.copy(self.from_z.at[z], self.from_z.at[z], self.z_send.at[0], self.z_recv.at[z], me.dp).wait_recv()
        add_rows(out_ref, (self.from_b.at[0],) + tuple(self.from_z.at[z] for z in others) + more, self.rows)

    def drain(self):
        for m in range(4):
            self.send_b(2 * m).wait_send()
            self.send_b(2 * m + 1).wait_send()
            self.send_a(m).wait_send()
            if m:
                self.send_z(m).wait_send()


def scatter_rows_scratch(rows, columns, dtype):
    dma = pltpu.SemaphoreType.DMA
    return [
        pltpu.VMEM((8, rows, columns), dtype),
        pltpu.VMEM((4, rows, columns), dtype),
        pltpu.VMEM((4, rows, columns), dtype),
        dma((8,)), dma((8,)), dma((4,)), dma((4,)), dma((4,)), dma((4,)),
    ]


def experts_kernel(
    x_ref, c_ref, g_ref, gate_ref, up_ref, down_ref,
    share_ref, two_ref, gu_out, down_out, xg_ref,
    wgu, wd, ag, ggu, share, p, xb, cb, from_b, from_a, from_z, b_send, b_recv, a_send, a_recv, z_send, z_recv,
    g_send, g_recv, w_send, w_recv, load_sem, tile_sem, keep_sem, share_sem,
):
    me = Place()
    rows, width = x_ref.shape
    hidden = wd.shape[0]
    half = hidden // 2
    dot = functools.partial(jnp.dot, preferred_element_type=jnp.float32)
    dot_t = functools.partial(lax.dot_general, dimension_numbers=(((1,), (1,)), ((), ())), preferred_element_type=jnp.float32)
    t_dot = functools.partial(lax.dot_general, dimension_numbers=(((0,), (0,)), ((), ())), preferred_element_type=jnp.float32)
    upper, lower = pl.ds(rows, rows), pl.ds(0, rows)

    z_of, block = me.z_of, me.block

    def part(source, to, slot, own=False):
        return me.copy(x_ref if own else xg_ref.at[source], xg_ref.at[source], g_send.at[slot], g_recv.at[source], to)

    def arrive(m):
        source = me.at_z(z_of(m))
        part(source, me.dp, 0).wait_recv()
        part(source, me.dp + me.db, 3 + 2 * m).start()
        part(source, me.dp + me.da, 4 + 2 * m).start()

    def arrive_a(m):
        source = me.at_z(z_of(m)) + me.da
        part(source, me.dp, 0).wait_recv()
        part(source, me.dp + me.db, 11 + m).start()

    def loads(n):
        slot = n % 2
        copies = []
        for j, source in enumerate((block(n), block(n) + me.db)):
            at = pl.ds(j * rows, rows)
            copies.append(pltpu.make_async_copy(xg_ref.at[source], xb.at[slot, at], load_sem.at[slot, j]))
            copies.append(pltpu.make_async_copy(c_ref.at[source], cb.at[slot, at], load_sem.at[slot, 2 + j]))
        return copies

    def fetch(n):
        part(block(n) + me.db, me.dp, 0).wait_recv()
        for c in loads(n):
            c.start()

    scatter = ScatterRows(
        me, lambda n: p.at[n, upper], lambda n: p.at[n, lower], from_b, from_a, from_z, (b_send, b_recv, a_send, a_recv, z_send, z_recv)
    )

    def keep_share(n):
        return pltpu.make_async_copy(share.at[n % 2], share_ref.at[n], share_sem.at[n % 2])

    own = p.at[7, lower]
    load = pltpu.make_async_copy(x_ref, own, keep_sem.at[0])
    store = pltpu.make_async_copy(own, xg_ref.at[me.dp], keep_sem.at[1])
    load.start()

    def half_of(core):
        at = core * half
        return (
            wgu.at[:, pl.ds(pl.multiple_of(at, 128), half)],
            wgu.at[:, pl.ds(pl.multiple_of(hidden + at, 128), half)],
            wd.at[pl.ds(pl.multiple_of(at, 128), half)],
        )

    mine = (gate_ref, up_ref, down_ref)
    locals_ = [pltpu.make_async_copy(src, dst, keep_sem.at[2 + j]) for j, (src, dst) in enumerate(zip(mine, half_of(me.core)))]
    for c in locals_:
        c.start()
    me.greet(column=True, near=True, partner=True)
    for m in range(1, 4):
        part(me.dp, me.at_z(z_of(m)), m - 1, True).start()
    part(me.dp, me.dp + me.db, 3, True).start()
    part(me.dp, me.dp + me.da, 4, True).start()
    shares = [
        me.copy(src, dst, w_send.at[j], w_recv.at[j], me.dp, 1 - me.core) for j, (src, dst) in enumerate(zip(mine, half_of(me.core)))
    ]
    for c in shares:
        c.start()
    load.wait()
    store.start()
    arrive_a(0)
    store.wait()
    for c in locals_:
        c.wait()
    for j, dst in enumerate(half_of(1 - me.core)):
        me.copy(dst, dst, w_send.at[j], w_recv.at[j], me.dp).wait_recv()
    fetch(0)

    tile = 256

    def step(n, _):
        slot = n % 2
        for c in loads(n):
            c.wait()
        gates = jnp.concatenate([g_ref[block(n)], g_ref[block(n) + me.db]], axis=0)

        def inner(j, _):
            at, at_up = pl.ds(pl.multiple_of(j * tile, tile), tile), pl.ds(pl.multiple_of(hidden + j * tile, tile), tile)
            gate, up, grad = dot(xb[slot], wgu[:, at]), dot(xb[slot], wgu[:, at_up]), dot_t(cb[slot], wd[at, :]) * gates
            sig = 1.0 / (1.0 + jnp.exp(-gate))
            act = gate * sig
            ag[n, :, at] = (act * up * gates).astype(ag.dtype)
            ggu[n, :, at] = (grad * up * sig * (1.0 + gate * (1.0 - sig))).astype(ggu.dtype)
            ggu[n, :, at_up] = (grad * act).astype(ggu.dtype)
            return 0

        lax.fori_loop(0, hidden // tile, inner, 0)

        def at_step(k, *calls):
            def go():
                for call, m in calls:
                    call(m)

            pl.when(n == k)(go)

        at_step(0, (arrive, 1))
        at_step(1, (arrive, 2), (arrive_a, 1))
        at_step(2, (arrive, 3))
        at_step(3, (arrive_a, 2))
        at_step(4, (arrive_a, 3))
        pl.when(n < 7)(lambda: fetch(n + 1))

        pl.when(n >= 2)(lambda: keep_share(n - 2).wait())

        def outer(j, _):
            at = pl.ds(pl.multiple_of(j * 2 * tile, 2 * tile), 2 * tile)
            share[slot, :, at] = dot(ag[n], wd[:, at]).astype(p.dtype)
            p[n, :, at] = dot_t(ggu[n], wgu[at, :]).astype(p.dtype)
            return 0

        lax.fori_loop(0, width // (2 * tile), outer, 0)
        scatter.send_b(n).start()
        keep_share(n).start()
        scatter.advance(n)
        return 0

    lax.fori_loop(0, 8, step, 0)

    def tiles(i):
        slot = i % 2
        cols = pl.ds(pl.multiple_of(i * tile, tile), tile)
        copies = []
        for which, src in enumerate((xg_ref, c_ref)):
            to = pl.ds(pl.multiple_of((2 * which + slot) * tile, tile), tile)

            def one(n, side, which=which, src=src, to=to):
                at = pl.ds(pl.multiple_of((2 * n + side) * rows, rows), rows)
                return pltpu.make_async_copy(src.at[block(n) + side * me.db, :, cols], wgu.at[at, to], tile_sem.at[which, slot, 2 * n + side])

            copies.append(one)
        return copies

    def each_tile(i, act):
        for one in tiles(i):

            def body(n, _):
                for side in (0, 1):
                    act(one(n, side))
                return 0

            lax.fori_loop(0, 8, body, 0)

    def outs(i):
        slot = i % 2
        at = pl.ds(pl.multiple_of(i * tile, tile), tile)
        return (
            pltpu.make_async_copy(xb.at[slot, :, pl.ds(0, 2 * hidden)], gu_out.at[at], load_sem.at[slot, 0]),
            pltpu.make_async_copy(cb.at[slot, :, pl.ds(0, hidden)], down_out.at[at], load_sem.at[slot, 1]),
        )

    each_tile(0, lambda c: c.start())

    def weight_step(i, _):
        slot = i % 2
        pl.when(i < 7)(lambda: each_tile(i + 1, lambda c: c.start()))
        each_tile(i, lambda c: c.wait())

        def free():
            for c in outs(i - 2):
                c.wait()

        pl.when(i >= 2)(free)
        x_tile = wgu[:, pl.ds(pl.multiple_of(slot * tile, tile), tile)]
        xb[slot, :, pl.ds(0, 2 * hidden)] = t_dot(x_tile, ggu[...].reshape(-1, 2 * hidden)).astype(xb.dtype)
        c_tile = wgu[:, pl.ds(pl.multiple_of((2 + slot) * tile, tile), tile)]
        cb[slot, :, pl.ds(0, hidden)] = t_dot(c_tile, ag[...].reshape(-1, hidden)).astype(cb.dtype)
        for c in outs(i):
            c.start()
        scatter.advance(i + 8)
        return 0

    lax.fori_loop(0, 8, weight_step, 0)
    scatter.finish(two_ref)

    for i in (6, 7):
        for c in outs(i):
            c.wait()
    for c in shares:
        c.wait_send()
    for slot in range(15):
        part(me.dp, me.dp, slot).wait_send()
    scatter.drain()
    keep_share(6).wait()
    keep_share(7).wait()


def expert_layer(x, grads, gates, gate, up, down, cid):
    rows, width = x.shape
    half = gate.shape[1]
    hbm, vmem = pl.BlockSpec(memory_space=pl.ANY), pl.BlockSpec(memory_space=pltpu.VMEM)
    dma = pltpu.SemaphoreType.DMA
    dtype = x.dtype
    return pl.pallas_call(
        experts_kernel,
        out_shape=[
            jax.ShapeDtypeStruct((8, 2 * rows, width), dtype),
            jax.ShapeDtypeStruct((rows, width), jnp.float32),
            jax.ShapeDtypeStruct((width, 4 * half), dtype),
            jax.ShapeDtypeStruct((width, 2 * half), dtype),
            jax.ShapeDtypeStruct((16, rows, width), dtype),
        ],
        in_specs=[hbm, hbm, vmem, hbm, hbm, hbm],
        out_specs=[hbm, vmem, hbm, hbm, hbm],
        scratch_shapes=[
            pltpu.VMEM((width, 4 * half), dtype),
            pltpu.VMEM((2 * half, width), dtype),
            pltpu.VMEM((8, 2 * rows, 2 * half), dtype),
            pltpu.VMEM((8, 2 * rows, 4 * half), dtype),
            pltpu.VMEM((2, 2 * rows, width), dtype),
            pltpu.VMEM((8, 2 * rows, width), dtype),
            pltpu.VMEM((2, 2 * rows, width), dtype),
            pltpu.VMEM((2, 2 * rows, width), dtype),
            *scatter_rows_scratch(rows, width, dtype),
            dma((15,)), dma((16,)),
            dma((3,)), dma((3,)),
            dma((2, 4)), dma((2, 2, 16)), dma((5,)), dma((2,)),
        ],
        compiler_params=pltpu.CompilerParams(collective_id=cid, has_side_effects=True, vmem_limit_bytes=67_043_328),
        name="experts",
    )(x, grads, gates, gate, up, down)


def per_device_any(
    tokens,
    cotangent,
    expert_ids,
    gate_values,
    w_query,
    w_key,
    w_value,
    w_out,
    w_gate,
    w_up,
    w_down,
    attn_gain,
    ffn_gain,
    query_gain,
    key_gain,
):
    contract = (((1,), (1,)), ((), ()))
    contract_rows = (((0,), (0,)), ((), ()))
    residual = tokens.astype(jnp.float32)
    model_width = residual.shape[1]
    inverse_one = rms_inverse(residual)
    seq_normed = gather_rows((residual * inverse_one * attn_gain).astype(jnp.bfloat16))
    full_query, full_key, full_value, full_out = (
        lax.all_gather(w_query, "dp", axis=0, tiled=True),
        lax.all_gather(w_key, "dp", axis=0, tiled=True),
        lax.all_gather(w_value, "dp", axis=0, tiled=True),
        lax.all_gather(w_out, "dp", axis=1, tiled=True),
    )
    seq_len = seq_normed.shape[0]
    head_dim = query_gain.shape[0]
    local_heads = full_query.shape[1] // head_dim
    local_kv = full_key.shape[1] // head_dim
    group_size = local_heads // local_kv
    attn_scale = head_dim ** (-0.5)
    cosine, sine_table = rotary_tables(seq_len, head_dim)
    query_raw = jnp.dot(seq_normed, full_query, preferred_element_type=jnp.float32).reshape(
        seq_len, local_heads, head_dim
    )
    key_raw = jnp.dot(seq_normed, full_key, preferred_element_type=jnp.float32).reshape(
        seq_len, local_kv, head_dim
    )
    value_low = (
        jnp.dot(seq_normed, full_value, preferred_element_type=jnp.float32)
        .astype(jnp.bfloat16)
        .reshape(seq_len, local_kv, head_dim)
    )
    query_inverse = rms_inverse(query_raw)
    key_inverse = rms_inverse(key_raw)
    query_low = (
        rotate(query_raw * query_inverse * query_gain, cosine, sine_table) * attn_scale
    ).astype(jnp.bfloat16)
    key_low = rotate(key_raw * key_inverse * key_gain, cosine, sine_table).astype(jnp.bfloat16)
    query_heads = query_low.reshape(seq_len, local_kv, group_size, head_dim).transpose(1, 0, 2, 3)
    key_heads = key_low.transpose(1, 0, 2)
    value_heads = value_low.transpose(1, 0, 2)
    mixed_heads, logsum = lax.map(head_forward, (query_heads, key_heads, value_heads))
    mixed_flat = mixed_heads.transpose(1, 0, 2, 3).reshape(seq_len, local_heads * head_dim)
    hidden = residual + scatter_rows(
        jnp.dot(mixed_flat, full_out, preferred_element_type=jnp.float32)
    )
    inverse_two = rms_inverse(hidden)
    seq_two = gather_rows((hidden * inverse_two * ffn_gain).astype(jnp.bfloat16))
    seq_grad = gather_rows(cotangent)
    experts = w_gate.shape[0]
    dp_rows = w_gate.shape[1]
    hidden_units = w_gate.shape[2]
    dp_count = lax.axis_size("dp")
    group = dp_count // experts
    routed_rows = seq_len * expert_ids.shape[1] * 9 // 8
    capacity = (routed_rows + experts * group - 1) // (experts * group) * group
    slot_table, gate_table = dispatch(expert_ids, gate_values, experts, capacity)
    blank_row = jnp.zeros((1, model_width), jnp.bfloat16)
    padded_in = jnp.concatenate([seq_two, blank_row], axis=0)
    padded_grad = jnp.concatenate([seq_grad, blank_row], axis=0)
    empty_rows = jnp.zeros((seq_len + 1, model_width), jnp.float32)
    piece_rows = capacity // group
    down_rows = jnp.transpose(w_down, (0, 2, 1))
    gate_mine, up_mine, down_mine = (
        lax.all_to_all(widen(w_gate, group), "dp", split_axis=0, concat_axis=1, tiled=True),
        lax.all_to_all(widen(w_up, group), "dp", split_axis=0, concat_axis=1, tiled=True),
        lax.all_to_all(widen(down_rows, group), "dp", split_axis=0, concat_axis=1, tiled=True),
    )
    gate_mine = gate_mine[0]
    up_mine = up_mine[0]
    down_mine = down_mine[0]
    blocks_in = padded_in[slot_table]
    grad_blocks = (padded_grad[slot_table].astype(jnp.float32) * gate_table[:, :, None]).astype(
        jnp.bfloat16
    )
    recv_in, recv_grad = (
        lax.all_to_all(
            blocks_in.reshape(dp_count, piece_rows, model_width),
            "dp",
            split_axis=0,
            concat_axis=0,
            tiled=True,
        ),
        lax.all_to_all(
            grad_blocks.reshape(dp_count, piece_rows, model_width),
            "dp",
            split_axis=0,
            concat_axis=0,
            tiled=True,
        ),
    )
    rows_in = recv_in.reshape(-1, model_width)
    rows_grad = recv_grad.reshape(-1, model_width)
    gate_pre = jnp.dot(rows_in, gate_mine, preferred_element_type=jnp.float32)
    up_pre = jnp.dot(rows_in, up_mine, preferred_element_type=jnp.float32)
    act_low = (jax.nn.silu(gate_pre) * up_pre).astype(jnp.bfloat16)
    expert_out = lax.dot_general(act_low, down_mine, contract, preferred_element_type=jnp.float32)
    grad_act = jnp.dot(rows_grad, down_mine, preferred_element_type=jnp.float32)
    sigmoid_gate = jax.nn.sigmoid(gate_pre)
    grad_gate = (grad_act * up_pre * sigmoid_gate * (1.0 + gate_pre * (1.0 - sigmoid_gate))).astype(
        jnp.bfloat16
    )
    grad_up = (grad_act * gate_pre * sigmoid_gate).astype(jnp.bfloat16)
    grad_input = lax.dot_general(
        grad_gate, gate_mine, contract, preferred_element_type=jnp.float32
    ) + lax.dot_general(grad_up, up_mine, contract, preferred_element_type=jnp.float32)
    back_out, back_grad = (
        lax.all_to_all(
            expert_out.reshape(dp_count, piece_rows, model_width).astype(jnp.bfloat16),
            "dp",
            split_axis=0,
            concat_axis=0,
            tiled=True,
        ).astype(jnp.float32),
        lax.all_to_all(
            grad_input.reshape(dp_count, piece_rows, model_width).astype(jnp.bfloat16),
            "dp",
            split_axis=0,
            concat_axis=0,
            tiled=True,
        ).astype(jnp.float32),
    )
    back_out = back_out.reshape(experts, capacity, model_width)
    back_grad = back_grad.reshape(experts * capacity, model_width)
    flat_slots = slot_table.reshape(-1)
    combined = empty_rows.at[flat_slots].add(
        (back_out * gate_table[:, :, None]).reshape(-1, model_width)
    )
    grad_acc = empty_rows.at[flat_slots].add(back_grad)
    grad_both = jnp.concatenate([grad_gate, grad_up], axis=1)
    grad_cols = jnp.concatenate(
        [
            lax.dot_general(rows_in, grad_both, contract_rows, preferred_element_type=jnp.float32),
            lax.dot_general(rows_grad, act_low, contract_rows, preferred_element_type=jnp.float32),
        ],
        axis=1,
    )
    returned = lax.all_to_all(
        grad_cols[None].astype(jnp.bfloat16), "dp", split_axis=1, concat_axis=0, tiled=True
    ).astype(jnp.float32)
    summed = jnp.sum(returned.reshape(experts, group, dp_rows, 3 * hidden_units), axis=1)
    grad_w_gate = summed[:, :, :hidden_units]
    grad_w_up = summed[:, :, hidden_units : 2 * hidden_units]
    grad_w_down = jnp.transpose(summed[:, :, 2 * hidden_units :], (0, 2, 1))
    output = (hidden + scatter_rows(combined[:seq_len])).astype(jnp.bfloat16)
    grad_two = scatter_rows(grad_acc[:seq_len])
    ffn_gain_part = jnp.sum(grad_two * hidden * inverse_two, axis=0)
    grad_hidden = cotangent.astype(jnp.float32) + norm_backward(
        grad_two, hidden, inverse_two, ffn_gain
    )
    grad_attn = gather_rows(grad_hidden.astype(jnp.bfloat16))
    grad_mixed = lax.dot_general(
        grad_attn, full_out, contract, preferred_element_type=jnp.float32
    ).astype(jnp.bfloat16)
    grad_mixed_heads = grad_mixed.reshape(seq_len, local_kv, group_size, head_dim).transpose(
        1, 0, 2, 3
    )
    grad_query_heads, grad_key_heads, grad_value_heads = lax.map(
        head_backward, (query_heads, key_heads, value_heads, logsum, grad_mixed_heads)
    )
    grad_query_rot = (
        grad_query_heads.transpose(1, 0, 2, 3).reshape(seq_len, local_heads, head_dim) * attn_scale
    )
    grad_query_norm = rotate_back(grad_query_rot, cosine, sine_table)
    query_gain_part = jnp.sum(grad_query_norm * query_raw * query_inverse, axis=(0, 1))
    grad_query_low = (
        norm_backward(grad_query_norm, query_raw, query_inverse, query_gain)
        .astype(jnp.bfloat16)
        .reshape(seq_len, local_heads * head_dim)
    )
    grad_key_norm = rotate_back(grad_key_heads.transpose(1, 0, 2), cosine, sine_table)
    key_gain_part = jnp.sum(grad_key_norm * key_raw * key_inverse, axis=(0, 1))
    grad_key_low = (
        norm_backward(grad_key_norm, key_raw, key_inverse, key_gain)
        .astype(jnp.bfloat16)
        .reshape(seq_len, local_kv * head_dim)
    )
    grad_value_low = (
        grad_value_heads.transpose(1, 0, 2)
        .reshape(seq_len, local_kv * head_dim)
        .astype(jnp.bfloat16)
    )
    grad_proj = jnp.concatenate([grad_query_low, grad_key_low, grad_value_low], axis=1)
    full_proj = jnp.concatenate([full_query, full_key, full_value], axis=1)
    grad_one = scatter_rows(
        lax.dot_general(grad_proj, full_proj, contract, preferred_element_type=jnp.float32)
    )
    first_part = jnp.einsum("sd,sf->df", seq_normed, grad_proj, preferred_element_type=jnp.float32)
    second = jnp.einsum("sd,sf->df", grad_attn, mixed_flat, preferred_element_type=jnp.float32)
    shares = lax.psum_scatter(
        jnp.concatenate([first_part, second], axis=1), "dp", scatter_dimension=0, tiled=True
    )
    query_cols = w_query.shape[1]
    key_cols = w_key.shape[1]
    grad_w_query = shares[:, :query_cols]
    grad_w_key = shares[:, query_cols : query_cols + key_cols]
    grad_w_value = shares[:, query_cols + key_cols : query_cols + 2 * key_cols]
    grad_w_out = jnp.transpose(shares[:, query_cols + 2 * key_cols :])
    attn_gain_part = jnp.sum(grad_one * residual * inverse_one, axis=0)
    grad_tokens = (grad_hidden + norm_backward(grad_one, residual, inverse_one, attn_gain)).astype(
        jnp.bfloat16
    )
    total_gains = lax.psum(
        (attn_gain_part, ffn_gain_part, query_gain_part, key_gain_part), ("dp", "tensor")
    )
    return (
        output,
        grad_tokens,
        grad_w_query,
        grad_w_key,
        grad_w_value,
        grad_w_out,
        grad_w_gate,
        grad_w_up,
        grad_w_down,
        total_gains[0],
        total_gains[1],
        total_gains[2],
        total_gains[3],
    )


def per_device_relay(
    tokens,
    cotangent,
    expert_ids,
    gate_values,
    w_query,
    w_key,
    w_value,
    w_out,
    w_gate,
    w_up,
    w_down,
    attn_gain,
    ffn_gain,
    query_gain,
    key_gain,
):
    dot = functools.partial(jnp.dot, preferred_element_type=jnp.float32)
    dot_t = functools.partial(lax.dot_general, dimension_numbers=(((1,), (1,)), ((), ())), preferred_element_type=jnp.float32)
    t_dot = functools.partial(lax.dot_general, dimension_numbers=(((0,), (0,)), ((), ())), preferred_element_type=jnp.float32)
    low = jnp.bfloat16
    rows, width = tokens.shape
    head_dim = query_gain.shape[0]
    experts = w_gate.shape[0]
    core = lax.axis_index("tensor")
    mine = lax.dynamic_slice_in_dim(expert_ids, core * rows, rows, 0)
    values = lax.dynamic_slice_in_dim(gate_values, core * rows, rows, 0)
    match = mine[None] == jnp.arange(experts, dtype=jnp.int32)[:, None, None]
    gates = jnp.sum(jnp.where(match, values[None], 0.0), axis=2)
    gates = jnp.broadcast_to(gates[:, None], (experts, 8, rows))

    q_cols, kv_cols = w_query.shape[1] // 2, w_key.shape[1] // 2
    w_out_rows = jnp.transpose(w_out)
    halves = jnp.stack(
        [
            jnp.concatenate([w[:, h * (w.shape[1] // 2) : (h + 1) * (w.shape[1] // 2)] for w in (w_query, w_key, w_value, w_out_rows)], axis=1)
            for h in range(2)
        ]
    )
    residual = tokens.astype(jnp.float32)
    inverse_one = rms_inverse(residual)
    normed_one = (residual * inverse_one * attn_gain).astype(low)
    cosine, sine_table = rotary_tables(2 * rows, head_dim)
    rope = jnp.stack([jnp.concatenate([v, w], axis=1) for v, w in ((cosine[:, 0], cosine[:, 0]), (sine_table[:, 0], -sine_table[:, 0]))])
    gain = jnp.stack([query_gain, key_gain])[:, None]
    weights, rows_grad, gates, seq_normed, raw, lows, mixed, hidden, normed_two, *projections = attention_first(
        halves, cotangent, gates, normed_one, rope, gain, tokens, ffn_gain[None], (w_gate, w_up, w_down), 1
    )
    weights, gates, seq_normed = weights.reshape(-1, weights.shape[2]), gates[:, 0][:, :, None], seq_normed.reshape(-1, width)
    proj_cols = q_cols + 2 * kv_cols
    share, grad_two, gu_part, down_part, _ = expert_layer(normed_two, rows_grad, gates, *projections, 2)
    norms = jnp.stack([attn_gain, ffn_gain])[:, None]
    output, grad_tokens, *grads, totals, grad_gate, grad_up, grad_down = attention_back(
        tokens, cotangent, hidden, grad_two, norms, weights, seq_normed, raw, lows, mixed, rope, gain, gu_part, down_part, share, 9
    )
    grad_w_gate, grad_w_up, grad_w_down = [v.astype(jnp.float32) for v in (grad_gate, grad_up, grad_down)]
    grad_w_down = jnp.transpose(grad_w_down, (0, 2, 1))
    totals = jnp.split(totals.reshape(-1), (width, 2 * width, 2 * width + head_dim, 2 * width + 2 * head_dim))[:4]
    return (output, grad_tokens, grads[0], grads[1], grads[2], jnp.transpose(grads[3]), grad_w_gate, grad_w_up, grad_w_down, *totals)


def solution(mesh):
    return jax.shard_map(
        per_device_relay if tuple(mesh.shape.values()) == (16, 2) else per_device_any,
        mesh=mesh,
        in_specs=(
            P(("dp", "tensor"), None),
            P(("dp", "tensor"), None),
            P("dp", None),
            P("dp", None),
            P("dp", "tensor"),
            P("dp", "tensor"),
            P("dp", "tensor"),
            P("tensor", "dp"),
            P(None, "dp", "tensor"),
            P(None, "dp", "tensor"),
            P(None, "tensor", "dp"),
            P(),
            P(),
            P(),
            P(),
        ),
        out_specs=(
            P(("dp", "tensor"), None),
            P(("dp", "tensor"), None),
            P("dp", "tensor"),
            P("dp", "tensor"),
            P("dp", "tensor"),
            P("tensor", "dp"),
            P(None, "dp", "tensor"),
            P(None, "dp", "tensor"),
            P(None, "tensor", "dp"),
            P(),
            P(),
            P(),
            P(),
        ),
        check_vma=False,
    )
```
